32 devices in a mesh: dp: 2 (over x), ctx: 4 (over z), tp: 4 (over y, core).
Axes of the slice: x: 2, y: 2, z: 4, core: 2. Of those that a mesh axis runs over, the one named last changes fastest.
Arguments:
- hidden_in: bfloat16 [2, 1024, 1536], P('dp', 'ctx'), may hold values from -6 to 6
- segment_ids: int32 [2, 1024], P('dp', 'ctx'), may hold values from 0 to 2, never falling along the last dimension, each value on 1 to 512 neighbouring positions
- cotangent: bfloat16 [2, 1024, 1536], P('dp', 'ctx'), may hold values from -6 to 6
- norm_gain: bfloat16 [2, 1536], replicated, may hold values from 0.5 to 1.5
- gate_proj: bfloat16 [2, 1536, 3072], P(None, ('dp', 'ctx'), 'tp'), may hold values from -0.15625 to 0.15625
- value_proj: bfloat16 [2, 1536, 3072], P(None, ('dp', 'ctx'), 'tp'), may hold values from -0.15625 to 0.15625
- bc_proj: bfloat16 [2, 1536, 256], P(None, ('dp', 'ctx')), may hold values from -0.15625 to 0.15625
- step_proj: bfloat16 [2, 1536, 48], P(None, ('dp', 'ctx'), 'tp'), may hold values from -0.15625 to 0.15625
- conv_value: bfloat16 [2, 4, 3072], P(None, None, 'tp'), may hold values from -3 to 3
- conv_value_bias: bfloat16 [2, 3072], P(None, 'tp'), may hold values from -3 to 3
- conv_bc: bfloat16 [2, 4, 256], replicated, may hold values from -3 to 3
- conv_bc_bias: bfloat16 [2, 256], replicated, may hold values from -3 to 3
- decay_log: float32 [2, 48], P(None, 'tp'), may hold values from -5 to 1
- step_bias: float32 [2, 48], P(None, 'tp'), may hold values from -6 to 0
- skip_gain: float32 [2, 48], P(None, 'tp'), may hold values from 0.5 to 1.5
- out_gain: bfloat16 [2, 3072], P(None, 'tp'), may hold values from 0.5 to 1.5
- out_proj: bfloat16 [2, 3072, 1536], P(None, 'tp', ('dp', 'ctx')), may hold values from -0.109375 to 0.109375
Outputs:
- hidden_out: bfloat16 [2, 1024, 1536], P('dp', 'ctx')
- grad_hidden: bfloat16 [2, 1024, 1536], P('dp', 'ctx')
- grad_norm_gain: float32 [2, 1536], replicated
- grad_gate_proj: float32 [2, 1536, 3072], P(None, ('dp', 'ctx'), 'tp')
- grad_value_proj: float32 [2, 1536, 3072], P(None, ('dp', 'ctx'), 'tp')
- grad_bc_proj: float32 [2, 1536, 256], P(None, ('dp', 'ctx'))
- grad_step_proj: float32 [2, 1536, 48], P(None, ('dp', 'ctx'), 'tp')
- grad_conv_value: float32 [2, 4, 3072], P(None, None, 'tp')
- grad_conv_value_bias: float32 [2, 3072], P(None, 'tp')
- grad_conv_bc: float32 [2, 4, 256], replicated
- grad_conv_bc_bias: float32 [2, 256], replicated
- grad_decay_log: float32 [2, 48], P(None, 'tp')
- grad_step_bias: float32 [2, 48], P(None, 'tp')
- grad_skip_gain: float32 [2, 48], P(None, 'tp')
- grad_out_gain: float32 [2, 3072], P(None, 'tp')
- grad_out_proj: float32 [2, 3072, 1536], P(None, 'tp', ('dp', 'ctx'))
The draws below stay inside these ranges and needn't reach their ends.
Inputs may be any that keep to these rules, and one draw needn't show every extreme that they name: `segment_ids`: along each sequence the numbers never fall and every number from 0 to the most occurs; a document is the run of positions with one number.
All inputs are finite; a program needn't handle non-finite values.
Results may differ from the reference program's by a relative error of at most 0.02.
Values may be sent and summed in bfloat16 or wider, within the bound.
A program may use at most 192 MiB of HBM per device.

```python
import math
from functools import partial
import jax
import jax.numpy as jnp
import numpy as np
from jax import lax

D = 1536
HEADS = 48
HEADDIM = 64
STATE = 128
CONV = 4
BLOCK = 256
LAYERS = 2
INNER = 3072
LEN = 1024
BATCH = 2


def level_of(rng, extent, cuts, smallest, top_value):
    level, own = 1.0, jax.random.fold_in(rng, 6)
    for axis_at, blocks in cuts:
        steps = jnp.exp(jax.random.uniform(jax.random.fold_in(own, axis_at), (blocks,), jnp.float32, smallest / len(cuts), top_value / len(cuts)))
        level = level * jnp.repeat(steps, extent[axis_at] // blocks).reshape([-1 if axis == axis_at else 1 for axis in range(len(extent))])
    return level


def length_profile(number_of, total, most, slope):
    portions = [(1 << 20) // math.isqrt(rank ** slope) + 1 for rank in range(2, number_of + 1)]
    surplus, counts = total - most - (number_of - 1), [1] * (number_of - 1)
    while surplus > 0:
        candidates = [i for i in range(number_of - 1) if counts[i] < most]
        pool, budget = sum([portions[i] for i in candidates]), surplus
        for i in candidates:
            more = min(most - counts[i], max(1, budget * portions[i] // pool), surplus)
            counts[i] = counts[i] + more
            surplus = surplus - more
    return np.array([most] + counts)


def uneven(own_key, amount, total, most, lean):
    if amount == 2:
        one = jax.random.randint(own_key, (), max(1, total - most), min(most, total - 1) + 1)
        return jnp.stack([one, total - one])
    tallies = jnp.asarray(length_profile(amount, total, most, lean), jnp.int32)
    twos = (amount - 1) // 2
    donor, receiver = tallies[1:1 + 2 * twos:2], tallies[2:2 + 2 * twos:2]
    room = jnp.minimum(donor - 1, most - receiver)
    passed = jax.random.randint(jax.random.fold_in(own_key, 1), (twos,), 0, 1 << 20) % (room + 1)
    tallies = tallies.at[1:1 + 2 * twos:2].set(donor - passed).at[2:2 + 2 * twos:2].set(receiver + passed)
    return tallies[jax.random.permutation(jax.random.fold_in(own_key, 2), amount)]


def scatter_about(rng, dims, deviation, limit, cuts=(), kind=jnp.bfloat16):
    array = deviation * jax.random.normal(rng, dims, jnp.float32)
    if cuts:
        array = array * level_of(rng, dims, cuts, -0.22, 0.18)
    return jnp.clip(array, -limit, limit).astype(kind)


def setup_inputs(seed: int = 0) -> dict:
    key_list = jax.random.split(jax.random.key(seed), 18)
    hidden_in = scatter_about(key_list[0], (BATCH, LEN, D), 1.0, 6.0, ((0, 2), (1, 4)))
    segment_ids = jax.vmap(lambda own: jnp.searchsorted(jnp.cumsum(uneven(own, max(3, LEN // 1024), LEN, LEN // 2, 2)), jnp.arange(LEN), side="right"))(jax.random.split(key_list[1], BATCH)).reshape((BATCH, LEN)).astype(jnp.int32)
    cotangent = scatter_about(key_list[2], (BATCH, LEN, D), 1.0, 6.0, ((0, 2), (1, 4)))
    norm_gain = jnp.clip(1.0 + 0.1 * jax.random.normal(key_list[3], (LAYERS, D), jnp.float32), 0.5, 1.5).astype(jnp.bfloat16)
    gate_proj = scatter_about(key_list[4], (LAYERS, D, INNER), D ** -0.5, 0.15625, ((1, 8), (2, 4)))
    value_proj = scatter_about(key_list[5], (LAYERS, D, INNER), D ** -0.5, 0.15625, ((1, 8), (2, 4)))
    bc_proj = scatter_about(key_list[6], (LAYERS, D, 2 * STATE), D ** -0.5, 0.15625, ((1, 8),))
    step_proj = scatter_about(key_list[7], (LAYERS, D, HEADS), D ** -0.5, 0.15625, ((1, 8), (2, 4)))
    conv_value = scatter_about(key_list[8], (LAYERS, CONV, INNER), CONV ** -0.5, 3.0, ((2, 4),))
    conv_value_bias = scatter_about(key_list[9], (LAYERS, INNER), 0.5, 3.0, ((1, 4),))
    conv_bc = scatter_about(key_list[10], (LAYERS, CONV, 2 * STATE), CONV ** -0.5, 3.0)
    conv_bc_bias = scatter_about(key_list[11], (LAYERS, 2 * STATE), 0.5, 3.0)
    decay_log = jnp.clip(-5.0 + 6.0 * jax.random.uniform(key_list[12], (LAYERS, HEADS), jnp.float32) ** level_of(key_list[12], (LAYERS, HEADS), ((1, 4),), -0.2, 0.2), -5.0, 1.0)
    step_bias = jnp.clip(-6.0 + 6.0 * jax.random.uniform(key_list[13], (LAYERS, HEADS), jnp.float32) ** level_of(key_list[13], (LAYERS, HEADS), ((1, 4),), -0.2, 0.2), -6.0, 0.0)
    skip_gain = jnp.clip(0.5 + 1.0 * jax.random.uniform(key_list[14], (LAYERS, HEADS), jnp.float32) ** level_of(key_list[14], (LAYERS, HEADS), ((1, 4),), -0.2, 0.2), 0.5, 1.5)
    out_gain = jnp.clip(1.0 + 0.1 * jax.random.normal(key_list[15], (LAYERS, INNER), jnp.float32), 0.5, 1.5).astype(jnp.bfloat16)
    out_proj = scatter_about(key_list[16], (LAYERS, INNER, D), INNER ** -0.5, 0.109375, ((1, 4), (2, 8)))
    return {"hidden_in": hidden_in, "segment_ids": segment_ids, "cotangent": cotangent, "norm_gain": norm_gain, "gate_proj": gate_proj, "value_proj": value_proj, "bc_proj": bc_proj, "step_proj": step_proj, "conv_value": conv_value, "conv_value_bias": conv_value_bias, "conv_bc": conv_bc, "conv_bc_bias": conv_bc_bias, "decay_log": decay_log, "step_bias": step_bias, "skip_gain": skip_gain, "out_gain": out_gain, "out_proj": out_proj}


epsilon = 1e-05
highest = lax.Precision.HIGHEST

@jax.custom_vjp
def low(v):
    return lax.optimization_barrier(v.astype(jnp.bfloat16)).astype(jnp.float32)

@jax.custom_vjp
def low_back(v):
    return v

def low_keep(v):
    return (low(v), None)

def low_pass(kept, grad):
    return (grad,)

def back_keep(v):
    return (v, None)

def back_low(kept, grad):
    return (low(grad),)
low.defvjp(low_keep, low_pass)
low_back.defvjp(back_keep, back_low)

def rms_scale(values, gains):
    inv_rms = lax.rsqrt(lax.optimization_barrier(jnp.mean(values * values, axis=-1, keepdims=True)) + epsilon)
    return values * inv_rms * gains

def causal_conv(signal, kernel, conv_bias, segment):
    tap_count = kernel.shape[0]
    length = signal.shape[0]
    padded = jnp.concatenate([jnp.zeros((tap_count - 1, signal.shape[1]), signal.dtype), signal], axis=0)
    seg_pad = jnp.concatenate([jnp.zeros((tap_count - 1,), jnp.int32), segment], axis=0)
    result = conv_bias + jnp.zeros_like(signal)
    for tap_index in range(tap_count):
        same_doc = (seg_pad[tap_index:tap_index + length] == segment).astype(jnp.float32)
        result = result + kernel[tap_index] * padded[tap_index:tap_index + length] * same_doc[:, None]
    return jax.nn.silu(result)

def block_step(decay_rates, carried, block_data):
    states, prev_segment = carried
    values, b_mat, c_mat, step_size, segment = block_data
    length = values.shape[0]
    log_decay = jnp.cumsum(step_size * decay_rates, axis=0)
    positions = jnp.arange(length)
    causal = positions[:, None] >= positions[None, :]
    same_doc = jnp.logical_and(segment[:, None] == segment[None, :], causal)[:, :, None]
    differ = jnp.where(same_doc, log_decay[:, None, :] - log_decay[None, :, :], 0.0)
    weights = jnp.where(same_doc, jnp.exp(differ), 0.0)
    cb_product = jnp.dot(c_mat, b_mat.T, precision=highest)
    scores = cb_product[:, :, None] * weights * step_size[None, :, :]
    intra_out = jnp.einsum('tsh,shp->thp', scores, values, precision=highest)
    alive_mask = (segment == prev_segment).astype(jnp.float32)
    reach = alive_mask[:, None] * jnp.exp(log_decay)
    inter_out = reach[:, :, None] * jnp.einsum('tn,hpn->thp', c_mat, states, precision=highest)
    end_same = (segment == segment[length - 1]).astype(jnp.float32)
    to_end = jnp.exp(log_decay[length - 1][None, :] - log_decay) * end_same[:, None] * step_size
    weighted_values = to_end[:, :, None] * values
    new_states = reach[length - 1][:, None, None] * states + jnp.einsum('shp,sn->hpn', weighted_values, b_mat, precision=highest)
    return ((new_states, segment[length - 1]), intra_out + inter_out)

def ssd_sequence(heads_in, b_mat, c_mat, step_size, decay_rates, segment):
    length = heads_in.shape[0]
    block_count = length // BLOCK
    blocks = (heads_in.reshape(block_count, BLOCK, HEADS, HEADDIM), b_mat.reshape(block_count, BLOCK, STATE), c_mat.reshape(block_count, BLOCK, STATE), step_size.reshape(block_count, BLOCK, HEADS), segment.reshape(block_count, BLOCK))
    initial = (jnp.zeros((HEADS, HEADDIM, STATE), jnp.float32), jnp.zeros((), jnp.int32))
    final_carry, outputs = lax.scan(jax.checkpoint(partial(block_step, decay_rates)), initial, blocks)
    return outputs.reshape(length, HEADS, HEADDIM)

def mixer_layer(hidden, segment, layer_params):
    norm_gain, gate_proj, value_proj, bc_proj, step_proj, conv_value, conv_value_bias, conv_bc, conv_bc_bias, decay_log, step_bias, skip_gain, out_gain, out_proj = layer_params
    normed = low(rms_scale(hidden, norm_gain))
    gate_pre = low_back(jnp.dot(normed, gate_proj, precision=highest))
    value_pre = low_back(jnp.dot(normed, value_proj, precision=highest))
    bc_pre = low_back(jnp.dot(normed, bc_proj, precision=highest))
    step_pre = low_back(jnp.dot(normed, step_proj, precision=highest))
    values = low(causal_conv(value_pre, conv_value, conv_value_bias, segment))
    bc_conv = low(causal_conv(bc_pre, conv_bc, conv_bc_bias, segment))
    step_size = jax.nn.softplus(step_pre + step_bias)
    decay_rates = -jnp.exp(decay_log)
    heads_in = values.reshape(-1, HEADS, HEADDIM)
    ssd_out = ssd_sequence(heads_in, bc_conv[:, :STATE], bc_conv[:, STATE:], step_size, decay_rates, segment)
    mixed = (ssd_out + skip_gain[:, None] * heads_in).reshape(-1, INNER)
    gated = mixed * jax.nn.silu(gate_pre)
    scaled = low(rms_scale(gated, out_gain))
    return hidden + low_back(jnp.dot(scaled, out_proj, precision=highest))

def reference(hidden_in, segment_ids, cotangent, norm_gain, gate_proj, value_proj, bc_proj, step_proj, conv_value, conv_value_bias, conv_bc, conv_bc_bias, decay_log, step_bias, skip_gain, out_gain, out_proj):
    params = tuple((stacked.astype(jnp.float32) for stacked in (norm_gain, gate_proj, value_proj, bc_proj, step_proj, conv_value, conv_value_bias, conv_bc, conv_bc_bias, decay_log, step_bias, skip_gain, out_gain, out_proj)))

    def per_sequence(totals, sequence):
        hidden_seq, segment, cot_seq = sequence

        def forward(hidden, param_set):
            for layer_index in range(LAYERS):
                hidden = mixer_layer(hidden, segment, tuple((stacked[layer_index] for stacked in param_set)))
            return hidden
        result, pullback = jax.vjp(forward, hidden_seq.astype(jnp.float32), params)
        grad_in, grad_params = pullback(cot_seq.astype(jnp.float32))
        return (jax.tree.map(jnp.add, totals, grad_params), (result.astype(jnp.bfloat16), grad_in.astype(jnp.bfloat16)))
    zero_grads = jax.tree.map(jnp.zeros_like, params)
    totals, outputs = lax.scan(per_sequence, zero_grads, (hidden_in, segment_ids, cotangent))
    return (outputs[0], outputs[1], totals[0], totals[1], totals[2], totals[3], totals[4], totals[5], totals[6], totals[7], totals[8], totals[9], totals[10], totals[11], totals[12], totals[13])
```

```python
from functools import partial

import jax
import jax.numpy as jnp
from jax import lax
from jax.experimental import pallas as pl
from jax.experimental.pallas import tpu as pltpu
from jax.sharding import PartitionSpec as P

HEADDIM = 64
BLOCK = 256
LAYERS = 2
INNER = 3072


epsilon = 1e-05
precise = lax.Precision.HIGH


def from_behind(block, axis, distance):
    devices = range(lax.axis_size(axis))
    route = [(i - distance, i) for i in devices if i - distance in devices]
    return lax.ppermute(block, axis, route)


def round_keep(values):
    return lax.optimization_barrier(values.astype(jnp.bfloat16)).astype(jnp.float32)


def dot_back(left_rows, right_rows):
    return lax.dot_general(
        left_rows, right_rows, (((1,), (1,)), ((), ())), preferred_element_type=jnp.float32
    )


def dot_left(left_rows, right_rows):
    return lax.dot_general(
        left_rows, right_rows, (((0,), (0,)), ((), ())), preferred_element_type=jnp.float32
    )


def conv_local(signal, edge_rows, kernel, conv_bias, segment, edge_segment):
    tap_count = kernel.shape[0]
    length = signal.shape[1]
    padded = jnp.concatenate([edge_rows, signal], axis=1)
    seg_pad = jnp.concatenate([edge_segment, segment], axis=1)
    result = conv_bias + jnp.zeros_like(signal)
    for tap_index in range(tap_count):
        same_doc = (seg_pad[:, tap_index : tap_index + length] == segment).astype(jnp.float32)
        result = (
            result
            + kernel[tap_index] * padded[:, tap_index : tap_index + length] * same_doc[:, :, None]
        )
    return jax.nn.silu(result)


def block_step(decay_rates, carried, block_data):
    states, prev_segment = carried
    values, b_mat, c_mat, step_size, segment = block_data
    length = values.shape[0]
    log_decay = jnp.cumsum(step_size * decay_rates, axis=0)
    positions = jnp.arange(length)
    causal = positions[:, None] >= positions[None, :]
    same_doc = jnp.logical_and(segment[:, None] == segment[None, :], causal)[:, :, None]
    differ = jnp.where(same_doc, log_decay[:, None, :] - log_decay[None, :, :], 0.0)
    weights = jnp.where(same_doc, jnp.exp(differ), 0.0)
    cb_product = jnp.dot(c_mat, b_mat.T, precision=precise)
    scores = cb_product[:, :, None] * weights * step_size[None, :, :]
    intra_out = jnp.einsum("tsh,shp->thp", scores, values, precision=precise)
    alive_mask = (segment == prev_segment).astype(jnp.float32)
    reach = alive_mask[:, None] * jnp.exp(log_decay)
    inter_out = reach[:, :, None] * jnp.einsum("tn,hpn->thp", c_mat, states, precision=precise)
    end_same = (segment == segment[length - 1]).astype(jnp.float32)
    to_end = jnp.exp(log_decay[length - 1][None, :] - log_decay) * end_same[:, None] * step_size
    weighted_values = to_end[:, :, None] * values
    new_states = reach[length - 1][:, None, None] * states + jnp.einsum(
        "shp,sn->hpn", weighted_values, b_mat, precision=precise
    )
    return ((new_states, segment[length - 1]), intra_out + inter_out)


def device_scan(values, b_mat, c_mat, step_size, decay_rates, segment, seg_prev):
    block_count = values.shape[0] // BLOCK
    heads_local = values.shape[1]
    state_dim = b_mat.shape[1]
    blocks = (
        values.reshape(block_count, BLOCK, heads_local, HEADDIM),
        b_mat.reshape(block_count, BLOCK, state_dim),
        c_mat.reshape(block_count, BLOCK, state_dim),
        step_size.reshape(block_count, BLOCK, heads_local),
        segment.reshape(block_count, BLOCK),
    )
    initial = (jnp.zeros((heads_local, HEADDIM, state_dim), jnp.float32), seg_prev)
    final_carry, outputs = lax.scan(partial(block_step, decay_rates), initial, blocks)
    return (outputs.reshape(values.shape), final_carry[0])


def step_terms(step_pre, step_bias, decay_log):
    return (jax.nn.softplus(step_pre + step_bias), -jnp.exp(decay_log))


def mixer_terms(values, bc_conv, step_size, decay_rates, skip_gain, segment, seg_prev):
    seq_count, tokens, inner_local = values.shape
    heads_local = step_size.shape[2]
    heads_in = values.reshape(seq_count, tokens, heads_local, HEADDIM)
    state_dim = bc_conv.shape[2] // 2
    scanner = jax.vmap(device_scan, in_axes=(0, 0, 0, 0, None, 0, 0))
    intra_out, local_states = scanner(
        heads_in,
        bc_conv[:, :, :state_dim],
        bc_conv[:, :, state_dim:],
        step_size,
        decay_rates,
        segment,
        seg_prev,
    )
    alive_last = (segment[:, tokens - 1] == seg_prev).astype(jnp.float32)
    decays = alive_last[:, None] * jnp.exp(jnp.sum(step_size * decay_rates, axis=1))
    return (intra_out + skip_gain[:, None] * heads_in, local_states, decays)


def carried_terms(bc_conv, step_size, decay_rates, entering, segment, seg_prev):
    state_dim = bc_conv.shape[2] // 2
    c_mat = bc_conv[:, :, state_dim:]
    log_decay = jnp.cumsum(step_size * decay_rates, axis=1)
    alive_mask = (segment == seg_prev[:, None]).astype(jnp.float32)
    reach = alive_mask[:, :, None] * jnp.exp(log_decay)
    carried = jnp.einsum("sqn,shpn->sqhp", c_mat, entering, precision=precise)
    return reach[:, :, :, None] * carried


def chain_forward(decays, local_states):

    def handoff(step_index, entering):
        return from_behind(decays[:, :, None, None] * entering + local_states, "ctx", 1)

    return lax.fori_loop(0, lax.axis_size("ctx") - 1, handoff, jnp.zeros_like(local_states))


def chain_backward(decays, grad_entering):

    def handback(step_index, beyond):
        return from_behind(
            (grad_entering + decays[:, :, None, None] * beyond).astype(jnp.bfloat16), "ctx", -1
        ).astype(jnp.float32)

    return lax.fori_loop(0, lax.axis_size("ctx") - 1, handback, jnp.zeros_like(grad_entering))


def layer_forward(hidden, segment, layer_params):
    (
        norm_gain,
        gate_proj,
        value_proj,
        bc_proj,
        step_proj,
        conv_value,
        conv_value_bias,
        conv_bc,
        conv_bc_bias,
        decay_log,
        step_bias,
        skip_gain,
        out_gain,
        out_proj,
    ) = layer_params
    seq_count, tokens, model_width = hidden.shape
    row_count = seq_count * tokens
    tap_count = conv_value.shape[0]
    gathered = (
        lax.all_gather(gate_proj, ("dp", "ctx"), axis=0, tiled=True),
        lax.all_gather(value_proj, ("dp", "ctx"), axis=0, tiled=True),
        lax.all_gather(bc_proj, ("dp", "ctx"), axis=0, tiled=True),
        lax.all_gather(step_proj, ("dp", "ctx"), axis=0, tiled=True),
        lax.all_gather(out_proj, ("dp", "ctx"), axis=1, tiled=True),
    )
    gate_full, value_full, bc_full, step_full, out_full = gathered
    hidden_rows = hidden.reshape(row_count, model_width)
    inv_norm = lax.rsqrt(jnp.mean(hidden_rows * hidden_rows, axis=1, keepdims=True) + epsilon)
    normed = (hidden_rows * inv_norm * norm_gain).astype(jnp.bfloat16)
    gate_pre = jnp.dot(normed, gate_full, preferred_element_type=jnp.float32)
    value_pre = jnp.dot(normed, value_full, preferred_element_type=jnp.float32).reshape(
        seq_count, tokens, -1
    )
    bc_pre = jnp.dot(normed, bc_full, preferred_element_type=jnp.float32).reshape(
        seq_count, tokens, -1
    )
    step_pre = jnp.dot(normed, step_full, preferred_element_type=jnp.float32).reshape(
        seq_count, tokens, -1
    )
    first_edge = tokens - tap_count + 1
    edge_value, edge_bc, edge_segment = from_behind(
        (value_pre[:, first_edge:], bc_pre[:, first_edge:], segment[:, first_edge:]), "ctx", 1
    )
    conv_fn = partial(conv_local, segment=segment, edge_segment=edge_segment)
    value_act, value_pull = jax.vjp(conv_fn, value_pre, edge_value, conv_value, conv_value_bias)
    bc_act, bc_pull = jax.vjp(conv_fn, bc_pre, edge_bc, conv_bc, conv_bc_bias)
    values = round_keep(value_act)
    bc_conv = round_keep(bc_act)
    seg_prev = edge_segment[:, tap_count - 2]
    (step_size, decay_rates), step_pull = jax.vjp(step_terms, step_pre, step_bias, decay_log)
    (local_out, local_states, decays), local_pull = jax.vjp(
        partial(mixer_terms, segment=segment, seg_prev=seg_prev),
        values,
        bc_conv,
        step_size,
        decay_rates,
        skip_gain,
    )
    entering = chain_forward(decays, local_states)
    carried_out, carried_pull = jax.vjp(
        partial(carried_terms, segment=segment, seg_prev=seg_prev),
        bc_conv,
        step_size,
        decay_rates,
        entering,
    )
    mixed = (local_out + carried_out).reshape(row_count, -1)
    gate_act = jax.nn.silu(gate_pre)
    gated = mixed * gate_act
    square_sum = lax.psum(jnp.sum(gated * gated, axis=1), "tp")
    inv_gate = lax.rsqrt(square_sum / INNER + epsilon)[:, None]
    scaled = (gated * inv_gate * out_gain).astype(jnp.bfloat16)
    mixer_sum = lax.psum(jnp.dot(scaled, out_full, preferred_element_type=jnp.float32), "tp")
    kept = {
        "scaled": scaled,
        "gated": gated,
        "inv_gate": inv_gate,
        "gate_pre": gate_pre,
        "gate_act": gate_act,
        "mixed": mixed,
        "carried_pull": carried_pull,
        "local_pull": local_pull,
        "step_pull": step_pull,
        "value_pull": value_pull,
        "bc_pull": bc_pull,
        "decays": decays,
        "entering": entering,
        "hidden_rows": hidden_rows,
        "inv_norm": inv_norm,
        "normed": normed,
    }
    return (hidden + mixer_sum.reshape(seq_count, tokens, model_width), kept)


def layer_backward(grad_hidden, kept, layer_params):
    (
        norm_gain,
        gate_proj,
        value_proj,
        bc_proj,
        step_proj,
        conv_value,
        conv_value_bias,
        conv_bc,
        conv_bc_bias,
        decay_log,
        step_bias,
        skip_gain,
        out_gain,
        out_proj,
    ) = layer_params
    seq_count, tokens, model_width = grad_hidden.shape
    row_count = seq_count * tokens
    tap_count = conv_value.shape[0]
    gate_full, value_full, bc_full, step_full, out_full = (
        lax.all_gather(gate_proj, ("dp", "ctx"), axis=0, tiled=True),
        lax.all_gather(value_proj, ("dp", "ctx"), axis=0, tiled=True),
        lax.all_gather(bc_proj, ("dp", "ctx"), axis=0, tiled=True),
        lax.all_gather(step_proj, ("dp", "ctx"), axis=0, tiled=True),
        lax.all_gather(out_proj, ("dp", "ctx"), axis=1, tiled=True),
    )
    grad_rows = grad_hidden.reshape(row_count, model_width)
    grad_low = grad_rows.astype(jnp.bfloat16)
    grad_scaled = dot_back(grad_low, out_full)
    grad_out_proj = dot_left(kept["scaled"], grad_low)
    gated = kept["gated"]
    inv_gate = kept["inv_gate"]
    weighted = grad_scaled * out_gain
    inner_sum = lax.psum(jnp.sum(weighted * gated, axis=1), "tp")
    grad_gated = inv_gate * weighted - gated * inv_gate**3 * (inner_sum / INNER)[:, None]
    grad_out_gain = jnp.sum(grad_scaled * gated * inv_gate, axis=0)
    gate_pre = kept["gate_pre"]
    sigmoid_gate = jax.nn.sigmoid(gate_pre)
    grad_gate_pre = (
        grad_gated * kept["mixed"] * sigmoid_gate * (1.0 + gate_pre * (1.0 - sigmoid_gate))
    )
    grad_heads = (grad_gated * kept["gate_act"]).reshape(
        seq_count, tokens, step_full.shape[1], HEADDIM
    )
    carried_bc, carried_step, carried_rates, grad_entering = kept["carried_pull"](grad_heads)
    beyond = chain_backward(kept["decays"], grad_entering)
    grad_decays = jnp.sum(beyond * kept["entering"], axis=(2, 3))
    local_values, local_bc, local_step, local_rates, grad_skip = kept["local_pull"](
        (grad_heads, beyond, grad_decays)
    )
    grad_step_pre, grad_step_bias, grad_decay_log = kept["step_pull"](
        (carried_step + local_step, carried_rates + local_rates)
    )
    grad_value_pre, grad_edge_value, grad_conv_value, grad_conv_value_bias = kept["value_pull"](
        local_values
    )
    grad_bc_pre, grad_edge_bc, grad_conv_bc, grad_conv_bc_bias = kept["bc_pull"](
        carried_bc + local_bc
    )
    from_value, from_bc = from_behind((grad_edge_value, grad_edge_bc), "ctx", -1)
    first_edge = tokens - tap_count + 1
    grad_value_pre = grad_value_pre.at[:, first_edge:].add(from_value)
    grad_bc_pre = grad_bc_pre.at[:, first_edge:].add(from_bc)
    grad_gate_low = grad_gate_pre.astype(jnp.bfloat16)
    grad_value_low = grad_value_pre.reshape(row_count, -1).astype(jnp.bfloat16)
    grad_step_low = grad_step_pre.reshape(row_count, -1).astype(jnp.bfloat16)
    input_part = (
        dot_back(grad_gate_low, gate_full)
        + dot_back(grad_value_low, value_full)
        + dot_back(grad_step_low, step_full)
    )
    input_sum, bc_sum, conv_bc_sum, conv_bc_bias_sum = (
        lax.psum(input_part.astype(jnp.bfloat16), "tp").astype(jnp.float32),
        lax.psum(grad_bc_pre.reshape(row_count, -1).astype(jnp.bfloat16), "tp").astype(jnp.float32),
        lax.psum(grad_conv_bc, "tp").astype(jnp.float32),
        lax.psum(grad_conv_bc_bias, "tp").astype(jnp.float32),
    )
    grad_bc_low = bc_sum.astype(jnp.bfloat16)
    grad_normed = input_sum + dot_back(grad_bc_low, bc_full)
    hidden_rows = kept["hidden_rows"]
    inv_norm = kept["inv_norm"]
    weighted_norm = grad_normed * norm_gain
    grad_norm_gain = jnp.sum(grad_normed * hidden_rows * inv_norm, axis=0)
    grad_rows = (
        grad_rows
        + inv_norm * weighted_norm
        - hidden_rows * inv_norm**3 * jnp.mean(weighted_norm * hidden_rows, axis=1, keepdims=True)
    )
    normed = kept["normed"]
    proj_grads = (
        lax.psum_scatter(
            dot_left(normed, grad_gate_low).astype(jnp.bfloat16),
            ("dp", "ctx"),
            scatter_dimension=0,
            tiled=True,
        ).astype(jnp.float32),
        lax.psum_scatter(
            dot_left(normed, grad_value_low).astype(jnp.bfloat16),
            ("dp", "ctx"),
            scatter_dimension=0,
            tiled=True,
        ).astype(jnp.float32),
        lax.psum_scatter(
            dot_left(normed, grad_bc_low).astype(jnp.bfloat16),
            ("dp", "ctx"),
            scatter_dimension=0,
            tiled=True,
        ).astype(jnp.float32),
        lax.psum_scatter(
            dot_left(normed, grad_step_low).astype(jnp.bfloat16),
            ("dp", "ctx"),
            scatter_dimension=0,
            tiled=True,
        ).astype(jnp.float32),
        lax.psum_scatter(
            grad_out_proj.astype(jnp.bfloat16), ("dp", "ctx"), scatter_dimension=1, tiled=True
        ).astype(jnp.float32),
    )
    small_grads = lax.psum(
        (
            grad_norm_gain,
            grad_conv_value.astype(jnp.float32),
            grad_conv_value_bias.astype(jnp.float32),
            conv_bc_sum,
            conv_bc_bias_sum,
            grad_decay_log,
            grad_step_bias,
            grad_skip,
            grad_out_gain,
        ),
        ("dp", "ctx"),
    )
    return (grad_rows.reshape(seq_count, tokens, model_width), proj_grads, small_grads)


def stack_layers(groups, member):
    return jnp.stack([groups[layer_index][member] for layer_index in range(LAYERS)])


def local(
    hidden_in,
    segment_ids,
    cotangent,
    norm_gain,
    gate_proj,
    value_proj,
    bc_proj,
    step_proj,
    conv_value,
    conv_value_bias,
    conv_bc,
    conv_bc_bias,
    decay_log,
    step_bias,
    skip_gain,
    out_gain,
    out_proj,
):
    params = (
        norm_gain,
        gate_proj,
        value_proj,
        bc_proj,
        step_proj,
        conv_value,
        conv_value_bias,
        conv_bc,
        conv_bc_bias,
        decay_log,
        step_bias,
        skip_gain,
        out_gain,
        out_proj,
    )
    segment = segment_ids.astype(jnp.float32)
    hidden = hidden_in.astype(jnp.float32)
    kept_layers = []
    for layer_index in range(LAYERS):
        hidden, kept = layer_forward(
            hidden, segment, tuple((stacked[layer_index] for stacked in params))
        )
        kept_layers.append(kept)
    grad_hidden = cotangent.astype(jnp.float32)
    proj_list = [None] * LAYERS
    small_list = [None] * LAYERS
    for layer_index in reversed(range(LAYERS)):
        grad_hidden, proj_list[layer_index], small_list[layer_index] = layer_backward(
            grad_hidden,
            kept_layers[layer_index],
            tuple((stacked[layer_index] for stacked in params)),
        )
    return (
        hidden.astype(jnp.bfloat16),
        grad_hidden.astype(jnp.bfloat16),
        stack_layers(small_list, 0),
        stack_layers(proj_list, 0),
        stack_layers(proj_list, 1),
        stack_layers(proj_list, 2),
        stack_layers(proj_list, 3),
        stack_layers(small_list, 1),
        stack_layers(small_list, 2),
        stack_layers(small_list, 3),
        stack_layers(small_list, 4),
        stack_layers(small_list, 5),
        stack_layers(small_list, 6),
        stack_layers(small_list, 7),
        stack_layers(small_list, 8),
        stack_layers(proj_list, 4),
    )


MESH = pl.DeviceIdType.MESH
PACK = 640


def params_of(collective_id):
    return pltpu.CompilerParams(
        collective_id=collective_id, has_side_effects=True, vmem_limit_bytes=60 << 20
    )


VMEM_SPEC = pl.BlockSpec(memory_space=pltpu.VMEM)


def greet(peers):
    barrier = pltpu.get_barrier_semaphore()
    for peer in peers:
        pl.semaphore_signal(barrier, inc=1, device_id=peer, device_id_type=MESH)
    pl.semaphore_wait(barrier, len(peers))


def remote(source, target, send_sem, recv_sem, peer):
    return pltpu.make_async_remote_copy(
        src_ref=source,
        dst_ref=target,
        send_sem=send_sem,
        recv_sem=recv_sem,
        device_id=peer,
        device_id_type=MESH,
    )


def other_core(t):
    return t + 1 - 2 * lax.rem(t, 2)


def other_chip(t):
    return lax.rem(t + 2, 4)


def gather_body(count, depth, pieces, fulls, send_sem, recv_sem):
    z = lax.axis_index("ctx")
    t = lax.axis_index("tp")
    core, chip = {"tp": other_core(t)}, {"tp": other_chip(t)}
    started = []

    def send(a, source, slot, kind, peer):
        copy = remote(source, fulls[a].at[slot], send_sem.at[a, kind], recv_sem.at[a, slot], peer)
        copy.start()
        started.append(copy)

    def arrived(a, slot):
        remote(
            fulls[a].at[slot], fulls[a].at[slot], send_sem.at[a, 0], recv_sem.at[a, slot], core
        ).wait_recv()

    mine = z * 4 + t
    for a in range(count):
        for hop in range(1, depth):
            send(a, pieces[a], mine, hop, {"ctx": lax.rem(z + hop, depth)})
        send(a, pieces[a], mine, depth, chip)
        send(a, pieces[a], mine, depth + 1, core)
        fulls[a][mine] = pieces[a][...]
    kind = depth + 2
    for hop in range(1, depth):
        slot = lax.rem(z + hop, depth) * 4 + t
        for a in range(count):
            arrived(a, slot)
            send(a, fulls[a].at[slot], slot, kind, chip)
            send(a, fulls[a].at[slot], slot, kind + 1, core)
        kind += 2
    for hop in range(depth):
        slot = lax.rem(z + hop, depth) * 4 + other_chip(t)
        for a in range(count):
            arrived(a, slot)
            send(a, fulls[a].at[slot], slot, kind, core)
        kind += 1
    for hop in range(depth):
        for row in (other_core(t), other_chip(other_core(t))):
            for a in range(count):
                arrived(a, lax.rem(z + hop, depth) * 4 + row)
    for copy in started:
        copy.wait_send()


def gather_peers(depth):
    z = lax.axis_index("ctx")
    t = lax.axis_index("tp")
    return [{"ctx": lax.rem(z + hop, depth)} for hop in range(1, depth)] + [
        {"tp": other_chip(t)},
        {"tp": other_core(t)},
    ]


def gather_kernel(count, depth, *refs):
    greet(gather_peers(depth))
    gather_body(count, depth, refs[:count], refs[count : 2 * count], *refs[2 * count :])


def gather_pieces(pieces, depth, collective_id):
    count = len(pieces)
    slots = depth * 4
    return pl.pallas_call(
        partial(gather_kernel, count, depth),
        out_shape=[jax.ShapeDtypeStruct((slots,) + p.shape, p.dtype) for p in pieces],
        in_specs=[VMEM_SPEC] * count,
        out_specs=[VMEM_SPEC] * count,
        scratch_shapes=[
            pltpu.SemaphoreType.DMA((count, 4 * depth)),
            pltpu.SemaphoreType.DMA((count, slots)),
        ],
        compiler_params=params_of(collective_id),
        name="gather_pieces",
    )(*pieces)


def reduce_body(count, depth, parts, outs, bufs, send_sem, recv_sem):
    z = lax.axis_index("ctx")
    t = lax.axis_index("tp")
    core, chip = {"tp": other_core(t)}, {"tp": other_chip(t)}
    started = []
    hops = list(range(1, depth)) + [0]

    def send(a, source, target, kind, peer):
        copy = remote(source, target, send_sem.at[a, kind], recv_sem.at[a, kind], peer)
        copy.start()
        started.append(copy)

    def arrived(a, ref, kind):
        remote(ref, ref, send_sem.at[a, kind], recv_sem.at[a, kind], core).wait_recv()

    for place, hop in enumerate(hops):
        far = lax.rem(z + hop, depth)
        for which, row in enumerate((other_chip(other_core(t)), other_core(t))):
            kind = place * 2 + which
            for a in range(count):
                send(a, parts[a].at[far * 4 + row], bufs[a].at[kind], kind, core)
    for place, hop in enumerate(hops):
        far = lax.rem(z + hop, depth)
        kind = place * 2
        for a in range(count):
            buf = bufs[a]
            arrived(a, buf.at[kind], kind)
            total = parts[a][far * 4 + other_chip(t)].astype(jnp.float32) + buf[kind].astype(
                jnp.float32
            )
            buf[kind] = total.astype(buf.dtype)
            send(a, buf.at[kind], buf.at[2 * depth + place], 2 * depth + place, chip)
    for place, hop in enumerate(hops):
        far = lax.rem(z + hop, depth)
        kind = place * 2 + 1
        for a in range(count):
            buf = bufs[a]
            arrived(a, buf.at[kind], kind)
            arrived(a, buf.at[2 * depth + place], 2 * depth + place)
            total = (
                parts[a][far * 4 + t].astype(jnp.float32)
                + buf[kind].astype(jnp.float32)
                + buf[2 * depth + place].astype(jnp.float32)
            )
            if hop:
                buf[kind] = total.astype(buf.dtype)
                target = 3 * depth + (depth - hop)
                copy = remote(
                    buf.at[kind],
                    buf.at[target],
                    send_sem.at[a, 3 * depth + hop],
                    recv_sem.at[a, target],
                    {"ctx": far},
                )
                copy.start()
                started.append(copy)
            else:
                outs[a][...] = total
    for hop in range(1, depth):
        for a in range(count):
            buf = bufs[a]
            target = 3 * depth + hop
            arrived(a, buf.at[target], target)
            outs[a][...] += buf[target].astype(jnp.float32)
    for copy in started:
        copy.wait_send()


def reduce_kernel(count, depth, *refs):
    greet(gather_peers(depth))
    reduce_body(
        count,
        depth,
        refs[:count],
        refs[count : 2 * count],
        refs[2 * count : 3 * count],
        *refs[3 * count :],
    )


def reduce_pieces(parts, depth, collective_id):
    count = len(parts)
    return pl.pallas_call(
        partial(reduce_kernel, count, depth),
        out_shape=[jax.ShapeDtypeStruct(p.shape[1:], jnp.float32) for p in parts],
        in_specs=[VMEM_SPEC] * count,
        out_specs=[VMEM_SPEC] * count,
        scratch_shapes=[pltpu.VMEM((4 * depth,) + p.shape[1:], p.dtype) for p in parts]
        + [
            pltpu.SemaphoreType.DMA((count, 4 * depth)),
            pltpu.SemaphoreType.DMA((count, 4 * depth)),
        ],
        compiler_params=params_of(collective_id),
        name="reduce_pieces",
    )(*parts)


def scatter_kernel(depth, grads_ref, shared_ref, out_ref, shared_out, x_buf, x_shared, send_sem, recv_sem):
    x = lax.axis_index("dp")
    z = lax.axis_index("ctx")
    far_x = {"dp": 1 - x}
    greet([{"ctx": lax.rem(z + hop, depth)} for hop in range(1, depth)] + [far_x])
    started = []

    def send(source, target, kind, recv, peer):
        copy = remote(source, target, send_sem.at[kind], recv_sem.at[recv], peer)
        copy.start()
        started.append(copy)

    def arrived(ref, recv):
        remote(ref, ref, send_sem.at[recv], recv_sem.at[recv], far_x).wait_recv()

    hops = list(range(1, depth)) + [0]
    for place, hop in enumerate(hops):
        far = lax.rem(z + hop, depth)
        send(grads_ref.at[(1 - x) * depth + far], x_buf.at[place], place, place, far_x)
    send(shared_ref.at[1 - x], x_shared, depth, depth, far_x)
    for place, hop in enumerate(hops):
        far = lax.rem(z + hop, depth)
        arrived(x_buf.at[place], place)
        total = grads_ref[x * depth + far].astype(jnp.float32) + x_buf[place].astype(jnp.float32)
        if hop:
            x_buf[place] = total.astype(x_buf.dtype)
            copy = remote(
                x_buf.at[place],
                out_ref.at[z],
                send_sem.at[depth + hop],
                recv_sem.at[depth + depth - hop],
                {"ctx": far},
            )
            copy.start()
            started.append(copy)
        else:
            out_ref[z] = total.astype(out_ref.dtype)
    arrived(x_shared, depth)
    shared_out[...] = shared_ref[x].astype(jnp.float32) + x_shared[...].astype(jnp.float32)
    for hop in range(1, depth):
        arrived(out_ref.at[lax.rem(z + hop, depth)], depth + hop)
    for copy in started:
        copy.wait_send()


def scatter_grads(grads, shared, depth, collective_id):
    return pl.pallas_call(
        partial(scatter_kernel, depth),
        out_shape=[
            jax.ShapeDtypeStruct((depth,) + grads.shape[1:], grads.dtype),
            jax.ShapeDtypeStruct(shared.shape[1:], jnp.float32),
        ],
        in_specs=[VMEM_SPEC] * 2,
        out_specs=[VMEM_SPEC] * 2,
        scratch_shapes=[
            pltpu.VMEM((depth,) + grads.shape[1:], grads.dtype),
            pltpu.VMEM(shared.shape[1:], shared.dtype),
            pltpu.SemaphoreType.DMA((2 * depth,)),
            pltpu.SemaphoreType.DMA((2 * depth,)),
        ],
        compiler_params=params_of(collective_id),
        name="scatter_grads",
    )(grads, shared)


def mxu(left, right, left_dim, right_dim, precision=None):
    return lax.dot_general(
        left,
        right,
        (((left_dim,), (right_dim,)), ((), ())),
        preferred_element_type=jnp.float32,
        precision=precision,
    )


def iota(shape, axis):
    return lax.broadcasted_iota(jnp.int32, shape, axis)


def ones_where(condition, kind):
    return jnp.where(condition, 1.0, 0.0).astype(kind)


def sigmoid(v):
    return 1.0 / (1.0 + jnp.exp(-v))


exact = lax.Precision.HIGHEST
LOW = jnp.bfloat16
OUT_AT, VALUE_AT = 128, 384


class BlockTerms:
    def __init__(self, start, segc_ref, segr_ref, small_ref, value_ref, bc_ref, step_in, width):
        self.start, self.width = start, width
        self.segc_ref, self.small_ref = segc_ref, small_ref
        rows = pl.ds(8 + start, BLOCK)
        seg = segc_ref[rows, :]
        row, col = iota((BLOCK, BLOCK), 0), iota((BLOCK, BLOCK), 1)
        self.row, self.col = row, col
        same = jnp.logical_and(seg == segr_ref[:, pl.ds(start, BLOCK)], row >= col)
        self.hidden_pairs = jnp.where(same, 0.0, -1e30)
        self.value_arg = self.conv(value_ref, 0, 4, width)
        self.bc_arg = self.conv(bc_ref, 9, 13, bc_ref.shape[1])
        self.value_sig = sigmoid(self.value_arg)
        self.bc_sig = sigmoid(self.bc_arg)
        self.values = (self.value_arg * self.value_sig).astype(LOW)
        bc_low = (self.bc_arg * self.bc_sig).astype(LOW)
        half = bc_ref.shape[1] // 2
        self.b_low, self.c_low = bc_low[:, :half], bc_low[:, half:]
        self.step = jnp.maximum(step_in, 0.0) + jnp.log1p(jnp.exp(-jnp.abs(step_in)))
        rates = small_ref[8:9, :width]
        self.log_decay = mxu(ones_where(row >= col, jnp.float32), self.step * rates, 1, 0, exact)
        self.log_rows = jnp.transpose(self.log_decay)
        self.step_rows = jnp.transpose(self.step)
        self.scores = mxu(self.c_low, self.b_low, 1, 1)
        seg = seg[:, :width]
        before = segc_ref[7 + start : 8 + start, :width]
        last = segc_ref[7 + start + BLOCK : 8 + start + BLOCK, :width]
        self.reach = jnp.where(seg == before, jnp.exp(self.log_decay), 0.0)
        self.reach_last = self.reach[BLOCK - 1 : BLOCK, :]
        self.fade = jnp.where(
            seg == last, jnp.exp(self.log_decay[BLOCK - 1 : BLOCK, :] - self.log_decay), 0.0
        )
        self.faded = self.fade * self.step * self.values.astype(jnp.float32)

    def conv(self, ref, taps_at, bias_at, width):
        total = self.small_ref[bias_at : bias_at + 1, :width]
        for distance in range(4):
            tap = self.small_ref[taps_at + 3 - distance : taps_at + 4 - distance, :width]
            total = total + tap * self.back(ref, distance, width)
        return total

    def back(self, ref, distance, width):
        rows = ref[pl.ds(8 + self.start - distance, BLOCK), :]
        if not distance:
            return rows
        here = self.segc_ref[pl.ds(8 + self.start, BLOCK), :width]
        there = self.segc_ref[pl.ds(8 + self.start - distance, BLOCK), :width]
        return jnp.where(here == there, rows, 0.0)

    def ahead(self, ref, distance, width):
        rows = ref[pl.ds(self.start + distance, BLOCK), :]
        if not distance:
            return rows
        here = self.segc_ref[pl.ds(8 + self.start, BLOCK), :width]
        there = self.segc_ref[pl.ds(8 + self.start + distance, BLOCK), :width]
        return jnp.where(here == there, rows, 0.0)

    def decay_pairs(self, head):
        at = head * HEADDIM
        return jnp.exp(
            self.log_decay[:, at : at + 1] - self.log_rows[at : at + 1, :] + self.hidden_pairs
        )

    def head_lanes(self, head):
        lanes = iota((BLOCK, self.width), 1)
        return jnp.logical_and(lanes >= head * HEADDIM, lanes < (head + 1) * HEADDIM)

    def of_head(self, array, head):
        return array * ones_where(self.head_lanes(head), array.dtype)


def lane_shift(width):
    return ones_where(iota((width, 256), 1) == iota((width, 256), 0) + 64, LOW)


def two_parts(array):
    high = array.astype(LOW)
    return high, (array - high.astype(jnp.float32)).astype(LOW)


def forward_kernel(
    precise,
    normed_ref,
    wall_ref,
    bcw_ref,
    small_ref,
    segr_ref,
    segc_ref,
    part_ref,
    squares_ref,
    gate_ref,
    value_ref,
    bc_ref,
    step_ref,
    mixed_ref,
    state_ref,
):
    tokens = normed_ref.shape[0]
    width = gate_ref.shape[1]
    heads = width // HEADDIM
    piece = 0 if precise else part_ref.shape[1]
    value_ref[0:8, :] = jnp.zeros((8, width), jnp.float32)
    bc_ref[0:8, :] = jnp.zeros((8, bc_ref.shape[1]), jnp.float32)
    spread = ones_where(
        iota((256, width), 0) - width == iota((256, width), 1) // HEADDIM, jnp.float32
    )
    shift = lane_shift(width)
    gains, skip = small_ref[5:6, :width], small_ref[6:7, :width]
    state = jnp.zeros(state_ref.shape[1:], jnp.float32)
    for block in range(tokens // BLOCK):
        start = block * BLOCK
        rows = pl.ds(start, BLOCK)
        normed = normed_ref[rows, :]
        gate_pre = mxu(normed, wall_ref[:, 0:256], 1, 0)[:, :width]
        both = mxu(normed, wall_ref[:, VALUE_AT : VALUE_AT + 256], 1, 0)
        value_ref[pl.ds(8 + start, BLOCK), :] = both[:, :width]
        bc_ref[pl.ds(8 + start, BLOCK), :] = mxu(normed, bcw_ref[...], 1, 0)
        step_in = mxu(both, spread, 1, 0, exact) + small_ref[7:8, :width]
        gate_ref[rows, :] = gate_pre
        step_ref[rows, :] = step_in
        terms = BlockTerms(start, segc_ref, segr_ref, small_ref, value_ref, bc_ref, step_in, width)
        mixed = skip * terms.values.astype(jnp.float32)
        for head in range(heads):
            at = head * HEADDIM
            weights = terms.scores * terms.decay_pairs(head) * terms.step_rows[at : at + 1, :]
            own_values = terms.of_head(terms.values, head)
            for term in two_parts(weights) if precise else (weights.astype(LOW),):
                mixed += mxu(term, own_values, 1, 0)
        state_ref[block] = state
        if block:
            for term in two_parts(state) if precise else (state.astype(LOW),):
                mixed += terms.reach * mxu(terms.c_low, term, 1, 0)
        state = terms.reach_last * state
        for term in two_parts(terms.faded) if precise else (terms.faded.astype(LOW),):
            state += mxu(terms.b_low, term, 0, 0)
        mixed_ref[rows, :] = mixed
        gated = mixed * gate_pre * sigmoid(gate_pre)
        squares = gated * gated
        if precise:
            part_ref[rows, :] = gated
            for at in range(0, BLOCK, 128):
                row = (start + at) // 128
                squares_ref[row : row + 1, :] = mxu(
                    jnp.ones((8, width), jnp.float32), squares[at : at + 128], 1, 1, exact
                )[0:1]
            continue
        for at in range(0, BLOCK, piece):
            slot = (start + at) // piece
            squares_ref[slot, :, 0:piece] = mxu(
                jnp.ones((8, width), jnp.float32), squares[at : at + piece], 1, 1, exact
            )
        moved = mxu((gated * gains).astype(LOW), shift, 1, 0).astype(LOW)
        part = mxu(moved, wall_ref[:, OUT_AT : OUT_AT + 256], 1, 1).astype(LOW)
        for at in range(0, BLOCK, piece):
            part_ref[(start + at) // piece] = part[at : at + piece]


def local_params():
    return pltpu.CompilerParams(vmem_limit_bytes=60 << 20)


def split_forward(normed, wall, bcw, small, segr, segc, slots, precise):
    tokens, model_width = normed.shape
    piece = tokens // slots
    width = INNER // slots
    bc_width = bcw.shape[1]
    f32 = jnp.float32
    if precise:
        first = [
            jax.ShapeDtypeStruct((tokens, width), f32),
            jax.ShapeDtypeStruct((tokens // 128, 128), f32),
        ]
    else:
        first = [
            jax.ShapeDtypeStruct((slots, piece, model_width), LOW),
            jax.ShapeDtypeStruct((slots, 8, 128), f32),
        ]
    return pl.pallas_call(
        partial(forward_kernel, precise),
        out_shape=first
        + [
            jax.ShapeDtypeStruct((tokens, width), f32),
            jax.ShapeDtypeStruct((tokens + 8, width), f32),
            jax.ShapeDtypeStruct((tokens + 8, bc_width), f32),
            jax.ShapeDtypeStruct((tokens, width), f32),
            jax.ShapeDtypeStruct((tokens, width), f32),
            jax.ShapeDtypeStruct((tokens // BLOCK, bc_width // 2, width), f32),
        ],
        in_specs=[VMEM_SPEC] * 6,
        out_specs=[VMEM_SPEC] * 8,
        compiler_params=local_params(),
        name="forward_block",
    )(normed, wall, bcw, small, segr, segc)


def row_sum(array):
    return jnp.sum(array, axis=0, keepdims=True)


def backward_kernel(
    grad_ref,
    scalar_ref,
    normed_ref,
    wall_ref,
    small_ref,
    segr_ref,
    segc_ref,
    gate_ref,
    value_ref,
    bc_ref,
    step_ref,
    mixed_ref,
    state_ref,
    both_ref,
    grads_ref,
    sums_ref,
    pre_ref,
    scaled_ref,
    e_ref,
    e_bc_ref,
):
    tokens, model_width = normed_ref.shape
    width = gate_ref.shape[1]
    bc_width = bc_ref.shape[1]
    heads = width // HEADDIM
    piece = both_ref.shape[1]
    blocks = tokens // BLOCK
    f32 = jnp.float32
    shift = lane_shift(width)
    gains, skip, rates = (small_ref[at : at + 1, :width] for at in (5, 6, 8))
    e_ref[tokens:, :] = jnp.zeros((8, width), f32)
    e_bc_ref[tokens:, :] = jnp.zeros((8, bc_width), f32)
    pre_ref[...] = jnp.zeros(pre_ref.shape, LOW)
    eye = ones_where(iota((piece, 128), 0) == iota((piece, 128), 1), f32)
    same_head = ones_where(
        iota((width, width), 0) // HEADDIM == iota((width, width), 1) // HEADDIM, f32
    )
    tail = ones_where(iota((width, 128), 0) == iota((width, 128), 1) + 128, LOW)
    pick = ones_where(
        jnp.logical_and(
            iota((width, 128), 0) == (iota((width, 128), 1) - 64) * HEADDIM, iota((width, 128), 1) >= 64
        ),
        LOW,
    )
    grad_state = jnp.zeros(state_ref.shape[1:], f32)
    sums = {}

    def add(name, term):
        sums[name] = sums[name] + term if name in sums else term

    for block in reversed(range(blocks)):
        start = block * BLOCK
        rows = pl.ds(start, BLOCK)
        step_in = step_ref[rows, :]
        terms = BlockTerms(start, segc_ref, segr_ref, small_ref, value_ref, bc_ref, step_in, width)
        columns = jnp.concatenate(
            [
                mxu(eye, scalar_ref[(start + at) // piece], 1, 1, exact)
                for at in range(0, BLOCK, piece)
            ],
            axis=0,
        )
        inv, inner = columns[:, 0:1], columns[:, 1:2]
        grad_low = grad_ref[rows, 0:model_width]
        grad_scaled = mxu(grad_low, wall_ref[:, OUT_AT : OUT_AT + 256], 1, 0)
        grad_scaled = pltpu.roll(grad_scaled, 192, 1)[:, :width]
        gate_pre, mixed = gate_ref[rows, :], mixed_ref[rows, :]
        sig = sigmoid(gate_pre)
        act = gate_pre * sig
        gated = mixed * act
        normal = gated * inv
        scaled_ref[rows, :] = mxu((normal * gains).astype(LOW), shift, 1, 0).astype(LOW)
        add("out_gain", row_sum(grad_scaled * normal))
        grad_gated = inv * (grad_scaled * gains) - gated * (inv * inv * inner)
        grad_gate = grad_gated * mixed * sig * (1.0 + gate_pre * (1.0 - sig))
        pre_ref[rows, 0:width] = grad_gate.astype(LOW)
        grad_mixed = grad_gated * act
        grad_mixed_low = grad_mixed.astype(LOW)
        values = terms.values.astype(f32)
        add("skip", row_sum(grad_mixed * values))
        grad_values = skip * grad_mixed
        direct = jnp.zeros((BLOCK, width), f32)
        between = jnp.zeros((BLOCK, width), f32)
        pair_sum = jnp.zeros((BLOCK, BLOCK), f32)
        from_here = ones_where(terms.col >= terms.row, LOW)
        for head in range(heads):
            at = head * HEADDIM
            decay = terms.decay_pairs(head)
            step_row = terms.step_rows[at : at + 1, :]
            grad_head = terms.of_head(grad_mixed_low, head)
            head_ones = ones_where(terms.head_lanes(head), LOW)
            products = mxu(grad_head, terms.values, 1, 1)
            scored = terms.scores * decay
            grad_values += mxu((scored * step_row).astype(LOW), grad_head, 0, 0)
            pair_sum += decay * step_row * products
            unstepped = scored * products
            direct += mxu(unstepped.astype(LOW), head_ones, 0, 0)
            later = mxu(from_here, (unstepped * step_row).astype(LOW), 1, 0)
            later = jnp.where(terms.col < terms.row, later, 0.0)
            between += mxu(later.astype(LOW), head_ones, 1, 0)
        pair_low = pair_sum.astype(LOW)
        grad_b = mxu(pair_low, terms.c_low, 0, 0)
        grad_c = mxu(pair_low, terms.b_low, 1, 0)
        across = jnp.zeros((BLOCK, width), f32)
        if block < blocks - 1:
            state_low = grad_state.astype(LOW)
            to_state = mxu(terms.b_low, state_low, 1, 0)
            grad_values += terms.fade * terms.step * to_state
            by_step = terms.fade * to_state * values
            direct += mxu(by_step, same_head, 1, 0, exact)
            grad_b += mxu(terms.faded.astype(LOW), state_low, 1, 1)
            across += mxu(
                ones_where(terms.col < terms.row, f32), terms.step * by_step, 1, 0, exact
            )
        if block:
            entering = state_ref[block]
            entering_low = entering.astype(LOW)
            carried = terms.reach * mxu(terms.c_low, entering_low, 1, 0)
            across += mxu(
                ones_where(terms.col >= terms.row, f32), grad_mixed * carried, 1, 0, exact
            )
            reached = (terms.reach * grad_mixed).astype(LOW)
            grad_c += mxu(reached, entering_low, 1, 1)
            if block < blocks - 1:
                across += row_sum(grad_state * terms.reach_last * entering)
            grad_state = terms.reach_last * grad_state + mxu(terms.c_low, reached, 0, 0)
        between += mxu(across, same_head, 1, 0, exact)
        grad_step = direct + rates * between
        add("rates", row_sum(terms.step * between))
        grad_step_in = grad_step * sigmoid(step_in)
        add("step_bias", row_sum(grad_step_in))
        e = grad_values * (terms.value_sig * (1.0 + terms.value_arg * (1.0 - terms.value_sig)))
        e_ref[rows, :] = e
        e_bc = jnp.concatenate([grad_b, grad_c], axis=1) * (
            terms.bc_sig * (1.0 + terms.bc_arg * (1.0 - terms.bc_sig))
        )
        e_bc_ref[rows, :] = e_bc
        add("value_bias", row_sum(e))
        add("bc_bias", row_sum(e_bc))
        grad_value = jnp.zeros((BLOCK, width), f32)
        grad_bc = jnp.zeros((BLOCK, bc_width), f32)
        for distance in range(4):
            tap = 3 - distance
            add(("value", tap), row_sum(e * terms.back(value_ref, distance, width)))
            add(("bc", tap), row_sum(e_bc * terms.back(bc_ref, distance, bc_width)))
            grad_value += small_ref[tap : tap + 1, :width] * terms.ahead(e_ref, distance, width)
            grad_bc += small_ref[9 + tap : 10 + tap, :] * terms.ahead(e_bc_ref, distance, bc_width)
        value_low = grad_value.astype(LOW)
        pre_ref[rows, VALUE_AT : VALUE_AT + 128] = value_low[:, 0:128]
        pre_ref[rows, VALUE_AT + 128 : VALUE_AT + 256] = (
            mxu(value_low, tail, 1, 0) + mxu(grad_step_in.astype(LOW), pick, 1, 0)
        ).astype(LOW)
        part = mxu(pre_ref[rows, :], wall_ref[...], 1, 1).astype(LOW)
        grad_bc = grad_bc.astype(LOW)
        for at in range(0, BLOCK, piece):
            slot = (start + at) // piece
            both_ref[slot, :, 0:model_width] = part[at : at + piece]
            both_ref[slot, :, model_width:] = grad_bc[at : at + piece]

    k_rows = grads_ref.shape[1]
    for pair in range(grads_ref.shape[0] // 2):
        lanes = pl.ds(pair * 2 * k_rows, 2 * k_rows)
        total = mxu(normed_ref[:, lanes], pre_ref[...], 0, 0)
        out = mxu(grad_ref[:, lanes], scaled_ref[...], 0, 0)
        for at in range(2):
            k_slice = slice(at * k_rows, (at + 1) * k_rows)
            slot = 2 * pair + at
            grads_ref[slot, :, 0:OUT_AT] = total[k_slice, 0:OUT_AT].astype(LOW)
            grads_ref[slot, :, OUT_AT:VALUE_AT] = (
                total[k_slice, OUT_AT:VALUE_AT] + out[k_slice]
            ).astype(LOW)
            grads_ref[slot, :, VALUE_AT:] = total[k_slice, VALUE_AT:].astype(LOW)

    sums_ref[...] = jnp.zeros(sums_ref.shape, f32)
    head_sums = mxu(
        jnp.concatenate([sums["skip"], jnp.zeros((7, width), f32)], axis=0), same_head, 1, 0, exact
    )
    for tap in range(4):
        sums_ref[tap : tap + 1, 0:width] = sums["value", tap]
        sums_ref[9 + tap : 10 + tap, :] = sums["bc", tap]
    sums_ref[4:5, 0:width] = sums["value_bias"]
    sums_ref[5:6, 0:width] = sums["out_gain"]
    sums_ref[6:7, 0:width] = head_sums[0:1]
    sums_ref[7:8, 0:width] = sums["step_bias"]
    sums_ref[8:9, 0:width] = sums["rates"] * rates
    sums_ref[13:14, :] = sums["bc_bias"]


def split_backward(grad, scalars, normed, wall, small, segr, segc, kept, slots):
    tokens, model_width = normed.shape
    piece = tokens // slots
    width = kept[0].shape[1]
    bc_width = kept[2].shape[1]
    k_slots = slots // 2
    return pl.pallas_call(
        backward_kernel,
        out_shape=[
            jax.ShapeDtypeStruct((slots, piece, model_width + bc_width), LOW),
            jax.ShapeDtypeStruct((k_slots, model_width // k_slots, PACK), LOW),
            jax.ShapeDtypeStruct((16, 256), jnp.float32),
        ],
        in_specs=[VMEM_SPEC] * 13,
        out_specs=[VMEM_SPEC] * 3,
        scratch_shapes=[
            pltpu.VMEM((tokens, PACK), LOW),
            pltpu.VMEM((tokens, 256), LOW),
            pltpu.VMEM((tokens + 8, width), jnp.float32),
            pltpu.VMEM((tokens + 8, bc_width), jnp.float32),
        ],
        compiler_params=local_params(),
        name="backward_block",
    )(grad, scalars, normed, wall, small, segr, segc, *kept)


def lane_rows(columns, slots):
    rows = jnp.stack([c.reshape(slots, -1) for c in columns], axis=1)
    return jnp.pad(rows, ((0, 0), (0, 8 - rows.shape[1]), (0, 128 - rows.shape[2])))


def norm_rows(hidden, gain):
    inv = lax.rsqrt(jnp.mean(hidden * hidden, axis=1, keepdims=True) + epsilon)
    return inv, (hidden * inv * gain).astype(jnp.bfloat16)


HALVES = 2


class Links:
    def __init__(self, depth):
        self.depth = depth
        self.x, self.z, self.t = (lax.axis_index(name) for name in ("dp", "ctx", "tp"))
        self.core, self.chip = {"tp": other_core(self.t)}, {"tp": other_chip(self.t)}
        self.far_x = {"dp": 1 - self.x}
        self.left = {"ctx": lax.rem(self.z + depth - 1, depth)}
        self.right = {"ctx": lax.rem(self.z + 1, depth)}
        self.sent = []

    def send(self, source, target, send_sem, recv_sem, peer, when=None):
        copy = remote(source, target, send_sem, recv_sem, peer)
        self.sent.append((copy, when))
        if when is None:
            copy.start()
        else:
            pl.when(when)(copy.start)

    def wait(self, ref, send_sem, recv_sem, when=None):
        copy = remote(ref, ref, send_sem, recv_sem, self.core)
        if when is None:
            copy.wait_recv()
        else:
            pl.when(when)(copy.wait_recv)

    def finish(self):
        for copy, when in self.sent:
            if when is None:
                copy.wait_send()
            else:
                pl.when(when)(copy.wait_send)

    def near_first(self):
        z = self.z
        first = z + 1 - 2 * lax.rem(z, 2)
        third = 3 - 3 * (z // 2)
        return [first, 6 - z - first - third, third]

    def far_first(self):
        z = self.z
        odd = lax.rem(z, 2)
        first = 3 - 3 * (z // 2)
        second = (1 - odd) * (2 + z // 2) + odd * (z // 2)
        return [first, second, 6 - z - first - second]


def everyone(depth):
    z, t = lax.axis_index("ctx"), lax.axis_index("tp")
    return [
        {"ctx": lax.rem(z + hop, depth), "tp": lax.rem(t + turn, 4)}
        for hop in range(depth)
        for turn in range(4)
        if hop or turn
    ]


def half(ref, part):
    rows = ref.shape[0] // HALVES
    return ref.at[pl.ds(part * rows, rows)]


def gather_task(links, pieces, fulls, send_sem, recv_sem):
    z, t = links.z, links.t
    last = links.depth - 1
    own = z * 4 + t

    def pass_on(a, ref, slot, part, to_left, to_right, chip=True):
        target = half(fulls[a].at[slot], part)
        recv = recv_sem.at[a, slot, part]

        def go(way, peer, when=None):
            links.send(ref, target, send_sem.at[a, slot, part, way], recv, peer, when)

        if chip:
            go(0, links.left, to_left)
            go(1, links.right, to_right)
            go(2, links.chip)
        go(3, links.core)

    def arrived(a, slot, part):
        ref = half(fulls[a].at[slot], part)
        links.wait(ref, send_sem.at[a, slot, part, 0], recv_sem.at[a, slot, part])
        return ref

    every = range(len(pieces))
    for part in range(HALVES):
        for a in every:
            pass_on(a, half(pieces[a], part), own, part, z > 0, z < last)
    for a in every:
        fulls[a][own] = pieces[a][...]
    yield
    column = other_chip(t)
    order = links.near_first()
    for place, far in enumerate(order):
        slot = far * 4 + t
        for part in range(HALVES):
            for a in every:
                ref = arrived(a, slot, part)
                to_left = jnp.logical_and(far > z, z > 0)
                to_right = jnp.logical_and(far < z, z < last)
                pass_on(a, ref, slot, part, to_left, to_right)
        yield
        slot = (order[place - 1] if place else z) * 4 + column
        for part in range(HALVES):
            for a in every:
                pass_on(a, arrived(a, slot, part), slot, part, None, None, False)
        yield
    for part in range(HALVES):
        for a in every:
            slot = order[-1] * 4 + column
            pass_on(a, arrived(a, slot, part), slot, part, None, None, False)
    yield
    for far in [z] + order:
        for row in (other_core(t), other_chip(other_core(t))):
            for part in range(HALVES):
                for a in every:
                    arrived(a, far * 4 + row, part)


def gather_sems(count, slots):
    return [
        pltpu.SemaphoreType.DMA((count, slots, HALVES, 4)),
        pltpu.SemaphoreType.DMA((count, slots, HALVES)),
    ]


def reduce_task(links, produce, parts, outs, bufs, send_sem, recv_sem):
    z, t = links.z, links.t
    depth = links.depth
    last = depth - 1
    order = links.far_first() + [z]
    every = range(len(parts))

    def rows_of(ref, part):
        rows = ref.shape[0] // HALVES
        return slice(part * rows, (part + 1) * rows)

    def sems(a, at, part):
        return send_sem.at[a, at, part], recv_sem.at[a, at, part]

    def loaded(a, at, part):
        return bufs[a][at, rows_of(bufs[a].at[at], part), :].astype(jnp.float32)

    def mine(a, slot, part):
        return parts[a][slot, rows_of(parts[a].at[slot], part), :].astype(jnp.float32)

    def wait(a, at, part, when=None):
        links.wait(half(bufs[a].at[at], part), *sems(a, at, part), when)

    def stage1(far):
        produce(far)
        for which, row in enumerate((other_chip(other_core(t)), other_core(t))):
            for part in range(HALVES):
                for a in every:
                    at = far * 2 + which
                    links.send(
                        half(parts[a].at[far * 4 + row], part),
                        half(bufs[a].at[at], part),
                        *sems(a, at, part),
                        links.core,
                    )

    def stage2(far):
        for part in range(HALVES):
            for a in every:
                at = far * 2
                wait(a, at, part)
                total = mine(a, far * 4 + other_chip(t), part) + loaded(a, at, part)
                bufs[a][at, rows_of(bufs[a].at[at], part), :] = total.astype(bufs[a].dtype)
                to = 2 * depth + far
                links.send(
                    half(bufs[a].at[at], part), half(bufs[a].at[to], part), *sems(a, to, part), links.chip
                )

    def stage3(far):
        at = far * 2 + 1
        for part in range(HALVES):
            for a in every:
                wait(a, at, part)
                wait(a, 2 * depth + far, part)
                total = mine(a, far * 4 + t, part) + loaded(a, at, part) + loaded(a, 2 * depth + far, part)
                out = outs[a]
                rows = rows_of(out, part)
                if far is z:
                    out[rows, :] = total
                    continue
                ref = bufs[a]
                here = (at, rows_of(ref.at[at], part), slice(None))
                for way, (peer, when, first) in enumerate(
                    ((links.right, far > z, z == 0), (links.left, far < z, z == last))
                ):
                    chain = 3 * depth + way * depth + far

                    def go(total=total, chain=chain, here=here, ref=ref, first=first, a=a, part=part):
                        @pl.when(first)
                        def _():
                            ref[here] = total.astype(ref.dtype)

                        @pl.when(jnp.logical_not(first))
                        def _():
                            wait(a, chain, part)
                            ref[here] = (total + loaded(a, chain, part)).astype(ref.dtype)

                    pl.when(when)(go)
                    links.send(
                        half(ref.at[at], part), half(ref.at[chain], part), *sems(a, chain, part), peer, when
                    )

    count = len(order)
    for place in range(count + 2):
        if place < count:
            stage1(order[place])
        if 1 <= place <= count:
            stage2(order[place - 1])
        if 2 <= place:
            stage3(order[place - 2])
        yield
    for way, when in enumerate((z > 0, z < last)):
        chain = 3 * depth + way * depth + z
        for part in range(HALVES):
            for a in every:

                @pl.when(when)
                def _(a=a, part=part, chain=chain):
                    wait(a, chain, part)
                    outs[a][rows_of(outs[a], part), :] += loaded(a, chain, part)


def reduce_scratch(shapes, dtypes, depth):
    return [pltpu.VMEM((5 * depth,) + s, d) for s, d in zip(shapes, dtypes)] + [
        pltpu.SemaphoreType.DMA((len(shapes), 5 * depth, HALVES)),
        pltpu.SemaphoreType.DMA((len(shapes), 5 * depth, HALVES)),
    ]


def run_tasks(*tasks):
    tasks = list(tasks)
    while tasks:
        for task in list(tasks):
            try:
                next(task)
            except StopIteration:
                tasks.remove(task)


def share_task(links, own, full, send_sem, recv_sem):
    depth = links.depth
    slot = links.z * 4 + links.t
    for at, peer in enumerate(everyone(depth)):
        links.send(own, full.at[slot], send_sem.at[at], recv_sem.at[slot], peer)
    full[slot] = own[...]
    yield
    for hop in range(depth):
        for turn in range(4):
            if hop or turn:
                source = lax.rem(links.z + hop, depth) * 4 + lax.rem(links.t + turn, 4)
                links.wait(full.at[source], send_sem.at[0], recv_sem.at[source])


def spread_rows(rows):
    size = rows.shape[1]
    eye = ones_where(iota((size, size), 0) == iota((size, size), 1), jnp.float32)
    return mxu(eye, rows, 1, 1, exact)


def turn_forward_kernel(
    depth,
    gated_ref,
    squares_ref,
    small_ref,
    wall_ref,
    hidden_ref,
    gain_ref,
    hidden_out,
    total_out,
    inv_out,
    full_out,
    parts,
    normed,
    shared,
    share_send,
    share_recv,
    bufs,
    reduce_send,
    reduce_recv,
    gather_send,
    gather_recv,
):
    links = Links(depth)
    greet(everyone(depth))
    width = gated_ref.shape[1]
    piece = hidden_ref.shape[0]
    block = 4 * piece
    run_tasks(share_task(links, squares_ref, shared, share_send, share_recv))
    total = shared[0]
    for slot in range(1, 4 * depth):
        total = total + shared[slot]
    inv_rows = lax.rsqrt(total / INNER + epsilon)
    inv_out[...] = inv_rows
    columns = spread_rows(inv_rows)
    shift = lane_shift(width)
    gains = small_ref[5:6, :width]
    which = iota((block, columns.shape[1]), 1)

    def produce(far):
        at = far * (block // 128)
        both = jnp.concatenate([columns] * (block // 128), axis=0)
        low = iota((block, columns.shape[1]), 0) // 128 + at
        inv = jnp.sum(jnp.where(which == low, both, 0.0), axis=1, keepdims=True)
        rows = pl.ds(pl.multiple_of(far * block, block), block)
        scaled = (gated_ref[rows, :] * inv * gains).astype(LOW)
        moved = mxu(scaled, shift, 1, 0).astype(LOW)
        part = mxu(moved, wall_ref[:, OUT_AT : OUT_AT + 256], 1, 1)
        for row in range(4):
            parts[far * 4 + row] = part[row * piece : (row + 1) * piece].astype(parts.dtype)

    run_tasks(
        reduce_task(links, produce, [parts], [total_out], [bufs], reduce_send, reduce_recv)
    )
    hidden = hidden_ref[...].astype(jnp.float32) + total_out[...]
    hidden_out[...] = hidden
    inv = lax.rsqrt(jnp.mean(hidden * hidden, axis=1, keepdims=True) + epsilon)
    normed[...] = (hidden * inv * gain_ref[...]).astype(LOW)
    run_tasks(gather_task(links, [normed], [full_out], gather_send, gather_recv))
    links.finish()


def turn_forward(gated, squares, small, wall, hidden, gain, depth, collective_id):
    piece, model_width = hidden.shape
    slots = 4 * depth
    f32 = jnp.float32
    return pl.pallas_call(
        partial(turn_forward_kernel, depth),
        out_shape=[
            jax.ShapeDtypeStruct((piece, model_width), f32),
            jax.ShapeDtypeStruct((piece, model_width), f32),
            jax.ShapeDtypeStruct(squares.shape, f32),
            jax.ShapeDtypeStruct((slots, piece, model_width), LOW),
        ],
        in_specs=[VMEM_SPEC] * 6,
        out_specs=[VMEM_SPEC] * 4,
        scratch_shapes=[
            pltpu.VMEM((slots, piece, model_width), f32),
            pltpu.VMEM((piece, model_width), LOW),
            pltpu.VMEM((slots,) + squares.shape, f32),
            pltpu.SemaphoreType.DMA((slots,)),
            pltpu.SemaphoreType.DMA((slots,)),
        ]
        + reduce_scratch([(piece, model_width)], [f32], depth)
        + gather_sems(1, slots),
        compiler_params=params_of(collective_id),
        name="turn_forward",
    )(gated, squares, small, wall, hidden, gain)


def turn_backward_kernel(
    depth,
    last,
    both_ref,
    grad_ref,
    hidden_ref,
    gain_ref,
    bcw_ref,
    total_ref,
    scalar_ref,
    grad_out,
    gain_out,
    low_out,
    *refs,
):
    links = Links(depth)
    greet(everyone(depth))
    if last:
        full_out, total, piece_low, bufs, reduce_send, reduce_recv, gather_send, gather_recv = refs
    else:
        full_out, scalar_out, total, piece_low, scalars, bufs, reduce_send, reduce_recv, gather_send, gather_recv = refs
    model_width = hidden_ref.shape[1]
    piece = hidden_ref.shape[0]
    run_tasks(
        reduce_task(
            links, lambda far: None, [both_ref], [total], [bufs], reduce_send, reduce_recv
        )
    )
    bc_low = total[:, model_width:].astype(LOW)
    grad_normed = total[:, :model_width] + mxu(bc_low, bcw_ref[...], 1, 1)
    hidden = hidden_ref[...].astype(jnp.float32)
    inv = lax.rsqrt(jnp.mean(hidden * hidden, axis=1, keepdims=True) + epsilon)
    weighted = grad_normed * gain_ref[...]
    gain_out[...] = row_sum(grad_normed * hidden * inv)
    grad = (
        grad_ref[...].astype(jnp.float32)
        + inv * weighted
        - hidden * (inv * inv * inv) * jnp.mean(weighted * hidden, axis=1, keepdims=True)
    )
    grad_low = grad.astype(LOW)
    low_out[...] = grad_low
    grad_out[...] = grad
    if last:
        piece_low[...] = bc_low
        run_tasks(gather_task(links, [piece_low], [full_out], gather_send, gather_recv))
    else:
        piece_low[:, :model_width] = grad_low
        piece_low[:, model_width:] = bc_low
        inner = jnp.sum(grad_low.astype(jnp.float32) * total_ref[...], axis=1, keepdims=True) / INNER
        eye = ones_where(iota((piece, 128), 0) == iota((piece, 128), 1), jnp.float32)
        row = mxu(jnp.broadcast_to(inner, (piece, 8)), eye, 0, 0, exact)
        scalars[...] = jnp.where(iota((8, 128), 0) == 1, row, scalar_ref[...])
        run_tasks(
            gather_task(links, [piece_low, scalars], [full_out, scalar_out], gather_send, gather_recv)
        )
    links.finish()


def turn_backward(both, grad, hidden, gain, bcw, total, scalars, last, depth, collective_id):
    piece, model_width = hidden.shape
    slots, _, whole_width = both.shape
    f32 = jnp.float32
    low_width = whole_width - model_width if last else whole_width
    fulls = [jax.ShapeDtypeStruct((slots, piece, low_width), LOW)]
    own = [pltpu.VMEM((piece, low_width), LOW)]
    if not last:
        fulls.append(jax.ShapeDtypeStruct((slots, 8, 128), f32))
        own.append(pltpu.VMEM((8, 128), f32))
    return pl.pallas_call(
        partial(turn_backward_kernel, depth, last),
        out_shape=[
            jax.ShapeDtypeStruct((piece, model_width), f32),
            jax.ShapeDtypeStruct((1, model_width), f32),
            jax.ShapeDtypeStruct((piece, model_width), LOW),
        ]
        + fulls,
        in_specs=[VMEM_SPEC] * 7,
        out_specs=[VMEM_SPEC] * (3 + len(fulls)),
        scratch_shapes=[pltpu.VMEM((piece, whole_width), f32)]
        + own
        + reduce_scratch([(piece, whole_width)], [LOW], depth)
        + gather_sems(len(fulls), slots),
        compiler_params=params_of(collective_id),
        name="turn_backward",
    )(both, grad, hidden, gain, bcw, total, scalars)


def weights_task(links, packs, fulls, send_sem, recv_sem):
    x, z, depth = links.x, links.z, links.depth
    every = range(len(packs))

    def source(a, far, part):
        ref = packs[a]
        return half(ref.at[far] if len(ref.shape) == len(fulls[a].shape) else ref, part)

    def send(a, ref, slot, part, kind, peer):
        links.send(
            ref, half(fulls[a].at[slot], part), send_sem.at[a, kind, part], recv_sem.at[a, slot, part], peer
        )

    def arrived(a, slot, part):
        ref = half(fulls[a].at[slot], part)
        links.wait(ref, send_sem.at[a, 0, part], recv_sem.at[a, slot, part])
        return ref

    mine = x * depth + z
    for a in every:
        for part in range(HALVES):
            send(a, source(a, z, part), mine, part, 0, links.far_x)
    for place, far in enumerate(links.far_first()):
        for a in every:
            for part in range(HALVES):
                send(a, source(a, far, part), mine, part, 1 + place, {"ctx": far})
    for a in every:
        ref = packs[a]
        fulls[a][mine] = ref[z] if len(ref.shape) == len(fulls[a].shape) else ref[...]
    yield
    for place, far in enumerate(links.near_first()):
        for part in range(HALVES):
            for a in every:
                slot = x * depth + far
                send(a, arrived(a, slot, part), slot, part, depth + place, links.far_x)
        yield
    for far in [z] + links.near_first():
        for part in range(HALVES):
            for a in every:
                arrived(a, (1 - x) * depth + far, part)


def weights_sems(count, depth):
    return [
        pltpu.SemaphoreType.DMA((count, 2 * depth, HALVES)),
        pltpu.SemaphoreType.DMA((count, 2 * depth, HALVES)),
    ]


def prepare_kernel(depth, count, *refs):
    pieces, packs = refs[:count], refs[count : count + 2]
    refs = refs[count + 2 :]
    fulls, full_packs = refs[:count], refs[count : count + 2]
    gather_send, gather_recv, pack_send, pack_recv = refs[count + 2 :]
    links = Links(depth)
    greet(everyone(depth) + [links.far_x])
    run_tasks(
        gather_task(links, pieces, fulls, gather_send, gather_recv),
        weights_task(links, packs, full_packs, pack_send, pack_recv),
    )
    links.finish()


def prepare(pieces, packs, depth, collective_id):
    count = len(pieces)
    slots = 4 * depth
    return pl.pallas_call(
        partial(prepare_kernel, depth, count),
        out_shape=[jax.ShapeDtypeStruct((slots,) + p.shape, p.dtype) for p in pieces]
        + [jax.ShapeDtypeStruct((2 * depth,) + p.shape[-2:], p.dtype) for p in packs],
        in_specs=[VMEM_SPEC] * (count + 2),
        out_specs=[VMEM_SPEC] * (count + 2),
        scratch_shapes=gather_sems(count, slots) + weights_sems(2, depth),
        compiler_params=params_of(collective_id),
        name="prepare",
    )(*pieces, *packs)


def finish_kernel(depth, channel_rows, sums_ref, hidden_ref, grad_ref, by_z_out, sum_out, hidden_out, grad_out, work, total, arrived_ref, send_sem, recv_sem, row_send, row_recv):
    links = Links(depth)
    z, t = links.z, links.t
    greet(everyone(depth) + [links.far_x])

    def rows():
        outs = (hidden_out, grad_out)
        for a, ref in enumerate((hidden_ref, grad_ref)):
            for way, peer in enumerate((links.chip, links.core)):
                links.send(ref, outs[a].at[t], row_send.at[a, way], row_recv.at[a, t], peer)
            outs[a][t] = ref[...]
        yield
        for a in range(2):
            column = other_chip(t)
            ref = outs[a].at[column]
            links.wait(ref, row_send.at[a, 0], row_recv.at[a, column])
            links.send(ref, ref, row_send.at[a, 2], row_recv.at[a, column], links.core)
        yield
        for a in range(2):
            for column in (other_core(t), other_chip(other_core(t))):
                links.wait(outs[a].at[column], row_send.at[a, 0], row_recv.at[a, column])

    def sums():
        links.send(sums_ref, arrived_ref.at[0], send_sem.at[0], recv_sem.at[0], links.far_x)
        yield
        links.wait(arrived_ref.at[0], send_sem.at[0], recv_sem.at[0])
        work[...] = sums_ref[...] + arrived_ref[0]
        links.send(work, arrived_ref.at[1], send_sem.at[1], recv_sem.at[1], links.core)
        yield
        links.wait(arrived_ref.at[1], send_sem.at[1], recv_sem.at[1])
        total[0] = work[...] + arrived_ref[1]
        links.send(total.at[0], arrived_ref.at[2], send_sem.at[2], recv_sem.at[2], links.chip)
        yield
        links.wait(arrived_ref.at[2], send_sem.at[2], recv_sem.at[2])
        row = iota(work.shape, 0)
        own = jnp.logical_and(row < 16 * LAYERS, lax.rem(row, 16) < channel_rows)
        total[1] = jnp.where(own, work[...], total[0] + arrived_ref[2])
        for hop in range(1, depth):
            links.send(
                total.at[1], by_z_out.at[z], send_sem.at[2 + hop], recv_sem.at[3 + z], {"ctx": lax.rem(z + hop, depth)}
            )
        by_z_out[z] = total[1]
        yield
        for hop in range(1, depth):
            far = lax.rem(z + hop, depth)
            links.wait(by_z_out.at[far], send_sem.at[0], recv_sem.at[3 + far])
        whole = by_z_out[0]
        for far in range(1, depth):
            whole = whole + by_z_out[far]
        sum_out[...] = whole

    run_tasks(rows(), sums())
    links.finish()


def finish(sums, hidden, grad, depth, collective_id):
    f32 = jnp.float32
    return pl.pallas_call(
        partial(finish_kernel, depth, 9),
        out_shape=[
            jax.ShapeDtypeStruct((depth,) + sums.shape, f32),
            jax.ShapeDtypeStruct(sums.shape, f32),
            jax.ShapeDtypeStruct((4,) + hidden.shape, hidden.dtype),
            jax.ShapeDtypeStruct((4,) + grad.shape, grad.dtype),
        ],
        in_specs=[VMEM_SPEC] * 3,
        out_specs=[VMEM_SPEC] * 4,
        scratch_shapes=[
            pltpu.VMEM(sums.shape, f32),
            pltpu.VMEM((2,) + sums.shape, f32),
            pltpu.VMEM((3,) + sums.shape, f32),
            pltpu.SemaphoreType.DMA((3 + depth,)),
            pltpu.SemaphoreType.DMA((3 + depth,)),
            pltpu.SemaphoreType.DMA((2, 3)),
            pltpu.SemaphoreType.DMA((2, 4)),
        ],
        compiler_params=params_of(collective_id),
        name="finish",
    )(sums, hidden, grad)


def split_local(
    depth,
    hidden_in,
    segment_ids,
    cotangent,
    norm_gain,
    gate_proj,
    value_proj,
    bc_proj,
    step_proj,
    conv_value,
    conv_value_bias,
    conv_bc,
    conv_bc_bias,
    decay_log,
    step_bias,
    skip_gain,
    out_gain,
    out_proj,
):
    tokens, model_width = hidden_in.shape[1:]
    slots = depth * 4
    piece = tokens // 4
    width = gate_proj.shape[2] // depth
    heads = step_proj.shape[2] // depth
    k_rows = gate_proj.shape[1]
    f32 = jnp.float32
    t = lax.axis_index("tp")
    z = lax.axis_index("ctx")

    def own_piece(array):
        return lax.dynamic_slice_in_dim(array, t * piece, piece, 0)

    my_hidden = own_piece(hidden_in[0])
    my_cotangent = own_piece(cotangent[0])
    gains = [norm_gain[layer].astype(f32) for layer in range(LAYERS)]

    def by_z(block):
        return block.reshape(block.shape[0], depth, -1).transpose(1, 0, 2)

    packs, shared = [], []
    for layer in range(LAYERS):
        pack = jnp.concatenate(
            [
                by_z(gate_proj[layer]),
                by_z(out_proj[layer].T),
                by_z(value_proj[layer]),
                by_z(step_proj[layer]),
            ],
            axis=2,
        )
        packs.append(jnp.pad(pack, ((0, 0), (0, 0), (0, PACK - pack.shape[2]))))
        shared.append(bc_proj[layer])
    hidden0 = my_hidden.astype(f32)
    _, my_normed0 = norm_rows(hidden0, gains[0])
    seg_rows = lane_rows([own_piece(segment_ids[0]).astype(f32)[None]], 1)[0]
    normed0, seg_full, pack0, shared0 = prepare([my_normed0, seg_rows], [packs[0], shared[0]], depth, 1)
    cotangent_full, pack1, shared1 = prepare([my_cotangent], [packs[1], shared[1]], depth, 2)
    walls = [pack0.reshape(-1, PACK), pack1.reshape(-1, PACK)]
    bc_walls = [shared0.reshape(-1, shared0.shape[2]), shared1.reshape(-1, shared1.shape[2])]
    normed0 = normed0.reshape(-1, model_width)
    cotangent_full = cotangent_full.reshape(-1, model_width)
    segment = seg_full[:, 0, :piece].reshape(-1)
    segr = segment[None]
    segc = jnp.broadcast_to(jnp.pad(segment, 8, constant_values=-1.0)[:, None], (segment.size + 16, 256))

    def per_lane(by_head):
        return jnp.repeat(by_head, HEADDIM, axis=1)[:, None]

    per_channel = jnp.concatenate(
        [
            conv_value.astype(f32),
            conv_value_bias.astype(f32)[:, None],
            out_gain.astype(f32)[:, None],
            per_lane(skip_gain),
            per_lane(step_bias),
            per_lane(-jnp.exp(decay_log)),
        ],
        axis=1,
    )
    per_channel = lax.dynamic_slice_in_dim(per_channel, z * width, width, 2)
    per_channel = jnp.pad(per_channel, ((0, 0), (0, 0), (0, 256 - width)))
    smalls = jnp.concatenate(
        [per_channel, conv_bc.astype(f32), conv_bc_bias.astype(f32)[:, None], jnp.zeros((LAYERS, 2, 256), f32)],
        axis=1,
    )

    def forward(layer, normed, precise):
        return split_forward(
            normed, walls[layer], bc_walls[layer], smalls[layer], segr, segc, slots, precise
        )

    def backward(layer, grad, scalars, normed, kept):
        return split_backward(
            grad, scalars, normed, walls[layer], smalls[layer], segr, segc, kept, slots
        )

    gated0, squares0, *kept0 = forward(0, normed0, True)
    hidden1, total0, inv_rows0, normed1 = turn_forward(
        gated0, squares0, smalls[0], walls[0], my_hidden, gains[1][None], depth, 3
    )
    inv0 = lax.dynamic_slice_in_dim(inv_rows0.reshape(-1), (z * 4 + t) * piece, piece, 0)
    normed1 = normed1.reshape(-1, model_width)
    part1, squares1, *kept1 = forward(1, normed1, False)
    total1, square_rows1 = reduce_pieces([part1, squares1], depth, 5)
    inv1 = lax.rsqrt(square_rows1[0, :piece] / INNER + epsilon)
    total1 = total1 * inv1[:, None]
    hidden_out = (hidden1 + total1).astype(LOW)

    def bc_grad(normed, bc_low):
        return jnp.stack(
            [
                dot_left(
                    lax.dynamic_slice_in_dim(normed, (far_x * depth + z) * k_rows, k_rows, 1), bc_low
                ).astype(LOW)
                for far_x in range(2)
            ]
        )

    def scalar_rows(inv, inner):
        return lane_rows([inv[None], inner[None] / INNER], 1)[0]

    inner1 = jnp.sum(my_cotangent.astype(f32) * total1, axis=1)
    (scalars1,) = gather_pieces([scalar_rows(inv1, inner1)], depth, 8)
    both1, grads1, sums1 = backward(1, cotangent_full, scalars1, normed1, kept1)
    grad1, gain_grad1, _, full0, scalars0 = turn_backward(
        both1,
        my_cotangent,
        hidden1,
        gains[1][None],
        bc_walls[1],
        total0,
        scalar_rows(inv0, jnp.zeros_like(inv0)),
        False,
        depth,
        6,
    )
    full0 = full0.reshape(-1, full0.shape[2])
    out1, bc_out1 = scatter_grads(grads1, bc_grad(normed1, full0[:, model_width:]), depth, 10)
    both0, grads0, sums0 = backward(0, full0, scalars0, normed0, kept0)
    _, gain_grad0, grad_low0, bc_all0 = turn_backward(
        both0, grad1, my_hidden, gains[0][None], bc_walls[0], total0, scalars0[0], True, depth, 7
    )
    out0, bc_out0 = scatter_grads(
        grads0, bc_grad(normed0, bc_all0.reshape(-1, bc_all0.shape[2])), depth, 12
    )

    outs = jnp.stack([out0, out1]).astype(f32)

    def channels(lo, hi):
        return outs[..., lo:hi].transpose(0, 2, 1, 3).reshape(LAYERS, k_rows, -1)

    gain_rows = jnp.concatenate([gain_grad0, gain_grad1], axis=0).reshape(-1, 256)
    gain_count = gain_rows.shape[0]
    sums = jnp.concatenate([sums0, sums1, gain_rows, jnp.zeros((16 - gain_count, 256), f32)], axis=0)
    by_z, whole, hidden_out, grad_hidden = finish(sums, hidden_out, grad_low0, depth, 13)
    by_channel = jnp.stack([by_z[:, 16 * layer : 16 * layer + 9, :width] for layer in range(LAYERS)])
    by_channel = by_channel.transpose(0, 2, 1, 3).reshape(LAYERS, 9, -1)
    bc_sums = jnp.stack([whole[16 * layer + 9 : 16 * layer + 14] for layer in range(LAYERS)])
    gain_grad = whole[16 * LAYERS : 16 * LAYERS + gain_count].reshape(LAYERS, model_width)

    def by_head(row):
        return by_channel[:, row].reshape(LAYERS, -1, HEADDIM)[:, :, 0]

    return (
        hidden_out.reshape(1, tokens, model_width),
        grad_hidden.reshape(1, tokens, model_width),
        gain_grad,
        channels(0, width),
        channels(2 * width, 3 * width),
        jnp.stack([bc_out0, bc_out1]),
        channels(3 * width, 3 * width + heads),
        by_channel[:, :4],
        by_channel[:, 4],
        bc_sums[:, :4],
        bc_sums[:, 4],
        by_head(8),
        by_head(7),
        by_head(6),
        by_channel[:, 5],
        channels(width, 2 * width).transpose(0, 2, 1),
    )


def solution(mesh):
    in_specs = (
        P("dp", "ctx", None),
        P("dp", "ctx"),
        P("dp", "ctx", None),
        P(),
        P(None, ("dp", "ctx"), "tp"),
        P(None, ("dp", "ctx"), "tp"),
        P(None, ("dp", "ctx"), None),
        P(None, ("dp", "ctx"), "tp"),
        P(None, None, "tp"),
        P(None, "tp"),
        P(),
        P(),
        P(None, "tp"),
        P(None, "tp"),
        P(None, "tp"),
        P(None, "tp"),
        P(None, "tp", ("dp", "ctx")),
    )
    out_specs = (
        P("dp", "ctx", None),
        P("dp", "ctx", None),
        P(),
        P(None, ("dp", "ctx"), "tp"),
        P(None, ("dp", "ctx"), "tp"),
        P(None, ("dp", "ctx"), None),
        P(None, ("dp", "ctx"), "tp"),
        P(None, None, "tp"),
        P(None, "tp"),
        P(),
        P(),
        P(None, "tp"),
        P(None, "tp"),
        P(None, "tp"),
        P(None, "tp"),
        P(None, "tp", ("dp", "ctx")),
    )
    depth = mesh.shape["ctx"]
    heads = 48 // mesh.shape["tp"]
    fits = mesh.shape["tp"] == 4 and mesh.shape["dp"] == 2 and depth == 4 and heads % depth == 0
    body = partial(split_local, depth) if fits else local
    return jax.shard_map(body, mesh=mesh, in_specs=in_specs, out_specs=out_specs, check_vma=False)
```

```python
from functools import partial

import jax
import jax.numpy as jnp
from jax import lax
from jax.experimental import pallas as pl
from jax.experimental.pallas import tpu as pltpu
from jax.sharding import PartitionSpec as P

HEADDIM = 64
BLOCK = 256
LAYERS = 2
INNER = 3072


epsilon = 1e-05
precise = lax.Precision.HIGH


def from_behind(block, axis, distance):
    devices = range(lax.axis_size(axis))
    route = [(i - distance, i) for i in devices if i - distance in devices]
    return lax.ppermute(block, axis, route)


def round_keep(values):
    return lax.optimization_barrier(values.astype(jnp.bfloat16)).astype(jnp.float32)


def dot_back(left_rows, right_rows):
    return lax.dot_general(
        left_rows, right_rows, (((1,), (1,)), ((), ())), preferred_element_type=jnp.float32
    )


def dot_left(left_rows, right_rows):
    return lax.dot_general(
        left_rows, right_rows, (((0,), (0,)), ((), ())), preferred_element_type=jnp.float32
    )


def conv_local(signal, edge_rows, kernel, conv_bias, segment, edge_segment):
    tap_count = kernel.shape[0]
    length = signal.shape[1]
    padded = jnp.concatenate([edge_rows, signal], axis=1)
    seg_pad = jnp.concatenate([edge_segment, segment], axis=1)
    result = conv_bias + jnp.zeros_like(signal)
    for tap_index in range(tap_count):
        same_doc = (seg_pad[:, tap_index : tap_index + length] == segment).astype(jnp.float32)
        result = (
            result
            + kernel[tap_index] * padded[:, tap_index : tap_index + length] * same_doc[:, :, None]
        )
    return jax.nn.silu(result)


def block_step(decay_rates, carried, block_data):
    states, prev_segment = carried
    values, b_mat, c_mat, step_size, segment = block_data
    length = values.shape[0]
    log_decay = jnp.cumsum(step_size * decay_rates, axis=0)
    positions = jnp.arange(length)
    causal = positions[:, None] >= positions[None, :]
    same_doc = jnp.logical_and(segment[:, None] == segment[None, :], causal)[:, :, None]
    differ = jnp.where(same_doc, log_decay[:, None, :] - log_decay[None, :, :], 0.0)
    weights = jnp.where(same_doc, jnp.exp(differ), 0.0)
    cb_product = jnp.dot(c_mat, b_mat.T, precision=precise)
    scores = cb_product[:, :, None] * weights * step_size[None, :, :]
    intra_out = jnp.einsum("tsh,shp->thp", scores, values, precision=precise)
    alive_mask = (segment == prev_segment).astype(jnp.float32)
    reach = alive_mask[:, None] * jnp.exp(log_decay)
    inter_out = reach[:, :, None] * jnp.einsum("tn,hpn->thp", c_mat, states, precision=precise)
    end_same = (segment == segment[length - 1]).astype(jnp.float32)
    to_end = jnp.exp(log_decay[length - 1][None, :] - log_decay) * end_same[:, None] * step_size
    weighted_values = to_end[:, :, None] * values
    new_states = reach[length - 1][:, None, None] * states + jnp.einsum(
        "shp,sn->hpn", weighted_values, b_mat, precision=precise
    )
    return ((new_states, segment[length - 1]), intra_out + inter_out)


def device_scan(values, b_mat, c_mat, step_size, decay_rates, segment, seg_prev):
    block_count = values.shape[0] // BLOCK
    heads_local = values.shape[1]
    state_dim = b_mat.shape[1]
    blocks = (
        values.reshape(block_count, BLOCK, heads_local, HEADDIM),
        b_mat.reshape(block_count, BLOCK, state_dim),
        c_mat.reshape(block_count, BLOCK, state_dim),
        step_size.reshape(block_count, BLOCK, heads_local),
        segment.reshape(block_count, BLOCK),
    )
    initial = (jnp.zeros((heads_local, HEADDIM, state_dim), jnp.float32), seg_prev)
    final_carry, outputs = lax.scan(partial(block_step, decay_rates), initial, blocks)
    return (outputs.reshape(values.shape), final_carry[0])


def step_terms(step_pre, step_bias, decay_log):
    return (jax.nn.softplus(step_pre + step_bias), -jnp.exp(decay_log))


def mixer_terms(values, bc_conv, step_size, decay_rates, skip_gain, segment, seg_prev):
    seq_count, tokens, inner_local = values.shape
    heads_local = step_size.shape[2]
    heads_in = values.reshape(seq_count, tokens, heads_local, HEADDIM)
    state_dim = bc_conv.shape[2] // 2
    scanner = jax.vmap(device_scan, in_axes=(0, 0, 0, 0, None, 0, 0))
    intra_out, local_states = scanner(
        heads_in,
        bc_conv[:, :, :state_dim],
        bc_conv[:, :, state_dim:],
        step_size,
        decay_rates,
        segment,
        seg_prev,
    )
    alive_last = (segment[:, tokens - 1] == seg_prev).astype(jnp.float32)
    decays = alive_last[:, None] * jnp.exp(jnp.sum(step_size * decay_rates, axis=1))
    return (intra_out + skip_gain[:, None] * heads_in, local_states, decays)


def carried_terms(bc_conv, step_size, decay_rates, entering, segment, seg_prev):
    state_dim = bc_conv.shape[2] // 2
    c_mat = bc_conv[:, :, state_dim:]
    log_decay = jnp.cumsum(step_size * decay_rates, axis=1)
    alive_mask = (segment == seg_prev[:, None]).astype(jnp.float32)
    reach = alive_mask[:, :, None] * jnp.exp(log_decay)
    carried = jnp.einsum("sqn,shpn->sqhp", c_mat, entering, precision=precise)
    return reach[:, :, :, None] * carried


def chain_forward(decays, local_states):

    def handoff(step_index, entering):
        return from_behind(decays[:, :, None, None] * entering + local_states, "ctx", 1)

    return lax.fori_loop(0, lax.axis_size("ctx") - 1, handoff, jnp.zeros_like(local_states))


def chain_backward(decays, grad_entering):

    def handback(step_index, beyond):
        return from_behind(
            (grad_entering + decays[:, :, None, None] * beyond).astype(jnp.bfloat16), "ctx", -1
        ).astype(jnp.float32)

    return lax.fori_loop(0, lax.axis_size("ctx") - 1, handback, jnp.zeros_like(grad_entering))


def layer_forward(hidden, segment, layer_params):
    (
        norm_gain,
        gate_proj,
        value_proj,
        bc_proj,
        step_proj,
        conv_value,
        conv_value_bias,
        conv_bc,
        conv_bc_bias,
        decay_log,
        step_bias,
        skip_gain,
        out_gain,
        out_proj,
    ) = layer_params
    seq_count, tokens, model_width = hidden.shape
    row_count = seq_count * tokens
    tap_count = conv_value.shape[0]
    gathered = (
        lax.all_gather(gate_proj, ("dp", "ctx"), axis=0, tiled=True),
        lax.all_gather(value_proj, ("dp", "ctx"), axis=0, tiled=True),
        lax.all_gather(bc_proj, ("dp", "ctx"), axis=0, tiled=True),
        lax.all_gather(step_proj, ("dp", "ctx"), axis=0, tiled=True),
        lax.all_gather(out_proj, ("dp", "ctx"), axis=1, tiled=True),
    )
    gate_full, value_full, bc_full, step_full, out_full = gathered
    hidden_rows = hidden.reshape(row_count, model_width)
    inv_norm = lax.rsqrt(jnp.mean(hidden_rows * hidden_rows, axis=1, keepdims=True) + epsilon)
    normed = (hidden_rows * inv_norm * norm_gain).astype(jnp.bfloat16)
    gate_pre = jnp.dot(normed, gate_full, preferred_element_type=jnp.float32)
    value_pre = jnp.dot(normed, value_full, preferred_element_type=jnp.float32).reshape(
        seq_count, tokens, -1
    )
    bc_pre = jnp.dot(normed, bc_full, preferred_element_type=jnp.float32).reshape(
        seq_count, tokens, -1
    )
    step_pre = jnp.dot(normed, step_full, preferred_element_type=jnp.float32).reshape(
        seq_count, tokens, -1
    )
    first_edge = tokens - tap_count + 1
    edge_value, edge_bc, edge_segment = from_behind(
        (value_pre[:, first_edge:], bc_pre[:, first_edge:], segment[:, first_edge:]), "ctx", 1
    )
    conv_fn = partial(conv_local, segment=segment, edge_segment=edge_segment)
    value_act, value_pull = jax.vjp(conv_fn, value_pre, edge_value, conv_value, conv_value_bias)
    bc_act, bc_pull = jax.vjp(conv_fn, bc_pre, edge_bc, conv_bc, conv_bc_bias)
    values = round_keep(value_act)
    bc_conv = round_keep(bc_act)
    seg_prev = edge_segment[:, tap_count - 2]
    (step_size, decay_rates), step_pull = jax.vjp(step_terms, step_pre, step_bias, decay_log)
    (local_out, local_states, decays), local_pull = jax.vjp(
        partial(mixer_terms, segment=segment, seg_prev=seg_prev),
        values,
        bc_conv,
        step_size,
        decay_rates,
        skip_gain,
    )
    entering = chain_forward(decays, local_states)
    carried_out, carried_pull = jax.vjp(
        partial(carried_terms, segment=segment, seg_prev=seg_prev),
        bc_conv,
        step_size,
        decay_rates,
        entering,
    )
    mixed = (local_out + carried_out).reshape(row_count, -1)
    gate_act = jax.nn.silu(gate_pre)
    gated = mixed * gate_act
    square_sum = lax.psum(jnp.sum(gated * gated, axis=1), "tp")
    inv_gate = lax.rsqrt(square_sum / INNER + epsilon)[:, None]
    scaled = (gated * inv_gate * out_gain).astype(jnp.bfloat16)
    mixer_sum = lax.psum(jnp.dot(scaled, out_full, preferred_element_type=jnp.float32), "tp")
    kept = {
        "scaled": scaled,
        "gated": gated,
        "inv_gate": inv_gate,
        "gate_pre": gate_pre,
        "gate_act": gate_act,
        "mixed": mixed,
        "carried_pull": carried_pull,
        "local_pull": local_pull,
        "step_pull": step_pull,
        "value_pull": value_pull,
        "bc_pull": bc_pull,
        "decays": decays,
        "entering": entering,
        "hidden_rows": hidden_rows,
        "inv_norm": inv_norm,
        "normed": normed,
    }
    return (hidden + mixer_sum.reshape(seq_count, tokens, model_width), kept)


def layer_backward(grad_hidden, kept, layer_params):
    (
        norm_gain,
        gate_proj,
        value_proj,
        bc_proj,
        step_proj,
        conv_value,
        conv_value_bias,
        conv_bc,
        conv_bc_bias,
        decay_log,
        step_bias,
        skip_gain,
        out_gain,
        out_proj,
    ) = layer_params
    seq_count, tokens, model_width = grad_hidden.shape
    row_count = seq_count * tokens
    tap_count = conv_value.shape[0]
    gate_full, value_full, bc_full, step_full, out_full = (
        lax.all_gather(gate_proj, ("dp", "ctx"), axis=0, tiled=True),
        lax.all_gather(value_proj, ("dp", "ctx"), axis=0, tiled=True),
        lax.all_gather(bc_proj, ("dp", "ctx"), axis=0, tiled=True),
        lax.all_gather(step_proj, ("dp", "ctx"), axis=0, tiled=True),
        lax.all_gather(out_proj, ("dp", "ctx"), axis=1, tiled=True),
    )
    grad_rows = grad_hidden.reshape(row_count, model_width)
    grad_low = grad_rows.astype(jnp.bfloat16)
    grad_scaled = dot_back(grad_low, out_full)
    grad_out_proj = dot_left(kept["scaled"], grad_low)
    gated = kept["gated"]
    inv_gate = kept["inv_gate"]
    weighted = grad_scaled * out_gain
    inner_sum = lax.psum(jnp.sum(weighted * gated, axis=1), "tp")
    grad_gated = inv_gate * weighted - gated * inv_gate**3 * (inner_sum / INNER)[:, None]
    grad_out_gain = jnp.sum(grad_scaled * gated * inv_gate, axis=0)
    gate_pre = kept["gate_pre"]
    sigmoid_gate = jax.nn.sigmoid(gate_pre)
    grad_gate_pre = (
        grad_gated * kept["mixed"] * sigmoid_gate * (1.0 + gate_pre * (1.0 - sigmoid_gate))
    )
    grad_heads = (grad_gated * kept["gate_act"]).reshape(
        seq_count, tokens, step_full.shape[1], HEADDIM
    )
    carried_bc, carried_step, carried_rates, grad_entering = kept["carried_pull"](grad_heads)
    beyond = chain_backward(kept["decays"], grad_entering)
    grad_decays = jnp.sum(beyond * kept["entering"], axis=(2, 3))
    local_values, local_bc, local_step, local_rates, grad_skip = kept["local_pull"](
        (grad_heads, beyond, grad_decays)
    )
    grad_step_pre, grad_step_bias, grad_decay_log = kept["step_pull"](
        (carried_step + local_step, carried_rates + local_rates)
    )
    grad_value_pre, grad_edge_value, grad_conv_value, grad_conv_value_bias = kept["value_pull"](
        local_values
    )
    grad_bc_pre, grad_edge_bc, grad_conv_bc, grad_conv_bc_bias = kept["bc_pull"](
        carried_bc + local_bc
    )
    from_value, from_bc = from_behind((grad_edge_value, grad_edge_bc), "ctx", -1)
    first_edge = tokens - tap_count + 1
    grad_value_pre = grad_value_pre.at[:, first_edge:].add(from_value)
    grad_bc_pre = grad_bc_pre.at[:, first_edge:].add(from_bc)
    grad_gate_low = grad_gate_pre.astype(jnp.bfloat16)
    grad_value_low = grad_value_pre.reshape(row_count, -1).astype(jnp.bfloat16)
    grad_step_low = grad_step_pre.reshape(row_count, -1).astype(jnp.bfloat16)
    input_part = (
        dot_back(grad_gate_low, gate_full)
        + dot_back(grad_value_low, value_full)
        + dot_back(grad_step_low, step_full)
    )
    input_sum, bc_sum, conv_bc_sum, conv_bc_bias_sum = (
        lax.psum(input_part.astype(jnp.bfloat16), "tp").astype(jnp.float32),
        lax.psum(grad_bc_pre.reshape(row_count, -1).astype(jnp.bfloat16), "tp").astype(jnp.float32),
        lax.psum(grad_conv_bc, "tp").astype(jnp.float32),
        lax.psum(grad_conv_bc_bias, "tp").astype(jnp.float32),
    )
    grad_bc_low = bc_sum.astype(jnp.bfloat16)
    grad_normed = input_sum + dot_back(grad_bc_low, bc_full)
    hidden_rows = kept["hidden_rows"]
    inv_norm = kept["inv_norm"]
    weighted_norm = grad_normed * norm_gain
    grad_norm_gain = jnp.sum(grad_normed * hidden_rows * inv_norm, axis=0)
    grad_rows = (
        grad_rows
        + inv_norm * weighted_norm
        - hidden_rows * inv_norm**3 * jnp.mean(weighted_norm * hidden_rows, axis=1, keepdims=True)
    )
    normed = kept["normed"]
    proj_grads = (
        lax.psum_scatter(
            dot_left(normed, grad_gate_low).astype(jnp.bfloat16),
            ("dp", "ctx"),
            scatter_dimension=0,
            tiled=True,
        ).astype(jnp.float32),
        lax.psum_scatter(
            dot_left(normed, grad_value_low).astype(jnp.bfloat16),
            ("dp", "ctx"),
            scatter_dimension=0,
            tiled=True,
        ).astype(jnp.float32),
        lax.psum_scatter(
            dot_left(normed, grad_bc_low).astype(jnp.bfloat16),
            ("dp", "ctx"),
            scatter_dimension=0,
            tiled=True,
        ).astype(jnp.float32),
        lax.psum_scatter(
            dot_left(normed, grad_step_low).astype(jnp.bfloat16),
            ("dp", "ctx"),
            scatter_dimension=0,
            tiled=True,
        ).astype(jnp.float32),
        lax.psum_scatter(
            grad_out_proj.astype(jnp.bfloat16), ("dp", "ctx"), scatter_dimension=1, tiled=True
        ).astype(jnp.float32),
    )
    small_grads = lax.psum(
        (
            grad_norm_gain,
            grad_conv_value.astype(jnp.float32),
            grad_conv_value_bias.astype(jnp.float32),
            conv_bc_sum,
            conv_bc_bias_sum,
            grad_decay_log,
            grad_step_bias,
            grad_skip,
            grad_out_gain,
        ),
        ("dp", "ctx"),
    )
    return (grad_rows.reshape(seq_count, tokens, model_width), proj_grads, small_grads)


def stack_layers(groups, member):
    return jnp.stack([groups[layer_index][member] for layer_index in range(LAYERS)])


def local(
    hidden_in,
    segment_ids,
    cotangent,
    norm_gain,
    gate_proj,
    value_proj,
    bc_proj,
    step_proj,
    conv_value,
    conv_value_bias,
    conv_bc,
    conv_bc_bias,
    decay_log,
    step_bias,
    skip_gain,
    out_gain,
    out_proj,
):
    params = (
        norm_gain,
        gate_proj,
        value_proj,
        bc_proj,
        step_proj,
        conv_value,
        conv_value_bias,
        conv_bc,
        conv_bc_bias,
        decay_log,
        step_bias,
        skip_gain,
        out_gain,
        out_proj,
    )
    segment = segment_ids.astype(jnp.float32)
    hidden = hidden_in.astype(jnp.float32)
    kept_layers = []
    for layer_index in range(LAYERS):
        hidden, kept = layer_forward(
            hidden, segment, tuple((stacked[layer_index] for stacked in params))
        )
        kept_layers.append(kept)
    grad_hidden = cotangent.astype(jnp.float32)
    proj_list = [None] * LAYERS
    small_list = [None] * LAYERS
    for layer_index in reversed(range(LAYERS)):
        grad_hidden, proj_list[layer_index], small_list[layer_index] = layer_backward(
            grad_hidden,
            kept_layers[layer_index],
            tuple((stacked[layer_index] for stacked in params)),
        )
    return (
        hidden.astype(jnp.bfloat16),
        grad_hidden.astype(jnp.bfloat16),
        stack_layers(small_list, 0),
        stack_layers(proj_list, 0),
        stack_layers(proj_list, 1),
        stack_layers(proj_list, 2),
        stack_layers(proj_list, 3),
        stack_layers(small_list, 1),
        stack_layers(small_list, 2),
        stack_layers(small_list, 3),
        stack_layers(small_list, 4),
        stack_layers(small_list, 5),
        stack_layers(small_list, 6),
        stack_layers(small_list, 7),
        stack_layers(small_list, 8),
        stack_layers(proj_list, 4),
    )


MESH = pl.DeviceIdType.MESH
PACK = 640


def params_of(collective_id):
    return pltpu.CompilerParams(
        collective_id=collective_id, has_side_effects=True, vmem_limit_bytes=60 << 20
    )


VMEM_SPEC = pl.BlockSpec(memory_space=pltpu.VMEM)


def greet(peers):
    barrier = pltpu.get_barrier_semaphore()
    for peer in peers:
        pl.semaphore_signal(barrier, inc=1, device_id=peer, device_id_type=MESH)
    pl.semaphore_wait(barrier, len(peers))


def remote(source, target, send_sem, recv_sem, peer):
    return pltpu.make_async_remote_copy(
        src_ref=source,
        dst_ref=target,
        send_sem=send_sem,
        recv_sem=recv_sem,
        device_id=peer,
        device_id_type=MESH,
    )


def other_core(t):
    return t + 1 - 2 * lax.rem(t, 2)


def other_chip(t):
    return lax.rem(t + 2, 4)


def mxu(left, right, left_dim, right_dim, precision=None):
    return lax.dot_general(
        left,
        right,
        (((left_dim,), (right_dim,)), ((), ())),
        preferred_element_type=jnp.float32,
        precision=precision,
    )


def iota(shape, axis):
    return lax.broadcasted_iota(jnp.int32, shape, axis)


def ones_where(condition, kind):
    return jnp.where(condition, 1.0, 0.0).astype(kind)


def sigmoid(v):
    return 1.0 / (1.0 + jnp.exp(-v))


exact = lax.Precision.HIGHEST
LOW = jnp.bfloat16
OUT_AT, VALUE_AT = 128, 384


class BlockTerms:
    def __init__(self, start, segc_ref, segr_ref, small_ref, value_ref, bc_ref, step_in, width):
        self.start, self.width = start, width
        self.segc_ref, self.small_ref = segc_ref, small_ref
        rows = pl.ds(8 + start, BLOCK)
        seg = segc_ref[rows, :]
        row, col = iota((BLOCK, BLOCK), 0), iota((BLOCK, BLOCK), 1)
        self.row, self.col = row, col
        same = jnp.logical_and(seg == segr_ref[:, pl.ds(start, BLOCK)], row >= col)
        self.hidden_pairs = jnp.where(same, 0.0, -1e30)
        self.value_arg = self.conv(value_ref, 0, 4, width)
        self.bc_arg = self.conv(bc_ref, 9, 13, bc_ref.shape[1])
        self.value_sig = sigmoid(self.value_arg)
        self.bc_sig = sigmoid(self.bc_arg)
        self.values = (self.value_arg * self.value_sig).astype(LOW)
        bc_low = (self.bc_arg * self.bc_sig).astype(LOW)
        half = bc_ref.shape[1] // 2
        self.b_low, self.c_low = bc_low[:, :half], bc_low[:, half:]
        self.step = jnp.maximum(step_in, 0.0) + jnp.log1p(jnp.exp(-jnp.abs(step_in)))
        rates = small_ref[8:9, :width]
        self.log_decay = mxu(ones_where(row >= col, jnp.float32), self.step * rates, 1, 0, exact)
        self.log_rows = jnp.transpose(self.log_decay)
        self.step_rows = jnp.transpose(self.step)
        self.scores = mxu(self.c_low, self.b_low, 1, 1)
        seg = seg[:, :width]
        before = segc_ref[7 + start : 8 + start, :width]
        last = segc_ref[7 + start + BLOCK : 8 + start + BLOCK, :width]
        self.reach = jnp.where(seg == before, jnp.exp(self.log_decay), 0.0)
        self.reach_last = self.reach[BLOCK - 1 : BLOCK, :]
        self.fade = jnp.where(
            seg == last, jnp.exp(self.log_decay[BLOCK - 1 : BLOCK, :] - self.log_decay), 0.0
        )
        self.faded = self.fade * self.step * self.values.astype(jnp.float32)

    def conv(self, ref, taps_at, bias_at, width):
        total = self.small_ref[bias_at : bias_at + 1, :width]
        for distance in range(4):
            tap = self.small_ref[taps_at + 3 - distance : taps_at + 4 - distance, :width]
            total = total + tap * self.back(ref, distance, width)
        return total

    def back(self, ref, distance, width):
        rows = ref[pl.ds(8 + self.start - distance, BLOCK), :]
        if not distance:
            return rows
        here = self.segc_ref[pl.ds(8 + self.start, BLOCK), :width]
        there = self.segc_ref[pl.ds(8 + self.start - distance, BLOCK), :width]
        return jnp.where(here == there, rows, 0.0)

    def ahead(self, ref, distance, width):
        rows = ref[pl.ds(self.start + distance, BLOCK), :]
        if not distance:
            return rows
        here = self.segc_ref[pl.ds(8 + self.start, BLOCK), :width]
        there = self.segc_ref[pl.ds(8 + self.start + distance, BLOCK), :width]
        return jnp.where(here == there, rows, 0.0)

    def decay_pairs(self, head):
        at = head * HEADDIM
        return jnp.exp(
            self.log_decay[:, at : at + 1] - self.log_rows[at : at + 1, :] + self.hidden_pairs
        )

    def head_lanes(self, head):
        lanes = iota((BLOCK, self.width), 1)
        return jnp.logical_and(lanes >= head * HEADDIM, lanes < (head + 1) * HEADDIM)

    def of_head(self, array, head):
        return array * ones_where(self.head_lanes(head), array.dtype)


def lane_shift(width):
    return ones_where(iota((width, 256), 1) == iota((width, 256), 0) + 64, LOW)


def two_parts(array):
    high = array.astype(LOW)
    return high, (array - high.astype(jnp.float32)).astype(LOW)


def forward_body(
    precise,
    plan,
    normed_ref,
    wall_ref,
    bcw_ref,
    small_ref,
    segr_ref,
    segc_ref,
    part_ref,
    squares_ref,
    gate_ref,
    value_ref,
    bc_ref,
    step_ref,
    mixed_ref,
    state_ref,
):
    tokens = normed_ref.shape[0]
    width = gate_ref.shape[1]
    heads = width // HEADDIM
    piece = 0 if precise else part_ref.shape[1]
    value_ref[0:8, :] = jnp.zeros((8, width), jnp.float32)
    bc_ref[0:8, :] = jnp.zeros((8, bc_ref.shape[1]), jnp.float32)
    spread = ones_where(
        iota((256, width), 0) - width == iota((256, width), 1) // HEADDIM, jnp.float32
    )
    shift = lane_shift(width)
    gains, skip = small_ref[5:6, :width], small_ref[6:7, :width]
    state = jnp.zeros(state_ref.shape[1:], jnp.float32)
    for block in range(tokens // BLOCK):
        start = block * BLOCK
        rows = pl.ds(start, BLOCK)
        normed = normed_ref[rows, :]
        gate_pre = mxu(normed, wall_ref[:, 0:256], 1, 0)[:, :width]
        both = mxu(normed, wall_ref[:, VALUE_AT : VALUE_AT + 256], 1, 0)
        value_ref[pl.ds(8 + start, BLOCK), :] = both[:, :width]
        bc_ref[pl.ds(8 + start, BLOCK), :] = mxu(normed, bcw_ref[...], 1, 0)
        step_in = mxu(both, spread, 1, 0, exact) + small_ref[7:8, :width]
        gate_ref[rows, :] = gate_pre
        step_ref[rows, :] = step_in
        terms = BlockTerms(start, segc_ref, segr_ref, small_ref, value_ref, bc_ref, step_in, width)
        mixed = skip * terms.values.astype(jnp.float32)
        for head in range(heads):
            at = head * HEADDIM
            weights = terms.scores * terms.decay_pairs(head) * terms.step_rows[at : at + 1, :]
            own_values = terms.of_head(terms.values, head)
            for term in two_parts(weights) if precise else (weights.astype(LOW),):
                mixed += mxu(term, own_values, 1, 0)
            plan(block, head)
        state_ref[block] = state
        if block:
            for term in two_parts(state) if precise else (state.astype(LOW),):
                mixed += terms.reach * mxu(terms.c_low, term, 1, 0)
        state = terms.reach_last * state
        for term in two_parts(terms.faded) if precise else (terms.faded.astype(LOW),):
            state += mxu(terms.b_low, term, 0, 0)
        mixed_ref[rows, :] = mixed
        gated = mixed * gate_pre * sigmoid(gate_pre)
        squares = gated * gated
        for at in range(0, BLOCK, 128):
            row = (start + at) // 128
            squares_ref[row : row + 1, :] = mxu(
                jnp.ones((8, width), jnp.float32), squares[at : at + 128], 1, 1, exact
            )[0:1]
        if precise:
            part_ref[rows, :] = gated
            plan(block, 3)
            continue
        moved = mxu((gated * gains).astype(LOW), shift, 1, 0).astype(LOW)
        part = mxu(moved, wall_ref[:, OUT_AT : OUT_AT + 256], 1, 1).astype(LOW)
        for at in range(0, BLOCK, piece):
            part_ref[(start + at) // piece] = part[at : at + piece]
        plan(block, 3)


def local_params():
    return pltpu.CompilerParams(vmem_limit_bytes=60 << 20)


def forward_shapes(normed, bcw, slots, precise):
    tokens, model_width = normed.shape
    width = INNER // slots
    bc_width = bcw.shape[1]
    f32 = jnp.float32
    if precise:
        first = jax.ShapeDtypeStruct((tokens, width), f32)
    else:
        first = jax.ShapeDtypeStruct((slots, tokens // slots, model_width), LOW)
    return [
        first,
        jax.ShapeDtypeStruct((tokens // 128, 128), f32),
        jax.ShapeDtypeStruct((tokens, width), f32),
        jax.ShapeDtypeStruct((tokens + 8, width), f32),
        jax.ShapeDtypeStruct((tokens + 8, bc_width), f32),
        jax.ShapeDtypeStruct((tokens, width), f32),
        jax.ShapeDtypeStruct((tokens, width), f32),
        jax.ShapeDtypeStruct((tokens // BLOCK, bc_width // 2, width), f32),
    ]


def row_sum(array):
    return jnp.sum(array, axis=0, keepdims=True)


def backward_body(
    plan,
    grad_ref,
    inv_ref,
    inner_ref,
    normed_ref,
    wall_ref,
    small_ref,
    segr_ref,
    segc_ref,
    gate_ref,
    value_ref,
    bc_ref,
    step_ref,
    mixed_ref,
    state_ref,
    both_ref,
    early_ref,
    late_ref,
    sums_ref,
    pre_ref,
    scaled_ref,
    e_ref,
    e_bc_ref,
    grad_mixed_ref,
):
    tokens, model_width = normed_ref.shape
    width = gate_ref.shape[1]
    bc_width = bc_ref.shape[1]
    heads = width // HEADDIM
    piece = both_ref.shape[1]
    blocks = tokens // BLOCK
    f32 = jnp.float32
    shift = lane_shift(width)
    gains, skip, rates = (small_ref[at : at + 1, :width] for at in (5, 6, 8))
    e_ref[tokens:, :] = jnp.zeros((8, width), f32)
    e_bc_ref[tokens:, :] = jnp.zeros((8, bc_width), f32)
    pre_ref[...] = jnp.zeros(pre_ref.shape, LOW)
    inv_columns, inner_columns = spread_rows(inv_ref[...]), spread_rows(inner_ref[...])
    same_head = ones_where(
        iota((width, width), 0) // HEADDIM == iota((width, width), 1) // HEADDIM, f32
    )
    tail = ones_where(iota((width, 128), 0) == iota((width, 128), 1) + 128, LOW)
    pick = ones_where(
        jnp.logical_and(
            iota((width, 128), 0) == (iota((width, 128), 1) - 64) * HEADDIM, iota((width, 128), 1) >= 64
        ),
        LOW,
    )
    grad_state = jnp.zeros(state_ref.shape[1:], f32)
    sums = {}

    def add(name, term):
        sums[name] = sums[name] + term if name in sums else term

    for block in range(blocks):
        start = block * BLOCK
        rows = pl.ds(start, BLOCK)
        inv, inner = (
            jnp.concatenate([c[:, at : at + 1] for at in range(start // 128, (start + BLOCK) // 128)], axis=0)
            for c in (inv_columns, inner_columns)
        )
        grad_low = grad_ref[rows, 0:model_width]
        grad_scaled = mxu(grad_low, wall_ref[:, OUT_AT : OUT_AT + 256], 1, 0)
        grad_scaled = pltpu.roll(grad_scaled, 192, 1)[:, :width]
        gate_pre, mixed = gate_ref[rows, :], mixed_ref[rows, :]
        sig = sigmoid(gate_pre)
        act = gate_pre * sig
        gated = mixed * act
        normal = gated * inv
        scaled_ref[rows, :] = mxu((normal * gains).astype(LOW), shift, 1, 0).astype(LOW)
        add("out_gain", row_sum(grad_scaled * normal))
        grad_gated = inv * (grad_scaled * gains) - gated * (inv * inv * inner)
        grad_gate = grad_gated * mixed * sig * (1.0 + gate_pre * (1.0 - sig))
        pre_ref[rows, 0:width] = grad_gate.astype(LOW)
        grad_mixed_ref[rows, :] = grad_gated * act
    plan(-1, 0)
    k_rows = early_ref.shape[1]

    def by_slices(pair):
        lanes = pl.ds(pair * 2 * k_rows, 2 * k_rows)
        return lanes, ((2 * pair + at, slice(at * k_rows, (at + 1) * k_rows)) for at in range(2))

    for pair in range(early_ref.shape[0] // 2):
        lanes, slices = by_slices(pair)
        total = mxu(normed_ref[:, lanes], pre_ref[:, 0:256], 0, 0)
        out = mxu(grad_ref[:, lanes], scaled_ref[...], 0, 0)
        for slot, k_slice in slices:
            early_ref[slot, :, 0:OUT_AT] = total[k_slice, 0:OUT_AT].astype(LOW)
            early_ref[slot, :, OUT_AT:256] = (
                total[k_slice, OUT_AT:256] + out[k_slice, 0 : 256 - OUT_AT]
            ).astype(LOW)
            early_ref[slot, :, 256:VALUE_AT] = out[k_slice, 256 - OUT_AT :].astype(LOW)
    plan(-1, 1)
    for turn, block in enumerate(reversed(range(blocks))):
        start = block * BLOCK
        rows = pl.ds(start, BLOCK)
        step_in = step_ref[rows, :]
        terms = BlockTerms(start, segc_ref, segr_ref, small_ref, value_ref, bc_ref, step_in, width)
        grad_mixed = grad_mixed_ref[rows, :]
        grad_mixed_low = grad_mixed.astype(LOW)
        values = terms.values.astype(f32)
        add("skip", row_sum(grad_mixed * values))
        grad_values = skip * grad_mixed
        direct = jnp.zeros((BLOCK, width), f32)
        between = jnp.zeros((BLOCK, width), f32)
        pair_sum = jnp.zeros((BLOCK, BLOCK), f32)
        from_here = ones_where(terms.col >= terms.row, LOW)
        for head in range(heads):
            at = head * HEADDIM
            decay = terms.decay_pairs(head)
            step_row = terms.step_rows[at : at + 1, :]
            grad_head = terms.of_head(grad_mixed_low, head)
            head_ones = ones_where(terms.head_lanes(head), LOW)
            products = mxu(grad_head, terms.values, 1, 1)
            scored = terms.scores * decay
            grad_values += mxu((scored * step_row).astype(LOW), grad_head, 0, 0)
            pair_sum += decay * step_row * products
            unstepped = scored * products
            direct += mxu(unstepped.astype(LOW), head_ones, 0, 0)
            later = mxu(from_here, (unstepped * step_row).astype(LOW), 1, 0)
            later = jnp.where(terms.col < terms.row, later, 0.0)
            between += mxu(later.astype(LOW), head_ones, 1, 0)
            plan(turn, head)
        pair_low = pair_sum.astype(LOW)
        grad_b = mxu(pair_low, terms.c_low, 0, 0)
        grad_c = mxu(pair_low, terms.b_low, 1, 0)
        across = jnp.zeros((BLOCK, width), f32)
        if block < blocks - 1:
            state_low = grad_state.astype(LOW)
            to_state = mxu(terms.b_low, state_low, 1, 0)
            grad_values += terms.fade * terms.step * to_state
            by_step = terms.fade * to_state * values
            direct += mxu(by_step, same_head, 1, 0, exact)
            grad_b += mxu(terms.faded.astype(LOW), state_low, 1, 1)
            across += mxu(
                ones_where(terms.col < terms.row, f32), terms.step * by_step, 1, 0, exact
            )
        if block:
            entering = state_ref[block]
            entering_low = entering.astype(LOW)
            carried = terms.reach * mxu(terms.c_low, entering_low, 1, 0)
            across += mxu(
                ones_where(terms.col >= terms.row, f32), grad_mixed * carried, 1, 0, exact
            )
            reached = (terms.reach * grad_mixed).astype(LOW)
            grad_c += mxu(reached, entering_low, 1, 1)
            if block < blocks - 1:
                across += row_sum(grad_state * terms.reach_last * entering)
            grad_state = terms.reach_last * grad_state + mxu(terms.c_low, reached, 0, 0)
        between += mxu(across, same_head, 1, 0, exact)
        grad_step = direct + rates * between
        add("rates", row_sum(terms.step * between))
        grad_step_in = grad_step * sigmoid(step_in)
        add("step_bias", row_sum(grad_step_in))
        e = grad_values * (terms.value_sig * (1.0 + terms.value_arg * (1.0 - terms.value_sig)))
        e_ref[rows, :] = e
        e_bc = jnp.concatenate([grad_b, grad_c], axis=1) * (
            terms.bc_sig * (1.0 + terms.bc_arg * (1.0 - terms.bc_sig))
        )
        e_bc_ref[rows, :] = e_bc
        add("value_bias", row_sum(e))
        add("bc_bias", row_sum(e_bc))
        grad_value = jnp.zeros((BLOCK, width), f32)
        grad_bc = jnp.zeros((BLOCK, bc_width), f32)
        for distance in range(4):
            tap = 3 - distance
            add(("value", tap), row_sum(e * terms.back(value_ref, distance, width)))
            add(("bc", tap), row_sum(e_bc * terms.back(bc_ref, distance, bc_width)))
            grad_value += small_ref[tap : tap + 1, :width] * terms.ahead(e_ref, distance, width)
            grad_bc += small_ref[9 + tap : 10 + tap, :] * terms.ahead(e_bc_ref, distance, bc_width)
        value_low = grad_value.astype(LOW)
        pre_ref[rows, VALUE_AT : VALUE_AT + 128] = value_low[:, 0:128]
        pre_ref[rows, VALUE_AT + 128 : VALUE_AT + 256] = (
            mxu(value_low, tail, 1, 0) + mxu(grad_step_in.astype(LOW), pick, 1, 0)
        ).astype(LOW)
        part = mxu(pre_ref[rows, :], wall_ref[...], 1, 1).astype(LOW)
        grad_bc = grad_bc.astype(LOW)
        for at in range(0, BLOCK, piece):
            slot = (start + at) // piece
            both_ref[slot, :, 0:model_width] = part[at : at + piece]
            both_ref[slot, :, model_width:] = grad_bc[at : at + piece]
        plan(turn, 3)

    for pair in range(late_ref.shape[0] // 2):
        lanes, slices = by_slices(pair)
        total = mxu(normed_ref[:, lanes], pre_ref[:, VALUE_AT:], 0, 0)
        for slot, k_slice in slices:
            late_ref[slot] = total[k_slice].astype(LOW)
        plan(blocks, pair)

    sums_ref[...] = jnp.zeros(sums_ref.shape, f32)
    head_sums = mxu(
        jnp.concatenate([sums["skip"], jnp.zeros((7, width), f32)], axis=0), same_head, 1, 0, exact
    )
    for tap in range(4):
        sums_ref[tap : tap + 1, 0:width] = sums["value", tap]
        sums_ref[9 + tap : 10 + tap, :] = sums["bc", tap]
    sums_ref[4:5, 0:width] = sums["value_bias"]
    sums_ref[5:6, 0:width] = sums["out_gain"]
    sums_ref[6:7, 0:width] = head_sums[0:1]
    sums_ref[7:8, 0:width] = sums["step_bias"]
    sums_ref[8:9, 0:width] = sums["rates"] * rates
    sums_ref[13:14, :] = sums["bc_bias"]


def backward_shapes(normed, kept, slots):
    tokens, model_width = normed.shape
    width = kept[0].shape[1]
    bc_width = kept[2].shape[1]
    k_slots = slots // 2
    shapes = [
        jax.ShapeDtypeStruct((slots, tokens // slots, model_width + bc_width), LOW),
        jax.ShapeDtypeStruct((k_slots, model_width // k_slots, VALUE_AT), LOW),
        jax.ShapeDtypeStruct((k_slots, model_width // k_slots, PACK - VALUE_AT), LOW),
        jax.ShapeDtypeStruct((16, 256), jnp.float32),
    ]
    work = [
        pltpu.VMEM((tokens, PACK), LOW),
        pltpu.VMEM((tokens, 256), LOW),
        pltpu.VMEM((tokens + 8, width), jnp.float32),
        pltpu.VMEM((tokens + 8, bc_width), jnp.float32),
        pltpu.VMEM((tokens, width), jnp.float32),
    ]
    return shapes, work


def norm_rows(hidden, gain):
    inv = lax.rsqrt(jnp.mean(hidden * hidden, axis=1, keepdims=True) + epsilon)
    return inv, (hidden * inv * gain).astype(jnp.bfloat16)


HALVES = 2


class Links:
    def __init__(self, depth):
        self.depth = depth
        self.x, self.z, self.t = (lax.axis_index(name) for name in ("dp", "ctx", "tp"))
        self.core, self.chip = {"tp": other_core(self.t)}, {"tp": other_chip(self.t)}
        self.far_x = {"dp": 1 - self.x}
        self.left = {"ctx": lax.rem(self.z + depth - 1, depth)}
        self.right = {"ctx": lax.rem(self.z + 1, depth)}
        self.sent = []

    def send(self, source, target, send_sem, recv_sem, peer, when=None):
        copy = remote(source, target, send_sem, recv_sem, peer)
        self.sent.append((copy, when))
        if when is None:
            copy.start()
        else:
            pl.when(when)(copy.start)

    def wait(self, ref, send_sem, recv_sem, when=None):
        copy = remote(ref, ref, send_sem, recv_sem, self.core)
        if when is None:
            copy.wait_recv()
        else:
            pl.when(when)(copy.wait_recv)

    def finish(self):
        for copy, when in self.sent:
            if when is None:
                copy.wait_send()
            else:
                pl.when(when)(copy.wait_send)

    def near_first(self):
        z = self.z
        first = z + 1 - 2 * lax.rem(z, 2)
        third = 3 - 3 * (z // 2)
        return [first, 6 - z - first - third, third]

    def far_first(self):
        z = self.z
        odd = lax.rem(z, 2)
        first = 3 - 3 * (z // 2)
        second = (1 - odd) * (2 + z // 2) + odd * (z // 2)
        return [first, second, 6 - z - first - second]


def everyone(depth):
    z, t = lax.axis_index("ctx"), lax.axis_index("tp")
    return [
        {"ctx": lax.rem(z + hop, depth), "tp": lax.rem(t + turn, 4)}
        for hop in range(depth)
        for turn in range(4)
        if hop or turn
    ]


def half(ref, part):
    rows = ref.shape[0] // HALVES
    return ref.at[pl.ds(part * rows, rows)]


def gather_task(links, pieces, fulls, send_sem, recv_sem):
    z, t = links.z, links.t
    last = links.depth - 1
    own = z * 4 + t

    def pass_on(a, ref, slot, part, to_left, to_right, chip=True):
        target = half(fulls[a].at[slot], part)
        recv = recv_sem.at[a, slot, part]

        def go(way, peer, when=None):
            links.send(ref, target, send_sem.at[a, slot, part, way], recv, peer, when)

        if chip:
            go(0, links.left, to_left)
            go(1, links.right, to_right)
            go(2, links.chip)
        go(3, links.core)

    def arrived(a, slot, part):
        ref = half(fulls[a].at[slot], part)
        links.wait(ref, send_sem.at[a, slot, part, 0], recv_sem.at[a, slot, part])
        return ref

    every = range(len(pieces))
    for part in range(HALVES):
        for a in every:
            pass_on(a, half(pieces[a], part), own, part, z > 0, z < last)
    for a in every:
        fulls[a][own] = pieces[a][...]
    yield
    column = other_chip(t)
    order = links.near_first()
    for place, far in enumerate(order):
        slot = far * 4 + t
        for part in range(HALVES):
            for a in every:
                ref = arrived(a, slot, part)
                to_left = jnp.logical_and(far > z, z > 0)
                to_right = jnp.logical_and(far < z, z < last)
                pass_on(a, ref, slot, part, to_left, to_right)
        slot = (order[place - 1] if place else z) * 4 + column
        for part in range(HALVES):
            for a in every:
                pass_on(a, arrived(a, slot, part), slot, part, None, None, False)
        yield
    for part in range(HALVES):
        for a in every:
            slot = order[-1] * 4 + column
            pass_on(a, arrived(a, slot, part), slot, part, None, None, False)
    yield
    for far in [z] + order:
        for row in (other_core(t), other_chip(other_core(t))):
            for part in range(HALVES):
                for a in every:
                    arrived(a, far * 4 + row, part)


def gather_sems(count, slots):
    return [
        pltpu.SemaphoreType.DMA((count, slots, HALVES, 4)),
        pltpu.SemaphoreType.DMA((count, slots, HALVES)),
    ]


def reduce_task(links, produce, parts, outs, bufs, send_sem, recv_sem):
    z, t = links.z, links.t
    depth = links.depth
    last = depth - 1
    order = links.far_first() + [z]
    every = range(len(parts))

    def rows_of(ref, part):
        rows = ref.shape[0] // HALVES
        return slice(part * rows, (part + 1) * rows)

    def sems(a, at, part):
        return send_sem.at[a, at, part], recv_sem.at[a, at, part]

    def loaded(a, at, part):
        return bufs[a][at, rows_of(bufs[a].at[at], part), :].astype(jnp.float32)

    def mine(a, slot, part):
        return parts[a][slot, rows_of(parts[a].at[slot], part), :].astype(jnp.float32)

    def wait(a, at, part, when=None):
        links.wait(half(bufs[a].at[at], part), *sems(a, at, part), when)

    def stage1(far):
        produce(far)
        for which, row in enumerate((other_chip(other_core(t)), other_core(t))):
            for part in range(HALVES):
                for a in every:
                    at = far * 2 + which
                    links.send(
                        half(parts[a].at[far * 4 + row], part),
                        half(bufs[a].at[at], part),
                        *sems(a, at, part),
                        links.core,
                    )

    def stage2(far):
        for part in range(HALVES):
            for a in every:
                at = far * 2
                wait(a, at, part)
                total = mine(a, far * 4 + other_chip(t), part) + loaded(a, at, part)
                bufs[a][at, rows_of(bufs[a].at[at], part), :] = total.astype(bufs[a].dtype)
                to = 2 * depth + far
                links.send(
                    half(bufs[a].at[at], part), half(bufs[a].at[to], part), *sems(a, to, part), links.chip
                )

    def stage3(far):
        at = far * 2 + 1
        for part in range(HALVES):
            for a in every:
                wait(a, at, part)
                wait(a, 2 * depth + far, part)
                total = mine(a, far * 4 + t, part) + loaded(a, at, part) + loaded(a, 2 * depth + far, part)
                out = outs[a]
                rows = rows_of(out, part)
                if far is z:
                    out[rows, :] = total
                    continue
                ref = bufs[a]
                here = (at, rows_of(ref.at[at], part), slice(None))
                for way, (peer, when, first) in enumerate(
                    ((links.right, far > z, z == 0), (links.left, far < z, z == last))
                ):
                    chain = 3 * depth + way * depth + far

                    def go(total=total, chain=chain, here=here, ref=ref, first=first, a=a, part=part):
                        @pl.when(first)
                        def _():
                            ref[here] = total.astype(ref.dtype)

                        @pl.when(jnp.logical_not(first))
                        def _():
                            wait(a, chain, part)
                            ref[here] = (total + loaded(a, chain, part)).astype(ref.dtype)

                    pl.when(when)(go)
                    links.send(
                        half(ref.at[at], part), half(ref.at[chain], part), *sems(a, chain, part), peer, when
                    )

    count = len(order)
    for place in range(count + 2):
        if place < count:
            stage1(order[place])
        if 1 <= place <= count:
            stage2(order[place - 1])
        if 2 <= place:
            stage3(order[place - 2])
        yield
    for way, when in enumerate((z > 0, z < last)):
        chain = 3 * depth + way * depth + z
        for part in range(HALVES):
            for a in every:

                @pl.when(when)
                def _(a=a, part=part, chain=chain):
                    wait(a, chain, part)
                    outs[a][rows_of(outs[a], part), :] += loaded(a, chain, part)


def reduce_scratch(shapes, dtypes, depth):
    return [pltpu.VMEM((5 * depth,) + s, d) for s, d in zip(shapes, dtypes)] + [
        pltpu.SemaphoreType.DMA((len(shapes), 5 * depth, HALVES)),
        pltpu.SemaphoreType.DMA((len(shapes), 5 * depth, HALVES)),
    ]


def run_tasks(*tasks):
    tasks = list(tasks)
    while tasks:
        for task in list(tasks):
            try:
                next(task)
            except StopIteration:
                tasks.remove(task)


def share_task(links, own, full, send_sem, recv_sem):
    depth = links.depth
    slot = links.z * 4 + links.t
    for at, peer in enumerate(everyone(depth)):
        links.send(own, full.at[slot], send_sem.at[at], recv_sem.at[slot], peer)
    full[slot] = own[...]
    yield
    for hop in range(depth):
        for turn in range(4):
            if hop or turn:
                source = lax.rem(links.z + hop, depth) * 4 + lax.rem(links.t + turn, 4)
                links.wait(full.at[source], send_sem.at[0], recv_sem.at[source])


def spread_rows(rows):
    size = rows.shape[1]
    eye = ones_where(iota((size, size), 0) == iota((size, size), 1), jnp.float32)
    return mxu(eye, rows, 1, 1, exact)


def turn_forward_kernel(
    depth,
    gated_ref,
    squares_ref,
    small_ref,
    wall_ref,
    hidden_ref,
    gain_ref,
    pack_ref,
    early_ref,
    bc_ref,
    hidden_out,
    total_out,
    inv_out,
    full_out,
    full_pack,
    full_bc,
    parts,
    normed,
    shared,
    share_send,
    share_recv,
    bufs,
    reduce_send,
    reduce_recv,
    gather_send,
    gather_recv,
    pack_send,
    pack_recv,
    bc_send,
    bc_recv,
):
    links = Links(depth)
    greet(everyone(depth) + [links.far_x])
    width = gated_ref.shape[1]
    piece = hidden_ref.shape[1] // 4
    block = 4 * piece
    share = share_task(links, squares_ref, shared, share_send, share_recv)
    next(share, None)
    weights = Weights(links, pack_ref, full_pack, pack_send, pack_recv)
    here = [links.z, weights.order[0], weights.order[1]]
    for far in here:
        full_pack[weights.base + far] = early_ref[weights.base + far]
    other = (1 - links.x) * depth + links.z
    full_pack[other] = early_ref[other]
    run_tasks(share)
    total = shared[0]
    for slot in range(1, 4 * depth):
        total = total + shared[slot]
    inv_rows = lax.rsqrt(total / INNER + epsilon)
    inv_out[...] = inv_rows
    columns = spread_rows(inv_rows)
    shift = lane_shift(width)
    gains = small_ref[5:6, :width]
    which = iota((block, columns.shape[1]), 1)

    def produce(far):
        at = far * (block // 128)
        both = jnp.concatenate([columns] * (block // 128), axis=0)
        low = iota((block, columns.shape[1]), 0) // 128 + at
        inv = jnp.sum(jnp.where(which == low, both, 0.0), axis=1, keepdims=True)
        rows = pl.ds(pl.multiple_of(far * block, block), block)
        scaled = (gated_ref[rows, :] * inv * gains).astype(LOW)
        moved = mxu(scaled, shift, 1, 0).astype(LOW)
        part = mxu(moved, wall_ref[:, OUT_AT : OUT_AT + 256], 1, 1)
        for row in range(4):
            parts[far * 4 + row] = part[row * piece : (row + 1) * piece].astype(parts.dtype)

    def background():
        weights.over(0, False)
        yield
        weights.along(2)
        yield
        weights.over(1, False)
        yield
        yield
        weights.over(2)

    shared_bc = shared_task(links, bc_ref.at[1], full_bc, bc_send, bc_recv)
    run_tasks(
        reduce_task(links, produce, [parts], [total_out], [bufs], reduce_send, reduce_recv),
        background(),
        shared_bc,
    )
    rows = pl.ds(pl.multiple_of(links.t * piece, piece), piece)
    hidden = hidden_ref[0, rows, :].astype(jnp.float32) + total_out[...]
    hidden_out[...] = hidden
    _, normed[...] = norm_rows(hidden, gain_ref[...].astype(jnp.float32)[1:2])
    run_tasks(gather_task(links, [normed], [full_out], gather_send, gather_recv))
    for far in weights.order:
        weights.over_landed(far)
    links.finish()


def turn_forward(gated, squares, small, wall, hidden, gain, pack, early, bc, depth, collective_id):
    piece, model_width = hidden.shape[1] // 4, hidden.shape[2]
    slots = 4 * depth
    f32 = jnp.float32
    return pl.pallas_call(
        partial(turn_forward_kernel, depth),
        out_shape=[
            jax.ShapeDtypeStruct((piece, model_width), f32),
            jax.ShapeDtypeStruct((piece, model_width), f32),
            jax.ShapeDtypeStruct(squares.shape, f32),
            jax.ShapeDtypeStruct((slots, piece, model_width), LOW),
        ]
        + pack_shapes(depth, pack.shape[1], bc.shape[2]),
        in_specs=[VMEM_SPEC] * 9,
        out_specs=[VMEM_SPEC] * 6,
        scratch_shapes=[
            pltpu.VMEM((slots, piece, model_width), f32),
            pltpu.VMEM((piece, model_width), LOW),
            pltpu.VMEM((slots,) + squares.shape, f32),
            pltpu.SemaphoreType.DMA((slots,)),
            pltpu.SemaphoreType.DMA((slots,)),
        ]
        + reduce_scratch([(piece, model_width)], [f32], depth)
        + gather_sems(1, slots)
        + weights_sems(depth)
        + shared_sems(depth),
        compiler_params=params_of(collective_id),
        name="turn_forward",
    )(gated, squares, small, wall, hidden, gain, pack, early, bc)


def partners(links):
    z = links.z
    return [lax.rem(z + 2, 4), z + 1 - 2 * lax.rem(z, 2), 3 - z]


class Weights:
    def __init__(self, links, pack, full, send_sem, recv_sem):
        self.links, self.pack, self.full = links, pack, full
        self.send_sem, self.recv_sem = send_sem, recv_sem
        self.order = partners(links)
        self.base = links.x * links.depth
        self.mine = self.base + links.z

    def send(self, ref, slot, part, kind, peer):
        self.links.send(
            ref,
            half(self.full.at[slot], part),
            self.send_sem.at[kind, part],
            self.recv_sem.at[slot, part],
            peer,
        )

    def arrived(self, slot, part):
        ref = half(self.full.at[slot], part)
        self.links.wait(ref, self.send_sem.at[0, part], self.recv_sem.at[slot, part])
        return ref

    def keep(self):
        self.full[self.mine] = self.pack[self.links.z]

    def own_over(self):
        for part in range(HALVES):
            self.send(half(self.pack.at[self.links.z], part), self.mine, part, 0, self.links.far_x)

    def along(self, place):
        far = self.order[place]
        for part in range(HALVES):
            self.send(half(self.pack.at[far], part), self.mine, part, 1 + place, {"ctx": far})

    def landed(self, place):
        for part in range(HALVES):
            self.arrived(self.base + self.order[place], part)

    def over(self, place, wait=True):
        slot = self.base + self.order[place]
        for part in range(HALVES):
            ref = self.arrived(slot, part) if wait else half(self.full.at[slot], part)
            self.send(ref, slot, part, self.links.depth + place, self.links.far_x)

    def own_over_landed(self):
        self.over_landed(self.links.z)

    def over_landed(self, far):
        slot = (1 - self.links.x) * self.links.depth + far
        for part in range(HALVES):
            self.arrived(slot, part)

    def task(self):
        self.own_over()
        self.keep()
        yield
        self.along(1)
        yield
        self.along(0)
        yield
        self.over(1)
        yield
        self.along(2)
        self.over(0)
        yield
        self.over(2)
        yield
        for far in [self.links.z] + self.order:
            self.over_landed(far)


def weights_sems(depth):
    return [
        pltpu.SemaphoreType.DMA((2 * depth, HALVES)),
        pltpu.SemaphoreType.DMA((2 * depth, HALVES)),
    ]


def shared_task(links, own, full, send_sem, recv_sem):
    x, z, t, depth = links.x, links.z, links.t, links.depth
    quarter = own.at[pl.ds(t * full.shape[2], full.shape[2])]
    mine = x * depth + z

    def send(ref, slot, column, kind, peer):
        links.send(ref, full.at[slot, column], send_sem.at[slot, column, kind], recv_sem.at[slot, column], peer)

    def arrived(slot, column):
        ref = full.at[slot, column]
        links.wait(ref, send_sem.at[slot, column, 0], recv_sem.at[slot, column])
        return ref

    order = partners(links)
    for place, far in enumerate(order):
        send(quarter, mine, t, place, {"ctx": far})
    send(quarter, mine, t, 3, links.far_x)
    full[mine] = own[...].reshape(full.shape[1:])
    yield
    for place in (1, 0, 2):
        slot = x * depth + order[place]
        ref = arrived(slot, t)
        send(ref, slot, t, 3, links.far_x)
        send(ref, slot, t, 4, links.chip)
        send(ref, slot, t, 5, links.core)
    yield
    for far in [z] + order:
        slot = (1 - x) * depth + far
        ref = arrived(slot, t)
        send(ref, slot, t, 4, links.chip)
        send(ref, slot, t, 5, links.core)
    others = [x * depth + far for far in order] + [(1 - x) * depth + far for far in [z] + order]
    yield
    for slot in others:
        send(arrived(slot, other_chip(t)), slot, other_chip(t), 5, links.core)
    yield
    for slot in others:
        for column in (other_core(t), other_chip(other_core(t))):
            arrived(slot, column)


def shared_sems(depth):
    return [
        pltpu.SemaphoreType.DMA((2 * depth, 4, 6)),
        pltpu.SemaphoreType.DMA((2 * depth, 4)),
    ]


def scatter_task(links, grads, out, bufs, send_sem, recv_sem):
    x, z, depth = links.x, links.z, links.depth
    order = partners(links) + [z]

    def rows_of(ref, part):
        rows = ref.shape[0] // HALVES
        return slice(part * rows, (part + 1) * rows)

    def over(place):
        for part in range(HALVES):
            links.send(
                half(grads.at[(1 - x) * depth + order[place]], part),
                half(bufs.at[place], part),
                send_sem.at[place, part],
                recv_sem.at[place, part],
                links.far_x,
            )

    over(0)
    over(1)
    yield
    for place, far in enumerate(order):
        for part in range(HALVES):
            ref = half(bufs.at[place], part)
            links.wait(ref, send_sem.at[place, part], recv_sem.at[place, part])
            rows = rows_of(out.at[0], part)
            total = grads[x * depth + far, rows, :].astype(jnp.float32) + bufs[place, rows, :].astype(
                jnp.float32
            )
            if place < 3:
                bufs[place, rows, :] = total.astype(LOW)
                links.send(
                    ref,
                    half(out.at[z], part),
                    send_sem.at[depth + place, part],
                    recv_sem.at[depth + z, part],
                    {"ctx": far},
                )
            else:
                out[z, rows, :] = total.astype(LOW)
        if place < 2:
            over(place + 2)
        yield
    for far in order[:3]:
        for part in range(HALVES):
            links.wait(half(out.at[far], part), send_sem.at[0, part], recv_sem.at[depth + far, part])


def scatter_scratch(shape, depth, keep=True):
    return [pltpu.VMEM((depth,) + shape, LOW)] * (2 if keep else 1) + [
        pltpu.SemaphoreType.DMA((2 * depth, HALVES)),
        pltpu.SemaphoreType.DMA((2 * depth, HALVES)),
    ]


def placed(far, width, whole):
    window, lane = iota((256, whole), 0), iota((256, whole), 1)
    return ones_where(jnp.logical_and(lane == window + far * width, window < width), LOW)


def unpack_early(early, width, layer, gate_out, proj_out):
    take = ones_where(iota((256, width), 0) == iota((256, width), 1) + 64, LOW)
    gate = 0.0
    for far in range(early.shape[0]):
        gate += mxu(early[far, :, 0:256], placed(far, width, gate_out.shape[2]), 1, 0)
        proj_out[layer, far * width : (far + 1) * width, :] = mxu(
            take, early[far, :, OUT_AT : OUT_AT + 256], 0, 1
        )
    gate_out[layer] = gate


def bc_products(normed_ref, bc_low, slots_ref):
    rows = slots_ref.shape[1]
    for pair in range(slots_ref.shape[0] // 2):
        total = mxu(normed_ref[:, pair * 2 * rows : (pair + 1) * 2 * rows], bc_low, 0, 0)
        slots_ref[2 * pair] = total[:rows].astype(LOW)
        slots_ref[2 * pair + 1] = total[rows:].astype(LOW)


def bc_task(links, slots_ref, arrived_ref, out_ref, layer, send_sem, recv_sem):
    x, z, depth = links.x, links.z, links.depth
    links.send(slots_ref.at[(1 - x) * depth + z], arrived_ref, send_sem, recv_sem, links.far_x)
    yield
    links.wait(arrived_ref, send_sem, recv_sem)
    out_ref[layer] = slots_ref[x * depth + z].astype(jnp.float32) + arrived_ref[...].astype(jnp.float32)


def rows_task(links, ref, out, send_sem, recv_sem):
    t = links.t
    for way, peer in enumerate((links.chip, links.core)):
        links.send(ref, out.at[t], send_sem.at[way], recv_sem.at[t], peer)
    out[t] = ref[...]
    yield
    column = other_chip(t)
    links.wait(out.at[column], send_sem.at[0], recv_sem.at[column])
    links.send(out.at[column], out.at[column], send_sem.at[2], recv_sem.at[column], links.core)
    yield
    for column in (other_core(t), other_chip(other_core(t))):
        links.wait(out.at[column], send_sem.at[0], recv_sem.at[column])


ROWS_SEMS = [pltpu.SemaphoreType.DMA((3,)), pltpu.SemaphoreType.DMA((4,))]


def sums_task(links, own, arrived_ref, work, by_z, sum_out, send_sem, recv_sem, channel_rows=9):
    z, depth = links.z, links.depth
    links.send(own, arrived_ref.at[0], send_sem.at[0], recv_sem.at[0], links.far_x)
    yield
    links.wait(arrived_ref.at[0], send_sem.at[0], recv_sem.at[0])
    over_dp = own[...] + arrived_ref[0]
    work[0] = over_dp
    links.send(work.at[0], arrived_ref.at[1], send_sem.at[1], recv_sem.at[1], links.core)
    yield
    links.wait(arrived_ref.at[1], send_sem.at[1], recv_sem.at[1])
    work[1] = work[0] + arrived_ref[1]
    links.send(work.at[1], arrived_ref.at[2], send_sem.at[2], recv_sem.at[2], links.chip)
    yield
    links.wait(arrived_ref.at[2], send_sem.at[2], recv_sem.at[2])
    row = iota(own.shape, 0)
    kept = jnp.logical_and(row < 16 * LAYERS, lax.rem(row, 16) < channel_rows)
    work[2] = jnp.where(kept, work[0], work[1] + arrived_ref[2])
    for hop in range(1, depth):
        links.send(
            work.at[2], by_z.at[z], send_sem.at[2 + hop], recv_sem.at[3 + z], {"ctx": lax.rem(z + hop, depth)}
        )
    by_z[z] = work[2]
    yield
    for hop in range(1, depth):
        far = lax.rem(z + hop, depth)
        links.wait(by_z.at[far], send_sem.at[0], recv_sem.at[3 + far])
    whole = by_z[0]
    for far in range(1, depth):
        whole = whole + by_z[far]
    sum_out[...] = whole


def sums_scratch(shape, depth):
    return [
        pltpu.VMEM((3,) + shape, jnp.float32),
        pltpu.VMEM((3,) + shape, jnp.float32),
        pltpu.SemaphoreType.DMA((3 + depth,)),
        pltpu.SemaphoreType.DMA((3 + depth,)),
    ]


ANY_SPEC = pl.BlockSpec(memory_space=pl.ANY)


class Fetch:
    def __init__(self, sources, targets, sems):
        self.copies = [
            pltpu.make_async_copy(source, target, sems.at[at])
            for at, (source, target) in enumerate(zip(sources, targets))
        ]
        self.waiting = set(range(len(self.copies)))
        for copy in self.copies:
            copy.start()

    def wait(self, *which):
        for at in which or range(len(self.copies)):
            if at in self.waiting:
                self.waiting.remove(at)
                self.copies[at].wait()


def build_pack(pack, gate, value, step, proj):
    depth, rows, _ = pack.shape
    width, heads = gate.shape[1] // depth, step.shape[1] // depth
    shift = lane_shift(width)
    blank = jnp.zeros((rows, 128), jnp.float32)
    inside = iota((rows, 256), 1) < width

    def own_lanes(ref, far):
        at = far * width // 128 * 128
        window = ref[:, at : at + 256].astype(jnp.float32)
        if far * width > at:
            window = pltpu.roll(window, 256 - (far * width - at), 1)
        return jnp.where(inside, window, 0.0)

    for far in range(depth):
        gate_lanes, value_lanes = own_lanes(gate, far), own_lanes(value, far)
        pack[far, :, 0:128] = gate_lanes[:, 0:128].astype(LOW)
        out = mxu(proj[far * width : (far + 1) * width, :], shift, 0, 0)
        pack[far, :, OUT_AT:VALUE_AT] = (
            out + jnp.concatenate([gate_lanes[:, 128:256], blank], axis=1)
        ).astype(LOW)
        pack[far, :, VALUE_AT : VALUE_AT + 128] = value_lanes[:, 0:128].astype(LOW)
        head = iota((depth * heads, 128), 0) - far * heads
        chosen = jnp.logical_and(jnp.logical_and(head >= 0, head < heads), iota(head.shape, 1) == head + 64)
        pack[far, :, VALUE_AT + 128 :] = (
            value_lanes[:, 128:256] + mxu(step[...], ones_where(chosen, LOW), 1, 0)
        ).astype(LOW)


def raw_scratch(gate, step, proj):
    return [pltpu.VMEM(a.shape[1:], LOW) for a in (gate, gate, step, proj)] + [pltpu.SemaphoreType.DMA((4,))]


def prepare_kernel(
    depth,
    hidden_ref,
    seg_ref,
    gain_ref,
    gate_ref,
    value_ref,
    step_ref,
    proj_ref,
    bc_ref,
    taps_ref,
    tap_bias_ref,
    out_gain_ref,
    skip_ref,
    step_bias_ref,
    decay_ref,
    bc_taps_ref,
    bc_bias_ref,
    full_out,
    pack_out,
    bc_out,
    smalls_out,
    segr_out,
    segc_out,
    normed,
    seg_piece,
    seg_full,
    pack,
    raw_gate,
    raw_value,
    raw_step,
    raw_proj,
    raw_sems,
    gather_send,
    gather_recv,
    pack_send,
    pack_recv,
    bc_send,
    bc_recv,
):
    f32 = jnp.float32
    links = Links(depth)
    raw = (raw_gate, raw_value, raw_step, raw_proj)
    fetch = Fetch([r.at[0] for r in (gate_ref, value_ref, step_ref, proj_ref)], raw, raw_sems)
    piece, model_width = normed.shape
    rows = pl.ds(pl.multiple_of(links.t * piece, piece), piece)
    _, normed[...] = norm_rows(hidden_ref[0, rows, :].astype(f32), gain_ref[0:1, :].astype(f32))
    tokens = seg_ref.shape[1]
    lane, place = iota((tokens, 128), 0) - links.t * piece, iota((tokens, 128), 1)
    pick = ones_where(jnp.logical_and(lane == place, place < piece), f32)
    seg_piece[...] = mxu(jnp.broadcast_to(seg_ref[...].astype(f32), (8, tokens)), pick, 1, 0, exact)
    greet(everyone(depth) + [links.far_x])
    gather = gather_task(links, [normed, seg_piece], [full_out, seg_full], gather_send, gather_recv)
    next(gather, None)
    shared = shared_task(links, bc_ref.at[0], bc_out, bc_send, bc_recv)
    fetch.wait()
    build_pack(pack, *raw)
    weights = Weights(links, pack, pack_out, pack_send, pack_recv)
    weights.own_over()
    weights.keep()
    next(gather, None)
    weights.along(1)
    next(gather, None)
    weights.along(0)
    next(shared, None)
    width = taps_ref.shape[2] // depth
    lane, place = iota((taps_ref.shape[2], 256), 0) - links.z * width, iota((taps_ref.shape[2], 256), 1)
    own = ones_where(jnp.logical_and(lane == place, place < width), f32)
    heads = skip_ref.shape[1] // depth
    head, place = iota((skip_ref.shape[1], 256), 0) - links.z * heads, iota((skip_ref.shape[1], 256), 1)
    spread = ones_where(jnp.logical_and(head == place // HEADDIM, place < width), f32)
    smalls_out[...] = jnp.zeros(smalls_out.shape, f32)
    for layer in range(LAYERS):
        one = slice(layer, layer + 1)
        smalls_out[layer, 0:4, :] = mxu(taps_ref[layer].astype(f32), own, 1, 0, exact)
        by_channel = jnp.concatenate(
            [tap_bias_ref[...].astype(f32)[one], out_gain_ref[...].astype(f32)[one]] * 4, axis=0
        )
        smalls_out[layer, 4:6, :] = mxu(by_channel, own, 1, 0, exact)[0:2]
        by_head = jnp.concatenate(
            [skip_ref[one, :], step_bias_ref[one, :], -jnp.exp(decay_ref[one, :])] + [skip_ref[one, :]] * 5,
            axis=0,
        )
        smalls_out[layer, 6:9, :] = mxu(by_head, spread, 1, 0, exact)[0:3]
        smalls_out[layer, 9:13, :] = bc_taps_ref[layer].astype(f32)
        smalls_out[layer, 13:14, :] = bc_bias_ref[...].astype(f32)[one]
    next(gather, None)
    weights.over(1)
    weights.along(2)
    next(gather, None)
    weights.over(0)
    next(gather, None)
    per = 128 // piece
    segc_out[...] = jnp.full(segc_out.shape, -1.0, f32)
    for row in range(4 * depth // per):
        lanes = iota((8, 128), 1)
        total = jnp.zeros((8, 128), f32)
        for at in range(per):
            part = seg_full[row * per + at]
            total = jnp.where(lanes // piece == at, pltpu.roll(part, at * piece, 1) if at else part, total)
        segr_out[:, row * 128 : (row + 1) * 128] = total[0:1]
        column = spread_rows(total)[:, 0:1]
        segc_out[8 + row * 128 : 8 + (row + 1) * 128, :] = jnp.broadcast_to(column, (128, 256))
    weights.over(2)
    run_tasks(shared)
    for far in [links.z] + weights.order:
        weights.over_landed(far)
    links.finish()


def pack_shapes(depth, rows, bc_width):
    return [
        jax.ShapeDtypeStruct((2 * depth, rows, PACK), LOW),
        jax.ShapeDtypeStruct((2 * depth, 4, rows // 4, bc_width), LOW),
    ]


def piece_shapes(pieces, depth):
    return [jax.ShapeDtypeStruct((4 * depth,) + p.shape, p.dtype) for p in pieces]


def prepare(hidden, segment, gain, gate, value, step, proj, bc, small, depth, collective_id):
    f32 = jnp.float32
    _, tokens, model_width = hidden.shape
    piece, slots = tokens // 4, 4 * depth
    rows = gate.shape[1]
    shapes = [
        jax.ShapeDtypeStruct((slots, piece, model_width), LOW),
        *pack_shapes(depth, rows, bc.shape[2]),
        jax.ShapeDtypeStruct((LAYERS, 16, 256), f32),
        jax.ShapeDtypeStruct((1, depth * tokens), f32),
        jax.ShapeDtypeStruct((depth * tokens + 16, 256), f32),
    ]
    return pl.pallas_call(
        partial(prepare_kernel, depth),
        out_shape=shapes,
        in_specs=[VMEM_SPEC] * 3 + [ANY_SPEC] * 4 + [VMEM_SPEC] * (1 + len(small)),
        out_specs=[VMEM_SPEC] * len(shapes),
        scratch_shapes=[
            pltpu.VMEM((piece, model_width), LOW),
            pltpu.VMEM((8, 128), f32),
            pltpu.VMEM((slots, 8, 128), f32),
            pltpu.VMEM((depth, rows, PACK), LOW),
        ]
        + raw_scratch(gate, step, proj)
        + gather_sems(2, slots)
        + weights_sems(depth)
        + shared_sems(depth),
        compiler_params=params_of(collective_id),
        name="prepare",
    )(hidden, segment, gain, gate, value, step, proj, bc, *small)


class SumStream:
    def __init__(self, links, parts, out, bufs, send_sem, recv_sem, low=0, high=4):
        self.links, self.parts, self.out, self.bufs = links, parts, out, bufs
        self.send_sem, self.recv_sem = send_sem, recv_sem
        self.receives = jnp.logical_and(links.z >= low, links.z < high)

    def rows(self, part):
        size = self.out.shape[0] // HALVES
        return slice(part * size, (part + 1) * size)

    def sems(self, at, part):
        return self.send_sem.at[at, part], self.recv_sem.at[at, part]

    def wait(self, at, part):
        self.links.wait(half(self.bufs.at[at], part), *self.sems(at, part))

    def loaded(self, at, part):
        return self.bufs[at, self.rows(part), :].astype(jnp.float32)

    def mine(self, slot, part):
        return self.parts[slot, self.rows(part), :].astype(jnp.float32)

    def first(self, far):
        t = self.links.t
        for which, row in enumerate((other_chip(other_core(t)), other_core(t))):
            for part in range(HALVES):
                at = far * 2 + which
                self.links.send(
                    half(self.parts.at[far * 4 + row], part),
                    half(self.bufs.at[at], part),
                    *self.sems(at, part),
                    self.links.core,
                )

    def second(self, far):
        at = far * 2
        for part in range(HALVES):
            self.wait(at, part)
            total = self.mine(far * 4 + other_chip(self.links.t), part) + self.loaded(at, part)
            self.bufs[at, self.rows(part), :] = total.astype(self.bufs.dtype)
            self.links.send(
                half(self.bufs.at[at], part),
                half(self.bufs.at[8 + far], part),
                *self.sems(8 + far, part),
                self.links.chip,
            )

    def third(self, far):
        at = far * 2 + 1
        z = self.links.z
        for part in range(HALVES):
            self.wait(at, part)
            self.wait(8 + far, part)
            total = (
                self.mine(far * 4 + self.links.t, part) + self.loaded(at, part) + self.loaded(8 + far, part)
            )
            rows = self.rows(part)

            @pl.when(z == far)
            def _(total=total, rows=rows):
                self.out[rows, :] = total

            @pl.when(z != far)
            def _(total=total, rows=rows):
                self.bufs[at, rows, :] = total.astype(self.bufs.dtype)

            self.links.send(
                half(self.bufs.at[at], part),
                half(self.bufs.at[12 + z], part),
                self.send_sem.at[12 + far, part],
                self.recv_sem.at[12 + z, part],
                {"ctx": far},
                z != far,
            )

    def end(self):
        @pl.when(self.receives)
        def _():
            for hop in range(1, self.links.depth):
                far = lax.rem(self.links.z + hop, self.links.depth)
                for part in range(HALVES):
                    self.wait(12 + far, part)
                    self.out[self.rows(part), :] += self.loaded(12 + far, part)


def stream_scratch(shape, dtype):
    return [
        pltpu.VMEM((16,) + shape, dtype),
        pltpu.SemaphoreType.DMA((16, HALVES)),
        pltpu.SemaphoreType.DMA((16, HALVES)),
    ]


class Plan:
    def __init__(self, calls):
        self.calls = calls

    def __call__(self, turn, point):
        for call in self.calls.get((turn, point), ()):
            call()


def advance(task):
    def step():
        next(task, None)

    return step


def forward_first_kernel(depth, *refs):
    compute, weights_in, results, (pack, full_pack) = refs[:6], refs[6:10], refs[10:18], refs[18:20]
    *raw, raw_sems, pack_send, pack_recv = refs[20:]
    links = Links(depth)
    fetch = Fetch([r.at[1] for r in weights_in], raw, raw_sems)
    greet(everyone(depth) + [links.far_x])
    fetch.wait()
    build_pack(pack, *raw)
    weights = Weights(links, pack, full_pack, pack_send, pack_recv)
    weights.along(0)
    weights.own_over()
    weights.keep()
    plan = Plan({(1, 1): [partial(weights.along, 1)]})
    forward_body(True, plan, *compute, *results)
    weights.landed(0)
    weights.landed(1)
    weights.own_over_landed()
    links.finish()


def forward_first(normed, wall, bcw, small, segr, segc, slots, gate, value, step, proj, depth, collective_id):
    rows = gate.shape[1]
    shapes = forward_shapes(normed, bcw, slots, True) + [
        jax.ShapeDtypeStruct((depth, rows, PACK), LOW),
        jax.ShapeDtypeStruct((2 * depth, rows, PACK), LOW),
    ]
    return pl.pallas_call(
        partial(forward_first_kernel, depth),
        out_shape=shapes,
        in_specs=[VMEM_SPEC] * 6 + [ANY_SPEC] * 4,
        out_specs=[VMEM_SPEC] * len(shapes),
        scratch_shapes=raw_scratch(gate, step, proj) + weights_sems(depth),
        compiler_params=params_of(collective_id),
        name="forward_first",
    )(normed, wall, bcw, small, segr, segc, gate, value, step, proj)


def forward_second_kernel(depth, *refs):
    compute, cotangent, results, (full, inv_out, inner_out), scratch = (
        refs[:6],
        refs[6],
        refs[7:15],
        refs[15:18],
        refs[18:],
    )
    gather_send, gather_recv, own, shared, share_send, share_recv = scratch
    links = Links(depth)
    greet(everyone(depth))
    piece = full.shape[1]
    mine = cotangent.at[0, pl.ds(pl.multiple_of(links.t * piece, piece), piece)]
    gather = gather_task(links, [mine], [full], gather_send, gather_recv)
    next(gather, None)
    go = [advance(gather)]
    forward_body(False, Plan({(1, 0): go, (2, 0): go, (3, 0): go}), *compute, *results)
    run_tasks(gather)
    _, wall_ref, _, small_ref = compute[:4]
    squares_ref, gate_ref, mixed_ref = results[1], results[2], results[6]
    width = gate_ref.shape[1]
    rows = squares_ref.shape[0]
    own[0:rows, :] = squares_ref[...]
    gains = small_ref[5:6, :width]
    per = 128 // piece
    for row in range(rows):
        grad = full[per * row : per * (row + 1)].reshape(128, full.shape[2])
        grad_scaled = mxu(grad, wall_ref[:, OUT_AT : OUT_AT + 256], 1, 0)
        grad_scaled = pltpu.roll(grad_scaled, 192, 1)[:, :width]
        at = pl.ds(row * 128, 128)
        gate_pre = gate_ref[at, :]
        terms = grad_scaled * gains * mixed_ref[at, :] * gate_pre * sigmoid(gate_pre)
        own[rows + row : rows + row + 1, :] = mxu(
            jnp.ones((8, width), jnp.float32), terms, 1, 1, exact
        )[0:1]
    run_tasks(share_task(links, own, shared, share_send, share_recv))
    summed = shared[0]
    for slot in range(1, 4 * depth):
        summed = summed + shared[slot]
    inv = lax.rsqrt(summed[0:rows] / INNER + epsilon)
    inv_out[...] = inv
    inner_out[...] = inv * summed[rows:] / INNER
    links.finish()


def forward_second(normed, wall, bcw, small, segr, segc, slots, cotangent, depth, collective_id):
    shapes = forward_shapes(normed, bcw, slots, False)
    rows = shapes[1].shape
    shapes = (
        shapes
        + [jax.ShapeDtypeStruct((4 * depth, cotangent.shape[1] // 4, cotangent.shape[2]), LOW)]
        + [jax.ShapeDtypeStruct(rows, jnp.float32)] * 2
    )
    return pl.pallas_call(
        partial(forward_second_kernel, depth),
        out_shape=shapes,
        in_specs=[VMEM_SPEC] * 7,
        out_specs=[VMEM_SPEC] * len(shapes),
        scratch_shapes=gather_sems(1, 4 * depth)
        + [
            pltpu.VMEM((2 * rows[0], 128), jnp.float32),
            pltpu.VMEM((4 * depth, 2 * rows[0], 128), jnp.float32),
            pltpu.SemaphoreType.DMA((4 * depth,)),
            pltpu.SemaphoreType.DMA((4 * depth,)),
        ],
        compiler_params=params_of(collective_id),
        name="forward_second",
    )(normed, wall, bcw, small, segr, segc, cotangent)


def own_column(rows, slot, piece):
    per = 128 // piece
    columns = spread_rows(rows)
    lane = iota(columns.shape, 1)
    column = jnp.sum(jnp.where(lane == slot // per, columns, 0.0), axis=1, keepdims=True)
    at = iota((piece, 128), 0) + lax.rem(slot, per) * piece
    pick = ones_where(at == iota((piece, 128), 1), jnp.float32)
    return mxu(pick, jnp.broadcast_to(column, (128, 128)), 1, 0, exact)[:, 0:1]


def norm_gradient(grad_rows, grad_normed, hidden, gain):
    inv = lax.rsqrt(jnp.mean(hidden * hidden, axis=1, keepdims=True) + epsilon)
    weighted = grad_normed * gain
    grad = (
        grad_rows
        + inv * weighted
        - hidden * (inv * inv * inv) * jnp.mean(weighted * hidden, axis=1, keepdims=True)
    )
    return grad, row_sum(grad_normed * hidden * inv)


def owner_norm(total, grad, hidden_ref, gain_ref, bcw_ref):
    model_width = hidden_ref.shape[1]
    bc_low = total[:, model_width:].astype(LOW)
    grad_normed = total[:, :model_width] + mxu(bc_low, bcw_ref[...], 1, 1)
    grad, gain = norm_gradient(grad, grad_normed, hidden_ref[...].astype(jnp.float32), gain_ref[...])
    return bc_low, grad, gain


def backward_second_kernel(depth, *refs):
    compute, (cotangent, hidden_ref, gain_ref, bcw_ref, before_ref) = refs[:14], refs[14:19]
    late, sums, grad_out, gain_out, full_out, inner_out, early_out = refs[19:26]
    both, early, *work = refs[26:33]
    (
        early_bufs, early_send, early_recv,
        back_total, piece_low, scalars, scalars_full, back_bufs, back_send, back_recv,
        gather_send, gather_recv,
    ) = refs[33:]
    links = Links(depth)
    greet(everyone(depth) + [links.far_x])
    piece, model_width = hidden_ref.shape
    scatter = scatter_task(links, early, early_out, early_bufs, early_send, early_recv)
    go = advance(scatter)
    stream = SumStream(links, both, back_total, back_bufs, back_send, back_recv)

    def call(method, far):
        return partial(method, far)

    plan = Plan(
        {
            (-1, 1): [go],
            (0, 3): [call(stream.first, 3)],
            (1, 0): [call(stream.second, 3)],
            (1, 2): [go],
            (1, 3): [call(stream.first, 2)],
            (2, 0): [call(stream.second, 2), call(stream.third, 3)],
            (2, 2): [go],
            (2, 3): [call(stream.first, 1)],
            (3, 0): [call(stream.second, 1), call(stream.third, 2)],
            (3, 3): [call(stream.first, 0)],
            (4, 0): [call(stream.second, 0), call(stream.third, 1)],
        }
    )
    backward_body(plan, *compute, both, early, late, sums, *work)
    stream.third(0)
    stream.end()
    rows = pl.ds(pl.multiple_of(links.t * piece, piece), piece)
    bc_low, grad, gain_out[...] = owner_norm(
        back_total,
        cotangent[0, rows, :].astype(jnp.float32),
        hidden_ref,
        gain_ref[...].astype(jnp.float32)[1:2],
        bcw_ref,
    )
    grad_low = grad.astype(LOW)
    piece_low[:, :model_width] = grad_low
    piece_low[:, model_width:] = bc_low
    inner = jnp.sum(grad_low.astype(jnp.float32) * before_ref[...], axis=1, keepdims=True) / INNER
    slot, per = links.z * 4 + links.t, 128 // piece
    lane = iota((piece, 128), 0) + lax.rem(slot, per) * piece
    place = ones_where(lane == iota((piece, 128), 1), jnp.float32)
    inner_rows = mxu(jnp.broadcast_to(inner, (piece, 8)), place, 0, 0, exact)
    scalars[...] = jnp.where(iota(inner_rows.shape, 0) == slot // per, inner_rows, 0.0)
    grad_out[...] = grad
    run_tasks(
        gather_task(links, [piece_low, scalars], [full_out, scalars_full], gather_send, gather_recv),
        scatter,
    )
    inner_rows = scalars_full[0]
    for other in range(1, 4 * depth):
        inner_rows = inner_rows + scalars_full[other]
    inner_out[...] = inner_rows
    links.finish()


def backward_second(
    grad, inv, inner, normed, wall, small, segr, segc, kept, slots, cotangent, hidden, gain, bcw, before, depth, collective_id
):
    f32 = jnp.float32
    piece, model_width = hidden.shape
    (both, early, late, sums), work = backward_shapes(normed, kept, slots)
    whole_width = both.shape[2]
    shapes = [
        late,
        sums,
        jax.ShapeDtypeStruct((piece, model_width), f32),
        jax.ShapeDtypeStruct((1, model_width), f32),
        jax.ShapeDtypeStruct(both.shape, LOW),
        jax.ShapeDtypeStruct(inv.shape, f32),
        jax.ShapeDtypeStruct((depth,) + early.shape[1:], LOW),
    ]
    return pl.pallas_call(
        partial(backward_second_kernel, depth),
        out_shape=shapes,
        in_specs=[VMEM_SPEC] * 19,
        out_specs=[VMEM_SPEC] * len(shapes),
        scratch_shapes=[pltpu.VMEM(both.shape, LOW), pltpu.VMEM(early.shape, LOW)]
        + work
        + scatter_scratch(early.shape[1:], depth, False)
        + [
            pltpu.VMEM((piece, whole_width), f32),
            pltpu.VMEM((piece, whole_width), LOW),
            pltpu.VMEM(inv.shape, f32),
            pltpu.VMEM((slots,) + inv.shape, f32),
        ]
        + stream_scratch((piece, whole_width), LOW)
        + gather_sems(2, slots),
        compiler_params=params_of(collective_id),
        name="backward_second",
    )(grad, inv, inner, normed, wall, small, segr, segc, *kept, cotangent, hidden, gain, bcw, before)


def backward_first_kernel(depth, *refs):
    compute, (late1, normed1, grad_in, hidden_ref, gain_ref, bcw_ref, sums1, gain1, part, hidden1, inv1) = (
        refs[:14],
        refs[14:25],
    )
    late1_out, early0_out, late0_out, bc_out, by_z_out, sum_out, hidden_grad_out, hidden_out = refs[25:33]
    both, early, late, sums, *work = refs[33:42]
    (
        out_total, out_low, out_bufs, out_send, out_recv, out_row_send, out_row_recv,
        total, low, bc_piece, bc_full, own,
        bufs, stream_send, stream_recv,
        gather_send, gather_recv,
        late1_bufs, late1_send, late1_recv,
        early0_bufs, early0_send, early0_recv,
        late0_bufs, late0_send, late0_recv,
        bc_slots, bc_arrived, bc_send, bc_recv,
        sums_arrived, sums_work, sums_send, sums_recv,
        row_send, row_recv,
    ) = refs[42:]
    links = Links(depth)
    greet(everyone(depth) + [links.far_x])
    piece, model_width = grad_in.shape
    normed_ref, grad_ref = compute[3], compute[0]
    output = SumStream(links, part, out_total, out_bufs, out_send, out_recv)
    stream = SumStream(links, both, total, bufs, stream_send, stream_recv)
    late_task1 = scatter_task(links, late1, late1_out, late1_bufs, late1_send, late1_recv)
    early_task0 = scatter_task(links, early, early0_out, early0_bufs, early0_send, early0_recv)
    late_task0 = scatter_task(links, late, late0_out, late0_bufs, late0_send, late0_recv)
    bc1 = bc_task(links, bc_slots.at[1], bc_arrived.at[1], bc_out, 1, bc_send.at[1], bc_recv.at[1])
    next(late_task1, None)
    for far in (3, 2, 1, 0):
        output.first(far)

    def call(method, far):
        return partial(method, far)

    def output_rows():
        output.end()
        inv = own_column(inv1[...], links.z * 4 + links.t, piece)
        out_low[...] = (hidden1[...] + out_total[...] * inv).astype(LOW)
        yield from rows_task(links, out_low, hidden_out, out_row_send, out_row_recv)

    def bc_first():
        bc_products(normed1, grad_ref[:, model_width:], bc_slots.at[1])
        next(bc1, None)

    go1, go0 = advance(late_task1), advance(early_task0)
    plan = Plan(
        {
            (-1, 0): [go1, call(output.second, 3)],
            (-1, 1): [go0, go1, call(output.second, 2)],
            (0, 1): [call(output.third, 3), go1],
            (0, 3): [call(stream.first, 3), go1, call(output.third, 2)],
            (1, 0): [call(stream.second, 3), go0],
            (1, 2): [call(output.second, 1)],
            (1, 3): [call(stream.first, 2), go0],
            (2, 0): [call(stream.second, 2), call(stream.third, 3), go1],
            (2, 2): [call(output.third, 1), call(output.second, 0)],
            (2, 3): [call(stream.first, 1), go0],
            (3, 0): [call(stream.second, 1), call(stream.third, 2)],
            (3, 2): [call(output.third, 0)],
            (3, 3): [call(stream.first, 0), go0],
            (4, 0): [call(stream.second, 0), call(stream.third, 1)],
        }
    )
    backward_body(plan, *compute, both, early, late, sums, *work)
    next(late_task0, None)
    bc_first()
    stream.third(0)
    next(late_task0, None)
    stream.end()
    rows = pl.ds(pl.multiple_of(links.t * piece, piece), piece)
    bc_low, grad, gain = owner_norm(
        total, grad_in[...], hidden_ref.at[0, rows], gain_ref[...].astype(jnp.float32)[0:1], bcw_ref
    )
    bc_piece[...] = bc_low
    low[...] = grad.astype(LOW)
    own[...] = jnp.zeros(own.shape, jnp.float32)
    own[0:16, :] = sums[...]
    own[16:32, :] = sums1[...]
    count = model_width // 256
    for layer, row in enumerate((gain, gain1[...])):
        for at in range(count):
            to = 16 * LAYERS + layer * count + at
            own[to : to + 1, :] = row[:, at * 256 : (at + 1) * 256]
    run_tasks(
        gather_task(links, [bc_piece], [bc_full], gather_send, gather_recv),
        sums_task(links, own, sums_arrived, sums_work, by_z_out, sum_out, sums_send, sums_recv),
        rows_task(links, low, hidden_grad_out, row_send, row_recv),
        late_task0,
        output_rows(),
        early_task0,
        late_task1,
        bc1,
    )
    tokens = bc_full.shape[0] * bc_full.shape[1]
    bc_products(normed_ref, bc_full[...].reshape(tokens, bc_full.shape[2]), bc_slots.at[0])
    bc0 = bc_task(links, bc_slots.at[0], bc_arrived.at[0], bc_out, 0, bc_send.at[0], bc_recv.at[0])
    run_tasks(bc0)
    links.finish()


def backward_first(
    grad, inv, inner, normed, wall, small, segr, segc, kept, slots, late1, normed1, grad_in, hidden, gain, bcw, sums1, gain1, part, hidden1, inv1, depth, collective_id
):
    f32 = jnp.float32
    piece, model_width = grad_in.shape
    (both, early, late, sums), work = backward_shapes(normed, kept, slots)
    whole_width = both.shape[2]
    k_slots, k_rows, _ = late1.shape
    bc_width = kept[2].shape[1]
    small_sums = (16 * LAYERS + 16, 256)
    shapes = [
        jax.ShapeDtypeStruct((depth,) + late.shape[1:], LOW),
        jax.ShapeDtypeStruct((depth,) + early.shape[1:], LOW),
        jax.ShapeDtypeStruct((depth,) + late.shape[1:], LOW),
        jax.ShapeDtypeStruct((LAYERS, k_rows, bc_width), f32),
        jax.ShapeDtypeStruct((depth,) + small_sums, f32),
        jax.ShapeDtypeStruct(small_sums, f32),
        jax.ShapeDtypeStruct((4, piece, model_width), LOW),
        jax.ShapeDtypeStruct((4, piece, model_width), LOW),
    ]
    return pl.pallas_call(
        partial(backward_first_kernel, depth),
        out_shape=shapes,
        in_specs=[VMEM_SPEC] * 25,
        out_specs=[VMEM_SPEC] * len(shapes),
        scratch_shapes=[pltpu.VMEM(a.shape, a.dtype) for a in (both, early, late, sums)]
        + work
        + [pltpu.VMEM((piece, model_width), f32), pltpu.VMEM((piece, model_width), LOW)]
        + stream_scratch((piece, model_width), LOW)
        + ROWS_SEMS
        + [
            pltpu.VMEM((piece, whole_width), f32),
            pltpu.VMEM((piece, model_width), LOW),
            pltpu.VMEM((piece, bc_width), LOW),
            pltpu.VMEM((slots, piece, bc_width), LOW),
            pltpu.VMEM(small_sums, f32),
        ]
        + stream_scratch((piece, whole_width), LOW)
        + gather_sems(1, slots)
        + scatter_scratch(late.shape[1:], depth, False)
        + scatter_scratch(early.shape[1:], depth, False)
        + scatter_scratch(late.shape[1:], depth, False)
        + [
            pltpu.VMEM((LAYERS, k_slots, k_rows, bc_width), LOW),
            pltpu.VMEM((LAYERS, k_rows, bc_width), LOW),
            pltpu.SemaphoreType.DMA((LAYERS,)),
            pltpu.SemaphoreType.DMA((LAYERS,)),
        ]
        + sums_scratch(small_sums, depth)
        + ROWS_SEMS,
        compiler_params=params_of(collective_id),
        name="backward_first",
    )(grad, inv, inner, normed, wall, small, segr, segc, *kept, late1, normed1, grad_in, hidden, gain, bcw, sums1, gain1, part, hidden1, inv1)


def emit_kernel(
    hidden_ref, grad_ref, early0, late0, early1, late1, bc_ref, by_z, whole,
    hidden_out, grad_out, gain_out, gate_out, value_out, bc_out, step_out,
    taps_out, tap_bias_out, bc_taps_out, bc_bias_out, decay_out, step_bias_out, skip_out, out_gain_out, proj_out,
):
    piece = hidden_ref.shape[1]
    depth, _, _ = by_z.shape
    channels, heads_whole = taps_out.shape[2], skip_out.shape[1]
    width, heads = channels // depth, heads_whole // depth
    for at in range(4):
        hidden_out[0, at * piece : (at + 1) * piece, :] = hidden_ref[at]
        grad_out[0, at * piece : (at + 1) * piece, :] = grad_ref[at]
    bc_out[...] = bc_ref[...]
    count = gain_out.shape[1] // 256
    for layer, (early, late) in enumerate(((early0, late0), (early1, late1))):
        one = slice(layer, layer + 1)
        unpack_early(early, width, layer, gate_out, proj_out)
        value = step = by_channel = by_head = 0.0
        rows = slice(16 * layer, 16 * layer + 16)
        for far in range(depth):
            place = placed(far, width, channels)
            value += mxu(late[far], place, 1, 0)
            window, head = iota((256, 16), 0), iota((256, 16), 1) - far * heads
            mine = jnp.logical_and(head >= 0, head < heads)
            step += mxu(ones_where(jnp.logical_and(mine, window == width + head), LOW), late[far], 0, 1)
            by_channel += mxu(by_z[far, rows, :], place.astype(jnp.float32), 1, 0, exact)
            window, head = iota((256, 128), 0), iota((256, 128), 1) - far * heads
            mine = jnp.logical_and(head >= 0, head < heads)
            by_head += mxu(
                by_z[far, rows, :],
                ones_where(jnp.logical_and(mine, window == head * HEADDIM), jnp.float32),
                1,
                0,
                exact,
            )
        value_out[layer] = value
        for head in range(heads_whole):
            step_out[head, one, :] = step[head : head + 1]
        taps_out[layer] = by_channel[0:4]
        tap_bias_out[one, :] = by_channel[4:5]
        out_gain_out[one, :] = by_channel[5:6]
        skip_out[one, :] = by_head[6:7, :heads_whole]
        step_bias_out[one, :] = by_head[7:8, :heads_whole]
        decay_out[one, :] = by_head[8:9, :heads_whole]
        bc_taps_out[layer] = whole[16 * layer + 9 : 16 * layer + 13, :]
        bc_bias_out[one, :] = whole[16 * layer + 13 : 16 * layer + 14, :]
        for at in range(count):
            row = 16 * LAYERS + layer * count + at
            gain_out[one, at * 256 : (at + 1) * 256] = whole[row : row + 1, :]


def emit(hidden, grad, early0, late0, early1, late1, bc, by_z, whole, tokens, heads, channels):
    f32 = jnp.float32
    rows, model_width = early0.shape[1], hidden.shape[2]
    bc_width = bc.shape[2]
    shapes = [
        ((1, tokens, model_width), LOW),
        ((1, tokens, model_width), LOW),
        ((LAYERS, model_width), f32),
        ((LAYERS, rows, channels), f32),
        ((LAYERS, rows, channels), f32),
        ((LAYERS, rows, bc_width), f32),
        ((heads, LAYERS, rows), f32),
        ((LAYERS, 4, channels), f32),
        ((LAYERS, channels), f32),
        ((LAYERS, 4, bc_width), f32),
        ((LAYERS, bc_width), f32),
        ((LAYERS, heads), f32),
        ((LAYERS, heads), f32),
        ((LAYERS, heads), f32),
        ((LAYERS, channels), f32),
        ((LAYERS, channels, rows), f32),
    ]
    return pl.pallas_call(
        emit_kernel,
        out_shape=[jax.ShapeDtypeStruct(*shape) for shape in shapes],
        in_specs=[VMEM_SPEC] * 9,
        out_specs=[VMEM_SPEC] * len(shapes),
        compiler_params=local_params(),
        name="emit",
    )(hidden, grad, early0, late0, early1, late1, bc, by_z, whole)


def split_local(
    depth,
    hidden_in,
    segment_ids,
    cotangent,
    norm_gain,
    gate_proj,
    value_proj,
    bc_proj,
    step_proj,
    conv_value,
    conv_value_bias,
    conv_bc,
    conv_bc_bias,
    decay_log,
    step_bias,
    skip_gain,
    out_gain,
    out_proj,
):
    tokens, model_width = hidden_in.shape[1:]
    slots = depth * 4
    heads, channels = step_proj.shape[2], gate_proj.shape[2]
    projections = (gate_proj, value_proj, step_proj, out_proj)
    small = (
        conv_value,
        conv_value_bias,
        out_gain,
        skip_gain,
        step_bias,
        decay_log,
        conv_bc,
        conv_bc_bias,
    )
    normed0, pack0, shared0, smalls, segr, segc = prepare(
        hidden_in, segment_ids, norm_gain, *projections, bc_proj, small, depth, 1
    )
    seg = (segr, segc)
    normed0 = normed0.reshape(-1, model_width)
    wall0, bc_wall0 = pack0.reshape(-1, PACK), shared0.reshape(model_width, -1)
    gated0, squares0, *kept0, packs1, early = forward_first(
        normed0, wall0, bc_wall0, smalls[0], *seg, slots, *projections, depth, 2
    )
    hidden1, total0, inv_rows0, normed1, pack1, shared1 = turn_forward(
        gated0, squares0, smalls[0], wall0, hidden_in, norm_gain, packs1, early, bc_proj, depth, 3
    )
    wall1, bc_wall1 = pack1.reshape(-1, PACK), shared1.reshape(model_width, -1)
    normed1 = normed1.reshape(-1, model_width)
    part1, _, *kept1, cotangent_full, inv_rows1, inner_rows1 = forward_second(
        normed1, wall1, bc_wall1, smalls[1], *seg, slots, cotangent, depth, 4
    )
    late1, sums1, grad1, gain1, full0, inner_rows0, early1 = backward_second(
        cotangent_full.reshape(-1, model_width),
        inv_rows1,
        inner_rows1,
        normed1,
        wall1,
        smalls[1],
        *seg,
        kept1,
        slots,
        cotangent,
        hidden1,
        norm_gain,
        bc_wall1,
        total0,
        depth,
        5,
    )
    late1, early0, late0, bc_grad, by_z, whole, grad_hidden, hidden_out = backward_first(
        full0.reshape(-1, full0.shape[2]),
        inv_rows0,
        inner_rows0,
        normed0,
        wall0,
        smalls[0],
        *seg,
        kept0,
        slots,
        late1,
        normed1,
        grad1,
        hidden_in,
        norm_gain,
        bc_wall0,
        sums1,
        gain1,
        part1,
        hidden1,
        inv_rows1,
        depth,
        6,
    )
    outs = emit(
        hidden_out, grad_hidden, early0, late0, early1, late1, bc_grad, by_z, whole, tokens, heads, channels
    )
    return (*outs[:6], outs[6].transpose(1, 2, 0), *outs[7:])


def solution(mesh):
    in_specs = (
        P("dp", "ctx", None),
        P("dp", "ctx"),
        P("dp", "ctx", None),
        P(),
        P(None, ("dp", "ctx"), "tp"),
        P(None, ("dp", "ctx"), "tp"),
        P(None, ("dp", "ctx"), None),
        P(None, ("dp", "ctx"), "tp"),
        P(None, None, "tp"),
        P(None, "tp"),
        P(),
        P(),
        P(None, "tp"),
        P(None, "tp"),
        P(None, "tp"),
        P(None, "tp"),
        P(None, "tp", ("dp", "ctx")),
    )
    out_specs = (
        P("dp", "ctx", None),
        P("dp", "ctx", None),
        P(),
        P(None, ("dp", "ctx"), "tp"),
        P(None, ("dp", "ctx"), "tp"),
        P(None, ("dp", "ctx"), None),
        P(None, ("dp", "ctx"), "tp"),
        P(None, None, "tp"),
        P(None, "tp"),
        P(),
        P(),
        P(None, "tp"),
        P(None, "tp"),
        P(None, "tp"),
        P(None, "tp"),
        P(None, "tp", ("dp", "ctx")),
    )
    depth = mesh.shape["ctx"]
    heads = 48 // mesh.shape["tp"]
    fits = mesh.shape["tp"] == 4 and mesh.shape["dp"] == 2 and depth == 4 and heads % depth == 0
    body = partial(split_local, depth) if fits else local
    return jax.shard_map(body, mesh=mesh, in_specs=in_specs, out_specs=out_specs, check_vma=False)
```

```python
from functools import partial

import jax
import jax.numpy as jnp
from jax import lax
from jax.experimental import pallas as pl
from jax.experimental.pallas import tpu as pltpu
from jax.sharding import PartitionSpec as P

HEADDIM = 64
BLOCK = 256
LAYERS = 2
INNER = 3072


epsilon = 1e-05
precise = lax.Precision.HIGH


def from_behind(block, axis, distance):
    devices = range(lax.axis_size(axis))
    route = [(i - distance, i) for i in devices if i - distance in devices]
    return lax.ppermute(block, axis, route)


def round_keep(values):
    return lax.optimization_barrier(values.astype(jnp.bfloat16)).astype(jnp.float32)


def dot_back(left_rows, right_rows):
    return lax.dot_general(
        left_rows, right_rows, (((1,), (1,)), ((), ())), preferred_element_type=jnp.float32
    )


def dot_left(left_rows, right_rows):
    return lax.dot_general(
        left_rows, right_rows, (((0,), (0,)), ((), ())), preferred_element_type=jnp.float32
    )


def conv_local(signal, edge_rows, kernel, conv_bias, segment, edge_segment):
    tap_count = kernel.shape[0]
    length = signal.shape[1]
    padded = jnp.concatenate([edge_rows, signal], axis=1)
    seg_pad = jnp.concatenate([edge_segment, segment], axis=1)
    result = conv_bias + jnp.zeros_like(signal)
    for tap_index in range(tap_count):
        same_doc = (seg_pad[:, tap_index : tap_index + length] == segment).astype(jnp.float32)
        result = (
            result
            + kernel[tap_index] * padded[:, tap_index : tap_index + length] * same_doc[:, :, None]
        )
    return jax.nn.silu(result)


def block_step(decay_rates, carried, block_data):
    states, prev_segment = carried
    values, b_mat, c_mat, step_size, segment = block_data
    length = values.shape[0]
    log_decay = jnp.cumsum(step_size * decay_rates, axis=0)
    positions = jnp.arange(length)
    causal = positions[:, None] >= positions[None, :]
    same_doc = jnp.logical_and(segment[:, None] == segment[None, :], causal)[:, :, None]
    differ = jnp.where(same_doc, log_decay[:, None, :] - log_decay[None, :, :], 0.0)
    weights = jnp.where(same_doc, jnp.exp(differ), 0.0)
    cb_product = jnp.dot(c_mat, b_mat.T, precision=precise)
    scores = cb_product[:, :, None] * weights * step_size[None, :, :]
    intra_out = jnp.einsum("tsh,shp->thp", scores, values, precision=precise)
    alive_mask = (segment == prev_segment).astype(jnp.float32)
    reach = alive_mask[:, None] * jnp.exp(log_decay)
    inter_out = reach[:, :, None] * jnp.einsum("tn,hpn->thp", c_mat, states, precision=precise)
    end_same = (segment == segment[length - 1]).astype(jnp.float32)
    to_end = jnp.exp(log_decay[length - 1][None, :] - log_decay) * end_same[:, None] * step_size
    weighted_values = to_end[:, :, None] * values
    new_states = reach[length - 1][:, None, None] * states + jnp.einsum(
        "shp,sn->hpn", weighted_values, b_mat, precision=precise
    )
    return ((new_states, segment[length - 1]), intra_out + inter_out)


def device_scan(values, b_mat, c_mat, step_size, decay_rates, segment, seg_prev):
    block_count = values.shape[0] // BLOCK
    heads_local = values.shape[1]
    state_dim = b_mat.shape[1]
    blocks = (
        values.reshape(block_count, BLOCK, heads_local, HEADDIM),
        b_mat.reshape(block_count, BLOCK, state_dim),
        c_mat.reshape(block_count, BLOCK, state_dim),
        step_size.reshape(block_count, BLOCK, heads_local),
        segment.reshape(block_count, BLOCK),
    )
    initial = (jnp.zeros((heads_local, HEADDIM, state_dim), jnp.float32), seg_prev)
    final_carry, outputs = lax.scan(partial(block_step, decay_rates), initial, blocks)
    return (outputs.reshape(values.shape), final_carry[0])


def step_terms(step_pre, step_bias, decay_log):
    return (jax.nn.softplus(step_pre + step_bias), -jnp.exp(decay_log))


def mixer_terms(values, bc_conv, step_size, decay_rates, skip_gain, segment, seg_prev):
    seq_count, tokens, inner_local = values.shape
    heads_local = step_size.shape[2]
    heads_in = values.reshape(seq_count, tokens, heads_local, HEADDIM)
    state_dim = bc_conv.shape[2] // 2
    scanner = jax.vmap(device_scan, in_axes=(0, 0, 0, 0, None, 0, 0))
    intra_out, local_states = scanner(
        heads_in,
        bc_conv[:, :, :state_dim],
        bc_conv[:, :, state_dim:],
        step_size,
        decay_rates,
        segment,
        seg_prev,
    )
    alive_last = (segment[:, tokens - 1] == seg_prev).astype(jnp.float32)
    decays = alive_last[:, None] * jnp.exp(jnp.sum(step_size * decay_rates, axis=1))
    return (intra_out + skip_gain[:, None] * heads_in, local_states, decays)


def carried_terms(bc_conv, step_size, decay_rates, entering, segment, seg_prev):
    state_dim = bc_conv.shape[2] // 2
    c_mat = bc_conv[:, :, state_dim:]
    log_decay = jnp.cumsum(step_size * decay_rates, axis=1)
    alive_mask = (segment == seg_prev[:, None]).astype(jnp.float32)
    reach = alive_mask[:, :, None] * jnp.exp(log_decay)
    carried = jnp.einsum("sqn,shpn->sqhp", c_mat, entering, precision=precise)
    return reach[:, :, :, None] * carried


def chain_forward(decays, local_states):

    def handoff(step_index, entering):
        return from_behind(decays[:, :, None, None] * entering + local_states, "ctx", 1)

    return lax.fori_loop(0, lax.axis_size("ctx") - 1, handoff, jnp.zeros_like(local_states))


def chain_backward(decays, grad_entering):

    def handback(step_index, beyond):
        return from_behind(
            (grad_entering + decays[:, :, None, None] * beyond).astype(jnp.bfloat16), "ctx", -1
        ).astype(jnp.float32)

    return lax.fori_loop(0, lax.axis_size("ctx") - 1, handback, jnp.zeros_like(grad_entering))


def layer_forward(hidden, segment, layer_params):
    (
        norm_gain,
        gate_proj,
        value_proj,
        bc_proj,
        step_proj,
        conv_value,
        conv_value_bias,
        conv_bc,
        conv_bc_bias,
        decay_log,
        step_bias,
        skip_gain,
        out_gain,
        out_proj,
    ) = layer_params
    seq_count, tokens, model_width = hidden.shape
    row_count = seq_count * tokens
    tap_count = conv_value.shape[0]
    gathered = (
        lax.all_gather(gate_proj, ("dp", "ctx"), axis=0, tiled=True),
        lax.all_gather(value_proj, ("dp", "ctx"), axis=0, tiled=True),
        lax.all_gather(bc_proj, ("dp", "ctx"), axis=0, tiled=True),
        lax.all_gather(step_proj, ("dp", "ctx"), axis=0, tiled=True),
        lax.all_gather(out_proj, ("dp", "ctx"), axis=1, tiled=True),
    )
    gate_full, value_full, bc_full, step_full, out_full = gathered
    hidden_rows = hidden.reshape(row_count, model_width)
    inv_norm = lax.rsqrt(jnp.mean(hidden_rows * hidden_rows, axis=1, keepdims=True) + epsilon)
    normed = (hidden_rows * inv_norm * norm_gain).astype(jnp.bfloat16)
    gate_pre = jnp.dot(normed, gate_full, preferred_element_type=jnp.float32)
    value_pre = jnp.dot(normed, value_full, preferred_element_type=jnp.float32).reshape(
        seq_count, tokens, -1
    )
    bc_pre = jnp.dot(normed, bc_full, preferred_element_type=jnp.float32).reshape(
        seq_count, tokens, -1
    )
    step_pre = jnp.dot(normed, step_full, preferred_element_type=jnp.float32).reshape(
        seq_count, tokens, -1
    )
    first_edge = tokens - tap_count + 1
    edge_value, edge_bc, edge_segment = from_behind(
        (value_pre[:, first_edge:], bc_pre[:, first_edge:], segment[:, first_edge:]), "ctx", 1
    )
    conv_fn = partial(conv_local, segment=segment, edge_segment=edge_segment)
    value_act, value_pull = jax.vjp(conv_fn, value_pre, edge_value, conv_value, conv_value_bias)
    bc_act, bc_pull = jax.vjp(conv_fn, bc_pre, edge_bc, conv_bc, conv_bc_bias)
    values = round_keep(value_act)
    bc_conv = round_keep(bc_act)
    seg_prev = edge_segment[:, tap_count - 2]
    (step_size, decay_rates), step_pull = jax.vjp(step_terms, step_pre, step_bias, decay_log)
    (local_out, local_states, decays), local_pull = jax.vjp(
        partial(mixer_terms, segment=segment, seg_prev=seg_prev),
        values,
        bc_conv,
        step_size,
        decay_rates,
        skip_gain,
    )
    entering = chain_forward(decays, local_states)
    carried_out, carried_pull = jax.vjp(
        partial(carried_terms, segment=segment, seg_prev=seg_prev),
        bc_conv,
        step_size,
        decay_rates,
        entering,
    )
    mixed = (local_out + carried_out).reshape(row_count, -1)
    gate_act = jax.nn.silu(gate_pre)
    gated = mixed * gate_act
    square_sum = lax.psum(jnp.sum(gated * gated, axis=1), "tp")
    inv_gate = lax.rsqrt(square_sum / INNER + epsilon)[:, None]
    scaled = (gated * inv_gate * out_gain).astype(jnp.bfloat16)
    mixer_sum = lax.psum(jnp.dot(scaled, out_full, preferred_element_type=jnp.float32), "tp")
    kept = {
        "scaled": scaled,
        "gated": gated,
        "inv_gate": inv_gate,
        "gate_pre": gate_pre,
        "gate_act": gate_act,
        "mixed": mixed,
        "carried_pull": carried_pull,
        "local_pull": local_pull,
        "step_pull": step_pull,
        "value_pull": value_pull,
        "bc_pull": bc_pull,
        "decays": decays,
        "entering": entering,
        "hidden_rows": hidden_rows,
        "inv_norm": inv_norm,
        "normed": normed,
    }
    return (hidden + mixer_sum.reshape(seq_count, tokens, model_width), kept)


def layer_backward(grad_hidden, kept, layer_params):
    (
        norm_gain,
        gate_proj,
        value_proj,
        bc_proj,
        step_proj,
        conv_value,
        conv_value_bias,
        conv_bc,
        conv_bc_bias,
        decay_log,
        step_bias,
        skip_gain,
        out_gain,
        out_proj,
    ) = layer_params
    seq_count, tokens, model_width = grad_hidden.shape
    row_count = seq_count * tokens
    tap_count = conv_value.shape[0]
    gate_full, value_full, bc_full, step_full, out_full = (
        lax.all_gather(gate_proj, ("dp", "ctx"), axis=0, tiled=True),
        lax.all_gather(value_proj, ("dp", "ctx"), axis=0, tiled=True),
        lax.all_gather(bc_proj, ("dp", "ctx"), axis=0, tiled=True),
        lax.all_gather(step_proj, ("dp", "ctx"), axis=0, tiled=True),
        lax.all_gather(out_proj, ("dp", "ctx"), axis=1, tiled=True),
    )
    grad_rows = grad_hidden.reshape(row_count, model_width)
    grad_low = grad_rows.astype(jnp.bfloat16)
    grad_scaled = dot_back(grad_low, out_full)
    grad_out_proj = dot_left(kept["scaled"], grad_low)
    gated = kept["gated"]
    inv_gate = kept["inv_gate"]
    weighted = grad_scaled * out_gain
    inner_sum = lax.psum(jnp.sum(weighted * gated, axis=1), "tp")
    grad_gated = inv_gate * weighted - gated * inv_gate**3 * (inner_sum / INNER)[:, None]
    grad_out_gain = jnp.sum(grad_scaled * gated * inv_gate, axis=0)
    gate_pre = kept["gate_pre"]
    sigmoid_gate = jax.nn.sigmoid(gate_pre)
    grad_gate_pre = (
        grad_gated * kept["mixed"] * sigmoid_gate * (1.0 + gate_pre * (1.0 - sigmoid_gate))
    )
    grad_heads = (grad_gated * kept["gate_act"]).reshape(
        seq_count, tokens, step_full.shape[1], HEADDIM
    )
    carried_bc, carried_step, carried_rates, grad_entering = kept["carried_pull"](grad_heads)
    beyond = chain_backward(kept["decays"], grad_entering)
    grad_decays = jnp.sum(beyond * kept["entering"], axis=(2, 3))
    local_values, local_bc, local_step, local_rates, grad_skip = kept["local_pull"](
        (grad_heads, beyond, grad_decays)
    )
    grad_step_pre, grad_step_bias, grad_decay_log = kept["step_pull"](
        (carried_step + local_step, carried_rates + local_rates)
    )
    grad_value_pre, grad_edge_value, grad_conv_value, grad_conv_value_bias = kept["value_pull"](
        local_values
    )
    grad_bc_pre, grad_edge_bc, grad_conv_bc, grad_conv_bc_bias = kept["bc_pull"](
        carried_bc + local_bc
    )
    from_value, from_bc = from_behind((grad_edge_value, grad_edge_bc), "ctx", -1)
    first_edge = tokens - tap_count + 1
    grad_value_pre = grad_value_pre.at[:, first_edge:].add(from_value)
    grad_bc_pre = grad_bc_pre.at[:, first_edge:].add(from_bc)
    grad_gate_low = grad_gate_pre.astype(jnp.bfloat16)
    grad_value_low = grad_value_pre.reshape(row_count, -1).astype(jnp.bfloat16)
    grad_step_low = grad_step_pre.reshape(row_count, -1).astype(jnp.bfloat16)
    input_part = (
        dot_back(grad_gate_low, gate_full)
        + dot_back(grad_value_low, value_full)
        + dot_back(grad_step_low, step_full)
    )
    input_sum, bc_sum, conv_bc_sum, conv_bc_bias_sum = (
        lax.psum(input_part.astype(jnp.bfloat16), "tp").astype(jnp.float32),
        lax.psum(grad_bc_pre.reshape(row_count, -1).astype(jnp.bfloat16), "tp").astype(jnp.float32),
        lax.psum(grad_conv_bc, "tp").astype(jnp.float32),
        lax.psum(grad_conv_bc_bias, "tp").astype(jnp.float32),
    )
    grad_bc_low = bc_sum.astype(jnp.bfloat16)
    grad_normed = input_sum + dot_back(grad_bc_low, bc_full)
    hidden_rows = kept["hidden_rows"]
    inv_norm = kept["inv_norm"]
    weighted_norm = grad_normed * norm_gain
    grad_norm_gain = jnp.sum(grad_normed * hidden_rows * inv_norm, axis=0)
    grad_rows = (
        grad_rows
        + inv_norm * weighted_norm
        - hidden_rows * inv_norm**3 * jnp.mean(weighted_norm * hidden_rows, axis=1, keepdims=True)
    )
    normed = kept["normed"]
    proj_grads = (
        lax.psum_scatter(
            dot_left(normed, grad_gate_low).astype(jnp.bfloat16),
            ("dp", "ctx"),
            scatter_dimension=0,
            tiled=True,
        ).astype(jnp.float32),
        lax.psum_scatter(
            dot_left(normed, grad_value_low).astype(jnp.bfloat16),
            ("dp", "ctx"),
            scatter_dimension=0,
            tiled=True,
        ).astype(jnp.float32),
        lax.psum_scatter(
            dot_left(normed, grad_bc_low).astype(jnp.bfloat16),
            ("dp", "ctx"),
            scatter_dimension=0,
            tiled=True,
        ).astype(jnp.float32),
        lax.psum_scatter(
            dot_left(normed, grad_step_low).astype(jnp.bfloat16),
            ("dp", "ctx"),
            scatter_dimension=0,
            tiled=True,
        ).astype(jnp.float32),
        lax.psum_scatter(
            grad_out_proj.astype(jnp.bfloat16), ("dp", "ctx"), scatter_dimension=1, tiled=True
        ).astype(jnp.float32),
    )
    small_grads = lax.psum(
        (
            grad_norm_gain,
            grad_conv_value.astype(jnp.float32),
            grad_conv_value_bias.astype(jnp.float32),
            conv_bc_sum,
            conv_bc_bias_sum,
            grad_decay_log,
            grad_step_bias,
            grad_skip,
            grad_out_gain,
        ),
        ("dp", "ctx"),
    )
    return (grad_rows.reshape(seq_count, tokens, model_width), proj_grads, small_grads)


def stack_layers(groups, member):
    return jnp.stack([groups[layer_index][member] for layer_index in range(LAYERS)])


def local(
    hidden_in,
    segment_ids,
    cotangent,
    norm_gain,
    gate_proj,
    value_proj,
    bc_proj,
    step_proj,
    conv_value,
    conv_value_bias,
    conv_bc,
    conv_bc_bias,
    decay_log,
    step_bias,
    skip_gain,
    out_gain,
    out_proj,
):
    params = (
        norm_gain,
        gate_proj,
        value_proj,
        bc_proj,
        step_proj,
        conv_value,
        conv_value_bias,
        conv_bc,
        conv_bc_bias,
        decay_log,
        step_bias,
        skip_gain,
        out_gain,
        out_proj,
    )
    segment = segment_ids.astype(jnp.float32)
    hidden = hidden_in.astype(jnp.float32)
    kept_layers = []
    for layer_index in range(LAYERS):
        hidden, kept = layer_forward(
            hidden, segment, tuple((stacked[layer_index] for stacked in params))
        )
        kept_layers.append(kept)
    grad_hidden = cotangent.astype(jnp.float32)
    proj_list = [None] * LAYERS
    small_list = [None] * LAYERS
    for layer_index in reversed(range(LAYERS)):
        grad_hidden, proj_list[layer_index], small_list[layer_index] = layer_backward(
            grad_hidden,
            kept_layers[layer_index],
            tuple((stacked[layer_index] for stacked in params)),
        )
    return (
        hidden.astype(jnp.bfloat16),
        grad_hidden.astype(jnp.bfloat16),
        stack_layers(small_list, 0),
        stack_layers(proj_list, 0),
        stack_layers(proj_list, 1),
        stack_layers(proj_list, 2),
        stack_layers(proj_list, 3),
        stack_layers(small_list, 1),
        stack_layers(small_list, 2),
        stack_layers(small_list, 3),
        stack_layers(small_list, 4),
        stack_layers(small_list, 5),
        stack_layers(small_list, 6),
        stack_layers(small_list, 7),
        stack_layers(small_list, 8),
        stack_layers(proj_list, 4),
    )


MESH = pl.DeviceIdType.MESH
PACK = 640


def params_of(collective_id):
    return pltpu.CompilerParams(
        collective_id=collective_id, has_side_effects=True, vmem_limit_bytes=60 << 20
    )


VMEM_SPEC = pl.BlockSpec(memory_space=pltpu.VMEM)


def greet(peers):
    barrier = pltpu.get_barrier_semaphore()
    for peer in peers:
        pl.semaphore_signal(barrier, inc=1, device_id=peer, device_id_type=MESH)
    pl.semaphore_wait(barrier, len(peers))


def remote(source, target, send_sem, recv_sem, peer):
    return pltpu.make_async_remote_copy(
        src_ref=source,
        dst_ref=target,
        send_sem=send_sem,
        recv_sem=recv_sem,
        device_id=peer,
        device_id_type=MESH,
    )


def other_core(t):
    return t + 1 - 2 * lax.rem(t, 2)


def other_chip(t):
    return lax.rem(t + 2, 4)


def mxu(left, right, left_dim, right_dim, precision=None):
    return lax.dot_general(
        left,
        right,
        (((left_dim,), (right_dim,)), ((), ())),
        preferred_element_type=jnp.float32,
        precision=precision,
    )


def parts_of(array, count):
    parts = []
    for _ in range(count - 1):
        high = array.astype(jnp.bfloat16)
        parts.append(high)
        array = array - high.astype(jnp.float32)
    return parts + [array.astype(jnp.bfloat16)]


def mxu_ones_left(ones, data, count):
    return sum(mxu(ones, part, 1, 0) for part in parts_of(data, count))


def mxu_ones_right(data, ones, count):
    return sum(mxu(part, ones, 1, 0) for part in parts_of(data, count))


def iota(shape, axis):
    return lax.broadcasted_iota(jnp.int32, shape, axis)


def ones_where(condition, kind):
    return jnp.where(condition, 1.0, 0.0).astype(kind)


def sigmoid(v):
    return 1.0 / (1.0 + jnp.exp(-v))


exact = lax.Precision.HIGHEST
LOW = jnp.bfloat16
OUT_AT, VALUE_AT = 128, 384


class BlockTerms:
    def __init__(self, start, segc_ref, segr_ref, small_ref, value_ref, bc_ref, step_in, width):
        self.start, self.width = start, width
        self.segc_ref, self.small_ref = segc_ref, small_ref
        rows = pl.ds(8 + start, BLOCK)
        seg = segc_ref[rows, :]
        row, col = iota((BLOCK, BLOCK), 0), iota((BLOCK, BLOCK), 1)
        self.row, self.col = row, col
        same = jnp.logical_and(seg == segr_ref[:, pl.ds(start, BLOCK)], row >= col)
        self.hidden_pairs = jnp.where(same, 0.0, -1e30)
        self.value_arg = self.conv(value_ref, 0, 4, width)
        self.bc_arg = self.conv(bc_ref, 9, 13, bc_ref.shape[1])
        self.value_sig = sigmoid(self.value_arg)
        self.bc_sig = sigmoid(self.bc_arg)
        self.values = (self.value_arg * self.value_sig).astype(LOW)
        bc_low = (self.bc_arg * self.bc_sig).astype(LOW)
        half = bc_ref.shape[1] // 2
        self.b_low, self.c_low = bc_low[:, :half], bc_low[:, half:]
        self.step = jnp.maximum(step_in, 0.0) + jnp.log1p(jnp.exp(-jnp.abs(step_in)))
        rates = small_ref[8:9, :width]
        self.log_decay = mxu_ones_left(ones_where(row >= col, LOW), self.step * rates, 3)
        self.log_rows = jnp.transpose(self.log_decay)
        self.step_rows = jnp.transpose(self.step)
        self.scores = mxu(self.c_low, self.b_low, 1, 1)
        seg = seg[:, :width]
        before = segc_ref[7 + start : 8 + start, :width]
        last = segc_ref[7 + start + BLOCK : 8 + start + BLOCK, :width]
        self.reach = jnp.where(seg == before, jnp.exp(self.log_decay), 0.0)
        self.reach_last = self.reach[BLOCK - 1 : BLOCK, :]
        self.fade = jnp.where(
            seg == last, jnp.exp(self.log_decay[BLOCK - 1 : BLOCK, :] - self.log_decay), 0.0
        )
        self.faded = self.fade * self.step * self.values.astype(jnp.float32)

    def conv(self, ref, taps_at, bias_at, width):
        total = self.small_ref[bias_at : bias_at + 1, :width]
        for distance in range(4):
            tap = self.small_ref[taps_at + 3 - distance : taps_at + 4 - distance, :width]
            total = total + tap * self.back(ref, distance, width)
        return total

    def back(self, ref, distance, width):
        rows = ref[pl.ds(8 + self.start - distance, BLOCK), :]
        if not distance:
            return rows
        here = self.segc_ref[pl.ds(8 + self.start, BLOCK), :width]
        there = self.segc_ref[pl.ds(8 + self.start - distance, BLOCK), :width]
        return jnp.where(here == there, rows, 0.0)

    def ahead(self, ref, distance, width):
        rows = ref[pl.ds(self.start + distance, BLOCK), :]
        if not distance:
            return rows
        here = self.segc_ref[pl.ds(8 + self.start, BLOCK), :width]
        there = self.segc_ref[pl.ds(8 + self.start + distance, BLOCK), :width]
        return jnp.where(here == there, rows, 0.0)

    def decay_pairs(self, head):
        at = head * HEADDIM
        return jnp.exp(
            self.log_decay[:, at : at + 1] - self.log_rows[at : at + 1, :] + self.hidden_pairs
        )

    def head_lanes(self, head):
        lanes = iota((BLOCK, self.width), 1)
        return jnp.logical_and(lanes >= head * HEADDIM, lanes < (head + 1) * HEADDIM)

    def of_head(self, array, head):
        return array * ones_where(self.head_lanes(head), array.dtype)


def lane_shift(width):
    return ones_where(iota((width, 256), 1) == iota((width, 256), 0) + 64, LOW)


def two_parts(array):
    high = array.astype(LOW)
    return high, (array - high.astype(jnp.float32)).astype(LOW)


def forward_body(
    precise,
    plan,
    normed_ref,
    wall_ref,
    bcw_ref,
    small_ref,
    segr_ref,
    segc_ref,
    part_ref,
    squares_ref,
    gate_ref,
    value_ref,
    bc_ref,
    step_ref,
    mixed_ref,
    state_ref,
):
    tokens = normed_ref.shape[0]
    width = gate_ref.shape[1]
    heads = width // HEADDIM
    piece = 0 if precise else part_ref.shape[1]
    value_ref[0:8, :] = jnp.zeros((8, width), jnp.float32)
    bc_ref[0:8, :] = jnp.zeros((8, bc_ref.shape[1]), jnp.float32)
    spread = ones_where(
        iota((256, width), 0) - width == iota((256, width), 1) // HEADDIM, LOW
    )
    shift = lane_shift(width)
    gains, skip = small_ref[5:6, :width], small_ref[6:7, :width]
    state = jnp.zeros(state_ref.shape[1:], jnp.float32)
    for block in range(tokens // BLOCK):
        start = block * BLOCK
        rows = pl.ds(start, BLOCK)
        normed = normed_ref[rows, :]
        gate_pre = mxu(normed, wall_ref[:, 0:256], 1, 0)[:, :width]
        both = mxu(normed, wall_ref[:, VALUE_AT : VALUE_AT + 256], 1, 0)
        value_ref[pl.ds(8 + start, BLOCK), :] = both[:, :width]
        bc_ref[pl.ds(8 + start, BLOCK), :] = mxu(normed, bcw_ref[...], 1, 0)
        step_in = mxu_ones_right(both, spread, 3) + small_ref[7:8, :width]
        gate_ref[rows, :] = gate_pre
        step_ref[rows, :] = step_in
        terms = BlockTerms(start, segc_ref, segr_ref, small_ref, value_ref, bc_ref, step_in, width)
        mixed = skip * terms.values.astype(jnp.float32)
        for head in range(heads):
            at = head * HEADDIM
            weights = terms.scores * terms.decay_pairs(head) * terms.step_rows[at : at + 1, :]
            own_values = terms.of_head(terms.values, head)
            for term in two_parts(weights) if precise else (weights.astype(LOW),):
                mixed += mxu(term, own_values, 1, 0)
            plan(block, head)
        state_ref[block] = state
        if block:
            for term in two_parts(state) if precise else (state.astype(LOW),):
                mixed += terms.reach * mxu(terms.c_low, term, 1, 0)
        state = terms.reach_last * state
        for term in two_parts(terms.faded) if precise else (terms.faded.astype(LOW),):
            state += mxu(terms.b_low, term, 0, 0)
        mixed_ref[rows, :] = mixed
        gated = mixed * gate_pre * sigmoid(gate_pre)
        squares = gated * gated
        for at in range(0, BLOCK, 128):
            row = (start + at) // 128
            squares_ref[row : row + 1, :] = mxu(
                jnp.ones((8, width), jnp.float32), squares[at : at + 128], 1, 1, exact
            )[0:1]
        if precise:
            part_ref[rows, :] = gated
            plan(block, 3)
            continue
        moved = mxu((gated * gains).astype(LOW), shift, 1, 0).astype(LOW)
        part = mxu(moved, wall_ref[:, OUT_AT : OUT_AT + 256], 1, 1).astype(LOW)
        for at in range(0, BLOCK, piece):
            part_ref[(start + at) // piece] = part[at : at + piece]
        plan(block, 3)


def local_params():
    return pltpu.CompilerParams(vmem_limit_bytes=60 << 20)


def forward_shapes(normed, bcw, slots, precise):
    tokens, model_width = normed.shape
    width = INNER // slots
    bc_width = bcw.shape[1]
    f32 = jnp.float32
    if precise:
        first = jax.ShapeDtypeStruct((tokens, width), f32)
    else:
        first = jax.ShapeDtypeStruct((slots, tokens // slots, model_width), LOW)
    return [
        first,
        jax.ShapeDtypeStruct((tokens // 128, 128), f32),
        jax.ShapeDtypeStruct((tokens, width), f32),
        jax.ShapeDtypeStruct((tokens + 8, width), f32),
        jax.ShapeDtypeStruct((tokens + 8, bc_width), f32),
        jax.ShapeDtypeStruct((tokens, width), f32),
        jax.ShapeDtypeStruct((tokens, width), f32),
        jax.ShapeDtypeStruct((tokens // BLOCK, bc_width // 2, width), f32),
    ]


def row_sum(array):
    return jnp.sum(array, axis=0, keepdims=True)


def backward_body(
    plan,
    grad_ref,
    inv_ref,
    inner_ref,
    normed_ref,
    wall_ref,
    small_ref,
    segr_ref,
    segc_ref,
    gate_ref,
    value_ref,
    bc_ref,
    step_ref,
    mixed_ref,
    state_ref,
    both_ref,
    early_ref,
    late_ref,
    sums_ref,
    pre_ref,
    scaled_ref,
    e_ref,
    e_bc_ref,
    grad_mixed_ref,
):
    tokens, model_width = normed_ref.shape
    width = gate_ref.shape[1]
    bc_width = bc_ref.shape[1]
    heads = width // HEADDIM
    piece = both_ref.shape[1]
    blocks = tokens // BLOCK
    f32 = jnp.float32
    shift = lane_shift(width)
    gains, skip, rates = (small_ref[at : at + 1, :width] for at in (5, 6, 8))
    e_ref[tokens:, :] = jnp.zeros((8, width), f32)
    e_bc_ref[tokens:, :] = jnp.zeros((8, bc_width), f32)
    pre_ref[...] = jnp.zeros(pre_ref.shape, LOW)
    inv_columns, inner_columns = spread_rows(inv_ref[...]), spread_rows(inner_ref[...])
    same_head = ones_where(
        iota((width, width), 0) // HEADDIM == iota((width, width), 1) // HEADDIM, LOW
    )
    tail = ones_where(iota((width, 128), 0) == iota((width, 128), 1) + 128, LOW)
    pick = ones_where(
        jnp.logical_and(
            iota((width, 128), 0) == (iota((width, 128), 1) - 64) * HEADDIM, iota((width, 128), 1) >= 64
        ),
        LOW,
    )
    grad_state = jnp.zeros(state_ref.shape[1:], f32)
    sums = {}

    def add(name, term):
        sums[name] = sums[name] + term if name in sums else term

    for block in range(blocks):
        start = block * BLOCK
        rows = pl.ds(start, BLOCK)
        inv, inner = (
            jnp.concatenate([c[:, at : at + 1] for at in range(start // 128, (start + BLOCK) // 128)], axis=0)
            for c in (inv_columns, inner_columns)
        )
        grad_low = grad_ref[rows, 0:model_width]
        grad_scaled = mxu(grad_low, wall_ref[:, OUT_AT : OUT_AT + 256], 1, 0)
        grad_scaled = pltpu.roll(grad_scaled, 192, 1)[:, :width]
        gate_pre, mixed = gate_ref[rows, :], mixed_ref[rows, :]
        sig = sigmoid(gate_pre)
        act = gate_pre * sig
        gated = mixed * act
        normal = gated * inv
        scaled_ref[rows, :] = mxu((normal * gains).astype(LOW), shift, 1, 0).astype(LOW)
        add("out_gain", row_sum(grad_scaled * normal))
        grad_gated = inv * (grad_scaled * gains) - gated * (inv * inv * inner)
        grad_gate = grad_gated * mixed * sig * (1.0 + gate_pre * (1.0 - sig))
        pre_ref[rows, 0:width] = grad_gate.astype(LOW)
        grad_mixed_ref[rows, :] = grad_gated * act
    plan(-1, 0)
    k_rows = early_ref.shape[1]

    def by_slices(pair):
        lanes = pl.ds(pair * 2 * k_rows, 2 * k_rows)
        return lanes, ((2 * pair + at, slice(at * k_rows, (at + 1) * k_rows)) for at in range(2))

    for pair in range(early_ref.shape[0] // 2):
        lanes, slices = by_slices(pair)
        total = mxu(normed_ref[:, lanes], pre_ref[:, 0:256], 0, 0)
        out = mxu(grad_ref[:, lanes], scaled_ref[...], 0, 0)
        for slot, k_slice in slices:
            early_ref[slot, :, 0:OUT_AT] = total[k_slice, 0:OUT_AT].astype(LOW)
            early_ref[slot, :, OUT_AT:256] = (
                total[k_slice, OUT_AT:256] + out[k_slice, 0 : 256 - OUT_AT]
            ).astype(LOW)
            early_ref[slot, :, 256:VALUE_AT] = out[k_slice, 256 - OUT_AT :].astype(LOW)
    plan(-1, 1)
    for turn, block in enumerate(reversed(range(blocks))):
        start = block * BLOCK
        rows = pl.ds(start, BLOCK)
        step_in = step_ref[rows, :]
        terms = BlockTerms(start, segc_ref, segr_ref, small_ref, value_ref, bc_ref, step_in, width)
        grad_mixed = grad_mixed_ref[rows, :]
        grad_mixed_low = grad_mixed.astype(LOW)
        values = terms.values.astype(f32)
        add("skip", row_sum(grad_mixed * values))
        grad_values = skip * grad_mixed
        direct = jnp.zeros((BLOCK, width), f32)
        between = jnp.zeros((BLOCK, width), f32)
        pair_sum = jnp.zeros((BLOCK, BLOCK), f32)
        from_here = ones_where(terms.col >= terms.row, LOW)
        for head in range(heads):
            at = head * HEADDIM
            decay = terms.decay_pairs(head)
            step_row = terms.step_rows[at : at + 1, :]
            grad_head = terms.of_head(grad_mixed_low, head)
            head_ones = ones_where(terms.head_lanes(head), LOW)
            products = mxu(grad_head, terms.values, 1, 1)
            scored = terms.scores * decay
            grad_values += mxu((scored * step_row).astype(LOW), grad_head, 0, 0)
            pair_sum += decay * step_row * products
            unstepped = scored * products
            direct += mxu(unstepped.astype(LOW), head_ones, 0, 0)
            later = mxu(from_here, (unstepped * step_row).astype(LOW), 1, 0)
            later = jnp.where(terms.col < terms.row, later, 0.0)
            between += mxu(later.astype(LOW), head_ones, 1, 0)
            plan(turn, head)
        pair_low = pair_sum.astype(LOW)
        grad_b = mxu(pair_low, terms.c_low, 0, 0)
        grad_c = mxu(pair_low, terms.b_low, 1, 0)
        across = jnp.zeros((BLOCK, width), f32)
        if block < blocks - 1:
            state_low = grad_state.astype(LOW)
            to_state = mxu(terms.b_low, state_low, 1, 0)
            grad_values += terms.fade * terms.step * to_state
            by_step = terms.fade * to_state * values
            direct += mxu_ones_right(by_step, same_head, 2)
            grad_b += mxu(terms.faded.astype(LOW), state_low, 1, 1)
            across += mxu_ones_left(ones_where(terms.col < terms.row, LOW), terms.step * by_step, 2)
        if block:
            entering = state_ref[block]
            entering_low = entering.astype(LOW)
            carried = terms.reach * mxu(terms.c_low, entering_low, 1, 0)
            across += mxu_ones_left(from_here, grad_mixed * carried, 2)
            reached = (terms.reach * grad_mixed).astype(LOW)
            grad_c += mxu(reached, entering_low, 1, 1)
            if block < blocks - 1:
                across += row_sum(grad_state * terms.reach_last * entering)
            grad_state = terms.reach_last * grad_state + mxu(terms.c_low, reached, 0, 0)
        between += mxu_ones_right(across, same_head, 2)
        grad_step = direct + rates * between
        add("rates", row_sum(terms.step * between))
        grad_step_in = grad_step * sigmoid(step_in)
        add("step_bias", row_sum(grad_step_in))
        e = grad_values * (terms.value_sig * (1.0 + terms.value_arg * (1.0 - terms.value_sig)))
        e_ref[rows, :] = e
        e_bc = jnp.concatenate([grad_b, grad_c], axis=1) * (
            terms.bc_sig * (1.0 + terms.bc_arg * (1.0 - terms.bc_sig))
        )
        e_bc_ref[rows, :] = e_bc
        add("value_bias", row_sum(e))
        add("bc_bias", row_sum(e_bc))
        grad_value = jnp.zeros((BLOCK, width), f32)
        grad_bc = jnp.zeros((BLOCK, bc_width), f32)
        for distance in range(4):
            tap = 3 - distance
            add(("value", tap), row_sum(e * terms.back(value_ref, distance, width)))
            add(("bc", tap), row_sum(e_bc * terms.back(bc_ref, distance, bc_width)))
            grad_value += small_ref[tap : tap + 1, :width] * terms.ahead(e_ref, distance, width)
            grad_bc += small_ref[9 + tap : 10 + tap, :] * terms.ahead(e_bc_ref, distance, bc_width)
        value_low = grad_value.astype(LOW)
        pre_ref[rows, VALUE_AT : VALUE_AT + 128] = value_low[:, 0:128]
        pre_ref[rows, VALUE_AT + 128 : VALUE_AT + 256] = (
            mxu(value_low, tail, 1, 0) + mxu(grad_step_in.astype(LOW), pick, 1, 0)
        ).astype(LOW)
        part = mxu(pre_ref[rows, :], wall_ref[...], 1, 1).astype(LOW)
        grad_bc = grad_bc.astype(LOW)
        for at in range(0, BLOCK, piece):
            slot = (start + at) // piece
            both_ref[slot, :, 0:model_width] = part[at : at + piece]
            both_ref[slot, :, model_width:] = grad_bc[at : at + piece]
        plan(turn, 3)

    for pair in range(late_ref.shape[0] // 2):
        lanes, slices = by_slices(pair)
        total = mxu(normed_ref[:, lanes], pre_ref[:, VALUE_AT:], 0, 0)
        for slot, k_slice in slices:
            late_ref[slot] = total[k_slice].astype(LOW)
        plan(blocks, pair)

    sums_ref[...] = jnp.zeros(sums_ref.shape, f32)
    head_sums = mxu_ones_right(
        jnp.concatenate([sums["skip"], jnp.zeros((7, width), f32)], axis=0), same_head, 3
    )
    for tap in range(4):
        sums_ref[tap : tap + 1, 0:width] = sums["value", tap]
        sums_ref[9 + tap : 10 + tap, :] = sums["bc", tap]
    sums_ref[4:5, 0:width] = sums["value_bias"]
    sums_ref[5:6, 0:width] = sums["out_gain"]
    sums_ref[6:7, 0:width] = head_sums[0:1]
    sums_ref[7:8, 0:width] = sums["step_bias"]
    sums_ref[8:9, 0:width] = sums["rates"] * rates
    sums_ref[13:14, :] = sums["bc_bias"]


def backward_shapes(normed, kept, slots):
    tokens, model_width = normed.shape
    width = kept[0].shape[1]
    bc_width = kept[2].shape[1]
    k_slots = slots // 2
    shapes = [
        jax.ShapeDtypeStruct((slots, tokens // slots, model_width + bc_width), LOW),
        jax.ShapeDtypeStruct((k_slots, model_width // k_slots, VALUE_AT), LOW),
        jax.ShapeDtypeStruct((k_slots, model_width // k_slots, PACK - VALUE_AT), LOW),
        jax.ShapeDtypeStruct((16, 256), jnp.float32),
    ]
    work = [
        pltpu.VMEM((tokens, PACK), LOW),
        pltpu.VMEM((tokens, 256), LOW),
        pltpu.VMEM((tokens + 8, width), jnp.float32),
        pltpu.VMEM((tokens + 8, bc_width), jnp.float32),
        pltpu.VMEM((tokens, width), jnp.float32),
    ]
    return shapes, work


def norm_rows(hidden, gain):
    inv = lax.rsqrt(jnp.mean(hidden * hidden, axis=1, keepdims=True) + epsilon)
    return inv, (hidden * inv * gain).astype(jnp.bfloat16)


HALVES = 2


class Links:
    def __init__(self, depth):
        self.depth = depth
        self.x, self.z, self.t = (lax.axis_index(name) for name in ("dp", "ctx", "tp"))
        self.core, self.chip = {"tp": other_core(self.t)}, {"tp": other_chip(self.t)}
        self.far_x = {"dp": 1 - self.x}
        self.left = {"ctx": lax.rem(self.z + depth - 1, depth)}
        self.right = {"ctx": lax.rem(self.z + 1, depth)}
        self.sent = []

    def send(self, source, target, send_sem, recv_sem, peer, when=None):
        copy = remote(source, target, send_sem, recv_sem, peer)
        self.sent.append((copy, when))
        if when is None:
            copy.start()
        else:
            pl.when(when)(copy.start)

    def wait(self, ref, send_sem, recv_sem, when=None):
        copy = remote(ref, ref, send_sem, recv_sem, self.core)
        if when is None:
            copy.wait_recv()
        else:
            pl.when(when)(copy.wait_recv)

    def finish(self):
        for copy, when in self.sent:
            if when is None:
                copy.wait_send()
            else:
                pl.when(when)(copy.wait_send)

    def near_first(self):
        z = self.z
        first = z + 1 - 2 * lax.rem(z, 2)
        third = 3 - 3 * (z // 2)
        return [first, 6 - z - first - third, third]

    def far_first(self):
        z = self.z
        odd = lax.rem(z, 2)
        first = 3 - 3 * (z // 2)
        second = (1 - odd) * (2 + z // 2) + odd * (z // 2)
        return [first, second, 6 - z - first - second]


def everyone(depth):
    z, t = lax.axis_index("ctx"), lax.axis_index("tp")
    return [
        {"ctx": lax.rem(z + hop, depth), "tp": lax.rem(t + turn, 4)}
        for hop in range(depth)
        for turn in range(4)
        if hop or turn
    ]


def half(ref, part):
    rows = ref.shape[0] // HALVES
    return ref.at[pl.ds(part * rows, rows)]


def gather_task(links, pieces, fulls, send_sem, recv_sem):
    z, t = links.z, links.t
    last = links.depth - 1
    own = z * 4 + t

    def pass_on(a, ref, slot, part, to_left, to_right, chip=True):
        target = half(fulls[a].at[slot], part)
        recv = recv_sem.at[a, slot, part]

        def go(way, peer, when=None):
            links.send(ref, target, send_sem.at[a, slot, part, way], recv, peer, when)

        if chip:
            go(0, links.left, to_left)
            go(1, links.right, to_right)
            go(2, links.chip)
        go(3, links.core)

    def arrived(a, slot, part):
        ref = half(fulls[a].at[slot], part)
        links.wait(ref, send_sem.at[a, slot, part, 0], recv_sem.at[a, slot, part])
        return ref

    every = range(len(pieces))
    for part in range(HALVES):
        for a in every:
            pass_on(a, half(pieces[a], part), own, part, z > 0, z < last)
    for a in every:
        fulls[a][own] = pieces[a][...]
    yield
    column = other_chip(t)
    order = links.near_first()
    for place, far in enumerate(order):
        slot = far * 4 + t
        for part in range(HALVES):
            for a in every:
                ref = arrived(a, slot, part)
                to_left = jnp.logical_and(far > z, z > 0)
                to_right = jnp.logical_and(far < z, z < last)
                pass_on(a, ref, slot, part, to_left, to_right)
        slot = (order[place - 1] if place else z) * 4 + column
        for part in range(HALVES):
            for a in every:
                pass_on(a, arrived(a, slot, part), slot, part, None, None, False)
        yield
    for part in range(HALVES):
        for a in every:
            slot = order[-1] * 4 + column
            pass_on(a, arrived(a, slot, part), slot, part, None, None, False)
    yield
    for far in [z] + order:
        for row in (other_core(t), other_chip(other_core(t))):
            for part in range(HALVES):
                for a in every:
                    arrived(a, far * 4 + row, part)


def gather_sems(count, slots):
    return [
        pltpu.SemaphoreType.DMA((count, slots, HALVES, 4)),
        pltpu.SemaphoreType.DMA((count, slots, HALVES)),
    ]


def reduce_task(links, produce, parts, outs, bufs, send_sem, recv_sem):
    z, t = links.z, links.t
    depth = links.depth
    last = depth - 1
    order = links.far_first() + [z]
    every = range(len(parts))

    def rows_of(ref, part):
        rows = ref.shape[0] // HALVES
        return slice(part * rows, (part + 1) * rows)

    def sems(a, at, part):
        return send_sem.at[a, at, part], recv_sem.at[a, at, part]

    def loaded(a, at, part):
        return bufs[a][at, rows_of(bufs[a].at[at], part), :].astype(jnp.float32)

    def mine(a, slot, part):
        return parts[a][slot, rows_of(parts[a].at[slot], part), :].astype(jnp.float32)

    def wait(a, at, part, when=None):
        links.wait(half(bufs[a].at[at], part), *sems(a, at, part), when)

    def stage1(far):
        produce(far)
        for which, row in enumerate((other_chip(other_core(t)), other_core(t))):
            for part in range(HALVES):
                for a in every:
                    at = far * 2 + which
                    links.send(
                        half(parts[a].at[far * 4 + row], part),
                        half(bufs[a].at[at], part),
                        *sems(a, at, part),
                        links.core,
                    )

    def stage2(far):
        for part in range(HALVES):
            for a in every:
                at = far * 2
                wait(a, at, part)
                total = mine(a, far * 4 + other_chip(t), part) + loaded(a, at, part)
                bufs[a][at, rows_of(bufs[a].at[at], part), :] = total.astype(bufs[a].dtype)
                to = 2 * depth + far
                links.send(
                    half(bufs[a].at[at], part), half(bufs[a].at[to], part), *sems(a, to, part), links.chip
                )

    def stage3(far):
        at = far * 2 + 1
        for part in range(HALVES):
            for a in every:
                wait(a, at, part)
                wait(a, 2 * depth + far, part)
                total = mine(a, far * 4 + t, part) + loaded(a, at, part) + loaded(a, 2 * depth + far, part)
                out = outs[a]
                rows = rows_of(out, part)
                if far is z:
                    out[rows, :] = total
                    continue
                ref = bufs[a]
                here = (at, rows_of(ref.at[at], part), slice(None))
                for way, (peer, when, first) in enumerate(
                    ((links.right, far > z, z == 0), (links.left, far < z, z == last))
                ):
                    chain = 3 * depth + way * depth + far

                    def go(total=total, chain=chain, here=here, ref=ref, first=first, a=a, part=part):
                        @pl.when(first)
                        def _():
                            ref[here] = total.astype(ref.dtype)

                        @pl.when(jnp.logical_not(first))
                        def _():
                            wait(a, chain, part)
                            ref[here] = (total + loaded(a, chain, part)).astype(ref.dtype)

                    pl.when(when)(go)
                    links.send(
                        half(ref.at[at], part), half(ref.at[chain], part), *sems(a, chain, part), peer, when
                    )

    count = len(order)
    for place in range(count + 2):
        if place < count:
            stage1(order[place])
        if 1 <= place <= count:
            stage2(order[place - 1])
        if 2 <= place:
            stage3(order[place - 2])
        yield
    for way, when in enumerate((z > 0, z < last)):
        chain = 3 * depth + way * depth + z
        for part in range(HALVES):
            for a in every:

                @pl.when(when)
                def _(a=a, part=part, chain=chain):
                    wait(a, chain, part)
                    outs[a][rows_of(outs[a], part), :] += loaded(a, chain, part)


def reduce_scratch(shapes, dtypes, depth):
    return [pltpu.VMEM((5 * depth,) + s, d) for s, d in zip(shapes, dtypes)] + [
        pltpu.SemaphoreType.DMA((len(shapes), 5 * depth, HALVES)),
        pltpu.SemaphoreType.DMA((len(shapes), 5 * depth, HALVES)),
    ]


def run_tasks(*tasks):
    tasks = list(tasks)
    while tasks:
        for task in list(tasks):
            try:
                next(task)
            except StopIteration:
                tasks.remove(task)


def share_task(links, own, full, send_sem, recv_sem):
    depth = links.depth
    slot = links.z * 4 + links.t
    for at, peer in enumerate(everyone(depth)):
        links.send(own, full.at[slot], send_sem.at[at], recv_sem.at[slot], peer)
    full[slot] = own[...]
    yield
    for hop in range(depth):
        for turn in range(4):
            if hop or turn:
                source = lax.rem(links.z + hop, depth) * 4 + lax.rem(links.t + turn, 4)
                links.wait(full.at[source], send_sem.at[0], recv_sem.at[source])


def spread_rows(rows):
    size = rows.shape[1]
    eye = ones_where(iota((size, size), 0) == iota((size, size), 1), jnp.float32)
    return mxu(eye, rows, 1, 1, exact)


ANY_SPEC = pl.BlockSpec(memory_space=pl.ANY)


class Fetch:
    def __init__(self, sources, targets, sems, names=None):
        self.copies = [
            pltpu.make_async_copy(source, target, sems.at[at])
            for at, (source, target) in enumerate(zip(sources, targets))
        ]
        self.place = {name: at for at, name in enumerate(names or range(len(self.copies)))}
        self.waiting = set(range(len(self.copies)))
        for copy in self.copies:
            copy.start()

    def need(self, *names):
        for name in names:
            at = self.place.get(name)
            if at in self.waiting:
                self.waiting.remove(at)
                self.copies[at].wait()

    def wait(self):
        self.need(*self.place)


def launch(kernel, operands, shapes, scratch, collective_id, name, raw=(), first=()):
    big = [
        at for at, a in enumerate(operands) if at not in raw and a.size * a.dtype.itemsize >= 2**18
    ]
    big = [at for at in first if at in big] + [at for at in big if at not in first]
    count, staged_at = len(operands), -len(big) - 1

    def body(*refs):
        ins, staged = list(refs[:count]), refs[staged_at:-1]
        fetch = Fetch([ins[at] for at in big], staged, refs[-1], big)
        for at, ref in zip(big, staged):
            ins[at] = ref
        kernel(fetch, *ins, *refs[count:staged_at])

    return pl.pallas_call(
        body,
        out_shape=shapes,
        in_specs=[ANY_SPEC if at in raw or at in big else VMEM_SPEC for at in range(count)],
        out_specs=[VMEM_SPEC] * len(shapes),
        scratch_shapes=list(scratch)
        + [pltpu.VMEM(operands[at].shape, operands[at].dtype) for at in big]
        + [pltpu.SemaphoreType.DMA((len(big),))],
        compiler_params=params_of(collective_id),
        name=name,
    )(*operands)


def turn_forward_kernel(
    depth,
    fetch,
    gated_ref,
    squares_ref,
    small_ref,
    wall_ref,
    hidden_ref,
    gain_ref,
    pack_ref,
    early_ref,
    bc_ref,
    hidden_out,
    total_out,
    inv_out,
    full_out,
    full_pack,
    full_bc,
    parts,
    normed,
    shared,
    share_send,
    share_recv,
    bufs,
    reduce_send,
    reduce_recv,
    gather_send,
    gather_recv,
    pack_send,
    pack_recv,
    bc_send,
    bc_recv,
):
    links = Links(depth)
    greet(everyone(depth) + [links.far_x])
    small_ref = small_ref.at[0]
    width = gated_ref.shape[1]
    piece = hidden_ref.shape[1] // 4
    block = 4 * piece
    share = share_task(links, squares_ref, shared, share_send, share_recv)
    next(share, None)
    weights = Weights(links, pack_ref, full_pack, pack_send, pack_recv)
    fetch.wait()
    here = [links.z, weights.order[0], weights.order[1]]
    for far in here:
        full_pack[weights.base + far] = early_ref[weights.base + far]
    other = (1 - links.x) * depth + links.z
    full_pack[other] = early_ref[other]
    run_tasks(share)
    total = shared[0]
    for slot in range(1, 4 * depth):
        total = total + shared[slot]
    inv_rows = lax.rsqrt(total / INNER + epsilon)
    inv_out[...] = inv_rows
    columns = spread_rows(inv_rows)
    shift = lane_shift(width)
    gains = small_ref[5:6, :width]
    which = iota((block, columns.shape[1]), 1)

    def produce(far):
        at = far * (block // 128)
        both = jnp.concatenate([columns] * (block // 128), axis=0)
        low = iota((block, columns.shape[1]), 0) // 128 + at
        inv = jnp.sum(jnp.where(which == low, both, 0.0), axis=1, keepdims=True)
        rows = pl.ds(pl.multiple_of(far * block, block), block)
        scaled = (gated_ref[rows, :] * inv * gains).astype(LOW)
        moved = mxu(scaled, shift, 1, 0).astype(LOW)
        part = mxu(moved, wall_ref[:, OUT_AT : OUT_AT + 256], 1, 1)
        for row in range(4):
            parts[far * 4 + row] = part[row * piece : (row + 1) * piece].astype(parts.dtype)

    def background():
        weights.over(0, False)
        yield
        weights.along(2)
        yield
        weights.over(1, False)
        yield
        yield
        weights.over(2)

    shared_bc = shared_task(links, bc_ref.at[1], full_bc, bc_send, bc_recv)
    run_tasks(
        reduce_task(links, produce, [parts], [total_out], [bufs], reduce_send, reduce_recv),
        background(),
        shared_bc,
    )
    rows = pl.ds(pl.multiple_of(links.t * piece, piece), piece)
    hidden = hidden_ref[0, rows, :].astype(jnp.float32) + total_out[...]
    hidden_out[...] = hidden
    _, normed[...] = norm_rows(hidden, gain_ref[...].astype(jnp.float32)[1:2])
    run_tasks(gather_task(links, [normed], [full_out], gather_send, gather_recv))
    for far in weights.order:
        weights.over_landed(far)
    links.finish()


def turn_forward(gated, squares, small, wall, hidden, gain, pack, early, bc, depth, collective_id):
    piece, model_width = hidden.shape[1] // 4, hidden.shape[2]
    slots = 4 * depth
    f32 = jnp.float32
    return launch(
        partial(turn_forward_kernel, depth),
        (gated, squares, small, wall, hidden, gain, pack, early, bc),
        [
            jax.ShapeDtypeStruct((piece, model_width), f32),
            jax.ShapeDtypeStruct((piece, model_width), f32),
            jax.ShapeDtypeStruct(squares.shape, f32),
            jax.ShapeDtypeStruct((slots, piece, model_width), LOW),
        ]
        + pack_shapes(depth, pack.shape[1], bc.shape[2]),
        [
            pltpu.VMEM((slots, piece, model_width), f32),
            pltpu.VMEM((piece, model_width), LOW),
            pltpu.VMEM((slots,) + squares.shape, f32),
            pltpu.SemaphoreType.DMA((slots,)),
            pltpu.SemaphoreType.DMA((slots,)),
        ]
        + reduce_scratch([(piece, model_width)], [f32], depth)
        + gather_sems(1, slots)
        + weights_sems(depth)
        + shared_sems(depth),
        collective_id,
        "turn_forward",
    )


def partners(links):
    z = links.z
    return [lax.rem(z + 2, 4), z + 1 - 2 * lax.rem(z, 2), 3 - z]


class Weights:
    def __init__(self, links, pack, full, send_sem, recv_sem):
        self.links, self.pack, self.full = links, pack, full
        self.send_sem, self.recv_sem = send_sem, recv_sem
        self.order = partners(links)
        self.base = links.x * links.depth
        self.mine = self.base + links.z

    def send(self, ref, slot, part, kind, peer):
        self.links.send(
            ref,
            half(self.full.at[slot], part),
            self.send_sem.at[kind, part],
            self.recv_sem.at[slot, part],
            peer,
        )

    def arrived(self, slot, part):
        ref = half(self.full.at[slot], part)
        self.links.wait(ref, self.send_sem.at[0, part], self.recv_sem.at[slot, part])
        return ref

    def keep(self):
        self.full[self.mine] = self.pack[self.links.z]

    def own_over(self):
        for part in range(HALVES):
            self.send(half(self.pack.at[self.links.z], part), self.mine, part, 0, self.links.far_x)

    def along(self, place):
        far = self.order[place]
        for part in range(HALVES):
            self.send(half(self.pack.at[far], part), self.mine, part, 1 + place, {"ctx": far})

    def landed(self, place):
        for part in range(HALVES):
            self.arrived(self.base + self.order[place], part)

    def over(self, place, wait=True):
        slot = self.base + self.order[place]
        for part in range(HALVES):
            ref = self.arrived(slot, part) if wait else half(self.full.at[slot], part)
            self.send(ref, slot, part, self.links.depth + place, self.links.far_x)

    def own_over_landed(self):
        self.over_landed(self.links.z)

    def over_landed(self, far):
        slot = (1 - self.links.x) * self.links.depth + far
        for part in range(HALVES):
            self.arrived(slot, part)

    def task(self):
        self.own_over()
        self.keep()
        yield
        self.along(1)
        yield
        self.along(0)
        yield
        self.over(1)
        yield
        self.along(2)
        self.over(0)
        yield
        self.over(2)
        yield
        for far in [self.links.z] + self.order:
            self.over_landed(far)


def weights_sems(depth):
    return [
        pltpu.SemaphoreType.DMA((2 * depth, HALVES)),
        pltpu.SemaphoreType.DMA((2 * depth, HALVES)),
    ]


def shared_task(links, own, full, send_sem, recv_sem):
    x, z, t, depth = links.x, links.z, links.t, links.depth
    quarter = own.at[pl.ds(t * full.shape[2], full.shape[2])]
    mine = x * depth + z

    def send(ref, slot, column, kind, peer):
        links.send(ref, full.at[slot, column], send_sem.at[slot, column, kind], recv_sem.at[slot, column], peer)

    def arrived(slot, column):
        ref = full.at[slot, column]
        links.wait(ref, send_sem.at[slot, column, 0], recv_sem.at[slot, column])
        return ref

    order = partners(links)
    for place, far in enumerate(order):
        send(quarter, mine, t, place, {"ctx": far})
    send(quarter, mine, t, 3, links.far_x)
    full[mine] = own[...].reshape(full.shape[1:])
    yield
    for place in (1, 0, 2):
        slot = x * depth + order[place]
        ref = arrived(slot, t)
        send(ref, slot, t, 3, links.far_x)
        send(ref, slot, t, 4, links.chip)
        send(ref, slot, t, 5, links.core)
    yield
    for far in [z] + order:
        slot = (1 - x) * depth + far
        ref = arrived(slot, t)
        send(ref, slot, t, 4, links.chip)
        send(ref, slot, t, 5, links.core)
    others = [x * depth + far for far in order] + [(1 - x) * depth + far for far in [z] + order]
    yield
    for slot in others:
        send(arrived(slot, other_chip(t)), slot, other_chip(t), 5, links.core)
    yield
    for slot in others:
        for column in (other_core(t), other_chip(other_core(t))):
            arrived(slot, column)


def shared_sems(depth):
    return [
        pltpu.SemaphoreType.DMA((2 * depth, 4, 6)),
        pltpu.SemaphoreType.DMA((2 * depth, 4)),
    ]


def scatter_task(links, grads, out, bufs, send_sem, recv_sem):
    x, z, depth = links.x, links.z, links.depth
    order = partners(links) + [z]

    def rows_of(ref, part):
        rows = ref.shape[0] // HALVES
        return slice(part * rows, (part + 1) * rows)

    def over(place):
        for part in range(HALVES):
            links.send(
                half(grads.at[(1 - x) * depth + order[place]], part),
                half(bufs.at[place], part),
                send_sem.at[place, part],
                recv_sem.at[place, part],
                links.far_x,
            )

    over(0)
    over(1)
    yield
    for place, far in enumerate(order):
        for part in range(HALVES):
            ref = half(bufs.at[place], part)
            links.wait(ref, send_sem.at[place, part], recv_sem.at[place, part])
            rows = rows_of(out.at[0], part)
            total = grads[x * depth + far, rows, :].astype(jnp.float32) + bufs[place, rows, :].astype(
                jnp.float32
            )
            if place < 3:
                bufs[place, rows, :] = total.astype(LOW)
                links.send(
                    ref,
                    half(out.at[z], part),
                    send_sem.at[depth + place, part],
                    recv_sem.at[depth + z, part],
                    {"ctx": far},
                )
            else:
                out[z, rows, :] = total.astype(LOW)
        if place < 2:
            over(place + 2)
        yield
    for far in order[:3]:
        for part in range(HALVES):
            links.wait(half(out.at[far], part), send_sem.at[0, part], recv_sem.at[depth + far, part])


def scatter_scratch(shape, depth, keep=True):
    return [pltpu.VMEM((depth,) + shape, LOW)] * (2 if keep else 1) + [
        pltpu.SemaphoreType.DMA((2 * depth, HALVES)),
        pltpu.SemaphoreType.DMA((2 * depth, HALVES)),
    ]


def side_by_side(parts, width):
    tiles = []
    lane = iota((parts[0].shape[0], 128), 1)
    for first, second in zip(parts[::2], parts[1::2]):
        moved = pltpu.roll(second, 64, 1)
        tiles += [
            first[:, 0:128],
            jnp.where(lane < 64, first[:, 128:256], moved[:, 0:128]),
            moved[:, 128:256],
        ]
    return tiles


def store_tiles(ref, layer, tiles):
    for at, tile in enumerate(tiles):
        ref[layer, :, at * 128 : (at + 1) * 128] = tile


def unpack_early(early, width, layer, gate_out, proj_out):
    gate, proj = [], []
    inside = iota((early.shape[1], 256), 1) < width
    for far in range(early.shape[0]):
        gate.append(jnp.where(inside, early[far, :, 0:256].astype(jnp.float32), 0.0))
        out = pltpu.roll(early[far, :, OUT_AT : OUT_AT + 256].astype(jnp.float32), 192, 1)
        proj.append(jnp.where(inside, out, 0.0))
    store_tiles(gate_out, layer, side_by_side(gate, width))
    store_tiles(proj_out, layer, side_by_side(proj, width))


def bc_products(normed_ref, bc_low, slots_ref):
    rows = slots_ref.shape[1]
    for pair in range(slots_ref.shape[0] // 2):
        total = mxu(normed_ref[:, pair * 2 * rows : (pair + 1) * 2 * rows], bc_low, 0, 0)
        slots_ref[2 * pair] = total[:rows].astype(LOW)
        slots_ref[2 * pair + 1] = total[rows:].astype(LOW)


def bc_task(links, slots_ref, arrived_ref, out_ref, layer, send_sem, recv_sem):
    x, z, depth = links.x, links.z, links.depth
    links.send(slots_ref.at[(1 - x) * depth + z], arrived_ref, send_sem, recv_sem, links.far_x)
    yield
    links.wait(arrived_ref, send_sem, recv_sem)
    out_ref[layer] = slots_ref[x * depth + z].astype(jnp.float32) + arrived_ref[...].astype(jnp.float32)


def rows_task(links, ref, out, send_sem, recv_sem):
    t = links.t
    for way, peer in enumerate((links.chip, links.core)):
        links.send(ref, out.at[t], send_sem.at[way], recv_sem.at[t], peer)
    out[t] = ref[...]
    yield
    column = other_chip(t)
    links.wait(out.at[column], send_sem.at[0], recv_sem.at[column])
    links.send(out.at[column], out.at[column], send_sem.at[2], recv_sem.at[column], links.core)
    yield
    for column in (other_core(t), other_chip(other_core(t))):
        links.wait(out.at[column], send_sem.at[0], recv_sem.at[column])


ROWS_SEMS = [pltpu.SemaphoreType.DMA((3,)), pltpu.SemaphoreType.DMA((4,))]


def sums_task(links, own, arrived_ref, work, by_z, sum_out, send_sem, recv_sem, channel_rows=9):
    z, depth = links.z, links.depth
    links.send(own, arrived_ref.at[0], send_sem.at[0], recv_sem.at[0], links.far_x)
    yield
    links.wait(arrived_ref.at[0], send_sem.at[0], recv_sem.at[0])
    over_dp = own[...] + arrived_ref[0]
    work[0] = over_dp
    links.send(work.at[0], arrived_ref.at[1], send_sem.at[1], recv_sem.at[1], links.core)
    yield
    links.wait(arrived_ref.at[1], send_sem.at[1], recv_sem.at[1])
    work[1] = work[0] + arrived_ref[1]
    links.send(work.at[1], arrived_ref.at[2], send_sem.at[2], recv_sem.at[2], links.chip)
    yield
    links.wait(arrived_ref.at[2], send_sem.at[2], recv_sem.at[2])
    row = iota(own.shape, 0)
    kept = jnp.logical_and(row < 16 * LAYERS, lax.rem(row, 16) < channel_rows)
    work[2] = jnp.where(kept, work[0], work[1] + arrived_ref[2])
    for hop in range(1, depth):
        links.send(
            work.at[2], by_z.at[z], send_sem.at[2 + hop], recv_sem.at[3 + z], {"ctx": lax.rem(z + hop, depth)}
        )
    by_z[z] = work[2]
    yield
    for hop in range(1, depth):
        far = lax.rem(z + hop, depth)
        links.wait(by_z.at[far], send_sem.at[0], recv_sem.at[3 + far])
    whole = by_z[0]
    for far in range(1, depth):
        whole = whole + by_z[far]
    sum_out[...] = whole


def sums_scratch(shape, depth):
    return [
        pltpu.VMEM((3,) + shape, jnp.float32),
        pltpu.VMEM((3,) + shape, jnp.float32),
        pltpu.SemaphoreType.DMA((3 + depth,)),
        pltpu.SemaphoreType.DMA((3 + depth,)),
    ]


def build_pack(pack, layer, gate, value, step, proj):
    depth, rows, _ = pack.shape
    width, heads = gate.shape[1] // depth, step.shape[0] // depth
    blank = jnp.zeros((rows, 128), jnp.float32)
    inside = iota((rows, 256), 1) < width

    def own_lanes(ref, far):
        at = far * width // 128 * 128
        window = ref[:, at : at + 256].astype(jnp.float32)
        if far * width > at:
            window = pltpu.roll(window, 256 - (far * width - at), 1)
        return jnp.where(inside, window, 0.0)

    for far in range(depth):
        gate_lanes, value_lanes = own_lanes(gate, far), own_lanes(value, far)
        pack[far, :, 0:128] = gate_lanes[:, 0:128].astype(LOW)
        out = pltpu.roll(own_lanes(proj, far), 64, 1)
        pack[far, :, OUT_AT:VALUE_AT] = (
            out + jnp.concatenate([gate_lanes[:, 128:256], blank], axis=1)
        ).astype(LOW)
        pack[far, :, VALUE_AT : VALUE_AT + 128] = value_lanes[:, 0:128].astype(LOW)
        head = iota((depth * heads, 128), 0) - far * heads
        chosen = jnp.logical_and(jnp.logical_and(head >= 0, head < heads), iota(head.shape, 1) == head + 64)
        pack[far, :, VALUE_AT + 128 :] = (
            value_lanes[:, 128:256] + mxu(step[:, layer, :], ones_where(chosen, LOW), 0, 0)
        ).astype(LOW)


def raw_layer(refs, layer):
    gate, value, step, proj = refs
    return [gate.at[layer], value.at[layer], step, proj.at[layer]]


def raw_scratch(gate, step):
    shapes = (gate.shape[1:], gate.shape[1:], step.shape, gate.shape[1:])
    return [pltpu.VMEM(shape, LOW) for shape in shapes] + [pltpu.SemaphoreType.DMA((4,))]


def prepare_kernel(
    depth,
    hidden_ref,
    seg_ref,
    gain_ref,
    gate_ref,
    value_ref,
    step_ref,
    proj_ref,
    bc_ref,
    taps_ref,
    tap_bias_ref,
    out_gain_ref,
    skip_ref,
    step_bias_ref,
    decay_ref,
    bc_taps_ref,
    bc_bias_ref,
    full_out,
    pack_out,
    bc_out,
    smalls_out,
    segr_out,
    segc_out,
    normed,
    seg_piece,
    seg_full,
    pack,
    raw_gate,
    raw_value,
    raw_step,
    raw_proj,
    raw_sems,
    gather_send,
    gather_recv,
    pack_send,
    pack_recv,
    bc_send,
    bc_recv,
):
    f32 = jnp.float32
    links = Links(depth)
    raw = (raw_gate, raw_value, raw_step, raw_proj)
    fetch = Fetch(raw_layer((gate_ref, value_ref, step_ref, proj_ref), 0), raw, raw_sems)
    piece, model_width = normed.shape
    rows = pl.ds(pl.multiple_of(links.t * piece, piece), piece)
    _, normed[...] = norm_rows(hidden_ref[0, rows, :].astype(f32), gain_ref[0:1, :].astype(f32))
    tokens = seg_ref.shape[1]
    lane, place = iota((tokens, 128), 0) - links.t * piece, iota((tokens, 128), 1)
    pick = ones_where(jnp.logical_and(lane == place, place < piece), f32)
    seg_piece[...] = mxu(jnp.broadcast_to(seg_ref[...].astype(f32), (8, tokens)), pick, 1, 0, exact)
    greet(everyone(depth) + [links.far_x])
    gather = gather_task(links, [normed, seg_piece], [full_out, seg_full], gather_send, gather_recv)
    next(gather, None)
    shared = shared_task(links, bc_ref.at[0], bc_out, bc_send, bc_recv)
    fetch.wait()
    build_pack(pack, 0, *raw)
    weights = Weights(links, pack, pack_out, pack_send, pack_recv)
    weights.along(0)
    weights.own_over()
    weights.keep()
    next(gather, None)
    weights.along(1)
    next(gather, None)
    weights.over(0)
    weights.along(2)
    next(shared, None)
    next(gather, None)
    weights.over(1)
    width = taps_ref.shape[2] // depth
    lane, place = iota((taps_ref.shape[2], 256), 0) - links.z * width, iota((taps_ref.shape[2], 256), 1)
    own = ones_where(jnp.logical_and(lane == place, place < width), f32)
    heads = skip_ref.shape[1] // depth
    head, place = iota((skip_ref.shape[1], 256), 0) - links.z * heads, iota((skip_ref.shape[1], 256), 1)
    spread = ones_where(jnp.logical_and(head == place // HEADDIM, place < width), f32)
    smalls_out[...] = jnp.zeros(smalls_out.shape, f32)
    for layer in range(LAYERS):
        one = slice(layer, layer + 1)
        smalls_out[layer, 0:4, :] = mxu(taps_ref[layer].astype(f32), own, 1, 0, exact)
        by_channel = jnp.concatenate(
            [tap_bias_ref[...].astype(f32)[one], out_gain_ref[...].astype(f32)[one]] * 4, axis=0
        )
        smalls_out[layer, 4:6, :] = mxu(by_channel, own, 1, 0, exact)[0:2]
        by_head = jnp.concatenate(
            [skip_ref[one, :], step_bias_ref[one, :], -jnp.exp(decay_ref[one, :])] + [skip_ref[one, :]] * 5,
            axis=0,
        )
        smalls_out[layer, 6:9, :] = mxu(by_head, spread, 1, 0, exact)[0:3]
        smalls_out[layer, 9:13, :] = bc_taps_ref[layer].astype(f32)
        smalls_out[layer, 13:14, :] = bc_bias_ref[...].astype(f32)[one]
    next(gather, None)
    next(gather, None)
    per = 128 // piece
    segc_out[...] = jnp.full(segc_out.shape, -1.0, f32)
    for row in range(4 * depth // per):
        lanes = iota((8, 128), 1)
        total = jnp.zeros((8, 128), f32)
        for at in range(per):
            part = seg_full[row * per + at]
            total = jnp.where(lanes // piece == at, pltpu.roll(part, at * piece, 1) if at else part, total)
        segr_out[:, row * 128 : (row + 1) * 128] = total[0:1]
        column = spread_rows(total)[:, 0:1]
        segc_out[8 + row * 128 : 8 + (row + 1) * 128, :] = jnp.broadcast_to(column, (128, 256))
    weights.over(2)
    run_tasks(shared)
    for far in [links.z] + weights.order:
        weights.over_landed(far)
    links.finish()


def pack_shapes(depth, rows, bc_width):
    return [
        jax.ShapeDtypeStruct((2 * depth, rows, PACK), LOW),
        jax.ShapeDtypeStruct((2 * depth, 4, rows // 4, bc_width), LOW),
    ]


def piece_shapes(pieces, depth):
    return [jax.ShapeDtypeStruct((4 * depth,) + p.shape, p.dtype) for p in pieces]


def prepare(hidden, segment, gain, gate, value, step, proj, bc, small, depth, collective_id):
    f32 = jnp.float32
    _, tokens, model_width = hidden.shape
    piece, slots = tokens // 4, 4 * depth
    rows = gate.shape[1]
    shapes = [
        jax.ShapeDtypeStruct((slots, piece, model_width), LOW),
        *pack_shapes(depth, rows, bc.shape[2]),
        jax.ShapeDtypeStruct((LAYERS, 16, 256), f32),
        jax.ShapeDtypeStruct((1, depth * tokens), f32),
        jax.ShapeDtypeStruct((depth * tokens + 16, 256), f32),
    ]
    return pl.pallas_call(
        partial(prepare_kernel, depth),
        out_shape=shapes,
        in_specs=[VMEM_SPEC] * 3 + [ANY_SPEC] * 4 + [VMEM_SPEC] * (1 + len(small)),
        out_specs=[VMEM_SPEC] * len(shapes),
        scratch_shapes=[
            pltpu.VMEM((piece, model_width), LOW),
            pltpu.VMEM((8, 128), f32),
            pltpu.VMEM((slots, 8, 128), f32),
            pltpu.VMEM((depth, rows, PACK), LOW),
        ]
        + raw_scratch(gate, step)
        + gather_sems(2, slots)
        + weights_sems(depth)
        + shared_sems(depth),
        compiler_params=params_of(collective_id),
        name="prepare",
    )(hidden, segment, gain, gate, value, step, proj, bc, *small)


class SumStream:
    def __init__(self, links, parts, out, bufs, send_sem, recv_sem, low=0, high=4):
        self.links, self.parts, self.out, self.bufs = links, parts, out, bufs
        self.send_sem, self.recv_sem = send_sem, recv_sem
        self.receives = jnp.logical_and(links.z >= low, links.z < high)

    def rows(self, part):
        size = self.out.shape[0] // HALVES
        return slice(part * size, (part + 1) * size)

    def sems(self, at, part):
        return self.send_sem.at[at, part], self.recv_sem.at[at, part]

    def wait(self, at, part):
        self.links.wait(half(self.bufs.at[at], part), *self.sems(at, part))

    def loaded(self, at, part):
        return self.bufs[at, self.rows(part), :].astype(jnp.float32)

    def mine(self, slot, part):
        return self.parts[slot, self.rows(part), :].astype(jnp.float32)

    def first(self, far):
        t = self.links.t
        for which, row in enumerate((other_chip(other_core(t)), other_core(t))):
            for part in range(HALVES):
                at = far * 2 + which
                self.links.send(
                    half(self.parts.at[far * 4 + row], part),
                    half(self.bufs.at[at], part),
                    *self.sems(at, part),
                    self.links.core,
                )

    def second(self, far):
        at = far * 2
        for part in range(HALVES):
            self.wait(at, part)
            total = self.mine(far * 4 + other_chip(self.links.t), part) + self.loaded(at, part)
            self.bufs[at, self.rows(part), :] = total.astype(self.bufs.dtype)
            self.links.send(
                half(self.bufs.at[at], part),
                half(self.bufs.at[8 + far], part),
                *self.sems(8 + far, part),
                self.links.chip,
            )

    def third(self, far):
        at = far * 2 + 1
        z = self.links.z
        for part in range(HALVES):
            self.wait(at, part)
            self.wait(8 + far, part)
            total = (
                self.mine(far * 4 + self.links.t, part) + self.loaded(at, part) + self.loaded(8 + far, part)
            )
            rows = self.rows(part)

            @pl.when(z == far)
            def _(total=total, rows=rows):
                self.out[rows, :] = total

            @pl.when(z != far)
            def _(total=total, rows=rows):
                self.bufs[at, rows, :] = total.astype(self.bufs.dtype)

            self.links.send(
                half(self.bufs.at[at], part),
                half(self.bufs.at[12 + z], part),
                self.send_sem.at[12 + far, part],
                self.recv_sem.at[12 + z, part],
                {"ctx": far},
                z != far,
            )

    def end(self):
        @pl.when(self.receives)
        def _():
            for hop in range(1, self.links.depth):
                far = lax.rem(self.links.z + hop, self.links.depth)
                for part in range(HALVES):
                    self.wait(12 + far, part)
                    self.out[self.rows(part), :] += self.loaded(12 + far, part)


def stream_scratch(shape, dtype):
    return [
        pltpu.VMEM((16,) + shape, dtype),
        pltpu.SemaphoreType.DMA((16, HALVES)),
        pltpu.SemaphoreType.DMA((16, HALVES)),
    ]


class Plan:
    def __init__(self, calls):
        self.calls = calls

    def __call__(self, turn, point):
        for call in self.calls.get((turn, point), ()):
            call()


def advance(task):
    def step():
        next(task, None)

    return step


def forward_first_kernel(depth, operands, *refs):
    compute, weights_in, results, (pack, full_pack) = list(refs[:6]), refs[6:10], refs[10:18], refs[18:20]
    compute[3] = compute[3].at[0]
    *raw, raw_sems, pack_send, pack_recv = refs[20:]
    links = Links(depth)
    fetch = Fetch(raw_layer(weights_in, 1), raw, raw_sems)
    greet(everyone(depth) + [links.far_x])
    fetch.wait()
    build_pack(pack, 1, *raw)
    weights = Weights(links, pack, full_pack, pack_send, pack_recv)
    weights.along(0)
    weights.own_over()
    weights.keep()
    plan = Plan({(1, 1): [partial(weights.along, 1)]})
    operands.wait()
    forward_body(True, plan, *compute, *results)
    weights.landed(0)
    weights.landed(1)
    weights.own_over_landed()
    links.finish()


def forward_first(normed, wall, bcw, small, segr, segc, slots, gate, value, step, proj, depth, collective_id):
    rows = gate.shape[1]
    shapes = forward_shapes(normed, bcw, slots, True) + [
        jax.ShapeDtypeStruct((depth, rows, PACK), LOW),
        jax.ShapeDtypeStruct((2 * depth, rows, PACK), LOW),
    ]
    return launch(
        partial(forward_first_kernel, depth),
        (normed, wall, bcw, small, segr, segc, gate, value, step, proj),
        shapes,
        raw_scratch(gate, step) + weights_sems(depth),
        collective_id,
        "forward_first",
        raw=(6, 7, 8, 9),
    )


def forward_second_kernel(depth, operands, *refs):
    compute, cotangent, results, (full, inv_out, inner_out), scratch = (
        [*refs[:3], refs[3].at[1], *refs[4:6]],
        refs[6],
        refs[7:15],
        refs[15:18],
        refs[18:],
    )
    gather_send, gather_recv, own, shared, share_send, share_recv = scratch
    links = Links(depth)
    greet(everyone(depth))
    operands.need(6)
    piece = full.shape[1]
    mine = cotangent.at[0, pl.ds(pl.multiple_of(links.t * piece, piece), piece)]
    gather = gather_task(links, [mine], [full], gather_send, gather_recv)
    next(gather, None)
    go = [advance(gather)]
    operands.wait()
    forward_body(False, Plan({(1, 0): go, (2, 0): go, (3, 0): go}), *compute, *results)
    run_tasks(gather)
    _, wall_ref, _, small_ref = compute[:4]
    squares_ref, gate_ref, mixed_ref = results[1], results[2], results[6]
    width = gate_ref.shape[1]
    rows = squares_ref.shape[0]
    own[0:rows, :] = squares_ref[...]
    gains = small_ref[5:6, :width]
    per = 128 // piece
    for row in range(rows):
        grad = full[per * row : per * (row + 1)].reshape(128, full.shape[2])
        grad_scaled = mxu(grad, wall_ref[:, OUT_AT : OUT_AT + 256], 1, 0)
        grad_scaled = pltpu.roll(grad_scaled, 192, 1)[:, :width]
        at = pl.ds(row * 128, 128)
        gate_pre = gate_ref[at, :]
        terms = grad_scaled * gains * mixed_ref[at, :] * gate_pre * sigmoid(gate_pre)
        own[rows + row : rows + row + 1, :] = mxu(
            jnp.ones((8, width), jnp.float32), terms, 1, 1, exact
        )[0:1]
    run_tasks(share_task(links, own, shared, share_send, share_recv))
    summed = shared[0]
    for slot in range(1, 4 * depth):
        summed = summed + shared[slot]
    inv = lax.rsqrt(summed[0:rows] / INNER + epsilon)
    inv_out[...] = inv
    inner_out[...] = inv * summed[rows:] / INNER
    links.finish()


def forward_second(normed, wall, bcw, small, segr, segc, slots, cotangent, depth, collective_id):
    shapes = forward_shapes(normed, bcw, slots, False)
    rows = shapes[1].shape
    shapes = (
        shapes
        + [jax.ShapeDtypeStruct((4 * depth, cotangent.shape[1] // 4, cotangent.shape[2]), LOW)]
        + [jax.ShapeDtypeStruct(rows, jnp.float32)] * 2
    )
    return launch(
        partial(forward_second_kernel, depth),
        (normed, wall, bcw, small, segr, segc, cotangent),
        shapes,
        gather_sems(1, 4 * depth)
        + [
            pltpu.VMEM((2 * rows[0], 128), jnp.float32),
            pltpu.VMEM((4 * depth, 2 * rows[0], 128), jnp.float32),
            pltpu.SemaphoreType.DMA((4 * depth,)),
            pltpu.SemaphoreType.DMA((4 * depth,)),
        ],
        collective_id,
        "forward_second",
        first=(6,),
    )


def own_column(rows, slot, piece):
    per = 128 // piece
    columns = spread_rows(rows)
    lane = iota(columns.shape, 1)
    column = jnp.sum(jnp.where(lane == slot // per, columns, 0.0), axis=1, keepdims=True)
    at = iota((piece, 128), 0) + lax.rem(slot, per) * piece
    pick = ones_where(at == iota((piece, 128), 1), jnp.float32)
    return mxu(pick, jnp.broadcast_to(column, (128, 128)), 1, 0, exact)[:, 0:1]


def norm_gradient(grad_rows, grad_normed, hidden, gain):
    inv = lax.rsqrt(jnp.mean(hidden * hidden, axis=1, keepdims=True) + epsilon)
    weighted = grad_normed * gain
    grad = (
        grad_rows
        + inv * weighted
        - hidden * (inv * inv * inv) * jnp.mean(weighted * hidden, axis=1, keepdims=True)
    )
    return grad, row_sum(grad_normed * hidden * inv)


def owner_norm(total, grad, hidden_ref, gain_ref, bcw_ref):
    model_width = hidden_ref.shape[1]
    bc_low = total[:, model_width:].astype(LOW)
    grad_normed = total[:, :model_width] + mxu(bc_low, bcw_ref[...], 1, 1)
    grad, gain = norm_gradient(grad, grad_normed, hidden_ref[...].astype(jnp.float32), gain_ref[...])
    return bc_low, grad, gain


def backward_second_kernel(depth, operands, *refs):
    compute, (cotangent, hidden_ref, gain_ref, bcw_ref, before_ref) = list(refs[:14]), refs[14:19]
    compute[5] = compute[5].at[1]
    late, sums, grad_out, gain_out, full_out, inner_out, early_out = refs[19:26]
    both, early, *work = refs[26:33]
    (
        early_bufs, early_send, early_recv,
        back_total, piece_low, scalars, scalars_full, back_bufs, back_send, back_recv,
        gather_send, gather_recv,
    ) = refs[33:]
    links = Links(depth)
    greet(everyone(depth) + [links.far_x])
    piece, model_width = hidden_ref.shape
    scatter = scatter_task(links, early, early_out, early_bufs, early_send, early_recv)
    go = advance(scatter)
    stream = SumStream(links, both, back_total, back_bufs, back_send, back_recv)

    def call(method, far):
        return partial(method, far)

    plan = Plan(
        {
            (-1, 0): [partial(operands.need, 3)],
            (-1, 1): [go, operands.wait],
            (0, 3): [call(stream.first, 3)],
            (1, 0): [call(stream.second, 3)],
            (1, 2): [go],
            (1, 3): [call(stream.first, 2)],
            (2, 0): [call(stream.second, 2), call(stream.third, 3)],
            (2, 2): [go],
            (2, 3): [call(stream.first, 1)],
            (3, 0): [call(stream.second, 1), call(stream.third, 2)],
            (3, 3): [call(stream.first, 0)],
            (4, 0): [call(stream.second, 0), call(stream.third, 1)],
        }
    )
    operands.need(0, 4, 8, 12)
    backward_body(plan, *compute, both, early, late, sums, *work)
    stream.third(0)
    stream.end()
    rows = pl.ds(pl.multiple_of(links.t * piece, piece), piece)
    bc_low, grad, gain_out[...] = owner_norm(
        back_total,
        cotangent[0, rows, :].astype(jnp.float32),
        hidden_ref,
        gain_ref[...].astype(jnp.float32)[1:2],
        bcw_ref,
    )
    grad_low = grad.astype(LOW)
    piece_low[:, :model_width] = grad_low
    piece_low[:, model_width:] = bc_low
    inner = jnp.sum(grad_low.astype(jnp.float32) * before_ref[...], axis=1, keepdims=True) / INNER
    slot, per = links.z * 4 + links.t, 128 // piece
    lane = iota((piece, 128), 0) + lax.rem(slot, per) * piece
    place = ones_where(lane == iota((piece, 128), 1), jnp.float32)
    inner_rows = mxu(jnp.broadcast_to(inner, (piece, 8)), place, 0, 0, exact)
    scalars[...] = jnp.where(iota(inner_rows.shape, 0) == slot // per, inner_rows, 0.0)
    grad_out[...] = grad
    run_tasks(
        gather_task(links, [piece_low, scalars], [full_out, scalars_full], gather_send, gather_recv),
        scatter,
    )
    inner_rows = scalars_full[0]
    for other in range(1, 4 * depth):
        inner_rows = inner_rows + scalars_full[other]
    inner_out[...] = inner_rows
    links.finish()


def backward_second(
    grad, inv, inner, normed, wall, small, segr, segc, kept, slots, cotangent, hidden, gain, bcw, before, depth, collective_id
):
    f32 = jnp.float32
    piece, model_width = hidden.shape
    (both, early, late, sums), work = backward_shapes(normed, kept, slots)
    whole_width = both.shape[2]
    shapes = [
        late,
        sums,
        jax.ShapeDtypeStruct((piece, model_width), f32),
        jax.ShapeDtypeStruct((1, model_width), f32),
        jax.ShapeDtypeStruct(both.shape, LOW),
        jax.ShapeDtypeStruct(inv.shape, f32),
        jax.ShapeDtypeStruct((depth,) + early.shape[1:], LOW),
    ]
    return launch(
        partial(backward_second_kernel, depth),
        (grad, inv, inner, normed, wall, small, segr, segc, *kept, cotangent, hidden, gain, bcw, before),
        shapes,
        [pltpu.VMEM(both.shape, LOW), pltpu.VMEM(early.shape, LOW)]
        + work
        + scatter_scratch(early.shape[1:], depth, False)
        + [
            pltpu.VMEM((piece, whole_width), f32),
            pltpu.VMEM((piece, whole_width), LOW),
            pltpu.VMEM(inv.shape, f32),
            pltpu.VMEM((slots,) + inv.shape, f32),
        ]
        + stream_scratch((piece, whole_width), LOW)
        + gather_sems(2, slots),
        collective_id,
        "backward_second",
        first=(0, 4, 8, 12, 3),
    )


def backward_first_kernel(depth, operands, *refs):
    compute, (late1, normed1, grad_in, hidden_ref, gain_ref, bcw_ref, sums1, gain1, part, hidden1, inv1) = (
        list(refs[:14]),
        refs[14:25],
    )
    compute[5] = compute[5].at[0]
    late1_out, early0_out, late0_out, bc_out, by_z_out, sum_out, hidden_grad_out, hidden_out = refs[25:33]
    both, early, late, sums, *work = refs[33:42]
    (
        out_total, out_low, out_bufs, out_send, out_recv, out_row_send, out_row_recv,
        total, low, bc_piece, bc_full, own,
        bufs, stream_send, stream_recv,
        gather_send, gather_recv,
        late1_bufs, late1_send, late1_recv,
        early0_bufs, early0_send, early0_recv,
        late0_bufs, late0_send, late0_recv,
        bc_slots, bc_arrived, bc_send, bc_recv,
        sums_arrived, sums_work, sums_send, sums_recv,
        row_send, row_recv,
    ) = refs[42:]
    links = Links(depth)
    greet(everyone(depth) + [links.far_x])
    piece, model_width = grad_in.shape
    normed_ref, grad_ref = compute[3], compute[0]
    output = SumStream(links, part, out_total, out_bufs, out_send, out_recv)
    stream = SumStream(links, both, total, bufs, stream_send, stream_recv)
    late_task1 = scatter_task(links, late1, late1_out, late1_bufs, late1_send, late1_recv)
    early_task0 = scatter_task(links, early, early0_out, early0_bufs, early0_send, early0_recv)
    late_task0 = scatter_task(links, late, late0_out, late0_bufs, late0_send, late0_recv)
    bc1 = bc_task(links, bc_slots.at[1], bc_arrived.at[1], bc_out, 1, bc_send.at[1], bc_recv.at[1])
    operands.need(14)
    next(late_task1, None)

    def call(method, far):
        return partial(method, far)

    def output_rows():
        for far in (3, 2, 1, 0):
            output.third(far)
            yield
        output.end()
        inv = own_column(inv1[...], links.z * 4 + links.t, piece)
        out_low[...] = (hidden1[...] + out_total[...] * inv).astype(LOW)
        yield from rows_task(links, out_low, hidden_out, out_row_send, out_row_recv)

    def output_first():
        operands.need(22)
        for far in (3, 2, 1, 0):
            output.first(far)

    def bc_first():
        bc_products(normed1, grad_ref[:, model_width:], bc_slots.at[1])
        next(bc1, None)

    go1, go0 = advance(late_task1), advance(early_task0)
    plan = Plan(
        {
            (-1, 0): [partial(operands.need, 3), go1],
            (-1, 1): [operands.wait, go0],
            (0, 1): [go1],
            (0, 3): [call(stream.first, 3), go0],
            (1, 0): [call(stream.second, 3)],
            (1, 2): [go1],
            (1, 3): [call(stream.first, 2), go0],
            (2, 0): [call(stream.second, 2), call(stream.third, 3)],
            (2, 2): [go1],
            (2, 3): [call(stream.first, 1), go0],
            (3, 0): [call(stream.second, 1), call(stream.third, 2)],
            (3, 3): [call(stream.first, 0), go0],
            (4, 0): [call(stream.second, 0), call(stream.third, 1)],
            (4, 2): [output_first],
        }
    )
    operands.need(0, 4, 8, 12)
    backward_body(plan, *compute, both, early, late, sums, *work)
    next(late_task0, None)
    stream.third(0)
    for far in (3, 2, 1, 0):
        output.second(far)
    bc_first()
    next(late_task0, None)
    stream.end()
    rows = pl.ds(pl.multiple_of(links.t * piece, piece), piece)
    bc_low, grad, gain = owner_norm(
        total, grad_in[...], hidden_ref.at[0, rows], gain_ref[...].astype(jnp.float32)[0:1], bcw_ref
    )
    bc_piece[...] = bc_low
    low[...] = grad.astype(LOW)
    own[...] = jnp.zeros(own.shape, jnp.float32)
    own[0:16, :] = sums[...]
    own[16:32, :] = sums1[...]
    count = model_width // 256
    for layer, row in enumerate((gain, gain1[...])):
        for at in range(count):
            to = 16 * LAYERS + layer * count + at
            own[to : to + 1, :] = row[:, at * 256 : (at + 1) * 256]
    run_tasks(
        gather_task(links, [bc_piece], [bc_full], gather_send, gather_recv),
        sums_task(links, own, sums_arrived, sums_work, by_z_out, sum_out, sums_send, sums_recv),
        rows_task(links, low, hidden_grad_out, row_send, row_recv),
        late_task0,
        output_rows(),
        early_task0,
        late_task1,
        bc1,
    )
    tokens = bc_full.shape[0] * bc_full.shape[1]
    bc_products(normed_ref, bc_full[...].reshape(tokens, bc_full.shape[2]), bc_slots.at[0])
    bc0 = bc_task(links, bc_slots.at[0], bc_arrived.at[0], bc_out, 0, bc_send.at[0], bc_recv.at[0])
    run_tasks(bc0)
    links.finish()


def backward_first(
    grad, inv, inner, normed, wall, small, segr, segc, kept, slots, late1, normed1, grad_in, hidden, gain, bcw, sums1, gain1, part, hidden1, inv1, depth, collective_id
):
    f32 = jnp.float32
    piece, model_width = grad_in.shape
    (both, early, late, sums), work = backward_shapes(normed, kept, slots)
    whole_width = both.shape[2]
    k_slots, k_rows, _ = late1.shape
    bc_width = kept[2].shape[1]
    small_sums = (16 * LAYERS + 16, 256)
    shapes = [
        jax.ShapeDtypeStruct((depth,) + late.shape[1:], LOW),
        jax.ShapeDtypeStruct((depth,) + early.shape[1:], LOW),
        jax.ShapeDtypeStruct((depth,) + late.shape[1:], LOW),
        jax.ShapeDtypeStruct((LAYERS, k_rows, bc_width), f32),
        jax.ShapeDtypeStruct((depth,) + small_sums, f32),
        jax.ShapeDtypeStruct(small_sums, f32),
        jax.ShapeDtypeStruct((4, piece, model_width), LOW),
        jax.ShapeDtypeStruct((4, piece, model_width), LOW),
    ]
    return launch(
        partial(backward_first_kernel, depth),
        (grad, inv, inner, normed, wall, small, segr, segc, *kept, late1, normed1, grad_in, hidden, gain, bcw, sums1, gain1, part, hidden1, inv1),
        shapes,
        [pltpu.VMEM(a.shape, a.dtype) for a in (both, early, late, sums)]
        + work
        + [pltpu.VMEM((piece, model_width), f32), pltpu.VMEM((piece, model_width), LOW)]
        + stream_scratch((piece, model_width), LOW)
        + ROWS_SEMS
        + [
            pltpu.VMEM((piece, whole_width), f32),
            pltpu.VMEM((piece, model_width), LOW),
            pltpu.VMEM((piece, bc_width), LOW),
            pltpu.VMEM((slots, piece, bc_width), LOW),
            pltpu.VMEM(small_sums, f32),
        ]
        + stream_scratch((piece, whole_width), LOW)
        + gather_sems(1, slots)
        + scatter_scratch(late.shape[1:], depth, False)
        + scatter_scratch(early.shape[1:], depth, False)
        + scatter_scratch(late.shape[1:], depth, False)
        + [
            pltpu.VMEM((LAYERS, k_slots, k_rows, bc_width), LOW),
            pltpu.VMEM((LAYERS, k_rows, bc_width), LOW),
            pltpu.SemaphoreType.DMA((LAYERS,)),
            pltpu.SemaphoreType.DMA((LAYERS,)),
        ]
        + sums_scratch(small_sums, depth)
        + ROWS_SEMS,
        collective_id,
        "backward_first",
        first=(0, 14, 4, 8, 12, 3, 22),
    )


def emit_kernel(
    hidden_ref, grad_ref, early0, late0, early1, late1, bc_ref, by_z, whole,
    hidden_out, grad_out, gain_out, gate_out, value_out, bc_out, step_out,
    taps_out, tap_bias_out, bc_taps_out, bc_bias_out, decay_out, step_bias_out, skip_out, out_gain_out, proj_out,
):
    piece = hidden_ref.shape[1]
    depth, _, _ = by_z.shape
    channels, heads_whole = taps_out.shape[2], skip_out.shape[1]
    width, heads = channels // depth, heads_whole // depth
    for at in range(4):
        hidden_out[0, at * piece : (at + 1) * piece, :] = hidden_ref[at]
        grad_out[0, at * piece : (at + 1) * piece, :] = grad_ref[at]
    bc_out[...] = bc_ref[...]
    count = gain_out.shape[1] // 256
    for layer, (early, late) in enumerate(((early0, late0), (early1, late1))):
        one = slice(layer, layer + 1)
        unpack_early(early, width, layer, gate_out, proj_out)
        step = by_head = 0.0
        values, channel_rows = [], []
        inside = iota((late.shape[1], 256), 1) < width
        rows = slice(16 * layer, 16 * layer + 16)
        for far in range(depth):
            values.append(jnp.where(inside, late[far].astype(jnp.float32), 0.0))
            channel_rows.append(jnp.where(inside[0:16], by_z[far, rows, :], 0.0))
            window, head = iota((256, 16), 0), iota((256, 16), 1) - far * heads
            mine = jnp.logical_and(head >= 0, head < heads)
            step += mxu(ones_where(jnp.logical_and(mine, window == width + head), LOW), late[far], 0, 1)
            window, head = iota((256, 128), 0), iota((256, 128), 1) - far * heads
            mine = jnp.logical_and(head >= 0, head < heads)
            by_head += mxu(
                by_z[far, rows, :],
                ones_where(jnp.logical_and(mine, window == head * HEADDIM), jnp.float32),
                1,
                0,
                exact,
            )
        store_tiles(value_out, layer, side_by_side(values, width))
        by_channel = jnp.concatenate(side_by_side(channel_rows, width), axis=1)
        for head in range(heads_whole):
            step_out[head, one, :] = step[head : head + 1]
        taps_out[layer] = by_channel[0:4]
        tap_bias_out[one, :] = by_channel[4:5]
        out_gain_out[one, :] = by_channel[5:6]
        skip_out[one, :] = by_head[6:7, :heads_whole]
        step_bias_out[one, :] = by_head[7:8, :heads_whole]
        decay_out[one, :] = by_head[8:9, :heads_whole]
        bc_taps_out[layer] = whole[16 * layer + 9 : 16 * layer + 13, :]
        bc_bias_out[one, :] = whole[16 * layer + 13 : 16 * layer + 14, :]
        for at in range(count):
            row = 16 * LAYERS + layer * count + at
            gain_out[one, at * 256 : (at + 1) * 256] = whole[row : row + 1, :]


def emit(hidden, grad, early0, late0, early1, late1, bc, by_z, whole, tokens, heads, channels):
    f32 = jnp.float32
    rows, model_width = early0.shape[1], hidden.shape[2]
    bc_width = bc.shape[2]
    shapes = [
        ((1, tokens, model_width), LOW),
        ((1, tokens, model_width), LOW),
        ((LAYERS, model_width), f32),
        ((LAYERS, rows, channels), f32),
        ((LAYERS, rows, channels), f32),
        ((LAYERS, rows, bc_width), f32),
        ((heads, LAYERS, rows), f32),
        ((LAYERS, 4, channels), f32),
        ((LAYERS, channels), f32),
        ((LAYERS, 4, bc_width), f32),
        ((LAYERS, bc_width), f32),
        ((LAYERS, heads), f32),
        ((LAYERS, heads), f32),
        ((LAYERS, heads), f32),
        ((LAYERS, channels), f32),
        ((LAYERS, rows, channels), f32),
    ]
    return pl.pallas_call(
        emit_kernel,
        out_shape=[jax.ShapeDtypeStruct(*shape) for shape in shapes],
        in_specs=[VMEM_SPEC] * 9,
        out_specs=[VMEM_SPEC] * len(shapes),
        compiler_params=local_params(),
        name="emit",
    )(hidden, grad, early0, late0, early1, late1, bc, by_z, whole)


def split_local(
    depth,
    hidden_in,
    segment_ids,
    cotangent,
    norm_gain,
    gate_proj,
    value_proj,
    bc_proj,
    step_proj,
    conv_value,
    conv_value_bias,
    conv_bc,
    conv_bc_bias,
    decay_log,
    step_bias,
    skip_gain,
    out_gain,
    out_proj,
):
    tokens, model_width = hidden_in.shape[1:]
    slots = depth * 4
    heads, channels = step_proj.shape[2], gate_proj.shape[2]
    projections = (gate_proj, value_proj, step_proj.transpose(2, 0, 1), out_proj.transpose(0, 2, 1))
    small = (
        conv_value,
        conv_value_bias,
        out_gain,
        skip_gain,
        step_bias,
        decay_log,
        conv_bc,
        conv_bc_bias,
    )
    normed0, pack0, shared0, smalls, segr, segc = prepare(
        hidden_in, segment_ids, norm_gain, *projections, bc_proj, small, depth, 1
    )
    seg = (segr, segc)
    normed0 = normed0.reshape(-1, model_width)
    wall0, bc_wall0 = pack0.reshape(-1, PACK), shared0.reshape(model_width, -1)
    gated0, squares0, *kept0, packs1, early = forward_first(
        normed0, wall0, bc_wall0, smalls, *seg, slots, *projections, depth, 2
    )
    hidden1, total0, inv_rows0, normed1, pack1, shared1 = turn_forward(
        gated0, squares0, smalls, wall0, hidden_in, norm_gain, packs1, early, bc_proj, depth, 3
    )
    wall1, bc_wall1 = pack1.reshape(-1, PACK), shared1.reshape(model_width, -1)
    normed1 = normed1.reshape(-1, model_width)
    part1, _, *kept1, cotangent_full, inv_rows1, inner_rows1 = forward_second(
        normed1, wall1, bc_wall1, smalls, *seg, slots, cotangent, depth, 4
    )
    late1, sums1, grad1, gain1, full0, inner_rows0, early1 = backward_second(
        cotangent_full.reshape(-1, model_width),
        inv_rows1,
        inner_rows1,
        normed1,
        wall1,
        smalls,
        *seg,
        kept1,
        slots,
        cotangent,
        hidden1,
        norm_gain,
        bc_wall1,
        total0,
        depth,
        5,
    )
    late1, early0, late0, bc_grad, by_z, whole, grad_hidden, hidden_out = backward_first(
        full0.reshape(-1, full0.shape[2]),
        inv_rows0,
        inner_rows0,
        normed0,
        wall0,
        smalls,
        *seg,
        kept0,
        slots,
        late1,
        normed1,
        grad1,
        hidden_in,
        norm_gain,
        bc_wall0,
        sums1,
        gain1,
        part1,
        hidden1,
        inv_rows1,
        depth,
        6,
    )
    outs = emit(
        hidden_out, grad_hidden, early0, late0, early1, late1, bc_grad, by_z, whole, tokens, heads, channels
    )
    return (*outs[:6], outs[6].transpose(1, 2, 0), *outs[7:15], outs[15].transpose(0, 2, 1))


def solution(mesh):
    in_specs = (
        P("dp", "ctx", None),
        P("dp", "ctx"),
        P("dp", "ctx", None),
        P(),
        P(None, ("dp", "ctx"), "tp"),
        P(None, ("dp", "ctx"), "tp"),
        P(None, ("dp", "ctx"), None),
        P(None, ("dp", "ctx"), "tp"),
        P(None, None, "tp"),
        P(None, "tp"),
        P(),
        P(),
        P(None, "tp"),
        P(None, "tp"),
        P(None, "tp"),
        P(None, "tp"),
        P(None, "tp", ("dp", "ctx")),
    )
    out_specs = (
        P("dp", "ctx", None),
        P("dp", "ctx", None),
        P(),
        P(None, ("dp", "ctx"), "tp"),
        P(None, ("dp", "ctx"), "tp"),
        P(None, ("dp", "ctx"), None),
        P(None, ("dp", "ctx"), "tp"),
        P(None, None, "tp"),
        P(None, "tp"),
        P(),
        P(),
        P(None, "tp"),
        P(None, "tp"),
        P(None, "tp"),
        P(None, "tp"),
        P(None, "tp", ("dp", "ctx")),
    )
    depth = mesh.shape["ctx"]
    heads = 48 // mesh.shape["tp"]
    fits = mesh.shape["tp"] == 4 and mesh.shape["dp"] == 2 and depth == 4 and heads % depth == 0
    body = partial(split_local, depth) if fits else local
    return jax.shard_map(body, mesh=mesh, in_specs=in_specs, out_specs=out_specs, check_vma=False)
```

```python
from functools import partial

import jax
import jax.numpy as jnp
from jax import lax
from jax.experimental import pallas as pl
from jax.experimental.pallas import tpu as pltpu
from jax.sharding import PartitionSpec as P

HEADDIM = 64
BLOCK = 256
LAYERS = 2
INNER = 3072


epsilon = 1e-05
precise = lax.Precision.HIGH


def from_behind(block, axis, distance):
    devices = range(lax.axis_size(axis))
    route = [(i - distance, i) for i in devices if i - distance in devices]
    return lax.ppermute(block, axis, route)


def round_keep(values):
    return lax.optimization_barrier(values.astype(jnp.bfloat16)).astype(jnp.float32)


def dot_back(left_rows, right_rows):
    return lax.dot_general(
        left_rows, right_rows, (((1,), (1,)), ((), ())), preferred_element_type=jnp.float32
    )


def dot_left(left_rows, right_rows):
    return lax.dot_general(
        left_rows, right_rows, (((0,), (0,)), ((), ())), preferred_element_type=jnp.float32
    )


def conv_local(signal, edge_rows, kernel, conv_bias, segment, edge_segment):
    tap_count = kernel.shape[0]
    length = signal.shape[1]
    padded = jnp.concatenate([edge_rows, signal], axis=1)
    seg_pad = jnp.concatenate([edge_segment, segment], axis=1)
    result = conv_bias + jnp.zeros_like(signal)
    for tap_index in range(tap_count):
        same_doc = (seg_pad[:, tap_index : tap_index + length] == segment).astype(jnp.float32)
        result = (
            result
            + kernel[tap_index] * padded[:, tap_index : tap_index + length] * same_doc[:, :, None]
        )
    return jax.nn.silu(result)


def block_step(decay_rates, carried, block_data):
    states, prev_segment = carried
    values, b_mat, c_mat, step_size, segment = block_data
    length = values.shape[0]
    log_decay = jnp.cumsum(step_size * decay_rates, axis=0)
    positions = jnp.arange(length)
    causal = positions[:, None] >= positions[None, :]
    same_doc = jnp.logical_and(segment[:, None] == segment[None, :], causal)[:, :, None]
    differ = jnp.where(same_doc, log_decay[:, None, :] - log_decay[None, :, :], 0.0)
    weights = jnp.where(same_doc, jnp.exp(differ), 0.0)
    cb_product = jnp.dot(c_mat, b_mat.T, precision=precise)
    scores = cb_product[:, :, None] * weights * step_size[None, :, :]
    intra_out = jnp.einsum("tsh,shp->thp", scores, values, precision=precise)
    alive_mask = (segment == prev_segment).astype(jnp.float32)
    reach = alive_mask[:, None] * jnp.exp(log_decay)
    inter_out = reach[:, :, None] * jnp.einsum("tn,hpn->thp", c_mat, states, precision=precise)
    end_same = (segment == segment[length - 1]).astype(jnp.float32)
    to_end = jnp.exp(log_decay[length - 1][None, :] - log_decay) * end_same[:, None] * step_size
    weighted_values = to_end[:, :, None] * values
    new_states = reach[length - 1][:, None, None] * states + jnp.einsum(
        "shp,sn->hpn", weighted_values, b_mat, precision=precise
    )
    return ((new_states, segment[length - 1]), intra_out + inter_out)


def device_scan(values, b_mat, c_mat, step_size, decay_rates, segment, seg_prev):
    block_count = values.shape[0] // BLOCK
    heads_local = values.shape[1]
    state_dim = b_mat.shape[1]
    blocks = (
        values.reshape(block_count, BLOCK, heads_local, HEADDIM),
        b_mat.reshape(block_count, BLOCK, state_dim),
        c_mat.reshape(block_count, BLOCK, state_dim),
        step_size.reshape(block_count, BLOCK, heads_local),
        segment.reshape(block_count, BLOCK),
    )
    initial = (jnp.zeros((heads_local, HEADDIM, state_dim), jnp.float32), seg_prev)
    final_carry, outputs = lax.scan(partial(block_step, decay_rates), initial, blocks)
    return (outputs.reshape(values.shape), final_carry[0])


def step_terms(step_pre, step_bias, decay_log):
    return (jax.nn.softplus(step_pre + step_bias), -jnp.exp(decay_log))


def mixer_terms(values, bc_conv, step_size, decay_rates, skip_gain, segment, seg_prev):
    seq_count, tokens, inner_local = values.shape
    heads_local = step_size.shape[2]
    heads_in = values.reshape(seq_count, tokens, heads_local, HEADDIM)
    state_dim = bc_conv.shape[2] // 2
    scanner = jax.vmap(device_scan, in_axes=(0, 0, 0, 0, None, 0, 0))
    intra_out, local_states = scanner(
        heads_in,
        bc_conv[:, :, :state_dim],
        bc_conv[:, :, state_dim:],
        step_size,
        decay_rates,
        segment,
        seg_prev,
    )
    alive_last = (segment[:, tokens - 1] == seg_prev).astype(jnp.float32)
    decays = alive_last[:, None] * jnp.exp(jnp.sum(step_size * decay_rates, axis=1))
    return (intra_out + skip_gain[:, None] * heads_in, local_states, decays)


def carried_terms(bc_conv, step_size, decay_rates, entering, segment, seg_prev):
    state_dim = bc_conv.shape[2] // 2
    c_mat = bc_conv[:, :, state_dim:]
    log_decay = jnp.cumsum(step_size * decay_rates, axis=1)
    alive_mask = (segment == seg_prev[:, None]).astype(jnp.float32)
    reach = alive_mask[:, :, None] * jnp.exp(log_decay)
    carried = jnp.einsum("sqn,shpn->sqhp", c_mat, entering, precision=precise)
    return reach[:, :, :, None] * carried


def chain_forward(decays, local_states):

    def handoff(step_index, entering):
        return from_behind(decays[:, :, None, None] * entering + local_states, "ctx", 1)

    return lax.fori_loop(0, lax.axis_size("ctx") - 1, handoff, jnp.zeros_like(local_states))


def chain_backward(decays, grad_entering):

    def handback(step_index, beyond):
        return from_behind(
            (grad_entering + decays[:, :, None, None] * beyond).astype(jnp.bfloat16), "ctx", -1
        ).astype(jnp.float32)

    return lax.fori_loop(0, lax.axis_size("ctx") - 1, handback, jnp.zeros_like(grad_entering))


def layer_forward(hidden, segment, layer_params):
    (
        norm_gain,
        gate_proj,
        value_proj,
        bc_proj,
        step_proj,
        conv_value,
        conv_value_bias,
        conv_bc,
        conv_bc_bias,
        decay_log,
        step_bias,
        skip_gain,
        out_gain,
        out_proj,
    ) = layer_params
    seq_count, tokens, model_width = hidden.shape
    row_count = seq_count * tokens
    tap_count = conv_value.shape[0]
    gathered = (
        lax.all_gather(gate_proj, ("dp", "ctx"), axis=0, tiled=True),
        lax.all_gather(value_proj, ("dp", "ctx"), axis=0, tiled=True),
        lax.all_gather(bc_proj, ("dp", "ctx"), axis=0, tiled=True),
        lax.all_gather(step_proj, ("dp", "ctx"), axis=0, tiled=True),
        lax.all_gather(out_proj, ("dp", "ctx"), axis=1, tiled=True),
    )
    gate_full, value_full, bc_full, step_full, out_full = gathered
    hidden_rows = hidden.reshape(row_count, model_width)
    inv_norm = lax.rsqrt(jnp.mean(hidden_rows * hidden_rows, axis=1, keepdims=True) + epsilon)
    normed = (hidden_rows * inv_norm * norm_gain).astype(jnp.bfloat16)
    gate_pre = jnp.dot(normed, gate_full, preferred_element_type=jnp.float32)
    value_pre = jnp.dot(normed, value_full, preferred_element_type=jnp.float32).reshape(
        seq_count, tokens, -1
    )
    bc_pre = jnp.dot(normed, bc_full, preferred_element_type=jnp.float32).reshape(
        seq_count, tokens, -1
    )
    step_pre = jnp.dot(normed, step_full, preferred_element_type=jnp.float32).reshape(
        seq_count, tokens, -1
    )
    first_edge = tokens - tap_count + 1
    edge_value, edge_bc, edge_segment = from_behind(
        (value_pre[:, first_edge:], bc_pre[:, first_edge:], segment[:, first_edge:]), "ctx", 1
    )
    conv_fn = partial(conv_local, segment=segment, edge_segment=edge_segment)
    value_act, value_pull = jax.vjp(conv_fn, value_pre, edge_value, conv_value, conv_value_bias)
    bc_act, bc_pull = jax.vjp(conv_fn, bc_pre, edge_bc, conv_bc, conv_bc_bias)
    values = round_keep(value_act)
    bc_conv = round_keep(bc_act)
    seg_prev = edge_segment[:, tap_count - 2]
    (step_size, decay_rates), step_pull = jax.vjp(step_terms, step_pre, step_bias, decay_log)
    (local_out, local_states, decays), local_pull = jax.vjp(
        partial(mixer_terms, segment=segment, seg_prev=seg_prev),
        values,
        bc_conv,
        step_size,
        decay_rates,
        skip_gain,
    )
    entering = chain_forward(decays, local_states)
    carried_out, carried_pull = jax.vjp(
        partial(carried_terms, segment=segment, seg_prev=seg_prev),
        bc_conv,
        step_size,
        decay_rates,
        entering,
    )
    mixed = (local_out + carried_out).reshape(row_count, -1)
    gate_act = jax.nn.silu(gate_pre)
    gated = mixed * gate_act
    square_sum = lax.psum(jnp.sum(gated * gated, axis=1), "tp")
    inv_gate = lax.rsqrt(square_sum / INNER + epsilon)[:, None]
    scaled = (gated * inv_gate * out_gain).astype(jnp.bfloat16)
    mixer_sum = lax.psum(jnp.dot(scaled, out_full, preferred_element_type=jnp.float32), "tp")
    kept = {
        "scaled": scaled,
        "gated": gated,
        "inv_gate": inv_gate,
        "gate_pre": gate_pre,
        "gate_act": gate_act,
        "mixed": mixed,
        "carried_pull": carried_pull,
        "local_pull": local_pull,
        "step_pull": step_pull,
        "value_pull": value_pull,
        "bc_pull": bc_pull,
        "decays": decays,
        "entering": entering,
        "hidden_rows": hidden_rows,
        "inv_norm": inv_norm,
        "normed": normed,
    }
    return (hidden + mixer_sum.reshape(seq_count, tokens, model_width), kept)


def layer_backward(grad_hidden, kept, layer_params):
    (
        norm_gain,
        gate_proj,
        value_proj,
        bc_proj,
        step_proj,
        conv_value,
        conv_value_bias,
        conv_bc,
        conv_bc_bias,
        decay_log,
        step_bias,
        skip_gain,
        out_gain,
        out_proj,
    ) = layer_params
    seq_count, tokens, model_width = grad_hidden.shape
    row_count = seq_count * tokens
    tap_count = conv_value.shape[0]
    gate_full, value_full, bc_full, step_full, out_full = (
        lax.all_gather(gate_proj, ("dp", "ctx"), axis=0, tiled=True),
        lax.all_gather(value_proj, ("dp", "ctx"), axis=0, tiled=True),
        lax.all_gather(bc_proj, ("dp", "ctx"), axis=0, tiled=True),
        lax.all_gather(step_proj, ("dp", "ctx"), axis=0, tiled=True),
        lax.all_gather(out_proj, ("dp", "ctx"), axis=1, tiled=True),
    )
    grad_rows = grad_hidden.reshape(row_count, model_width)
    grad_low = grad_rows.astype(jnp.bfloat16)
    grad_scaled = dot_back(grad_low, out_full)
    grad_out_proj = dot_left(kept["scaled"], grad_low)
    gated = kept["gated"]
    inv_gate = kept["inv_gate"]
    weighted = grad_scaled * out_gain
    inner_sum = lax.psum(jnp.sum(weighted * gated, axis=1), "tp")
    grad_gated = inv_gate * weighted - gated * inv_gate**3 * (inner_sum / INNER)[:, None]
    grad_out_gain = jnp.sum(grad_scaled * gated * inv_gate, axis=0)
    gate_pre = kept["gate_pre"]
    sigmoid_gate = jax.nn.sigmoid(gate_pre)
    grad_gate_pre = (
        grad_gated * kept["mixed"] * sigmoid_gate * (1.0 + gate_pre * (1.0 - sigmoid_gate))
    )
    grad_heads = (grad_gated * kept["gate_act"]).reshape(
        seq_count, tokens, step_full.shape[1], HEADDIM
    )
    carried_bc, carried_step, carried_rates, grad_entering = kept["carried_pull"](grad_heads)
    beyond = chain_backward(kept["decays"], grad_entering)
    grad_decays = jnp.sum(beyond * kept["entering"], axis=(2, 3))
    local_values, local_bc, local_step, local_rates, grad_skip = kept["local_pull"](
        (grad_heads, beyond, grad_decays)
    )
    grad_step_pre, grad_step_bias, grad_decay_log = kept["step_pull"](
        (carried_step + local_step, carried_rates + local_rates)
    )
    grad_value_pre, grad_edge_value, grad_conv_value, grad_conv_value_bias = kept["value_pull"](
        local_values
    )
    grad_bc_pre, grad_edge_bc, grad_conv_bc, grad_conv_bc_bias = kept["bc_pull"](
        carried_bc + local_bc
    )
    from_value, from_bc = from_behind((grad_edge_value, grad_edge_bc), "ctx", -1)
    first_edge = tokens - tap_count + 1
    grad_value_pre = grad_value_pre.at[:, first_edge:].add(from_value)
    grad_bc_pre = grad_bc_pre.at[:, first_edge:].add(from_bc)
    grad_gate_low = grad_gate_pre.astype(jnp.bfloat16)
    grad_value_low = grad_value_pre.reshape(row_count, -1).astype(jnp.bfloat16)
    grad_step_low = grad_step_pre.reshape(row_count, -1).astype(jnp.bfloat16)
    input_part = (
        dot_back(grad_gate_low, gate_full)
        + dot_back(grad_value_low, value_full)
        + dot_back(grad_step_low, step_full)
    )
    input_sum, bc_sum, conv_bc_sum, conv_bc_bias_sum = (
        lax.psum(input_part.astype(jnp.bfloat16), "tp").astype(jnp.float32),
        lax.psum(grad_bc_pre.reshape(row_count, -1).astype(jnp.bfloat16), "tp").astype(jnp.float32),
        lax.psum(grad_conv_bc, "tp").astype(jnp.float32),
        lax.psum(grad_conv_bc_bias, "tp").astype(jnp.float32),
    )
    grad_bc_low = bc_sum.astype(jnp.bfloat16)
    grad_normed = input_sum + dot_back(grad_bc_low, bc_full)
    hidden_rows = kept["hidden_rows"]
    inv_norm = kept["inv_norm"]
    weighted_norm = grad_normed * norm_gain
    grad_norm_gain = jnp.sum(grad_normed * hidden_rows * inv_norm, axis=0)
    grad_rows = (
        grad_rows
        + inv_norm * weighted_norm
        - hidden_rows * inv_norm**3 * jnp.mean(weighted_norm * hidden_rows, axis=1, keepdims=True)
    )
    normed = kept["normed"]
    proj_grads = (
        lax.psum_scatter(
            dot_left(normed, grad_gate_low).astype(jnp.bfloat16),
            ("dp", "ctx"),
            scatter_dimension=0,
            tiled=True,
        ).astype(jnp.float32),
        lax.psum_scatter(
            dot_left(normed, grad_value_low).astype(jnp.bfloat16),
            ("dp", "ctx"),
            scatter_dimension=0,
            tiled=True,
        ).astype(jnp.float32),
        lax.psum_scatter(
            dot_left(normed, grad_bc_low).astype(jnp.bfloat16),
            ("dp", "ctx"),
            scatter_dimension=0,
            tiled=True,
        ).astype(jnp.float32),
        lax.psum_scatter(
            dot_left(normed, grad_step_low).astype(jnp.bfloat16),
            ("dp", "ctx"),
            scatter_dimension=0,
            tiled=True,
        ).astype(jnp.float32),
        lax.psum_scatter(
            grad_out_proj.astype(jnp.bfloat16), ("dp", "ctx"), scatter_dimension=1, tiled=True
        ).astype(jnp.float32),
    )
    small_grads = lax.psum(
        (
            grad_norm_gain,
            grad_conv_value.astype(jnp.float32),
            grad_conv_value_bias.astype(jnp.float32),
            conv_bc_sum,
            conv_bc_bias_sum,
            grad_decay_log,
            grad_step_bias,
            grad_skip,
            grad_out_gain,
        ),
        ("dp", "ctx"),
    )
    return (grad_rows.reshape(seq_count, tokens, model_width), proj_grads, small_grads)


def stack_layers(groups, member):
    return jnp.stack([groups[layer_index][member] for layer_index in range(LAYERS)])


def local(
    hidden_in,
    segment_ids,
    cotangent,
    norm_gain,
    gate_proj,
    value_proj,
    bc_proj,
    step_proj,
    conv_value,
    conv_value_bias,
    conv_bc,
    conv_bc_bias,
    decay_log,
    step_bias,
    skip_gain,
    out_gain,
    out_proj,
):
    params = (
        norm_gain,
        gate_proj,
        value_proj,
        bc_proj,
        step_proj,
        conv_value,
        conv_value_bias,
        conv_bc,
        conv_bc_bias,
        decay_log,
        step_bias,
        skip_gain,
        out_gain,
        out_proj,
    )
    segment = segment_ids.astype(jnp.float32)
    hidden = hidden_in.astype(jnp.float32)
    kept_layers = []
    for layer_index in range(LAYERS):
        hidden, kept = layer_forward(
            hidden, segment, tuple((stacked[layer_index] for stacked in params))
        )
        kept_layers.append(kept)
    grad_hidden = cotangent.astype(jnp.float32)
    proj_list = [None] * LAYERS
    small_list = [None] * LAYERS
    for layer_index in reversed(range(LAYERS)):
        grad_hidden, proj_list[layer_index], small_list[layer_index] = layer_backward(
            grad_hidden,
            kept_layers[layer_index],
            tuple((stacked[layer_index] for stacked in params)),
        )
    return (
        hidden.astype(jnp.bfloat16),
        grad_hidden.astype(jnp.bfloat16),
        stack_layers(small_list, 0),
        stack_layers(proj_list, 0),
        stack_layers(proj_list, 1),
        stack_layers(proj_list, 2),
        stack_layers(proj_list, 3),
        stack_layers(small_list, 1),
        stack_layers(small_list, 2),
        stack_layers(small_list, 3),
        stack_layers(small_list, 4),
        stack_layers(small_list, 5),
        stack_layers(small_list, 6),
        stack_layers(small_list, 7),
        stack_layers(small_list, 8),
        stack_layers(proj_list, 4),
    )


MESH = pl.DeviceIdType.MESH
PACK = 640


def params_of(collective_id):
    return pltpu.CompilerParams(
        collective_id=collective_id, has_side_effects=True, vmem_limit_bytes=60 << 20
    )


VMEM_SPEC = pl.BlockSpec(memory_space=pltpu.VMEM)


def greet(peers):
    barrier = pltpu.get_barrier_semaphore()
    for peer in peers:
        pl.semaphore_signal(barrier, inc=1, device_id=peer, device_id_type=MESH)
    pl.semaphore_wait(barrier, len(peers))


def remote(source, target, send_sem, recv_sem, peer):
    return pltpu.make_async_remote_copy(
        src_ref=source,
        dst_ref=target,
        send_sem=send_sem,
        recv_sem=recv_sem,
        device_id=peer,
        device_id_type=MESH,
    )


def other_core(t):
    return t + 1 - 2 * lax.rem(t, 2)


def other_chip(t):
    return lax.rem(t + 2, 4)


def mxu(left, right, left_dim, right_dim, precision=None):
    return lax.dot_general(
        left,
        right,
        (((left_dim,), (right_dim,)), ((), ())),
        preferred_element_type=jnp.float32,
        precision=precision,
    )


def parts_of(array, count):
    parts = []
    for _ in range(count - 1):
        high = array.astype(jnp.bfloat16)
        parts.append(high)
        array = array - high.astype(jnp.float32)
    return parts + [array.astype(jnp.bfloat16)]


def mxu_ones_left(ones, data, count):
    return sum(mxu(ones, part, 1, 0) for part in parts_of(data, count))


def mxu_ones_right(data, ones, count):
    return sum(mxu(part, ones, 1, 0) for part in parts_of(data, count))


def iota(shape, axis):
    return lax.broadcasted_iota(jnp.int32, shape, axis)


def ones_where(condition, kind):
    return jnp.where(condition, 1.0, 0.0).astype(kind)


def sigmoid(v):
    return 1.0 / (1.0 + jnp.exp(-v))


exact = lax.Precision.HIGHEST
LOW = jnp.bfloat16
OUT_AT, VALUE_AT = 128, 384


class BlockTerms:
    def __init__(self, start, segc_ref, segr_ref, small_ref, value_ref, bc_ref, step_in, width):
        self.start, self.width = start, width
        self.segc_ref, self.small_ref = segc_ref, small_ref
        rows = pl.ds(8 + start, BLOCK)
        seg = segc_ref[rows, :]
        row, col = iota((BLOCK, BLOCK), 0), iota((BLOCK, BLOCK), 1)
        self.row, self.col = row, col
        same = jnp.logical_and(seg == segr_ref[:, pl.ds(start, BLOCK)], row >= col)
        self.hidden_pairs = jnp.where(same, 0.0, -1e30)
        self.value_arg = self.conv(value_ref, 0, 4, width)
        self.bc_arg = self.conv(bc_ref, 9, 13, bc_ref.shape[1])
        self.value_sig = sigmoid(self.value_arg)
        self.bc_sig = sigmoid(self.bc_arg)
        self.values = (self.value_arg * self.value_sig).astype(LOW)
        bc_low = (self.bc_arg * self.bc_sig).astype(LOW)
        half = bc_ref.shape[1] // 2
        self.b_low, self.c_low = bc_low[:, :half], bc_low[:, half:]
        self.step = jnp.maximum(step_in, 0.0) + jnp.log1p(jnp.exp(-jnp.abs(step_in)))
        rates = small_ref[8:9, :width]
        self.log_decay = mxu_ones_left(ones_where(row >= col, LOW), self.step * rates, 3)
        self.log_rows = jnp.transpose(self.log_decay)
        self.step_rows = jnp.transpose(self.step)
        self.scores = mxu(self.c_low, self.b_low, 1, 1)
        seg = seg[:, :width]
        before = segc_ref[7 + start : 8 + start, :width]
        last = segc_ref[7 + start + BLOCK : 8 + start + BLOCK, :width]
        self.reach = jnp.where(seg == before, jnp.exp(self.log_decay), 0.0)
        self.reach_last = self.reach[BLOCK - 1 : BLOCK, :]
        self.fade = jnp.where(
            seg == last, jnp.exp(self.log_decay[BLOCK - 1 : BLOCK, :] - self.log_decay), 0.0
        )
        self.faded = self.fade * self.step * self.values.astype(jnp.float32)

    def conv(self, ref, taps_at, bias_at, width):
        total = self.small_ref[bias_at : bias_at + 1, :width]
        for distance in range(4):
            tap = self.small_ref[taps_at + 3 - distance : taps_at + 4 - distance, :width]
            total = total + tap * self.back(ref, distance, width)
        return total

    def back(self, ref, distance, width):
        rows = ref[pl.ds(8 + self.start - distance, BLOCK), :]
        if not distance:
            return rows
        here = self.segc_ref[pl.ds(8 + self.start, BLOCK), :width]
        there = self.segc_ref[pl.ds(8 + self.start - distance, BLOCK), :width]
        return jnp.where(here == there, rows, 0.0)

    def ahead(self, ref, distance, width):
        rows = ref[pl.ds(self.start + distance, BLOCK), :]
        if not distance:
            return rows
        here = self.segc_ref[pl.ds(8 + self.start, BLOCK), :width]
        there = self.segc_ref[pl.ds(8 + self.start + distance, BLOCK), :width]
        return jnp.where(here == there, rows, 0.0)

    def decay_pairs(self, head):
        at = head * HEADDIM
        return jnp.exp(
            self.log_decay[:, at : at + 1] - self.log_rows[at : at + 1, :] + self.hidden_pairs
        )

    def head_lanes(self, head):
        lanes = iota((BLOCK, self.width), 1)
        return jnp.logical_and(lanes >= head * HEADDIM, lanes < (head + 1) * HEADDIM)

    def of_head(self, array, head):
        return array * ones_where(self.head_lanes(head), array.dtype)


def lane_shift(width):
    return ones_where(iota((width, 256), 1) == iota((width, 256), 0) + 64, LOW)


def two_parts(array):
    high = array.astype(LOW)
    return high, (array - high.astype(jnp.float32)).astype(LOW)


def forward_body(
    precise,
    plan,
    normed_ref,
    wall_ref,
    bcw_ref,
    small_ref,
    segr_ref,
    segc_ref,
    part_ref,
    squares_ref,
    gate_ref,
    value_ref,
    bc_ref,
    step_ref,
    mixed_ref,
    state_ref,
):
    tokens = normed_ref.shape[0]
    width = gate_ref.shape[1]
    heads = width // HEADDIM
    piece = 0 if precise else part_ref.shape[1]
    value_ref[0:8, :] = jnp.zeros((8, width), jnp.float32)
    bc_ref[0:8, :] = jnp.zeros((8, bc_ref.shape[1]), jnp.float32)
    spread = ones_where(
        iota((256, width), 0) - width == iota((256, width), 1) // HEADDIM, LOW
    )
    shift = lane_shift(width)
    gains, skip = small_ref[5:6, :width], small_ref[6:7, :width]
    state = jnp.zeros(state_ref.shape[1:], jnp.float32)
    for block in range(tokens // BLOCK):
        start = block * BLOCK
        rows = pl.ds(start, BLOCK)
        normed = normed_ref[rows, :]
        gate_pre = mxu(normed, wall_ref[:, 0:256], 1, 0)[:, :width]
        both = mxu(normed, wall_ref[:, VALUE_AT : VALUE_AT + 256], 1, 0)
        value_ref[pl.ds(8 + start, BLOCK), :] = both[:, :width]
        bc_ref[pl.ds(8 + start, BLOCK), :] = mxu(normed, bcw_ref[...], 1, 0)
        step_in = mxu_ones_right(both, spread, 3) + small_ref[7:8, :width]
        gate_ref[rows, :] = gate_pre
        step_ref[rows, :] = step_in
        terms = BlockTerms(start, segc_ref, segr_ref, small_ref, value_ref, bc_ref, step_in, width)
        mixed = skip * terms.values.astype(jnp.float32)
        for head in range(heads):
            at = head * HEADDIM
            weights = terms.scores * terms.decay_pairs(head) * terms.step_rows[at : at + 1, :]
            own_values = terms.of_head(terms.values, head)
            for term in two_parts(weights) if precise else (weights.astype(LOW),):
                mixed += mxu(term, own_values, 1, 0)
            plan(block, head)
        state_ref[block] = state
        if block:
            for term in two_parts(state) if precise else (state.astype(LOW),):
                mixed += terms.reach * mxu(terms.c_low, term, 1, 0)
        state = terms.reach_last * state
        for term in two_parts(terms.faded) if precise else (terms.faded.astype(LOW),):
            state += mxu(terms.b_low, term, 0, 0)
        mixed_ref[rows, :] = mixed
        gated = mixed * gate_pre * sigmoid(gate_pre)
        squares = gated * gated
        for at in range(0, BLOCK, 128):
            row = (start + at) // 128
            squares_ref[row : row + 1, :] = mxu(
                jnp.ones((8, width), jnp.float32), squares[at : at + 128], 1, 1, exact
            )[0:1]
        if precise:
            part_ref[rows, :] = gated
            plan(block, 3)
            continue
        moved = mxu((gated * gains).astype(LOW), shift, 1, 0).astype(LOW)
        part = mxu(moved, wall_ref[:, OUT_AT : OUT_AT + 256], 1, 1).astype(LOW)
        for at in range(0, BLOCK, piece):
            part_ref[(start + at) // piece] = part[at : at + piece]
        plan(block, 3)


def local_params():
    return pltpu.CompilerParams(vmem_limit_bytes=60 << 20)


def forward_shapes(normed, bcw, slots, precise):
    tokens, model_width = normed.shape
    width = INNER // slots
    bc_width = bcw.shape[1]
    f32 = jnp.float32
    if precise:
        first = jax.ShapeDtypeStruct((tokens, width), f32)
    else:
        first = jax.ShapeDtypeStruct((slots, tokens // slots, model_width), LOW)
    return [
        first,
        jax.ShapeDtypeStruct((tokens // 128, 128), f32),
        jax.ShapeDtypeStruct((tokens, width), f32),
        jax.ShapeDtypeStruct((tokens + 8, width), f32),
        jax.ShapeDtypeStruct((tokens + 8, bc_width), f32),
        jax.ShapeDtypeStruct((tokens, width), f32),
        jax.ShapeDtypeStruct((tokens, width), f32),
        jax.ShapeDtypeStruct((tokens // BLOCK, bc_width // 2, width), f32),
    ]


def row_sum(array):
    return jnp.sum(array, axis=0, keepdims=True)


def backward_body(
    plan,
    grad_ref,
    inv_ref,
    inner_ref,
    normed_ref,
    wall_ref,
    small_ref,
    segr_ref,
    segc_ref,
    gate_ref,
    value_ref,
    bc_ref,
    step_ref,
    mixed_ref,
    state_ref,
    both_ref,
    early_ref,
    late_ref,
    sums_ref,
    pre_ref,
    scaled_ref,
    e_ref,
    e_bc_ref,
    grad_mixed_ref,
):
    tokens, model_width = normed_ref.shape
    width = gate_ref.shape[1]
    bc_width = bc_ref.shape[1]
    heads = width // HEADDIM
    piece = both_ref.shape[1]
    blocks = tokens // BLOCK
    f32 = jnp.float32
    shift = lane_shift(width)
    gains, skip, rates = (small_ref[at : at + 1, :width] for at in (5, 6, 8))
    e_ref[tokens:, :] = jnp.zeros((8, width), f32)
    e_bc_ref[tokens:, :] = jnp.zeros((8, bc_width), f32)
    pre_ref[...] = jnp.zeros(pre_ref.shape, LOW)
    inv_columns, inner_columns = spread_rows(inv_ref[...]), spread_rows(inner_ref[...])
    same_head = ones_where(
        iota((width, width), 0) // HEADDIM == iota((width, width), 1) // HEADDIM, LOW
    )
    tail = ones_where(iota((width, 128), 0) == iota((width, 128), 1) + 128, LOW)
    pick = ones_where(
        jnp.logical_and(
            iota((width, 128), 0) == (iota((width, 128), 1) - 64) * HEADDIM, iota((width, 128), 1) >= 64
        ),
        LOW,
    )
    grad_state = jnp.zeros(state_ref.shape[1:], f32)
    sums = {}

    def add(name, term):
        sums[name] = sums[name] + term if name in sums else term

    for block in range(blocks):
        start = block * BLOCK
        rows = pl.ds(start, BLOCK)
        inv, inner = (
            jnp.concatenate([c[:, at : at + 1] for at in range(start // 128, (start + BLOCK) // 128)], axis=0)
            for c in (inv_columns, inner_columns)
        )
        grad_low = grad_ref[rows, 0:model_width]
        grad_scaled = mxu(grad_low, wall_ref[:, OUT_AT : OUT_AT + 256], 1, 0)
        grad_scaled = pltpu.roll(grad_scaled, 192, 1)[:, :width]
        gate_pre, mixed = gate_ref[rows, :], mixed_ref[rows, :]
        sig = sigmoid(gate_pre)
        act = gate_pre * sig
        gated = mixed * act
        normal = gated * inv
        scaled_ref[rows, :] = mxu((normal * gains).astype(LOW), shift, 1, 0).astype(LOW)
        add("out_gain", row_sum(grad_scaled * normal))
        grad_gated = inv * (grad_scaled * gains) - gated * (inv * inv * inner)
        grad_gate = grad_gated * mixed * sig * (1.0 + gate_pre * (1.0 - sig))
        pre_ref[rows, 0:width] = grad_gate.astype(LOW)
        grad_mixed_ref[rows, :] = grad_gated * act
    plan(-1, 0)
    k_rows = early_ref.shape[1]

    def by_slices(pair):
        lanes = pl.ds(pair * 2 * k_rows, 2 * k_rows)
        return lanes, ((2 * pair + at, slice(at * k_rows, (at + 1) * k_rows)) for at in range(2))

    for pair in range(early_ref.shape[0] // 2):
        lanes, slices = by_slices(pair)
        total = mxu(normed_ref[:, lanes], pre_ref[:, 0:256], 0, 0)
        out = mxu(grad_ref[:, lanes], scaled_ref[...], 0, 0)
        for slot, k_slice in slices:
            early_ref[slot, :, 0:OUT_AT] = total[k_slice, 0:OUT_AT].astype(LOW)
            early_ref[slot, :, OUT_AT:256] = (
                total[k_slice, OUT_AT:256] + out[k_slice, 0 : 256 - OUT_AT]
            ).astype(LOW)
            early_ref[slot, :, 256:VALUE_AT] = out[k_slice, 256 - OUT_AT :].astype(LOW)
    plan(-1, 1)
    for turn, block in enumerate(reversed(range(blocks))):
        start = block * BLOCK
        rows = pl.ds(start, BLOCK)
        step_in = step_ref[rows, :]
        terms = BlockTerms(start, segc_ref, segr_ref, small_ref, value_ref, bc_ref, step_in, width)
        grad_mixed = grad_mixed_ref[rows, :]
        grad_mixed_low = grad_mixed.astype(LOW)
        values = terms.values.astype(f32)
        add("skip", row_sum(grad_mixed * values))
        grad_values = skip * grad_mixed
        direct = jnp.zeros((BLOCK, width), f32)
        between = jnp.zeros((BLOCK, width), f32)
        pair_sum = jnp.zeros((BLOCK, BLOCK), f32)
        from_here = ones_where(terms.col >= terms.row, LOW)
        for head in range(heads):
            at = head * HEADDIM
            decay = terms.decay_pairs(head)
            step_row = terms.step_rows[at : at + 1, :]
            grad_head = terms.of_head(grad_mixed_low, head)
            head_ones = ones_where(terms.head_lanes(head), LOW)
            products = mxu(grad_head, terms.values, 1, 1)
            scored = terms.scores * decay
            grad_values += mxu((scored * step_row).astype(LOW), grad_head, 0, 0)
            pair_sum += decay * step_row * products
            unstepped = scored * products
            direct += mxu(unstepped.astype(LOW), head_ones, 0, 0)
            later = mxu(from_here, (unstepped * step_row).astype(LOW), 1, 0)
            later = jnp.where(terms.col < terms.row, later, 0.0)
            between += mxu(later.astype(LOW), head_ones, 1, 0)
            plan(turn, head)
        pair_low = pair_sum.astype(LOW)
        grad_b = mxu(pair_low, terms.c_low, 0, 0)
        grad_c = mxu(pair_low, terms.b_low, 1, 0)
        across = jnp.zeros((BLOCK, width), f32)
        if block < blocks - 1:
            state_low = grad_state.astype(LOW)
            to_state = mxu(terms.b_low, state_low, 1, 0)
            grad_values += terms.fade * terms.step * to_state
            by_step = terms.fade * to_state * values
            direct += mxu_ones_right(by_step, same_head, 2)
            grad_b += mxu(terms.faded.astype(LOW), state_low, 1, 1)
            across += mxu_ones_left(ones_where(terms.col < terms.row, LOW), terms.step * by_step, 2)
        if block:
            entering = state_ref[block]
            entering_low = entering.astype(LOW)
            carried = terms.reach * mxu(terms.c_low, entering_low, 1, 0)
            across += mxu_ones_left(from_here, grad_mixed * carried, 2)
            reached = (terms.reach * grad_mixed).astype(LOW)
            grad_c += mxu(reached, entering_low, 1, 1)
            if block < blocks - 1:
                across += row_sum(grad_state * terms.reach_last * entering)
            grad_state = terms.reach_last * grad_state + mxu(terms.c_low, reached, 0, 0)
        between += mxu_ones_right(across, same_head, 2)
        grad_step = direct + rates * between
        add("rates", row_sum(terms.step * between))
        grad_step_in = grad_step * sigmoid(step_in)
        add("step_bias", row_sum(grad_step_in))
        e = grad_values * (terms.value_sig * (1.0 + terms.value_arg * (1.0 - terms.value_sig)))
        e_ref[rows, :] = e
        e_bc = jnp.concatenate([grad_b, grad_c], axis=1) * (
            terms.bc_sig * (1.0 + terms.bc_arg * (1.0 - terms.bc_sig))
        )
        e_bc_ref[rows, :] = e_bc
        add("value_bias", row_sum(e))
        add("bc_bias", row_sum(e_bc))
        grad_value = jnp.zeros((BLOCK, width), f32)
        grad_bc = jnp.zeros((BLOCK, bc_width), f32)
        for distance in range(4):
            tap = 3 - distance
            add(("value", tap), row_sum(e * terms.back(value_ref, distance, width)))
            add(("bc", tap), row_sum(e_bc * terms.back(bc_ref, distance, bc_width)))
            grad_value += small_ref[tap : tap + 1, :width] * terms.ahead(e_ref, distance, width)
            grad_bc += small_ref[9 + tap : 10 + tap, :] * terms.ahead(e_bc_ref, distance, bc_width)
        value_low = grad_value.astype(LOW)
        pre_ref[rows, VALUE_AT : VALUE_AT + 128] = value_low[:, 0:128]
        pre_ref[rows, VALUE_AT + 128 : VALUE_AT + 256] = (
            mxu(value_low, tail, 1, 0) + mxu(grad_step_in.astype(LOW), pick, 1, 0)
        ).astype(LOW)
        part = mxu(pre_ref[rows, :], wall_ref[...], 1, 1).astype(LOW)
        grad_bc = grad_bc.astype(LOW)
        for at in range(0, BLOCK, piece):
            slot = (start + at) // piece
            both_ref[slot, :, 0:model_width] = part[at : at + piece]
            both_ref[slot, :, model_width:] = grad_bc[at : at + piece]
        plan(turn, 3)

    for pair in range(late_ref.shape[0] // 2):
        lanes, slices = by_slices(pair)
        total = mxu(normed_ref[:, lanes], pre_ref[:, VALUE_AT:], 0, 0)
        for slot, k_slice in slices:
            late_ref[slot] = total[k_slice].astype(LOW)
        plan(blocks, pair)

    sums_ref[...] = jnp.zeros(sums_ref.shape, f32)
    head_sums = mxu_ones_right(
        jnp.concatenate([sums["skip"], jnp.zeros((7, width), f32)], axis=0), same_head, 3
    )
    for tap in range(4):
        sums_ref[tap : tap + 1, 0:width] = sums["value", tap]
        sums_ref[9 + tap : 10 + tap, :] = sums["bc", tap]
    sums_ref[4:5, 0:width] = sums["value_bias"]
    sums_ref[5:6, 0:width] = sums["out_gain"]
    sums_ref[6:7, 0:width] = head_sums[0:1]
    sums_ref[7:8, 0:width] = sums["step_bias"]
    sums_ref[8:9, 0:width] = sums["rates"] * rates
    sums_ref[13:14, :] = sums["bc_bias"]


def backward_shapes(normed, kept, slots):
    tokens, model_width = normed.shape
    width = kept[0].shape[1]
    bc_width = kept[2].shape[1]
    k_slots = slots // 2
    shapes = [
        jax.ShapeDtypeStruct((slots, tokens // slots, model_width + bc_width), LOW),
        jax.ShapeDtypeStruct((k_slots, model_width // k_slots, VALUE_AT), LOW),
        jax.ShapeDtypeStruct((k_slots, model_width // k_slots, PACK - VALUE_AT), LOW),
        jax.ShapeDtypeStruct((16, 256), jnp.float32),
    ]
    work = [
        pltpu.VMEM((tokens, PACK), LOW),
        pltpu.VMEM((tokens, 256), LOW),
        pltpu.VMEM((tokens + 8, width), jnp.float32),
        pltpu.VMEM((tokens + 8, bc_width), jnp.float32),
        pltpu.VMEM((tokens, width), jnp.float32),
    ]
    return shapes, work


def norm_rows(hidden, gain):
    inv = lax.rsqrt(jnp.mean(hidden * hidden, axis=1, keepdims=True) + epsilon)
    return inv, (hidden * inv * gain).astype(jnp.bfloat16)


HALVES = 2


class Links:
    def __init__(self, depth):
        self.depth = depth
        self.x, self.z, self.t = (lax.axis_index(name) for name in ("dp", "ctx", "tp"))
        self.core, self.chip = {"tp": other_core(self.t)}, {"tp": other_chip(self.t)}
        self.far_x = {"dp": 1 - self.x}
        self.left = {"ctx": lax.rem(self.z + depth - 1, depth)}
        self.right = {"ctx": lax.rem(self.z + 1, depth)}
        self.sent = []

    def send(self, source, target, send_sem, recv_sem, peer, when=None):
        copy = remote(source, target, send_sem, recv_sem, peer)
        self.sent.append((copy, when))
        if when is None:
            copy.start()
        else:
            pl.when(when)(copy.start)

    def wait(self, ref, send_sem, recv_sem, when=None):
        copy = remote(ref, ref, send_sem, recv_sem, self.core)
        if when is None:
            copy.wait_recv()
        else:
            pl.when(when)(copy.wait_recv)

    def finish(self):
        for copy, when in self.sent:
            if when is None:
                copy.wait_send()
            else:
                pl.when(when)(copy.wait_send)

    def near_first(self):
        z = self.z
        first = z + 1 - 2 * lax.rem(z, 2)
        third = 3 - 3 * (z // 2)
        return [first, 6 - z - first - third, third]

    def far_first(self):
        z = self.z
        odd = lax.rem(z, 2)
        first = 3 - 3 * (z // 2)
        second = (1 - odd) * (2 + z // 2) + odd * (z // 2)
        return [first, second, 6 - z - first - second]


def everyone(depth):
    z, t = lax.axis_index("ctx"), lax.axis_index("tp")
    return [
        {"ctx": lax.rem(z + hop, depth), "tp": lax.rem(t + turn, 4)}
        for hop in range(depth)
        for turn in range(4)
        if hop or turn
    ]


def half(ref, part):
    rows = ref.shape[0] // HALVES
    return ref.at[pl.ds(part * rows, rows)]


def gather_task(links, pieces, fulls, send_sem, recv_sem):
    z, t = links.z, links.t
    last = links.depth - 1
    own = z * 4 + t

    def pass_on(a, ref, slot, part, to_left, to_right, chip=True):
        target = half(fulls[a].at[slot], part)
        recv = recv_sem.at[a, slot, part]

        def go(way, peer, when=None):
            links.send(ref, target, send_sem.at[a, slot, part, way], recv, peer, when)

        if chip:
            go(0, links.left, to_left)
            go(1, links.right, to_right)
            go(2, links.chip)
        go(3, links.core)

    def arrived(a, slot, part):
        ref = half(fulls[a].at[slot], part)
        links.wait(ref, send_sem.at[a, slot, part, 0], recv_sem.at[a, slot, part])
        return ref

    every = range(len(pieces))
    for part in range(HALVES):
        for a in every:
            pass_on(a, half(pieces[a], part), own, part, z > 0, z < last)
    for a in every:
        fulls[a][own] = pieces[a][...]
    yield
    column = other_chip(t)
    order = links.near_first()
    for place, far in enumerate(order):
        slot = far * 4 + t
        for part in range(HALVES):
            for a in every:
                ref = arrived(a, slot, part)
                to_left = jnp.logical_and(far > z, z > 0)
                to_right = jnp.logical_and(far < z, z < last)
                pass_on(a, ref, slot, part, to_left, to_right)
        slot = (order[place - 1] if place else z) * 4 + column
        for part in range(HALVES):
            for a in every:
                pass_on(a, arrived(a, slot, part), slot, part, None, None, False)
        yield
    for part in range(HALVES):
        for a in every:
            slot = order[-1] * 4 + column
            pass_on(a, arrived(a, slot, part), slot, part, None, None, False)
    yield
    for far in [z] + order:
        for row in (other_core(t), other_chip(other_core(t))):
            for part in range(HALVES):
                for a in every:
                    arrived(a, far * 4 + row, part)


def gather_sems(count, slots):
    return [
        pltpu.SemaphoreType.DMA((count, slots, HALVES, 4)),
        pltpu.SemaphoreType.DMA((count, slots, HALVES)),
    ]


def reduce_task(links, produce, parts, outs, bufs, send_sem, recv_sem):
    z, t = links.z, links.t
    depth = links.depth
    last = depth - 1
    order = links.far_first() + [z]
    every = range(len(parts))

    def rows_of(ref, part):
        rows = ref.shape[0] // HALVES
        return slice(part * rows, (part + 1) * rows)

    def sems(a, at, part):
        return send_sem.at[a, at, part], recv_sem.at[a, at, part]

    def loaded(a, at, part):
        return bufs[a][at, rows_of(bufs[a].at[at], part), :].astype(jnp.float32)

    def mine(a, slot, part):
        return parts[a][slot, rows_of(parts[a].at[slot], part), :].astype(jnp.float32)

    def wait(a, at, part, when=None):
        links.wait(half(bufs[a].at[at], part), *sems(a, at, part), when)

    def stage1(far):
        produce(far)
        for which, row in enumerate((other_chip(other_core(t)), other_core(t))):
            for part in range(HALVES):
                for a in every:
                    at = far * 2 + which
                    links.send(
                        half(parts[a].at[far * 4 + row], part),
                        half(bufs[a].at[at], part),
                        *sems(a, at, part),
                        links.core,
                    )

    def stage2(far):
        for part in range(HALVES):
            for a in every:
                at = far * 2
                wait(a, at, part)
                total = mine(a, far * 4 + other_chip(t), part) + loaded(a, at, part)
                bufs[a][at, rows_of(bufs[a].at[at], part), :] = total.astype(bufs[a].dtype)
                to = 2 * depth + far
                links.send(
                    half(bufs[a].at[at], part), half(bufs[a].at[to], part), *sems(a, to, part), links.chip
                )

    def stage3(far):
        at = far * 2 + 1
        for part in range(HALVES):
            for a in every:
                wait(a, at, part)
                wait(a, 2 * depth + far, part)
                total = mine(a, far * 4 + t, part) + loaded(a, at, part) + loaded(a, 2 * depth + far, part)
                out = outs[a]
                rows = rows_of(out, part)
                if far is z:
                    out[rows, :] = total
                    continue
                ref = bufs[a]
                here = (at, rows_of(ref.at[at], part), slice(None))
                for way, (peer, when, first) in enumerate(
                    ((links.right, far > z, z == 0), (links.left, far < z, z == last))
                ):
                    chain = 3 * depth + way * depth + far

                    def go(total=total, chain=chain, here=here, ref=ref, first=first, a=a, part=part):
                        @pl.when(first)
                        def _():
                            ref[here] = total.astype(ref.dtype)

                        @pl.when(jnp.logical_not(first))
                        def _():
                            wait(a, chain, part)
                            ref[here] = (total + loaded(a, chain, part)).astype(ref.dtype)

                    pl.when(when)(go)
                    links.send(
                        half(ref.at[at], part), half(ref.at[chain], part), *sems(a, chain, part), peer, when
                    )

    count = len(order)
    for place in range(count + 2):
        if place < count:
            stage1(order[place])
        if 1 <= place <= count:
            stage2(order[place - 1])
        if 2 <= place:
            stage3(order[place - 2])
        yield
    for way, when in enumerate((z > 0, z < last)):
        chain = 3 * depth + way * depth + z
        for part in range(HALVES):
            for a in every:

                @pl.when(when)
                def _(a=a, part=part, chain=chain):
                    wait(a, chain, part)
                    outs[a][rows_of(outs[a], part), :] += loaded(a, chain, part)


def reduce_scratch(shapes, dtypes, depth):
    return [pltpu.VMEM((5 * depth,) + s, d) for s, d in zip(shapes, dtypes)] + [
        pltpu.SemaphoreType.DMA((len(shapes), 5 * depth, HALVES)),
        pltpu.SemaphoreType.DMA((len(shapes), 5 * depth, HALVES)),
    ]


def run_tasks(*tasks):
    tasks = list(tasks)
    while tasks:
        for task in list(tasks):
            try:
                next(task)
            except StopIteration:
                tasks.remove(task)


def share_task(links, own, full, send_sem, recv_sem):
    depth = links.depth
    slot = links.z * 4 + links.t
    for at, peer in enumerate(everyone(depth)):
        links.send(own, full.at[slot], send_sem.at[at], recv_sem.at[slot], peer)
    full[slot] = own[...]
    yield
    for hop in range(depth):
        for turn in range(4):
            if hop or turn:
                source = lax.rem(links.z + hop, depth) * 4 + lax.rem(links.t + turn, 4)
                links.wait(full.at[source], send_sem.at[0], recv_sem.at[source])


def spread_rows(rows):
    size = rows.shape[1]
    eye = ones_where(iota((size, size), 0) == iota((size, size), 1), jnp.float32)
    return mxu(eye, rows, 1, 1, exact)


ANY_SPEC = pl.BlockSpec(memory_space=pl.ANY)


class Fetch:
    def __init__(self, sources, targets, sems, names=None):
        self.copies = [
            pltpu.make_async_copy(source, target, sems.at[at])
            for at, (source, target) in enumerate(zip(sources, targets))
        ]
        self.place = {name: at for at, name in enumerate(names or range(len(self.copies)))}
        self.waiting = set(range(len(self.copies)))
        for copy in self.copies:
            copy.start()

    def need(self, *names):
        for name in names:
            at = self.place.get(name)
            if at in self.waiting:
                self.waiting.remove(at)
                self.copies[at].wait()

    def wait(self):
        self.need(*self.place)


def launch(kernel, operands, shapes, scratch, collective_id, name, raw=(), first=(), flushed=()):
    big = [
        at for at, a in enumerate(operands) if at not in raw and a.size * a.dtype.itemsize >= 2**18
    ]
    big = [at for at in first if at in big] + [at for at in big if at not in first]
    count, back = len(operands), len(flushed) + 1 if flushed else 0
    results = len(shapes)

    def body(*refs):
        refs = list(refs)
        held, refs = (refs[-back:], refs[:-back]) if back else ([], refs)
        ins, staged = refs[:count], refs[-len(big) - 1 : -1]
        fetch = Fetch([ins[at] for at in big], staged, refs[-1], big)
        for at, ref in zip(big, staged):
            ins[at] = ref
        outs = refs[count : count + results]
        copies = []
        for place, at in enumerate(flushed):
            copies.append(pltpu.make_async_copy(held[place], outs[at], held[-1].at[place]))
            outs[at] = held[place]

        def flush():
            for copy in copies:
                copy.start()

        fetch.flush = flush
        kernel(fetch, *ins, *outs, *refs[count + results : -len(big) - 1])
        for copy in copies:
            copy.wait()

    return pl.pallas_call(
        body,
        out_shape=shapes,
        in_specs=[ANY_SPEC if at in raw or at in big else VMEM_SPEC for at in range(count)],
        out_specs=[ANY_SPEC if at in flushed else VMEM_SPEC for at in range(results)],
        scratch_shapes=list(scratch)
        + [pltpu.VMEM(operands[at].shape, operands[at].dtype) for at in big]
        + [pltpu.SemaphoreType.DMA((len(big),))]
        + [pltpu.VMEM(shapes[at].shape, shapes[at].dtype) for at in flushed]
        + ([pltpu.SemaphoreType.DMA((len(flushed),))] if flushed else []),
        compiler_params=params_of(collective_id),
        name=name,
    )(*operands)


def turn_forward_kernel(
    depth,
    fetch,
    gated_ref,
    squares_ref,
    small_ref,
    wall_ref,
    hidden_ref,
    gain_ref,
    pack_ref,
    early_ref,
    bc_ref,
    hidden_out,
    total_out,
    inv_out,
    full_out,
    full_pack,
    full_bc,
    parts,
    normed,
    shared,
    share_send,
    share_recv,
    bufs,
    reduce_send,
    reduce_recv,
    gather_send,
    gather_recv,
    pack_send,
    pack_recv,
    bc_send,
    bc_recv,
):
    links = Links(depth)
    greet(everyone(depth) + [links.far_x])
    small_ref = small_ref.at[0]
    width = gated_ref.shape[1]
    piece = hidden_ref.shape[1] // 4
    block = 4 * piece
    share = share_task(links, squares_ref, shared, share_send, share_recv)
    next(share, None)
    weights = Weights(links, pack_ref, full_pack, pack_send, pack_recv)
    fetch.wait()
    here = [links.z, weights.order[0], weights.order[1]]
    for far in here:
        full_pack[weights.base + far] = early_ref[weights.base + far]
    other = (1 - links.x) * depth + links.z
    full_pack[other] = early_ref[other]
    run_tasks(share)
    total = shared[0]
    for slot in range(1, 4 * depth):
        total = total + shared[slot]
    inv_rows = lax.rsqrt(total / INNER + epsilon)
    inv_out[...] = inv_rows
    columns = spread_rows(inv_rows)
    shift = lane_shift(width)
    gains = small_ref[5:6, :width]
    which = iota((block, columns.shape[1]), 1)

    def produce(far):
        at = far * (block // 128)
        both = jnp.concatenate([columns] * (block // 128), axis=0)
        low = iota((block, columns.shape[1]), 0) // 128 + at
        inv = jnp.sum(jnp.where(which == low, both, 0.0), axis=1, keepdims=True)
        rows = pl.ds(pl.multiple_of(far * block, block), block)
        scaled = (gated_ref[rows, :] * inv * gains).astype(LOW)
        moved = mxu(scaled, shift, 1, 0).astype(LOW)
        part = mxu(moved, wall_ref[:, OUT_AT : OUT_AT + 256], 1, 1)
        for row in range(4):
            parts[far * 4 + row] = part[row * piece : (row + 1) * piece].astype(parts.dtype)

    def background():
        weights.over(0, False)
        yield
        weights.along(2)
        yield
        weights.over(1, False)
        yield
        yield
        weights.over(2)

    shared_bc = shared_task(links, bc_ref.at[1], full_bc, bc_send, bc_recv)
    run_tasks(
        reduce_task(links, produce, [parts], [total_out], [bufs], reduce_send, reduce_recv),
        background(),
        shared_bc,
    )
    rows = pl.ds(pl.multiple_of(links.t * piece, piece), piece)
    hidden = hidden_ref[0, rows, :].astype(jnp.float32) + total_out[...]
    hidden_out[...] = hidden
    _, normed[...] = norm_rows(hidden, gain_ref[...].astype(jnp.float32)[1:2])
    run_tasks(gather_task(links, [normed], [full_out], gather_send, gather_recv))
    for far in weights.order:
        weights.over_landed(far)
    links.finish()


def turn_forward(gated, squares, small, wall, hidden, gain, pack, early, bc, depth, collective_id):
    piece, model_width = hidden.shape[1] // 4, hidden.shape[2]
    slots = 4 * depth
    f32 = jnp.float32
    return launch(
        partial(turn_forward_kernel, depth),
        (gated, squares, small, wall, hidden, gain, pack, early, bc),
        [
            jax.ShapeDtypeStruct((piece, model_width), f32),
            jax.ShapeDtypeStruct((piece, model_width), f32),
            jax.ShapeDtypeStruct(squares.shape, f32),
            jax.ShapeDtypeStruct((slots, piece, model_width), LOW),
        ]
        + pack_shapes(depth, pack.shape[1], bc.shape[2]),
        [
            pltpu.VMEM((slots, piece, model_width), f32),
            pltpu.VMEM((piece, model_width), LOW),
            pltpu.VMEM((slots,) + squares.shape, f32),
            pltpu.SemaphoreType.DMA((slots,)),
            pltpu.SemaphoreType.DMA((slots,)),
        ]
        + reduce_scratch([(piece, model_width)], [f32], depth)
        + gather_sems(1, slots)
        + weights_sems(depth)
        + shared_sems(depth),
        collective_id,
        "turn_forward",
    )


def partners(links):
    z = links.z
    return [lax.rem(z + 2, 4), z + 1 - 2 * lax.rem(z, 2), 3 - z]


class Weights:
    def __init__(self, links, pack, full, send_sem, recv_sem):
        self.links, self.pack, self.full = links, pack, full
        self.send_sem, self.recv_sem = send_sem, recv_sem
        self.order = partners(links)
        self.base = links.x * links.depth
        self.mine = self.base + links.z

    def send(self, ref, slot, part, kind, peer):
        self.links.send(
            ref,
            half(self.full.at[slot], part),
            self.send_sem.at[kind, part],
            self.recv_sem.at[slot, part],
            peer,
        )

    def arrived(self, slot, part):
        ref = half(self.full.at[slot], part)
        self.links.wait(ref, self.send_sem.at[0, part], self.recv_sem.at[slot, part])
        return ref

    def keep(self):
        self.full[self.mine] = self.pack[self.links.z]

    def own_over(self):
        for part in range(HALVES):
            self.send(half(self.pack.at[self.links.z], part), self.mine, part, 0, self.links.far_x)

    def along(self, place):
        far = self.order[place]
        for part in range(HALVES):
            self.send(half(self.pack.at[far], part), self.mine, part, 1 + place, {"ctx": far})

    def landed(self, place):
        for part in range(HALVES):
            self.arrived(self.base + self.order[place], part)

    def over(self, place, wait=True):
        slot = self.base + self.order[place]
        for part in range(HALVES):
            ref = self.arrived(slot, part) if wait else half(self.full.at[slot], part)
            self.send(ref, slot, part, self.links.depth + place, self.links.far_x)

    def own_over_landed(self):
        self.over_landed(self.links.z)

    def over_landed(self, far):
        slot = (1 - self.links.x) * self.links.depth + far
        for part in range(HALVES):
            self.arrived(slot, part)

    def task(self):
        self.own_over()
        self.keep()
        yield
        self.along(1)
        yield
        self.along(0)
        yield
        self.over(1)
        yield
        self.along(2)
        self.over(0)
        yield
        self.over(2)
        yield
        for far in [self.links.z] + self.order:
            self.over_landed(far)


def weights_sems(depth):
    return [
        pltpu.SemaphoreType.DMA((2 * depth, HALVES)),
        pltpu.SemaphoreType.DMA((2 * depth, HALVES)),
    ]


def shared_task(links, own, full, send_sem, recv_sem):
    x, z, t, depth = links.x, links.z, links.t, links.depth
    quarter = own.at[pl.ds(t * full.shape[2], full.shape[2])]
    mine = x * depth + z

    def send(ref, slot, column, kind, peer):
        links.send(ref, full.at[slot, column], send_sem.at[slot, column, kind], recv_sem.at[slot, column], peer)

    def arrived(slot, column):
        ref = full.at[slot, column]
        links.wait(ref, send_sem.at[slot, column, 0], recv_sem.at[slot, column])
        return ref

    order = partners(links)
    for place, far in enumerate(order):
        send(quarter, mine, t, place, {"ctx": far})
    send(quarter, mine, t, 3, links.far_x)
    full[mine] = own[...].reshape(full.shape[1:])
    yield
    for place in (1, 0, 2):
        slot = x * depth + order[place]
        ref = arrived(slot, t)
        send(ref, slot, t, 3, links.far_x)
        send(ref, slot, t, 4, links.chip)
        send(ref, slot, t, 5, links.core)
    yield
    for far in [z] + order:
        slot = (1 - x) * depth + far
        ref = arrived(slot, t)
        send(ref, slot, t, 4, links.chip)
        send(ref, slot, t, 5, links.core)
    others = [x * depth + far for far in order] + [(1 - x) * depth + far for far in [z] + order]
    yield
    for slot in others:
        send(arrived(slot, other_chip(t)), slot, other_chip(t), 5, links.core)
    yield
    for slot in others:
        for column in (other_core(t), other_chip(other_core(t))):
            arrived(slot, column)


def shared_sems(depth):
    return [
        pltpu.SemaphoreType.DMA((2 * depth, 4, 6)),
        pltpu.SemaphoreType.DMA((2 * depth, 4)),
    ]


def scatter_task(links, grads, out, bufs, send_sem, recv_sem):
    x, z, depth = links.x, links.z, links.depth
    order = partners(links) + [z]

    def rows_of(ref, part):
        rows = ref.shape[0] // HALVES
        return slice(part * rows, (part + 1) * rows)

    def over(place):
        for part in range(HALVES):
            links.send(
                half(grads.at[(1 - x) * depth + order[place]], part),
                half(bufs.at[place], part),
                send_sem.at[place, part],
                recv_sem.at[place, part],
                links.far_x,
            )

    over(0)
    over(1)
    yield
    for place, far in enumerate(order):
        for part in range(HALVES):
            ref = half(bufs.at[place], part)
            links.wait(ref, send_sem.at[place, part], recv_sem.at[place, part])
            rows = rows_of(out.at[0], part)
            total = grads[x * depth + far, rows, :].astype(jnp.float32) + bufs[place, rows, :].astype(
                jnp.float32
            )
            if place < 3:
                bufs[place, rows, :] = total.astype(LOW)
                links.send(
                    ref,
                    half(out.at[z], part),
                    send_sem.at[depth + place, part],
                    recv_sem.at[depth + z, part],
                    {"ctx": far},
                )
            else:
                out[z, rows, :] = total.astype(LOW)
        if place < 2:
            over(place + 2)
        yield
    for far in order[:3]:
        for part in range(HALVES):
            links.wait(half(out.at[far], part), send_sem.at[0, part], recv_sem.at[depth + far, part])


def scatter_scratch(shape, depth, keep=True):
    return [pltpu.VMEM((depth,) + shape, LOW)] * (2 if keep else 1) + [
        pltpu.SemaphoreType.DMA((2 * depth, HALVES)),
        pltpu.SemaphoreType.DMA((2 * depth, HALVES)),
    ]


def side_by_side(parts, width):
    tiles = []
    lane = iota((parts[0].shape[0], 128), 1)
    for first, second in zip(parts[::2], parts[1::2]):
        moved = pltpu.roll(second, 64, 1)
        tiles += [
            first[:, 0:128],
            jnp.where(lane < 64, first[:, 128:256], moved[:, 0:128]),
            moved[:, 128:256],
        ]
    return tiles


def store_tiles(ref, layer, tiles):
    for at, tile in enumerate(tiles):
        ref[layer, :, at * 128 : (at + 1) * 128] = tile


def unpack_early(early, width, layer, gate_out, proj_out):
    gate, proj = [], []
    inside = iota((early.shape[1], 256), 1) < width
    for far in range(early.shape[0]):
        gate.append(jnp.where(inside, early[far, :, 0:256].astype(jnp.float32), 0.0))
        out = pltpu.roll(early[far, :, OUT_AT : OUT_AT + 256].astype(jnp.float32), 192, 1)
        proj.append(jnp.where(inside, out, 0.0))
    store_tiles(gate_out, layer, side_by_side(gate, width))
    store_tiles(proj_out, layer, side_by_side(proj, width))


def bc_products(normed_ref, bc_low, slots_ref):
    rows = slots_ref.shape[1]
    for pair in range(slots_ref.shape[0] // 2):
        total = mxu(normed_ref[:, pair * 2 * rows : (pair + 1) * 2 * rows], bc_low, 0, 0)
        slots_ref[2 * pair] = total[:rows].astype(LOW)
        slots_ref[2 * pair + 1] = total[rows:].astype(LOW)


def bc_task(links, slots_ref, arrived_ref, out_ref, layer, send_sem, recv_sem):
    x, z, depth = links.x, links.z, links.depth
    links.send(slots_ref.at[(1 - x) * depth + z], arrived_ref, send_sem, recv_sem, links.far_x)
    yield
    links.wait(arrived_ref, send_sem, recv_sem)
    out_ref[layer] = slots_ref[x * depth + z].astype(jnp.float32) + arrived_ref[...].astype(jnp.float32)


def rows_task(links, ref, out, send_sem, recv_sem):
    t = links.t
    for way, peer in enumerate((links.chip, links.core)):
        links.send(ref, out.at[t], send_sem.at[way], recv_sem.at[t], peer)
    out[t] = ref[...]
    yield
    column = other_chip(t)
    links.wait(out.at[column], send_sem.at[0], recv_sem.at[column])
    links.send(out.at[column], out.at[column], send_sem.at[2], recv_sem.at[column], links.core)
    yield
    for column in (other_core(t), other_chip(other_core(t))):
        links.wait(out.at[column], send_sem.at[0], recv_sem.at[column])


ROWS_SEMS = [pltpu.SemaphoreType.DMA((3,)), pltpu.SemaphoreType.DMA((4,))]


def sums_task(links, own, arrived_ref, work, by_z, sum_out, send_sem, recv_sem, channel_rows=9):
    z, depth = links.z, links.depth
    links.send(own, arrived_ref.at[0], send_sem.at[0], recv_sem.at[0], links.far_x)
    yield
    links.wait(arrived_ref.at[0], send_sem.at[0], recv_sem.at[0])
    over_dp = own[...] + arrived_ref[0]
    work[0] = over_dp
    links.send(work.at[0], arrived_ref.at[1], send_sem.at[1], recv_sem.at[1], links.core)
    yield
    links.wait(arrived_ref.at[1], send_sem.at[1], recv_sem.at[1])
    work[1] = work[0] + arrived_ref[1]
    links.send(work.at[1], arrived_ref.at[2], send_sem.at[2], recv_sem.at[2], links.chip)
    yield
    links.wait(arrived_ref.at[2], send_sem.at[2], recv_sem.at[2])
    row = iota(own.shape, 0)
    kept = jnp.logical_and(row < 16 * LAYERS, lax.rem(row, 16) < channel_rows)
    work[2] = jnp.where(kept, work[0], work[1] + arrived_ref[2])
    for hop in range(1, depth):
        links.send(
            work.at[2], by_z.at[z], send_sem.at[2 + hop], recv_sem.at[3 + z], {"ctx": lax.rem(z + hop, depth)}
        )
    by_z[z] = work[2]
    yield
    for hop in range(1, depth):
        far = lax.rem(z + hop, depth)
        links.wait(by_z.at[far], send_sem.at[0], recv_sem.at[3 + far])
    whole = by_z[0]
    for far in range(1, depth):
        whole = whole + by_z[far]
    sum_out[...] = whole


def sums_scratch(shape, depth):
    return [
        pltpu.VMEM((3,) + shape, jnp.float32),
        pltpu.VMEM((3,) + shape, jnp.float32),
        pltpu.SemaphoreType.DMA((3 + depth,)),
        pltpu.SemaphoreType.DMA((3 + depth,)),
    ]


def build_pack(pack, layer, gate, value, step, proj):
    depth, rows, _ = pack.shape
    width, heads = gate.shape[1] // depth, step.shape[0] // depth
    blank = jnp.zeros((rows, 128), jnp.float32)
    inside = iota((rows, 256), 1) < width

    def own_lanes(ref, far):
        at = far * width // 128 * 128
        window = ref[:, at : at + 256].astype(jnp.float32)
        if far * width > at:
            window = pltpu.roll(window, 256 - (far * width - at), 1)
        return jnp.where(inside, window, 0.0)

    for far in range(depth):
        gate_lanes, value_lanes = own_lanes(gate, far), own_lanes(value, far)
        pack[far, :, 0:128] = gate_lanes[:, 0:128].astype(LOW)
        out = pltpu.roll(own_lanes(proj, far), 64, 1)
        pack[far, :, OUT_AT:VALUE_AT] = (
            out + jnp.concatenate([gate_lanes[:, 128:256], blank], axis=1)
        ).astype(LOW)
        pack[far, :, VALUE_AT : VALUE_AT + 128] = value_lanes[:, 0:128].astype(LOW)
        head = iota((depth * heads, 128), 0) - far * heads
        chosen = jnp.logical_and(jnp.logical_and(head >= 0, head < heads), iota(head.shape, 1) == head + 64)
        pack[far, :, VALUE_AT + 128 :] = (
            value_lanes[:, 128:256] + mxu(step[:, layer, :], ones_where(chosen, LOW), 0, 0)
        ).astype(LOW)


def raw_layer(refs, layer):
    gate, value, step, proj = refs
    return [gate.at[layer], value.at[layer], step, proj.at[layer]]


def raw_scratch(gate, step):
    shapes = (gate.shape[1:], gate.shape[1:], step.shape, gate.shape[1:])
    return [pltpu.VMEM(shape, LOW) for shape in shapes] + [pltpu.SemaphoreType.DMA((4,))]


def prepare_kernel(
    depth,
    hidden_ref,
    seg_ref,
    gain_ref,
    gate_ref,
    value_ref,
    step_ref,
    proj_ref,
    bc_ref,
    taps_ref,
    tap_bias_ref,
    out_gain_ref,
    skip_ref,
    step_bias_ref,
    decay_ref,
    bc_taps_ref,
    bc_bias_ref,
    full_out,
    pack_out,
    bc_out,
    smalls_out,
    segr_out,
    segc_out,
    next_pack,
    normed,
    seg_piece,
    seg_full,
    pack,
    raw_gate,
    raw_value,
    raw_step,
    raw_proj,
    raw_sems,
    next_gate,
    next_value,
    next_step,
    next_proj,
    next_sems,
    gather_send,
    gather_recv,
    pack_send,
    pack_recv,
    bc_send,
    bc_recv,
):
    f32 = jnp.float32
    links = Links(depth)
    raw = (raw_gate, raw_value, raw_step, raw_proj)
    fetch = Fetch(raw_layer((gate_ref, value_ref, step_ref, proj_ref), 0), raw, raw_sems)
    next_raw = (next_gate, next_value, next_step, next_proj)
    next_fetch = Fetch(raw_layer((gate_ref, value_ref, step_ref, proj_ref), 1), next_raw, next_sems)
    piece, model_width = normed.shape
    rows = pl.ds(pl.multiple_of(links.t * piece, piece), piece)
    _, normed[...] = norm_rows(hidden_ref[0, rows, :].astype(f32), gain_ref[0:1, :].astype(f32))
    tokens = seg_ref.shape[1]
    lane, place = iota((tokens, 128), 0) - links.t * piece, iota((tokens, 128), 1)
    pick = ones_where(jnp.logical_and(lane == place, place < piece), f32)
    seg_piece[...] = mxu(jnp.broadcast_to(seg_ref[...].astype(f32), (8, tokens)), pick, 1, 0, exact)
    greet(everyone(depth) + [links.far_x])
    gather = gather_task(links, [normed, seg_piece], [full_out, seg_full], gather_send, gather_recv)
    next(gather, None)
    shared = shared_task(links, bc_ref.at[0], bc_out, bc_send, bc_recv)
    fetch.wait()
    build_pack(pack, 0, *raw)
    weights = Weights(links, pack, pack_out, pack_send, pack_recv)
    weights.along(0)
    weights.own_over()
    weights.keep()
    next(gather, None)
    weights.along(1)
    next(gather, None)
    weights.over(0)
    weights.along(2)
    next(shared, None)
    next(gather, None)
    weights.over(1)
    next(shared, None)
    width = taps_ref.shape[2] // depth
    lane, place = iota((taps_ref.shape[2], 256), 0) - links.z * width, iota((taps_ref.shape[2], 256), 1)
    own = ones_where(jnp.logical_and(lane == place, place < width), f32)
    heads = skip_ref.shape[1] // depth
    head, place = iota((skip_ref.shape[1], 256), 0) - links.z * heads, iota((skip_ref.shape[1], 256), 1)
    spread = ones_where(jnp.logical_and(head == place // HEADDIM, place < width), f32)
    smalls_out[...] = jnp.zeros(smalls_out.shape, f32)
    for layer in range(LAYERS):
        one = slice(layer, layer + 1)
        smalls_out[layer, 0:4, :] = mxu(taps_ref[layer].astype(f32), own, 1, 0, exact)
        by_channel = jnp.concatenate(
            [tap_bias_ref[...].astype(f32)[one], out_gain_ref[...].astype(f32)[one]] * 4, axis=0
        )
        smalls_out[layer, 4:6, :] = mxu(by_channel, own, 1, 0, exact)[0:2]
        by_head = jnp.concatenate(
            [skip_ref[one, :], step_bias_ref[one, :], -jnp.exp(decay_ref[one, :])] + [skip_ref[one, :]] * 5,
            axis=0,
        )
        smalls_out[layer, 6:9, :] = mxu(by_head, spread, 1, 0, exact)[0:3]
        smalls_out[layer, 9:13, :] = bc_taps_ref[layer].astype(f32)
        smalls_out[layer, 13:14, :] = bc_bias_ref[...].astype(f32)[one]
    next(shared, None)
    next(gather, None)
    next_fetch.wait()
    build_pack(next_pack, 1, *next_raw)
    next(shared, None)
    next(gather, None)
    per = 128 // piece
    segc_out[...] = jnp.full(segc_out.shape, -1.0, f32)
    for row in range(4 * depth // per):
        lanes = iota((8, 128), 1)
        total = jnp.zeros((8, 128), f32)
        for at in range(per):
            part = seg_full[row * per + at]
            total = jnp.where(lanes // piece == at, pltpu.roll(part, at * piece, 1) if at else part, total)
        segr_out[:, row * 128 : (row + 1) * 128] = total[0:1]
        column = spread_rows(total)[:, 0:1]
        segc_out[8 + row * 128 : 8 + (row + 1) * 128, :] = jnp.broadcast_to(column, (128, 256))
    run_tasks(shared)
    weights.over(2)
    for far in [links.z] + weights.order:
        weights.over_landed(far)
    links.finish()


def pack_shapes(depth, rows, bc_width):
    return [
        jax.ShapeDtypeStruct((2 * depth, rows, PACK), LOW),
        jax.ShapeDtypeStruct((2 * depth, 4, rows // 4, bc_width), LOW),
    ]


def piece_shapes(pieces, depth):
    return [jax.ShapeDtypeStruct((4 * depth,) + p.shape, p.dtype) for p in pieces]


def prepare(hidden, segment, gain, gate, value, step, proj, bc, small, depth, collective_id):
    f32 = jnp.float32
    _, tokens, model_width = hidden.shape
    piece, slots = tokens // 4, 4 * depth
    rows = gate.shape[1]
    shapes = [
        jax.ShapeDtypeStruct((slots, piece, model_width), LOW),
        *pack_shapes(depth, rows, bc.shape[2]),
        jax.ShapeDtypeStruct((LAYERS, 16, 256), f32),
        jax.ShapeDtypeStruct((1, depth * tokens), f32),
        jax.ShapeDtypeStruct((depth * tokens + 16, 256), f32),
        jax.ShapeDtypeStruct((depth, rows, PACK), LOW),
    ]
    return pl.pallas_call(
        partial(prepare_kernel, depth),
        out_shape=shapes,
        in_specs=[VMEM_SPEC] * 3 + [ANY_SPEC] * 4 + [VMEM_SPEC] * (1 + len(small)),
        out_specs=[VMEM_SPEC] * len(shapes),
        scratch_shapes=[
            pltpu.VMEM((piece, model_width), LOW),
            pltpu.VMEM((8, 128), f32),
            pltpu.VMEM((slots, 8, 128), f32),
            pltpu.VMEM((depth, rows, PACK), LOW),
        ]
        + raw_scratch(gate, step)
        + raw_scratch(gate, step)
        + gather_sems(2, slots)
        + weights_sems(depth)
        + shared_sems(depth),
        compiler_params=params_of(collective_id),
        name="prepare",
    )(hidden, segment, gain, gate, value, step, proj, bc, *small)


class SumStream:
    def __init__(self, links, parts, out, bufs, send_sem, recv_sem, low=1, high=4):
        self.links, self.parts, self.out, self.bufs = links, parts, out, bufs
        self.send_sem, self.recv_sem = send_sem, recv_sem
        self.receives = jnp.logical_and(links.z >= low, links.z < high)

    def rows(self, part):
        size = self.out.shape[0] // HALVES
        return slice(part * size, (part + 1) * size)

    def sems(self, at, part):
        return self.send_sem.at[at, part], self.recv_sem.at[at, part]

    def wait(self, at, part):
        self.links.wait(half(self.bufs.at[at], part), *self.sems(at, part))

    def loaded(self, at, part):
        return self.bufs[at, self.rows(part), :].astype(jnp.float32)

    def mine(self, slot, part):
        return self.parts[slot, self.rows(part), :].astype(jnp.float32)

    def first(self, far):
        t = self.links.t
        for which, row in enumerate((other_chip(other_core(t)), other_core(t))):
            for part in range(HALVES):
                at = far * 2 + which
                self.links.send(
                    half(self.parts.at[far * 4 + row], part),
                    half(self.bufs.at[at], part),
                    *self.sems(at, part),
                    self.links.core,
                )

    def second(self, far):
        at = far * 2
        for part in range(HALVES):
            self.wait(at, part)
            total = self.mine(far * 4 + other_chip(self.links.t), part) + self.loaded(at, part)
            self.bufs[at, self.rows(part), :] = total.astype(self.bufs.dtype)
            self.links.send(
                half(self.bufs.at[at], part),
                half(self.bufs.at[8 + far], part),
                *self.sems(8 + far, part),
                self.links.chip,
            )

    def third(self, far):
        at = far * 2 + 1
        z = self.links.z
        for part in range(HALVES):
            self.wait(at, part)
            self.wait(8 + far, part)
            total = (
                self.mine(far * 4 + self.links.t, part) + self.loaded(at, part) + self.loaded(8 + far, part)
            )
            rows = self.rows(part)

            @pl.when(z == far)
            def _(total=total, rows=rows):
                self.out[rows, :] = total

            @pl.when(z != far)
            def _(total=total, rows=rows):
                self.bufs[at, rows, :] = total.astype(self.bufs.dtype)

            self.links.send(
                half(self.bufs.at[at], part),
                half(self.bufs.at[12 + z], part),
                self.send_sem.at[12 + far, part],
                self.recv_sem.at[12 + z, part],
                {"ctx": far},
                z != far,
            )

    def last(self):
        z, bufs = self.links.z, self.bufs
        size = self.out.shape[0] // 4
        for quarter in range(4):
            if quarter % 2 == 0:
                self.wait(1, quarter // 2)
                self.wait(8, quarter // 2)
            rows = slice(quarter * size, (quarter + 1) * size)

            def of(ref, at, rows=rows):
                return ref[at, rows, :].astype(jnp.float32)

            total = of(self.parts, self.links.t) + of(bufs, 1) + of(bufs, 8)

            def piece(at, rows=rows):
                return bufs.at[at, pl.ds(rows.start, size)]

            @pl.when(z == self.links.depth - 1)
            def _(total=total, rows=rows):
                bufs[1, rows, :] = total.astype(bufs.dtype)

            @pl.when(z < self.links.depth - 1)
            def _(total=total, rows=rows, quarter=quarter):
                come = 17 + z
                self.links.wait(
                    piece(come), self.send_sem.at[come, quarter], self.recv_sem.at[come, quarter]
                )
                more = total + of(bufs, come)

                @pl.when(z == 0)
                def _():
                    self.out[rows, :] = more

                @pl.when(z > 0)
                def _():
                    bufs[1, rows, :] = more.astype(bufs.dtype)

            self.links.send(
                piece(1),
                piece(16 + z),
                self.send_sem.at[16 + z, quarter],
                self.recv_sem.at[16 + z, quarter],
                self.links.left,
                z > 0,
            )

    def end(self):
        @pl.when(self.receives)
        def _():
            for hop in range(1, self.links.depth):
                far = lax.rem(self.links.z + hop, self.links.depth)
                for part in range(HALVES):
                    self.wait(12 + far, part)
                    self.out[self.rows(part), :] += self.loaded(12 + far, part)


def stream_scratch(shape, dtype):
    return [
        pltpu.VMEM((20,) + shape, dtype),
        pltpu.SemaphoreType.DMA((20, 4)),
        pltpu.SemaphoreType.DMA((20, 4)),
    ]


class Plan:
    def __init__(self, calls):
        self.calls = calls

    def __call__(self, turn, point):
        for call in self.calls.get((turn, point), ()):
            call()


def advance(task):
    def step():
        next(task, None)

    return step


def forward_first_kernel(depth, operands, *refs):
    compute, pack, results, full_pack = list(refs[:6]), refs[6], refs[7:15], refs[15]
    compute[3] = compute[3].at[0]
    pack_send, pack_recv = refs[16:]
    links = Links(depth)
    greet(everyone(depth) + [links.far_x])
    operands.need(6)
    weights = Weights(links, pack, full_pack, pack_send, pack_recv)
    weights.along(0)
    weights.own_over()
    weights.keep()
    plan = Plan({(1, 1): [partial(weights.along, 1)]})
    operands.wait()
    forward_body(True, plan, *compute, *results)
    operands.flush()
    weights.landed(0)
    weights.landed(1)
    weights.own_over_landed()
    links.finish()


def forward_first(normed, wall, bcw, small, segr, segc, slots, pack, depth, collective_id):
    rows = pack.shape[1]
    shapes = forward_shapes(normed, bcw, slots, True) + [
        jax.ShapeDtypeStruct((2 * depth, rows, PACK), LOW),
    ]
    return launch(
        partial(forward_first_kernel, depth),
        (normed, wall, bcw, small, segr, segc, pack),
        shapes,
        weights_sems(depth),
        collective_id,
        "forward_first",
        first=(6,),
        flushed=(0, 2, 3, 4, 5, 6, 7),
    )


def forward_second_kernel(depth, operands, *refs):
    compute, cotangent, results, (full, inv_out, inner_out), scratch = (
        [*refs[:3], refs[3].at[1], *refs[4:6]],
        refs[6],
        refs[7:15],
        refs[15:18],
        refs[18:],
    )
    gather_send, gather_recv, own, shared, share_send, share_recv = scratch
    links = Links(depth)
    greet(everyone(depth))
    operands.need(6)
    piece = full.shape[1]
    mine = cotangent.at[0, pl.ds(pl.multiple_of(links.t * piece, piece), piece)]
    gather = gather_task(links, [mine], [full], gather_send, gather_recv)
    next(gather, None)
    go = [advance(gather)]
    operands.wait()
    forward_body(False, Plan({(1, 0): go, (2, 0): go, (3, 0): go}), *compute, *results)
    operands.flush()
    run_tasks(gather)
    _, wall_ref, _, small_ref = compute[:4]
    squares_ref, gate_ref, mixed_ref = results[1], results[2], results[6]
    width = gate_ref.shape[1]
    rows = squares_ref.shape[0]
    own[0:rows, :] = squares_ref[...]
    gains = small_ref[5:6, :width]
    per = 128 // piece
    for row in range(rows):
        grad = full[per * row : per * (row + 1)].reshape(128, full.shape[2])
        grad_scaled = mxu(grad, wall_ref[:, OUT_AT : OUT_AT + 256], 1, 0)
        grad_scaled = pltpu.roll(grad_scaled, 192, 1)[:, :width]
        at = pl.ds(row * 128, 128)
        gate_pre = gate_ref[at, :]
        terms = grad_scaled * gains * mixed_ref[at, :] * gate_pre * sigmoid(gate_pre)
        own[rows + row : rows + row + 1, :] = mxu(
            jnp.ones((8, width), jnp.float32), terms, 1, 1, exact
        )[0:1]
    run_tasks(share_task(links, own, shared, share_send, share_recv))
    summed = shared[0]
    for slot in range(1, 4 * depth):
        summed = summed + shared[slot]
    inv = lax.rsqrt(summed[0:rows] / INNER + epsilon)
    inv_out[...] = inv
    inner_out[...] = inv * summed[rows:] / INNER
    links.finish()


def forward_second(normed, wall, bcw, small, segr, segc, slots, cotangent, depth, collective_id):
    shapes = forward_shapes(normed, bcw, slots, False)
    rows = shapes[1].shape
    shapes = (
        shapes
        + [jax.ShapeDtypeStruct((4 * depth, cotangent.shape[1] // 4, cotangent.shape[2]), LOW)]
        + [jax.ShapeDtypeStruct(rows, jnp.float32)] * 2
    )
    return launch(
        partial(forward_second_kernel, depth),
        (normed, wall, bcw, small, segr, segc, cotangent),
        shapes,
        gather_sems(1, 4 * depth)
        + [
            pltpu.VMEM((2 * rows[0], 128), jnp.float32),
            pltpu.VMEM((4 * depth, 2 * rows[0], 128), jnp.float32),
            pltpu.SemaphoreType.DMA((4 * depth,)),
            pltpu.SemaphoreType.DMA((4 * depth,)),
        ],
        collective_id,
        "forward_second",
        first=(6,),
        flushed=(0, 2, 3, 4, 5, 6, 7),
    )


def own_column(rows, slot, piece):
    per = 128 // piece
    columns = spread_rows(rows)
    lane = iota(columns.shape, 1)
    column = jnp.sum(jnp.where(lane == slot // per, columns, 0.0), axis=1, keepdims=True)
    at = iota((piece, 128), 0) + lax.rem(slot, per) * piece
    pick = ones_where(at == iota((piece, 128), 1), jnp.float32)
    return mxu(pick, jnp.broadcast_to(column, (128, 128)), 1, 0, exact)[:, 0:1]


def norm_gradient(grad_rows, grad_normed, hidden, gain):
    inv = lax.rsqrt(jnp.mean(hidden * hidden, axis=1, keepdims=True) + epsilon)
    weighted = grad_normed * gain
    grad = (
        grad_rows
        + inv * weighted
        - hidden * (inv * inv * inv) * jnp.mean(weighted * hidden, axis=1, keepdims=True)
    )
    return grad, row_sum(grad_normed * hidden * inv)


def owner_norm(total, grad, hidden_ref, gain_ref, bcw_ref):
    model_width = hidden_ref.shape[1]
    bc_low = total[:, model_width:].astype(LOW)
    grad_normed = total[:, :model_width] + mxu(bc_low, bcw_ref[...], 1, 1)
    grad, gain = norm_gradient(grad, grad_normed, hidden_ref[...].astype(jnp.float32), gain_ref[...])
    return bc_low, grad, gain


def backward_second_kernel(depth, operands, *refs):
    compute, (cotangent, hidden_ref, gain_ref, bcw_ref, before_ref) = list(refs[:14]), refs[14:19]
    compute[5] = compute[5].at[1]
    late, sums, grad_out, gain_out, full_out, inner_out, early_out = refs[19:26]
    both, early, *work = refs[26:33]
    (
        early_bufs, early_send, early_recv,
        back_total, piece_low, scalars, scalars_full, back_bufs, back_send, back_recv,
        gather_send, gather_recv,
    ) = refs[33:]
    links = Links(depth)
    greet(everyone(depth) + [links.far_x])
    piece, model_width = hidden_ref.shape
    scatter = scatter_task(links, early, early_out, early_bufs, early_send, early_recv)
    go = advance(scatter)
    stream = SumStream(links, both, back_total, back_bufs, back_send, back_recv)

    def call(method, far):
        return partial(method, far)

    plan = Plan(
        {
            (-1, 0): [partial(operands.need, 3)],
            (-1, 1): [go, operands.wait],
            (0, 3): [call(stream.first, 3)],
            (1, 1): [call(stream.second, 3)],
            (1, 2): [go],
            (1, 3): [call(stream.first, 2)],
            (2, 1): [call(stream.second, 2)],
            (2, 2): [call(stream.third, 3), go],
            (2, 3): [call(stream.first, 1)],
            (3, 1): [call(stream.second, 1)],
            (3, 2): [call(stream.third, 2)],
            (3, 3): [call(stream.first, 0), go],
            (4, 1): [call(stream.second, 0)],
        }
    )
    operands.need(0, 4, 8, 12)
    backward_body(plan, *compute, both, early, late, sums, *work)
    stream.third(1)
    stream.last()
    stream.end()
    rows = pl.ds(pl.multiple_of(links.t * piece, piece), piece)
    bc_low, grad, gain_out[...] = owner_norm(
        back_total,
        cotangent[0, rows, :].astype(jnp.float32),
        hidden_ref,
        gain_ref[...].astype(jnp.float32)[1:2],
        bcw_ref,
    )
    grad_low = grad.astype(LOW)
    piece_low[:, :model_width] = grad_low
    piece_low[:, model_width:] = bc_low
    inner = jnp.sum(grad_low.astype(jnp.float32) * before_ref[...], axis=1, keepdims=True) / INNER
    slot, per = links.z * 4 + links.t, 128 // piece
    lane = iota((piece, 128), 0) + lax.rem(slot, per) * piece
    place = ones_where(lane == iota((piece, 128), 1), jnp.float32)
    inner_rows = mxu(jnp.broadcast_to(inner, (piece, 8)), place, 0, 0, exact)
    scalars[...] = jnp.where(iota(inner_rows.shape, 0) == slot // per, inner_rows, 0.0)
    grad_out[...] = grad
    run_tasks(
        gather_task(links, [piece_low, scalars], [full_out, scalars_full], gather_send, gather_recv),
        scatter,
    )
    inner_rows = scalars_full[0]
    for other in range(1, 4 * depth):
        inner_rows = inner_rows + scalars_full[other]
    inner_out[...] = inner_rows
    links.finish()


def backward_second(
    grad, inv, inner, normed, wall, small, segr, segc, kept, slots, cotangent, hidden, gain, bcw, before, depth, collective_id
):
    f32 = jnp.float32
    piece, model_width = hidden.shape
    (both, early, late, sums), work = backward_shapes(normed, kept, slots)
    whole_width = both.shape[2]
    shapes = [
        late,
        sums,
        jax.ShapeDtypeStruct((piece, model_width), f32),
        jax.ShapeDtypeStruct((1, model_width), f32),
        jax.ShapeDtypeStruct(both.shape, LOW),
        jax.ShapeDtypeStruct(inv.shape, f32),
        jax.ShapeDtypeStruct((depth,) + early.shape[1:], LOW),
    ]
    return launch(
        partial(backward_second_kernel, depth),
        (grad, inv, inner, normed, wall, small, segr, segc, *kept, cotangent, hidden, gain, bcw, before),
        shapes,
        [pltpu.VMEM(both.shape, LOW), pltpu.VMEM(early.shape, LOW)]
        + work
        + scatter_scratch(early.shape[1:], depth, False)
        + [
            pltpu.VMEM((piece, whole_width), f32),
            pltpu.VMEM((piece, whole_width), LOW),
            pltpu.VMEM(inv.shape, f32),
            pltpu.VMEM((slots,) + inv.shape, f32),
        ]
        + stream_scratch((piece, whole_width), LOW)
        + gather_sems(2, slots),
        collective_id,
        "backward_second",
        first=(0, 4, 8, 12, 3),
    )


def backward_first_kernel(depth, operands, *refs):
    compute, (late1, normed1, grad_in, hidden_ref, gain_ref, bcw_ref, sums1, gain1, part, hidden1, inv1) = (
        list(refs[:14]),
        refs[14:25],
    )
    compute[5] = compute[5].at[0]
    late1_out, early0_out, late0_out, bc_out, by_z_out, sum_out, hidden_grad_out, hidden_out = refs[25:33]
    both, early, late, sums, *work = refs[33:42]
    (
        out_total, out_low, out_bufs, out_send, out_recv, out_row_send, out_row_recv,
        total, low, bc_piece, bc_full, own,
        bufs, stream_send, stream_recv,
        gather_send, gather_recv,
        late1_bufs, late1_send, late1_recv,
        early0_bufs, early0_send, early0_recv,
        late0_bufs, late0_send, late0_recv,
        bc_slots, bc_arrived, bc_send, bc_recv,
        sums_arrived, sums_work, sums_send, sums_recv,
        row_send, row_recv,
    ) = refs[42:]
    links = Links(depth)
    greet(everyone(depth) + [links.far_x])
    piece, model_width = grad_in.shape
    normed_ref, grad_ref = compute[3], compute[0]
    output = SumStream(links, part, out_total, out_bufs, out_send, out_recv)
    stream = SumStream(links, both, total, bufs, stream_send, stream_recv)
    late_task1 = scatter_task(links, late1, late1_out, late1_bufs, late1_send, late1_recv)
    early_task0 = scatter_task(links, early, early0_out, early0_bufs, early0_send, early0_recv)
    late_task0 = scatter_task(links, late, late0_out, late0_bufs, late0_send, late0_recv)
    bc1 = bc_task(links, bc_slots.at[1], bc_arrived.at[1], bc_out, 1, bc_send.at[1], bc_recv.at[1])
    operands.need(14)
    next(late_task1, None)

    def call(method, far):
        return partial(method, far)

    def output_rows():
        output.third(1)
        yield
        output.last()
        yield
        output.end()
        inv = own_column(inv1[...], links.z * 4 + links.t, piece)
        out_low[...] = (hidden1[...] + out_total[...] * inv).astype(LOW)
        yield from rows_task(links, out_low, hidden_out, out_row_send, out_row_recv)

    def output_first():
        operands.need(22)
        for far in (3, 2, 1, 0):
            output.first(far)

    def bc_first():
        bc_products(normed1, grad_ref[:, model_width:], bc_slots.at[1])
        next(bc1, None)

    go1, go0 = advance(late_task1), advance(early_task0)
    plan = Plan(
        {
            (-1, 0): [partial(operands.need, 3), output_first, go1],
            (-1, 1): [operands.wait, go0, call(output.second, 3), call(output.second, 2)],
            (0, 1): [go1],
            (0, 3): [call(stream.first, 3), go0],
            (1, 1): [call(stream.second, 3), call(output.third, 3)],
            (1, 2): [go1],
            (1, 3): [call(stream.first, 2), call(output.third, 2), go0],
            (2, 1): [call(stream.second, 2)],
            (2, 2): [call(stream.third, 3), go1],
            (2, 3): [call(stream.first, 1), go0],
            (3, 1): [call(stream.second, 1)],
            (3, 2): [call(stream.third, 2)],
            (3, 3): [call(stream.first, 0), go0],
            (4, 1): [call(stream.second, 0)],
        }
    )
    operands.need(0, 4, 8, 12)
    backward_body(plan, *compute, both, early, late, sums, *work)
    next(late_task0, None)
    bc_first()
    stream.third(1)
    output.second(1)
    stream.last()
    output.second(0)
    next(late_task0, None)
    stream.end()
    rows = pl.ds(pl.multiple_of(links.t * piece, piece), piece)
    bc_low, grad, gain = owner_norm(
        total, grad_in[...], hidden_ref.at[0, rows], gain_ref[...].astype(jnp.float32)[0:1], bcw_ref
    )
    bc_piece[...] = bc_low
    low[...] = grad.astype(LOW)
    own[...] = jnp.zeros(own.shape, jnp.float32)
    own[0:16, :] = sums[...]
    own[16:32, :] = sums1[...]
    count = model_width // 256
    for layer, row in enumerate((gain, gain1[...])):
        for at in range(count):
            to = 16 * LAYERS + layer * count + at
            own[to : to + 1, :] = row[:, at * 256 : (at + 1) * 256]
    run_tasks(
        gather_task(links, [bc_piece], [bc_full], gather_send, gather_recv),
        sums_task(links, own, sums_arrived, sums_work, by_z_out, sum_out, sums_send, sums_recv),
        rows_task(links, low, hidden_grad_out, row_send, row_recv),
        late_task0,
        output_rows(),
        early_task0,
        late_task1,
        bc1,
    )
    tokens = bc_full.shape[0] * bc_full.shape[1]
    bc_products(normed_ref, bc_full[...].reshape(tokens, bc_full.shape[2]), bc_slots.at[0])
    bc0 = bc_task(links, bc_slots.at[0], bc_arrived.at[0], bc_out, 0, bc_send.at[0], bc_recv.at[0])
    run_tasks(bc0)
    links.finish()


def backward_first(
    grad, inv, inner, normed, wall, small, segr, segc, kept, slots, late1, normed1, grad_in, hidden, gain, bcw, sums1, gain1, part, hidden1, inv1, depth, collective_id
):
    f32 = jnp.float32
    piece, model_width = grad_in.shape
    (both, early, late, sums), work = backward_shapes(normed, kept, slots)
    whole_width = both.shape[2]
    k_slots, k_rows, _ = late1.shape
    bc_width = kept[2].shape[1]
    small_sums = (16 * LAYERS + 16, 256)
    shapes = [
        jax.ShapeDtypeStruct((depth,) + late.shape[1:], LOW),
        jax.ShapeDtypeStruct((depth,) + early.shape[1:], LOW),
        jax.ShapeDtypeStruct((depth,) + late.shape[1:], LOW),
        jax.ShapeDtypeStruct((LAYERS, k_rows, bc_width), f32),
        jax.ShapeDtypeStruct((depth,) + small_sums, f32),
        jax.ShapeDtypeStruct(small_sums, f32),
        jax.ShapeDtypeStruct((4, piece, model_width), LOW),
        jax.ShapeDtypeStruct((4, piece, model_width), LOW),
    ]
    return launch(
        partial(backward_first_kernel, depth),
        (grad, inv, inner, normed, wall, small, segr, segc, *kept, late1, normed1, grad_in, hidden, gain, bcw, sums1, gain1, part, hidden1, inv1),
        shapes,
        [pltpu.VMEM(a.shape, a.dtype) for a in (both, early, late, sums)]
        + work
        + [pltpu.VMEM((piece, model_width), f32), pltpu.VMEM((piece, model_width), LOW)]
        + stream_scratch((piece, model_width), LOW)
        + ROWS_SEMS
        + [
            pltpu.VMEM((piece, whole_width), f32),
            pltpu.VMEM((piece, model_width), LOW),
            pltpu.VMEM((piece, bc_width), LOW),
            pltpu.VMEM((slots, piece, bc_width), LOW),
            pltpu.VMEM(small_sums, f32),
        ]
        + stream_scratch((piece, whole_width), LOW)
        + gather_sems(1, slots)
        + scatter_scratch(late.shape[1:], depth, False)
        + scatter_scratch(early.shape[1:], depth, False)
        + scatter_scratch(late.shape[1:], depth, False)
        + [
            pltpu.VMEM((LAYERS, k_slots, k_rows, bc_width), LOW),
            pltpu.VMEM((LAYERS, k_rows, bc_width), LOW),
            pltpu.SemaphoreType.DMA((LAYERS,)),
            pltpu.SemaphoreType.DMA((LAYERS,)),
        ]
        + sums_scratch(small_sums, depth)
        + ROWS_SEMS,
        collective_id,
        "backward_first",
        first=(0, 14, 4, 8, 12, 3, 22),
    )


def emit_kernel(
    hidden_ref, grad_ref, early0, late0, early1, late1, bc_ref, by_z, whole,
    hidden_out, grad_out, gain_out, gate_out, value_out, bc_out, step_out,
    taps_out, tap_bias_out, bc_taps_out, bc_bias_out, decay_out, step_bias_out, skip_out, out_gain_out, proj_out,
):
    piece = hidden_ref.shape[1]
    depth, _, _ = by_z.shape
    channels, heads_whole = taps_out.shape[2], skip_out.shape[1]
    width, heads = channels // depth, heads_whole // depth
    for at in range(4):
        hidden_out[0, at * piece : (at + 1) * piece, :] = hidden_ref[at]
        grad_out[0, at * piece : (at + 1) * piece, :] = grad_ref[at]
    bc_out[...] = bc_ref[...]
    count = gain_out.shape[1] // 256
    for layer, (early, late) in enumerate(((early0, late0), (early1, late1))):
        one = slice(layer, layer + 1)
        unpack_early(early, width, layer, gate_out, proj_out)
        step = by_head = 0.0
        values, channel_rows = [], []
        inside = iota((late.shape[1], 256), 1) < width
        rows = slice(16 * layer, 16 * layer + 16)
        for far in range(depth):
            values.append(jnp.where(inside, late[far].astype(jnp.float32), 0.0))
            channel_rows.append(jnp.where(inside[0:16], by_z[far, rows, :], 0.0))
            window, head = iota((256, 16), 0), iota((256, 16), 1) - far * heads
            mine = jnp.logical_and(head >= 0, head < heads)
            step += mxu(ones_where(jnp.logical_and(mine, window == width + head), LOW), late[far], 0, 1)
            window, head = iota((256, 128), 0), iota((256, 128), 1) - far * heads
            mine = jnp.logical_and(head >= 0, head < heads)
            by_head += mxu(
                by_z[far, rows, :],
                ones_where(jnp.logical_and(mine, window == head * HEADDIM), jnp.float32),
                1,
                0,
                exact,
            )
        store_tiles(value_out, layer, side_by_side(values, width))
        by_channel = jnp.concatenate(side_by_side(channel_rows, width), axis=1)
        for head in range(heads_whole):
            step_out[head, one, :] = step[head : head + 1]
        taps_out[layer] = by_channel[0:4]
        tap_bias_out[one, :] = by_channel[4:5]
        out_gain_out[one, :] = by_channel[5:6]
        skip_out[one, :] = by_head[6:7, :heads_whole]
        step_bias_out[one, :] = by_head[7:8, :heads_whole]
        decay_out[one, :] = by_head[8:9, :heads_whole]
        bc_taps_out[layer] = whole[16 * layer + 9 : 16 * layer + 13, :]
        bc_bias_out[one, :] = whole[16 * layer + 13 : 16 * layer + 14, :]
        for at in range(count):
            row = 16 * LAYERS + layer * count + at
            gain_out[one, at * 256 : (at + 1) * 256] = whole[row : row + 1, :]


def emit(hidden, grad, early0, late0, early1, late1, bc, by_z, whole, tokens, heads, channels):
    f32 = jnp.float32
    rows, model_width = early0.shape[1], hidden.shape[2]
    bc_width = bc.shape[2]
    shapes = [
        ((1, tokens, model_width), LOW),
        ((1, tokens, model_width), LOW),
        ((LAYERS, model_width), f32),
        ((LAYERS, rows, channels), f32),
        ((LAYERS, rows, channels), f32),
        ((LAYERS, rows, bc_width), f32),
        ((heads, LAYERS, rows), f32),
        ((LAYERS, 4, channels), f32),
        ((LAYERS, channels), f32),
        ((LAYERS, 4, bc_width), f32),
        ((LAYERS, bc_width), f32),
        ((LAYERS, heads), f32),
        ((LAYERS, heads), f32),
        ((LAYERS, heads), f32),
        ((LAYERS, channels), f32),
        ((LAYERS, rows, channels), f32),
    ]
    return pl.pallas_call(
        emit_kernel,
        out_shape=[jax.ShapeDtypeStruct(*shape) for shape in shapes],
        in_specs=[VMEM_SPEC] * 9,
        out_specs=[VMEM_SPEC] * len(shapes),
        compiler_params=local_params(),
        name="emit",
    )(hidden, grad, early0, late0, early1, late1, bc, by_z, whole)


def split_local(
    depth,
    hidden_in,
    segment_ids,
    cotangent,
    norm_gain,
    gate_proj,
    value_proj,
    bc_proj,
    step_proj,
    conv_value,
    conv_value_bias,
    conv_bc,
    conv_bc_bias,
    decay_log,
    step_bias,
    skip_gain,
    out_gain,
    out_proj,
):
    tokens, model_width = hidden_in.shape[1:]
    slots = depth * 4
    heads, channels = step_proj.shape[2], gate_proj.shape[2]
    projections = (gate_proj, value_proj, step_proj.transpose(2, 0, 1), out_proj.transpose(0, 2, 1))
    small = (
        conv_value,
        conv_value_bias,
        out_gain,
        skip_gain,
        step_bias,
        decay_log,
        conv_bc,
        conv_bc_bias,
    )
    normed0, pack0, shared0, smalls, segr, segc, packs1 = prepare(
        hidden_in, segment_ids, norm_gain, *projections, bc_proj, small, depth, 1
    )
    seg = (segr, segc)
    normed0 = normed0.reshape(-1, model_width)
    wall0, bc_wall0 = pack0.reshape(-1, PACK), shared0.reshape(model_width, -1)
    gated0, squares0, *kept0, early = forward_first(
        normed0, wall0, bc_wall0, smalls, *seg, slots, packs1, depth, 2
    )
    hidden1, total0, inv_rows0, normed1, pack1, shared1 = turn_forward(
        gated0, squares0, smalls, wall0, hidden_in, norm_gain, packs1, early, bc_proj, depth, 3
    )
    wall1, bc_wall1 = pack1.reshape(-1, PACK), shared1.reshape(model_width, -1)
    normed1 = normed1.reshape(-1, model_width)
    part1, _, *kept1, cotangent_full, inv_rows1, inner_rows1 = forward_second(
        normed1, wall1, bc_wall1, smalls, *seg, slots, cotangent, depth, 4
    )
    late1, sums1, grad1, gain1, full0, inner_rows0, early1 = backward_second(
        cotangent_full.reshape(-1, model_width),
        inv_rows1,
        inner_rows1,
        normed1,
        wall1,
        smalls,
        *seg,
        kept1,
        slots,
        cotangent,
        hidden1,
        norm_gain,
        bc_wall1,
        total0,
        depth,
        5,
    )
    late1, early0, late0, bc_grad, by_z, whole, grad_hidden, hidden_out = backward_first(
        full0.reshape(-1, full0.shape[2]),
        inv_rows0,
        inner_rows0,
        normed0,
        wall0,
        smalls,
        *seg,
        kept0,
        slots,
        late1,
        normed1,
        grad1,
        hidden_in,
        norm_gain,
        bc_wall0,
        sums1,
        gain1,
        part1,
        hidden1,
        inv_rows1,
        depth,
        6,
    )
    outs = emit(
        hidden_out, grad_hidden, early0, late0, early1, late1, bc_grad, by_z, whole, tokens, heads, channels
    )
    return (*outs[:6], outs[6].transpose(1, 2, 0), *outs[7:15], outs[15].transpose(0, 2, 1))


def solution(mesh):
    in_specs = (
        P("dp", "ctx", None),
        P("dp", "ctx"),
        P("dp", "ctx", None),
        P(),
        P(None, ("dp", "ctx"), "tp"),
        P(None, ("dp", "ctx"), "tp"),
        P(None, ("dp", "ctx"), None),
        P(None, ("dp", "ctx"), "tp"),
        P(None, None, "tp"),
        P(None, "tp"),
        P(),
        P(),
        P(None, "tp"),
        P(None, "tp"),
        P(None, "tp"),
        P(None, "tp"),
        P(None, "tp", ("dp", "ctx")),
    )
    out_specs = (
        P("dp", "ctx", None),
        P("dp", "ctx", None),
        P(),
        P(None, ("dp", "ctx"), "tp"),
        P(None, ("dp", "ctx"), "tp"),
        P(None, ("dp", "ctx"), None),
        P(None, ("dp", "ctx"), "tp"),
        P(None, None, "tp"),
        P(None, "tp"),
        P(),
        P(),
        P(None, "tp"),
        P(None, "tp"),
        P(None, "tp"),
        P(None, "tp"),
        P(None, "tp", ("dp", "ctx")),
    )
    depth = mesh.shape["ctx"]
    heads = 48 // mesh.shape["tp"]
    fits = mesh.shape["tp"] == 4 and mesh.shape["dp"] == 2 and depth == 4 and heads % depth == 0
    body = partial(split_local, depth) if fits else local
    return jax.shard_map(body, mesh=mesh, in_specs=in_specs, out_specs=out_specs, check_vma=False)
```
